32 devices in a mesh: ctx: 8 (over z, x), head: 4 (over y, core).
Axes of the slice: x: 2, y: 2, z: 4, core: 2. Of those that a mesh axis runs over, the one named last changes fastest.
Arguments:
- queries: bfloat16 [256, 4096], P(None, 'head'), may hold values from -40 to 40
- keys: bfloat16 [16, 2048, 2048], P('ctx', None, 'head'), may hold values from -6 to 6
- values: bfloat16 [16, 2048, 2048], P('ctx', None, 'head'), may hold values from -6 to 6
- page_map: int32 [16], replicated, may hold values from 0 to 15, each once
- selected: int32 [2, 8], replicated, may hold values from 0 to 15, as said below
- residual_in: bfloat16 [256, 5376], P('head', 'ctx'), may hold values from -7 to 7
- out_weight: bfloat16 [4096, 5376], P('head', 'ctx'), may hold values from -0.09375 to 0.09375
- norm_gain: float32 [5376], P('ctx'), may hold values from 0.5 to 1.5
- gate_weight: bfloat16 [5376, 21504], P('head', 'ctx'), may hold values from -0.078125 to 0.078125
- up_weight: bfloat16 [5376, 21504], P('head', 'ctx'), may hold values from -0.078125 to 0.078125
- down_weight: bfloat16 [21504, 5376], P('ctx', 'head'), may hold values from -0.0390625 to 0.0390625
Outputs:
- layer_out: bfloat16 [256, 5376], P('ctx', 'head')
The draws below stay inside these ranges and needn't reach their ends.
Inputs may be any that keep to these rules, and one draw needn't show every extreme that they name: `selected`: each row names 8 different logical pages, among them 16 - 1, the page that holds the block's own positions.
All inputs are finite; a program needn't handle non-finite values.
Results may differ from the reference program's by a relative error of at most 0.02.
Values may be sent and summed in bfloat16 or wider, within the bound.
A program may use at most 128 MiB of HBM per device.

```python
import jax
import jax.numpy as jnp
from jax import lax

D = 5376
FF = 21504
QUERY_HEADS = 32
KEY_VALUE_HEADS = 16
HEAD_SIZE = 128
PAGE_TOKENS = 2048
TILE_QUERY_ROWS = 128
PAGES_PER_TILE = 8
TILES = 2
CACHE_PAGES = 16


def insert_vectors(key):
    sign_values = jax.random.bernoulli(jax.random.fold_in(key, 7), 0.5, (KEY_VALUE_HEADS, HEAD_SIZE))
    return jnp.where(sign_values, 1.0, -1.0).astype(jnp.float32)


def marked_slots(key):
    chosen = jax.random.bernoulli(jax.random.fold_in(key, 8), 0.5, (CACHE_PAGES,))
    return chosen.at[0].set(True)


def draw_queries(key, part):
    row_count = TILES * TILE_QUERY_ROWS
    base_vector = jnp.clip(3.0 * jax.random.normal(jax.random.fold_in(key, 1), (row_count, QUERY_HEADS * HEAD_SIZE), jnp.float32), -24.0, 24.0)
    vector_rows = insert_vectors(key)
    inserted_rows = jnp.repeat(vector_rows, QUERY_HEADS // KEY_VALUE_HEADS, axis=0).reshape(QUERY_HEADS * HEAD_SIZE)
    row_ids = jnp.arange(row_count)
    target = 130.0 + 50.0 * (row_ids // TILE_QUERY_ROWS % 3).astype(jnp.float32)
    strength = jnp.minimum(target * 168.0 ** 0.5 / (5.0 * HEAD_SIZE), 40.0)
    marked = row_ids % TILE_QUERY_ROWS == TILE_QUERY_ROWS // 2
    base_vector = jnp.where(marked[:, None], strength[:, None] * inserted_rows[None, :], base_vector)
    return base_vector.astype(jnp.bfloat16)


def draw_keys(key, part):
    base_vector = jnp.clip(jax.random.normal(jax.random.fold_in(key, 2), (CACHE_PAGES, PAGE_TOKENS, KEY_VALUE_HEADS * HEAD_SIZE), jnp.float32), -6.0, 6.0)
    vector_rows = 5.0 * insert_vectors(key).reshape(KEY_VALUE_HEADS * HEAD_SIZE)
    hot = marked_slots(key)[:, None]
    base_vector = base_vector.at[:, 0, :].set(jnp.where(hot, vector_rows[None, :], base_vector[:, 0, :]))
    base_vector = base_vector.at[:, 1, :].set(jnp.where(hot, 0.992 * vector_rows[None, :], base_vector[:, 1, :]))
    return base_vector.astype(jnp.bfloat16)


def draw_selected(key, part):
    popular = jax.random.randint(jax.random.fold_in(key, 3), (CACHE_PAGES,), 0, 4)
    jitter = jax.random.randint(jax.random.fold_in(key, 4), (TILES, CACHE_PAGES), 0, 64)
    page_ids = jnp.arange(CACHE_PAGES, dtype=jnp.int32)
    ranking = (popular[None, :] * 64 + jitter) * CACHE_PAGES + page_ids[None, :]
    ranking = jnp.where(page_ids[None, :] == CACHE_PAGES - 1, 1 << 29, ranking)
    picked = lax.top_k(ranking, PAGES_PER_TILE)[1]
    return picked.astype(jnp.int32)


def draw_residual_in(key, part):
    row_count = TILES * TILE_QUERY_ROWS
    row_scale = jnp.exp(jax.random.uniform(jax.random.fold_in(key, 5), (row_count, 1), jnp.float32, -0.69, 0.4))
    column = jnp.arange(D).astype(jnp.float32) / D
    column_scale = 0.5 * 3.0 ** column
    base_vector = jnp.clip(jax.random.normal(jax.random.fold_in(key, 6), (row_count, D), jnp.float32), -3.0, 3.0)
    return (base_vector * row_scale * column_scale[None, :]).astype(jnp.bfloat16)


def levels(own_key, extent, cuts, least, top_value):
    def one(dim, blocks):
        heights = jax.random.uniform(jax.random.fold_in(jax.random.fold_in(own_key, 6), dim), (blocks,), jnp.float32, least / len(cuts), top_value / len(cuts))
        return jnp.repeat(jnp.exp(heights), extent[dim] // blocks).reshape((-1,) + (1,) * (len(extent) - dim - 1))

    gain = one(*cuts[0])
    for cut in cuts[1:]:
        gain = gain * one(*cut)
    return gain


def gaussian(stream_key, extent, width, reach, split=(), kind=jnp.bfloat16):
    entries = width * jax.random.normal(stream_key, extent, jnp.float32)
    if split:
        entries = entries * levels(stream_key, extent, split, -0.22, 0.18)
    return jnp.clip(entries, -reach, reach).astype(kind)


def setup_inputs(seed: int = 0) -> dict:
    splits = jax.random.split(jax.random.key(seed), 12)
    queries = draw_queries(jax.random.fold_in(splits[11], 71), 0)
    keys = draw_keys(jax.random.fold_in(splits[11], 71), 0)
    values = gaussian(splits[2], (CACHE_PAGES, PAGE_TOKENS, KEY_VALUE_HEADS * HEAD_SIZE), 1.0, 6.0, ((0, 8), (2, 4)))
    page_map = jax.random.permutation(splits[3], CACHE_PAGES).astype(jnp.int32)
    selected = draw_selected(jax.random.fold_in(splits[11], 71), 0)
    residual_in = draw_residual_in(jax.random.fold_in(splits[11], 71), 0)
    out_weight = gaussian(splits[6], (QUERY_HEADS * HEAD_SIZE, D), (QUERY_HEADS * HEAD_SIZE) ** -0.5, 0.09375, ((0, 4), (1, 8)))
    norm_gain = jnp.clip(0.5 + 1.0 * jax.random.uniform(splits[7], (D,), jnp.float32) ** levels(splits[7], (D,), ((0, 8),), -0.2, 0.2), 0.5, 1.5)
    gate_weight = gaussian(splits[8], (D, FF), D ** -0.5, 0.078125, ((0, 4), (1, 8)))
    up_weight = gaussian(splits[9], (D, FF), D ** -0.5, 0.078125, ((0, 4), (1, 8)))
    down_weight = gaussian(splits[10], (FF, D), FF ** -0.5, 0.0390625, ((0, 8), (1, 4)))
    return dict(queries=queries, keys=keys, values=values, page_map=page_map, selected=selected, residual_in=residual_in, out_weight=out_weight, norm_gain=norm_gain, gate_weight=gate_weight, up_weight=up_weight, down_weight=down_weight)


score_scale = 168.0 ** (-0.5)
masked_score = -1e+30
norm_epsilon = 1e-06

def reference(queries, keys, values, page_map, selected, residual_in, out_weight, norm_gain, gate_weight, up_weight, down_weight):
    row_count = TILES * TILE_QUERY_ROWS
    offset = PAGE_TOKENS - row_count
    query_group_size = QUERY_HEADS // KEY_VALUE_HEADS
    slot_ids = jnp.take(page_map, selected, axis=0).astype(jnp.int32)
    is_causal = selected == CACHE_PAGES - 1
    key_position = jnp.arange(PAGE_TOKENS, dtype=jnp.int32)

    def one_tile(inputs):
        tile_query_rows, tile_page_slots, tile_causal, tile_index = inputs
        tile_key_rows = jnp.take(keys, tile_page_slots, axis=0).reshape(PAGES_PER_TILE * PAGE_TOKENS, KEY_VALUE_HEADS, HEAD_SIZE).astype(jnp.float32)
        tile_value_rows = jnp.take(values, tile_page_slots, axis=0).reshape(PAGES_PER_TILE * PAGE_TOKENS, KEY_VALUE_HEADS, HEAD_SIZE).astype(jnp.float32)
        grouped_queries = tile_query_rows.reshape(TILE_QUERY_ROWS, KEY_VALUE_HEADS, query_group_size, HEAD_SIZE).astype(jnp.float32)
        scores = jnp.einsum('qkgd,jkd->kgqj', grouped_queries, tile_key_rows) * score_scale
        query_position = offset + tile_index * TILE_QUERY_ROWS + jnp.arange(TILE_QUERY_ROWS, dtype=jnp.int32)
        visible = jnp.logical_or(jnp.logical_not(tile_causal)[:, None, None], key_position[None, None, :] <= query_position[None, :, None])
        visible = jnp.transpose(visible, (1, 0, 2)).reshape(TILE_QUERY_ROWS, PAGES_PER_TILE * PAGE_TOKENS)
        scores = jnp.where(visible[None, None], scores, masked_score)
        row_max = lax.optimization_barrier(jnp.max(scores, axis=-1, keepdims=True))
        weights = jnp.where(visible[None, None], jnp.exp(scores - row_max), 0.0)
        row_total = lax.optimization_barrier(jnp.sum(weights, axis=-1))
        rounded = lax.optimization_barrier(weights.astype(jnp.bfloat16)).astype(jnp.float32)
        mixture = jnp.einsum('kgqj,jkd->qkgd', rounded, tile_value_rows)
        mixture = mixture / jnp.transpose(row_total, (2, 0, 1))[..., None]
        return mixture.reshape(TILE_QUERY_ROWS, QUERY_HEADS * HEAD_SIZE).astype(jnp.bfloat16)
    tiled = queries.reshape(TILES, TILE_QUERY_ROWS, QUERY_HEADS * HEAD_SIZE)
    attention = lax.map(one_tile, (tiled, slot_ids, is_causal, jnp.arange(TILES, dtype=jnp.int32)))
    attention = attention.reshape(row_count, QUERY_HEADS * HEAD_SIZE)
    projected = jnp.dot(attention, out_weight, preferred_element_type=jnp.float32)
    stream = (residual_in.astype(jnp.float32) + projected).astype(jnp.bfloat16)
    stream_float = stream.astype(jnp.float32)
    mean_square = lax.optimization_barrier(jnp.mean(stream_float * stream_float, axis=-1, keepdims=True))
    normed = (stream_float * lax.rsqrt(mean_square + norm_epsilon) * norm_gain).astype(jnp.bfloat16)
    gate = jnp.dot(normed, gate_weight, preferred_element_type=jnp.float32)
    upward = jnp.dot(normed, up_weight, preferred_element_type=jnp.float32)
    hidden = (jax.nn.gelu(gate, approximate=True) * upward).astype(jnp.bfloat16)
    mlp_out = jnp.dot(hidden, down_weight, preferred_element_type=jnp.float32)
    return (stream_float + mlp_out).astype(jnp.bfloat16)
```

```python
import jax
import jax.numpy as jnp
import functools
from jax import lax
from jax.experimental import pallas as pl
from jax.experimental.pallas import tpu as pltpu
from jax.sharding import PartitionSpec as P

D = 5376
HEAD_SIZE = 128


score_scale = 168.0 ** (-0.5)
masked_score = -1e30
norm_epsilon = 1e-06


def attention_kernel(
    logical_ref, chosen_ref, page_total, q_ref, k_ref, v_ref, mix_ref, m_ref, l_ref, acc, top, total
):
    page = pl.program_id(1)
    tile_count = chosen_ref.shape[0]
    tile_rows = q_ref.shape[0] // tile_count
    group = q_ref.shape[1] // k_ref.shape[2]
    page_len = k_ref.shape[1]
    offset = page_len - q_ref.shape[0]
    f32 = jnp.float32

    @pl.when(page == 0)
    def _():
        acc[...] = jnp.zeros_like(acc)
        top[...] = jnp.full_like(top, masked_score)
        total[...] = jnp.zeros_like(total)

    causal = logical_ref[page] == page_total - 1

    def visit(t, masked):
        rows = slice(t * tile_rows, (t + 1) * tile_rows)
        for g in range(group):
            cols = slice(g * HEAD_SIZE, (g + 1) * HEAD_SIZE)
            scores = (
                lax.dot_general(
                    q_ref[rows, cols],
                    k_ref[0],
                    (((1,), (1,)), ((), ())),
                    preferred_element_type=f32,
                )
                * score_scale
            )
            if masked:
                position = offset + t * tile_rows + lax.broadcasted_iota(jnp.int32, scores.shape, 0)
                key = lax.broadcasted_iota(jnp.int32, scores.shape, 1)
                scores = jnp.where(key <= position, scores, masked_score)
            old = top[g, rows, :1]
            new = jnp.maximum(old, jnp.max(scores, axis=1, keepdims=True))
            weights = jnp.exp(scores - new)
            keep = jnp.exp(old - new)
            total[g, rows] = total[g, rows] * keep + jnp.sum(weights, axis=1, keepdims=True)
            top[g, rows] = jnp.broadcast_to(new, (tile_rows, 128))
            acc[rows, cols] = acc[rows, cols] * keep + jnp.dot(
                weights.astype(jnp.bfloat16), v_ref[0], preferred_element_type=f32
            )

    for t in range(tile_count):
        picked = chosen_ref[t, page] != 0
        pl.when(jnp.logical_and(picked, causal))(functools.partial(visit, t, True))
        pl.when(jnp.logical_and(picked, jnp.logical_not(causal)))(
            functools.partial(visit, t, False)
        )

    @pl.when(page == pl.num_programs(1) - 1)
    def _():
        mix_ref[...] = acc[...].astype(jnp.bfloat16)
        lane = lax.broadcasted_iota(jnp.int32, m_ref.shape[1:], 1)
        maxima = jnp.zeros(m_ref.shape[1:], f32)
        sums = jnp.zeros(m_ref.shape[1:], f32)
        for g in range(group):
            maxima = jnp.where(lane == g, top[g], maxima)
            sums = jnp.where(lane == g, total[g], sums)
        m_ref[0] = maxima
        l_ref[0] = sums


def owner_pass(queries, keys, values, page_map, selected, ctx_index, ctx_count):
    pages_local, page_len, kv_width = keys.shape
    row_count, query_width = queries.shape
    kv_local = kv_width // HEAD_SIZE
    group = query_width // kv_width
    tile_count = selected.shape[0]
    page_total = pages_local * ctx_count
    slot_ids = ctx_index * pages_local + jnp.arange(pages_local, dtype=jnp.int32)
    all_pages = jnp.arange(page_total, dtype=jnp.int32)
    logical = jnp.sum(
        jnp.where(page_map[None, :] == slot_ids[:, None], all_pages[None, :], 0), axis=1
    )
    chosen = jnp.any(selected[:, None, :] == logical[None, :, None], axis=2).astype(jnp.int32)
    stat = jax.ShapeDtypeStruct((kv_local, row_count, 128), jnp.float32)
    stat_spec = pl.BlockSpec((1, row_count, 128), lambda k, p, a, b: (k, 0, 0))
    kv_spec = pl.BlockSpec((1, page_len, HEAD_SIZE), lambda k, p, a, b: (p, 0, k))
    q_spec = pl.BlockSpec((row_count, group * HEAD_SIZE), lambda k, p, a, b: (0, k))

    def kernel(logical_ref, chosen_ref, *refs):
        attention_kernel(logical_ref, chosen_ref, page_total, *refs)

    mixture, top, total = pl.pallas_call(
        kernel,
        grid_spec=pltpu.PrefetchScalarGridSpec(
            num_scalar_prefetch=2,
            grid=(kv_local, pages_local),
            in_specs=[q_spec, kv_spec, kv_spec],
            out_specs=(q_spec, stat_spec, stat_spec),
            scratch_shapes=[
                pltpu.VMEM((row_count, group * HEAD_SIZE), jnp.float32),
                pltpu.VMEM((group, row_count, 128), jnp.float32),
                pltpu.VMEM((group, row_count, 128), jnp.float32),
            ],
        ),
        out_shape=(jax.ShapeDtypeStruct((row_count, query_width), jnp.bfloat16), stat, stat),
    )(logical.astype(jnp.int32), chosen, queries, keys, values)

    def heads(stacked):
        return stacked[:, :, :group].transpose(1, 0, 2).reshape(row_count, kv_local * group)

    return heads(top), heads(total), mixture


MESH = pl.DeviceIdType.MESH
CORES = 2


def column_tile(width):
    for tile in (896, 768, 640, 512, 384, 256, 128):
        if width % tile == 0:
            return tile
    return width


def flat(block, rows):
    if block.shape[1] % 16:
        return block.astype(jnp.float32).reshape(rows, -1).astype(jnp.bfloat16)
    return block.reshape(rows, -1)


def tail_kernel(
    C,
    H,
    mix_ref,
    stat_ref,
    res_ref,
    gain_ref,
    ow_hbm,
    gw_hbm,
    uw_hbm,
    dw_hbm,
    mlp_ref,
    own_ref,
    ow,
    gw,
    uw,
    dw,
    mix_in,
    stat_in,
    att,
    po,
    po_in,
    u_out,
    st_out,
    ss,
    ublk,
    own_st,
    first,
    first_in,
    second,
    second_in,
    hid,
    acc,
    part,
    part_in,
    w_sem,
    mix_s,
    mix_r,
    stat_s,
    stat_r,
    att_s,
    att_r,
    po_s,
    po_r,
    u_s,
    u_r,
    st_s,
    st_r,
    ss_s,
    ss_r,
    f_s,
    f_r,
    g_s,
    g_r,
    h_s,
    h_r,
    fw_s,
    part_s,
    part_r,
):
    c = lax.axis_index("ctx")
    h = lax.axis_index("head")
    Y = H // CORES
    y = h // CORES
    core = h % CORES
    partner = y * CORES + (CORES - 1 - core)
    R = mix_ref.shape[1]
    rows = C * R
    rb = C // H
    bph = C // H
    width = ow.shape[0]
    head_rows = rows // H
    heads = mix_ref.shape[2] // HEAD_SIZE
    tiles, _, _, _, _, tile = first.shape
    f32 = jnp.float32
    bf16 = jnp.bfloat16

    def remote(src, dst, send_sem, recv_sem, ctx, head):
        return pltpu.make_async_remote_copy(
            src_ref=src,
            dst_ref=dst,
            send_sem=send_sem,
            recv_sem=recv_sem,
            device_id=(ctx, head),
            device_id_type=MESH,
        )

    sent = []

    def send(*args):
        copy = remote(*args)
        copy.start()
        sent.append(copy)

    loads = [
        pltpu.make_async_copy(src, dst, w_sem.at[i])
        for i, (src, dst) in enumerate(
            ((ow_hbm, ow), (gw_hbm, gw), (uw_hbm, uw), (dw_hbm, dw))
        )
    ]
    for load in loads:
        load.start()

    for d in range(1, C):
        peer = (c + d) % C
        send(stat_ref.at[peer], stat_in.at[c], stat_s.at[d], stat_r.at[c], peer, h)
        send(mix_ref.at[peer], mix_in.at[c], mix_s.at[d], mix_r.at[c], peer, h)
    stat_in[c] = stat_ref[c]
    mix_in[c] = mix_ref[c]
    for d in range(1, C):
        peer = (c + C - d) % C
        remote(stat_in.at[peer], stat_in.at[peer], stat_s.at[d], stat_r.at[peer], peer, h).wait_recv()
        remote(mix_in.at[peer], mix_in.at[peer], mix_s.at[d], mix_r.at[peer], peer, h).wait_recv()
    maxima = [stat_in[k][:, :heads] for k in range(C)]
    top = functools.reduce(jnp.maximum, maxima)
    scales = [jnp.exp(m - top) for m in maxima]
    total = sum(stat_in[k][:, heads : 2 * heads] * scales[k] for k in range(C))
    inverse = 1.0 / total
    for g in range(heads):
        cols = slice(g * HEAD_SIZE, (g + 1) * HEAD_SIZE)
        mixed = sum(mix_in[k, :, cols].astype(f32) * scales[k][:, g : g + 1] for k in range(C))
        att[c, :, cols] = (mixed * inverse[:, g : g + 1]).astype(bf16)

    for d in range(1, C):
        peer = (c + d) % C
        send(att.at[c], att.at[c], att_s.at[d], att_r.at[c], peer, h)
    loads[0].wait()
    for d in range(1, C):
        peer = (c + C - d) % C
        remote(att.at[peer], att.at[peer], att_s.at[d], att_r.at[peer], peer, h).wait_recv()
    projected = lax.dot_general(
        flat(att[...], rows), ow[...], (((1,), (1,)), ((), ())), preferred_element_type=f32
    )
    po[...] = projected.reshape(H, head_rows, width).astype(bf16)

    for d in range(1, H):
        peer = (h + d) % H
        send(po.at[peer], po_in.at[h], po_s.at[d], po_r.at[h], c, peer)
    po_in[h] = po[h]
    for d in range(1, H):
        peer = (h + H - d) % H
        remote(po_in.at[peer], po_in.at[peer], po_s.at[d], po_r.at[peer], c, peer).wait_recv()
    projected = sum(po_in[k].astype(f32) for k in range(H))
    stream = (res_ref[...].astype(f32) + projected).astype(bf16).astype(f32)
    st_out[...] = stream.reshape(rb, R, width).astype(bf16)
    u_out[...] = (stream * gain_ref[...]).reshape(rb, R, width).astype(bf16)
    squares = jnp.sum(stream * stream, axis=1, keepdims=True)
    ss[c] = jnp.broadcast_to(squares, (head_rows, 128))

    block_head = c // bph
    block_part = c % bph
    u_dst = ublk.at[block_part, pl.ds(h * rb, rb)]
    kept = []
    for d in range(C):
        peer = (c + d) % C
        copy = remote(u_out, u_dst, u_s.at[d], u_r.at[block_part, h], peer, block_head)
        if d == 0:
            kept.append((block_head != h, copy))
            pl.when(block_head != h)(copy.start)

            @pl.when(block_head == h)
            def _():
                ublk[block_part, pl.ds(h * rb, rb)] = u_out[...]

        else:
            copy.start()
            sent.append(copy)
    for d in range(1, C):
        peer = (c + d) % C
        send(ss.at[c], ss.at[c], ss_s.at[d], ss_r.at[c], peer, h)
    for i in range(rb):
        owner = h * rb + i
        other = jnp.logical_or(owner != c, block_head != h)
        copy = remote(
            st_out.at[i], own_st.at[block_part], st_s.at[i], st_r.at[block_part], owner, block_head
        )
        kept.append((other, copy))
        pl.when(other)(copy.start)

        @pl.when(jnp.logical_not(other))
        def _(i=i):
            own_st[block_part] = st_out[i]

    for j in range(bph):
        for k in range(H):
            source = h * bph + j
            block = ublk.at[j, pl.ds(k * rb, rb)]
            arrival = remote(block, block, u_s.at[0], u_r.at[j, k], source, k)
            pl.when(jnp.logical_or(source != c, h != k))(arrival.wait_recv)
    loads[1].wait()
    loads[2].wait()

    def matmul(i, which, weight):
        cols = slice(i * tile, (i + 1) * tile)
        value = None
        for j in range(bph):
            term = jnp.dot(
                flat(ublk[j], rows),
                weight[j * width : (j + 1) * width, cols],
                preferred_element_type=f32,
            )
            value = term if value is None else value + term
        first[i, which] = value.reshape(Y, CORES, head_rows, tile).swapaxes(0, 1).astype(bf16)
        send(
            first.at[i, which, CORES - 1 - core],
            first_in.at[i, which],
            f_s.at[i, which],
            f_r.at[i, which],
            c,
            partner,
        )

    def middle(i, which):
        remote(
            first_in.at[i, which], first_in.at[i, which], f_s.at[i, which], f_r.at[i, which], c, partner
        ).wait_recv()
        both = first[i, which, core].astype(f32) + first_in[i, which].astype(f32)
        second[i, which] = both.astype(bf16)
        for d in range(1, Y):
            peer = (y + d) % Y
            send(
                second.at[i, which, peer],
                second_in.at[i, which, y],
                g_s.at[i, which, d],
                g_r.at[i, which, y],
                c,
                peer * CORES + core,
            )

    def finish(i, inverse_rms):
        sums = []
        for which in range(2):
            value = second[i, which, y].astype(f32)
            for d in range(1, Y):
                peer = (y + Y - d) % Y
                slot = second_in.at[i, which, peer]
                remote(
                    slot, slot, g_s.at[i, which, d], g_r.at[i, which, peer], c, peer * CORES + core
                ).wait_recv()
                value = value + second_in[i, which, peer].astype(f32)
            sums.append(value * inverse_rms)
        hid[i, h] = (jax.nn.gelu(sums[0], approximate=True) * sums[1]).astype(bf16)
        send(hid.at[i, h], hid.at[i, h], h_s.at[i, 0], h_r.at[i, h], c, partner)
        for d in range(1, Y):
            peer = ((y + d) % Y) * CORES + core
            send(hid.at[i, h], hid.at[i, h], h_s.at[i, d], h_r.at[i, h], c, peer)

    def forward(i):
        for d in range(1, Y):
            origin = ((y + Y - d) % Y) * CORES + core
            slot = hid.at[i, origin]
            remote(slot, slot, h_s.at[i, d], h_r.at[i, origin], c, origin).wait_recv()
            send(slot, slot, fw_s.at[i, d], h_r.at[i, origin], c, partner)

    def down(i):
        for d in range(Y):
            origin = ((y + Y - d) % Y) * CORES + (CORES - 1 - core)
            slot = hid.at[i, origin]
            remote(slot, slot, h_s.at[i, 0], h_r.at[i, origin], c, partner).wait_recv()
        term = lax.dot_general(
            flat(hid[i], rows),
            dw[:, i * tile : (i + 1) * tile],
            (((1,), (1,)), ((), ())),
            preferred_element_type=f32,
        )
        if i == 0:
            acc[...] = term
        else:
            acc[...] += term

    steps = [(i, which) for i in range(tiles) for which in range(2)]
    for n, (i, which) in enumerate(steps):
        matmul(i, which, (gw, uw)[which])
        if n:
            middle(*steps[n - 1])
    middle(*steps[-1])
    for d in range(1, C):
        peer = (c + C - d) % C
        remote(ss.at[peer], ss.at[peer], ss_s.at[d], ss_r.at[peer], peer, h).wait_recv()
    squares = sum(ss[k] for k in range(C))
    inverse_rms = lax.rsqrt(squares[:, :1] / (C * width) + norm_epsilon)
    loads[3].wait()
    for i in range(tiles):
        finish(i, inverse_rms)
        if i:
            forward(i - 1)
    forward(tiles - 1)
    for i in range(tiles):
        down(i)
    part[...] = acc[...].reshape(C, R, acc.shape[1]).astype(bf16)

    for d in range(1, C):
        peer = (c + d) % C
        send(part.at[peer], part_in.at[c], part_s.at[d], part_r.at[c], peer, h)
    part_in[c] = part[c]
    for j in range(bph):
        source = h * bph + j
        arrival = remote(own_st.at[j], own_st.at[j], st_s.at[0], st_r.at[j], source, c // rb)
        pl.when(jnp.logical_or(source != c, c // rb != h))(arrival.wait_recv)
    own_ref[...] = own_st[...]
    for d in range(1, C):
        peer = (c + C - d) % C
        remote(part_in.at[peer], part_in.at[peer], part_s.at[d], part_r.at[peer], peer, h).wait_recv()
    mlp_ref[...] = sum(part_in[k].astype(f32) for k in range(C))
    for copy in sent:
        copy.wait_send()
    for condition, copy in kept:
        pl.when(condition)(copy.wait_send)


def tail(C, H, mixture, stats, residual_in, norm_gain, out_weight, gate_weight, up_weight, down_weight):
    rows, query_width = mixture.shape
    R = rows // C
    width = out_weight.shape[1]
    hidden = gate_weight.shape[1]
    out_width = down_weight.shape[1]
    out_weight = out_weight.T
    down_weight = down_weight.T
    rb = C // H
    bph = C // H
    Y = H // CORES
    head_rows = rows // H
    tile = column_tile(hidden)
    tiles = hidden // tile
    bf16 = jnp.bfloat16
    vmem = pl.BlockSpec(memory_space=pltpu.VMEM)
    hbm = pl.BlockSpec(memory_space=pl.ANY)
    V = pltpu.VMEM
    S = pltpu.SemaphoreType.DMA
    return pl.pallas_call(
        functools.partial(tail_kernel, C, H),
        out_shape=(
            jax.ShapeDtypeStruct((R, out_width), jnp.float32),
            jax.ShapeDtypeStruct((bph, R, width), bf16),
        ),
        in_specs=[vmem] * 4 + [hbm] * 4,
        out_specs=(vmem, vmem),
        scratch_shapes=[
            V(out_weight.shape, bf16),
            V(gate_weight.shape, bf16),
            V(up_weight.shape, bf16),
            V(down_weight.shape, bf16),
            V((C, R, query_width), bf16),
            V((C, R, 128), jnp.float32),
            V((C, R, query_width), bf16),
            V((H, head_rows, width), bf16),
            V((H, head_rows, width), bf16),
            V((rb, R, width), bf16),
            V((rb, R, width), bf16),
            V((C, head_rows, 128), jnp.float32),
            V((bph, C, R, width), bf16),
            V((bph, R, width), bf16),
            V((tiles, 2, CORES, Y, head_rows, tile), bf16),
            V((tiles, 2, Y, head_rows, tile), bf16),
            V((tiles, 2, Y, head_rows, tile), bf16),
            V((tiles, 2, Y, head_rows, tile), bf16),
            V((tiles, H, head_rows, tile), bf16),
            V((rows, out_width), jnp.float32),
            V((C, R, out_width), bf16),
            V((C, R, out_width), bf16),
            S((4,)),
            S((C,)),
            S((C,)),
            S((C,)),
            S((C,)),
            S((C,)),
            S((C,)),
            S((H,)),
            S((H,)),
            S((C,)),
            S((bph, H)),
            S((rb,)),
            S((bph,)),
            S((C,)),
            S((C,)),
            S((tiles, 2)),
            S((tiles, 2)),
            S((tiles, 2, Y)),
            S((tiles, 2, Y)),
            S((tiles, Y)),
            S((tiles, H)),
            S((tiles, Y)),
            S((C,)),
            S((C,)),
        ],
        compiler_params=pltpu.CompilerParams(
            has_side_effects=True, vmem_limit_bytes=60 * 2**20
        ),
    )(
        mixture.reshape(C, R, query_width),
        stats.reshape(C, R, 128),
        residual_in,
        norm_gain.reshape(1, width),
        out_weight,
        gate_weight,
        up_weight,
        down_weight,
    )


def shards(
    queries,
    keys,
    values,
    page_map,
    selected,
    residual_in,
    out_weight,
    norm_gain,
    gate_weight,
    up_weight,
    down_weight,
):
    ctx_index = lax.axis_index("ctx")
    C = lax.axis_size("ctx")
    H = lax.axis_size("head")
    row_max, row_total, mixture = owner_pass(
        queries, keys, values, page_map, selected, ctx_index, C
    )
    stats = jnp.concatenate([row_max, row_total], axis=1)
    stats = jnp.pad(stats, ((0, 0), (0, 128 - stats.shape[1])))
    mlp_out, own_stream = tail(
        C,
        H,
        mixture.astype(jnp.bfloat16),
        stats,
        residual_in,
        norm_gain,
        out_weight,
        gate_weight,
        up_weight,
        down_weight,
    )
    own_stream = jnp.concatenate([own_stream[j] for j in range(own_stream.shape[0])], axis=1)
    return (own_stream.astype(jnp.float32) + mlp_out).astype(jnp.bfloat16)


def solution(mesh):
    in_specs = (
        P(None, "head"),
        P("ctx", None, "head"),
        P("ctx", None, "head"),
        P(),
        P(),
        P("head", "ctx"),
        P("head", "ctx"),
        P("ctx"),
        P("head", "ctx"),
        P("head", "ctx"),
        P("ctx", "head"),
    )
    out_specs = P("ctx", "head")
    return jax.shard_map(shards, mesh=mesh, in_specs=in_specs, out_specs=out_specs, check_vma=False)
```

```python
import jax
import jax.numpy as jnp
import functools
from jax import lax
from jax.experimental import pallas as pl
from jax.experimental.pallas import tpu as pltpu
from jax.sharding import PartitionSpec as P

D = 5376
HEAD_SIZE = 128


score_scale = 168.0 ** (-0.5)
masked_score = -1e30
norm_epsilon = 1e-06


def attention_kernel(
    logical_ref, chosen_ref, page_total, q_ref, k_ref, v_ref, mix_ref, m_ref, l_ref, acc, top, total
):
    page = pl.program_id(1)
    tile_count = chosen_ref.shape[0]
    tile_rows = q_ref.shape[0] // tile_count
    group = q_ref.shape[1] // k_ref.shape[2]
    page_len = k_ref.shape[1]
    offset = page_len - q_ref.shape[0]
    f32 = jnp.float32

    @pl.when(page == 0)
    def _():
        acc[...] = jnp.zeros_like(acc)
        top[...] = jnp.full_like(top, masked_score)
        total[...] = jnp.zeros_like(total)

    causal = logical_ref[page] == page_total - 1

    def visit(t, masked):
        rows = slice(t * tile_rows, (t + 1) * tile_rows)
        for g in range(group):
            cols = slice(g * HEAD_SIZE, (g + 1) * HEAD_SIZE)
            scores = (
                lax.dot_general(
                    q_ref[rows, cols],
                    k_ref[0],
                    (((1,), (1,)), ((), ())),
                    preferred_element_type=f32,
                )
                * score_scale
            )
            if masked:
                position = offset + t * tile_rows + lax.broadcasted_iota(jnp.int32, scores.shape, 0)
                key = lax.broadcasted_iota(jnp.int32, scores.shape, 1)
                scores = jnp.where(key <= position, scores, masked_score)
            old = top[g, rows, :1]
            new = jnp.maximum(old, jnp.max(scores, axis=1, keepdims=True))
            weights = jnp.exp(scores - new)
            keep = jnp.exp(old - new)
            total[g, rows] = total[g, rows] * keep + jnp.sum(weights, axis=1, keepdims=True)
            top[g, rows] = jnp.broadcast_to(new, (tile_rows, 128))
            acc[rows, cols] = acc[rows, cols] * keep + jnp.dot(
                weights.astype(jnp.bfloat16), v_ref[0], preferred_element_type=f32
            )

    for t in range(tile_count):
        picked = chosen_ref[t, page] != 0
        pl.when(jnp.logical_and(picked, causal))(functools.partial(visit, t, True))
        pl.when(jnp.logical_and(picked, jnp.logical_not(causal)))(
            functools.partial(visit, t, False)
        )

    @pl.when(page == pl.num_programs(1) - 1)
    def _():
        mix_ref[...] = acc[...].astype(jnp.bfloat16)
        lane = lax.broadcasted_iota(jnp.int32, m_ref.shape[1:], 1)
        maxima = jnp.zeros(m_ref.shape[1:], f32)
        sums = jnp.zeros(m_ref.shape[1:], f32)
        for g in range(group):
            maxima = jnp.where(lane == g, top[g], maxima)
            sums = jnp.where(lane == g, total[g], sums)
        m_ref[0] = maxima
        l_ref[0] = sums


def owner_pass(queries, keys, values, page_map, selected, ctx_index, ctx_count):
    pages_local, page_len, kv_width = keys.shape
    row_count, query_width = queries.shape
    kv_local = kv_width // HEAD_SIZE
    group = query_width // kv_width
    tile_count = selected.shape[0]
    page_total = pages_local * ctx_count
    slot_ids = ctx_index * pages_local + jnp.arange(pages_local, dtype=jnp.int32)
    all_pages = jnp.arange(page_total, dtype=jnp.int32)
    logical = jnp.sum(
        jnp.where(page_map[None, :] == slot_ids[:, None], all_pages[None, :], 0), axis=1
    )
    chosen = jnp.any(selected[:, None, :] == logical[None, :, None], axis=2).astype(jnp.int32)
    stat = jax.ShapeDtypeStruct((kv_local, row_count, 128), jnp.float32)
    stat_spec = pl.BlockSpec((1, row_count, 128), lambda k, p, a, b: (k, 0, 0))
    kv_spec = pl.BlockSpec((1, page_len, HEAD_SIZE), lambda k, p, a, b: (p, 0, k))
    q_spec = pl.BlockSpec((row_count, group * HEAD_SIZE), lambda k, p, a, b: (0, k))

    def kernel(logical_ref, chosen_ref, *refs):
        attention_kernel(logical_ref, chosen_ref, page_total, *refs)

    mixture, top, total = pl.pallas_call(
        kernel,
        grid_spec=pltpu.PrefetchScalarGridSpec(
            num_scalar_prefetch=2,
            grid=(kv_local, pages_local),
            in_specs=[q_spec, kv_spec, kv_spec],
            out_specs=(q_spec, stat_spec, stat_spec),
            scratch_shapes=[
                pltpu.VMEM((row_count, group * HEAD_SIZE), jnp.float32),
                pltpu.VMEM((group, row_count, 128), jnp.float32),
                pltpu.VMEM((group, row_count, 128), jnp.float32),
            ],
        ),
        out_shape=(jax.ShapeDtypeStruct((row_count, query_width), jnp.bfloat16), stat, stat),
    )(logical.astype(jnp.int32), chosen, queries, keys, values)

    def heads(stacked):
        return stacked[:, :, :group].transpose(1, 0, 2).reshape(row_count, kv_local * group)

    return heads(top), heads(total), mixture


MESH = pl.DeviceIdType.MESH
CORES = 2


def column_tile(width):
    for tile in (896, 768, 640, 512, 384, 256, 128):
        if width % tile == 0:
            return tile
    return width


def flat(block, rows):
    if block.shape[1] % 16:
        return block.astype(jnp.float32).reshape(rows, -1).astype(jnp.bfloat16)
    return block.reshape(rows, -1)


def tail_kernel(
    C,
    H,
    mix_ref,
    stat_ref,
    res_ref,
    gain_ref,
    ow_hbm,
    gw_hbm,
    uw_hbm,
    dw_hbm,
    mlp_ref,
    own_ref,
    ow,
    gw,
    uw,
    dw,
    mix_in,
    stat_in,
    att,
    po,
    po_in,
    u_out,
    st_out,
    ss,
    ublk,
    own_st,
    first,
    first_in,
    second,
    second_in,
    hid,
    acc,
    part,
    part_in,
    w_sem,
    mix_s,
    mix_r,
    stat_s,
    stat_r,
    att_s,
    att_r,
    po_s,
    po_r,
    u_s,
    u_r,
    st_s,
    st_r,
    ss_s,
    ss_r,
    f_s,
    f_r,
    g_s,
    g_r,
    h_s,
    h_r,
    fw_s,
    part_s,
    part_r,
):
    c = lax.axis_index("ctx")
    h = lax.axis_index("head")
    Y = H // CORES
    y = h // CORES
    core = h % CORES
    partner = y * CORES + (CORES - 1 - core)
    R = mix_ref.shape[1]
    rows = C * R
    rb = C // H
    bph = C // H
    width = ow.shape[0]
    head_rows = rows // H
    heads = mix_ref.shape[2] // HEAD_SIZE
    tiles, _, _, _, _, tile = first.shape
    f32 = jnp.float32
    bf16 = jnp.bfloat16

    def remote(src, dst, send_sem, recv_sem, ctx, head):
        return pltpu.make_async_remote_copy(
            src_ref=src,
            dst_ref=dst,
            send_sem=send_sem,
            recv_sem=recv_sem,
            device_id=(ctx, head),
            device_id_type=MESH,
        )

    sent = []

    def send(*args):
        copy = remote(*args)
        copy.start()
        sent.append(copy)

    loads = [
        pltpu.make_async_copy(src, dst, w_sem.at[i])
        for i, (src, dst) in enumerate(
            ((ow_hbm, ow), (gw_hbm, gw), (uw_hbm, uw), (dw_hbm, dw))
        )
    ]
    for load in loads:
        load.start()

    for d in range(1, C):
        peer = (c + d) % C
        send(stat_ref.at[peer], stat_in.at[c], stat_s.at[d], stat_r.at[c], peer, h)
        send(mix_ref.at[peer], mix_in.at[c], mix_s.at[d], mix_r.at[c], peer, h)
    stat_in[c] = stat_ref[c]
    mix_in[c] = mix_ref[c]
    for d in range(1, C):
        peer = (c + C - d) % C
        remote(stat_in.at[peer], stat_in.at[peer], stat_s.at[d], stat_r.at[peer], peer, h).wait_recv()
        remote(mix_in.at[peer], mix_in.at[peer], mix_s.at[d], mix_r.at[peer], peer, h).wait_recv()
    maxima = [stat_in[k][:, :heads] for k in range(C)]
    top = functools.reduce(jnp.maximum, maxima)
    scales = [jnp.exp(m - top) for m in maxima]
    total = sum(stat_in[k][:, heads : 2 * heads] * scales[k] for k in range(C))
    inverse = 1.0 / total
    for g in range(heads):
        cols = slice(g * HEAD_SIZE, (g + 1) * HEAD_SIZE)
        mixed = sum(mix_in[k, :, cols].astype(f32) * scales[k][:, g : g + 1] for k in range(C))
        att[c, :, cols] = (mixed * inverse[:, g : g + 1]).astype(bf16)

    for d in range(1, C):
        peer = (c + d) % C
        send(att.at[c], att.at[c], att_s.at[d], att_r.at[c], peer, h)
    loads[0].wait()
    for d in range(1, C):
        peer = (c + C - d) % C
        remote(att.at[peer], att.at[peer], att_s.at[d], att_r.at[peer], peer, h).wait_recv()
    projected = lax.dot_general(
        flat(att[...], rows), ow[...], (((1,), (1,)), ((), ())), preferred_element_type=f32
    )
    po[...] = projected.reshape(H, head_rows, width).astype(bf16)

    for d in range(1, H):
        peer = (h + d) % H
        send(po.at[peer], po_in.at[h], po_s.at[d], po_r.at[h], c, peer)
    po_in[h] = po[h]
    for d in range(1, H):
        peer = (h + H - d) % H
        remote(po_in.at[peer], po_in.at[peer], po_s.at[d], po_r.at[peer], c, peer).wait_recv()
    projected = sum(po_in[k].astype(f32) for k in range(H))
    stream = (res_ref[...].astype(f32) + projected).astype(bf16).astype(f32)
    st_out[...] = stream.reshape(rb, R, width).astype(bf16)
    u_out[...] = (stream * gain_ref[...]).reshape(rb, R, width).astype(bf16)
    squares = jnp.sum(stream * stream, axis=1, keepdims=True)
    ss[c] = jnp.broadcast_to(squares, (head_rows, 128))

    block_head = c // bph
    block_part = c % bph
    u_dst = ublk.at[block_part, pl.ds(h * rb, rb)]
    kept = []
    for d in range(C):
        peer = (c + d) % C
        copy = remote(u_out, u_dst, u_s.at[d], u_r.at[block_part, h], peer, block_head)
        if d == 0:
            kept.append((block_head != h, copy))
            pl.when(block_head != h)(copy.start)

            @pl.when(block_head == h)
            def _():
                ublk[block_part, pl.ds(h * rb, rb)] = u_out[...]

        else:
            copy.start()
            sent.append(copy)
    for d in range(1, C):
        peer = (c + d) % C
        send(ss.at[c], ss.at[c], ss_s.at[d], ss_r.at[c], peer, h)
    for i in range(rb):
        owner = h * rb + i
        other = jnp.logical_or(owner != c, block_head != h)
        copy = remote(
            st_out.at[i], own_st.at[block_part], st_s.at[i], st_r.at[block_part], owner, block_head
        )
        kept.append((other, copy))
        pl.when(other)(copy.start)

        @pl.when(jnp.logical_not(other))
        def _(i=i):
            own_st[block_part] = st_out[i]

    for j in range(bph):
        for k in range(H):
            source = h * bph + j
            block = ublk.at[j, pl.ds(k * rb, rb)]
            arrival = remote(block, block, u_s.at[0], u_r.at[j, k], source, k)
            pl.when(jnp.logical_or(source != c, h != k))(arrival.wait_recv)
    loads[1].wait()
    loads[2].wait()

    def matmul(i, which, weight):
        cols = slice(i * tile, (i + 1) * tile)
        value = None
        for j in range(bph):
            term = jnp.dot(
                flat(ublk[j], rows),
                weight[j * width : (j + 1) * width, cols],
                preferred_element_type=f32,
            )
            value = term if value is None else value + term
        first[i, which] = value.reshape(Y, CORES, head_rows, tile).swapaxes(0, 1).astype(bf16)
        send(
            first.at[i, which, CORES - 1 - core],
            first_in.at[i, which],
            f_s.at[i, which],
            f_r.at[i, which],
            c,
            partner,
        )

    def middle(i, which):
        remote(
            first_in.at[i, which], first_in.at[i, which], f_s.at[i, which], f_r.at[i, which], c, partner
        ).wait_recv()
        both = first[i, which, core].astype(f32) + first_in[i, which].astype(f32)
        second[i, which] = both.astype(bf16)
        for d in range(1, Y):
            peer = (y + d) % Y
            send(
                second.at[i, which, peer],
                second_in.at[i, which, y],
                g_s.at[i, which, d],
                g_r.at[i, which, y],
                c,
                peer * CORES + core,
            )

    def finish(i, inverse_rms):
        sums = []
        for which in range(2):
            value = second[i, which, y].astype(f32)
            for d in range(1, Y):
                peer = (y + Y - d) % Y
                slot = second_in.at[i, which, peer]
                remote(
                    slot, slot, g_s.at[i, which, d], g_r.at[i, which, peer], c, peer * CORES + core
                ).wait_recv()
                value = value + second_in[i, which, peer].astype(f32)
            sums.append(value * inverse_rms)
        hid[i, h] = (jax.nn.gelu(sums[0], approximate=True) * sums[1]).astype(bf16)
        send(hid.at[i, h], hid.at[i, h], h_s.at[i, 0], h_r.at[i, h], c, partner)
        for d in range(1, Y):
            peer = ((y + d) % Y) * CORES + core
            send(hid.at[i, h], hid.at[i, h], h_s.at[i, d], h_r.at[i, h], c, peer)

    def forward(i):
        for d in range(1, Y):
            origin = ((y + Y - d) % Y) * CORES + core
            slot = hid.at[i, origin]
            remote(slot, slot, h_s.at[i, d], h_r.at[i, origin], c, origin).wait_recv()
            send(slot, slot, fw_s.at[i, d], h_r.at[i, origin], c, partner)

    def down(i):
        for d in range(Y):
            origin = ((y + Y - d) % Y) * CORES + (CORES - 1 - core)
            slot = hid.at[i, origin]
            remote(slot, slot, h_s.at[i, 0], h_r.at[i, origin], c, partner).wait_recv()
        term = lax.dot_general(
            flat(hid[i], rows),
            dw[:, i * tile : (i + 1) * tile],
            (((1,), (1,)), ((), ())),
            preferred_element_type=f32,
        )
        if i == 0:
            acc[...] = term
        else:
            acc[...] += term

    steps = [(i, which) for i in range(tiles) for which in range(2)]
    for n, (i, which) in enumerate(steps):
        matmul(i, which, (gw, uw)[which])
        if n:
            middle(*steps[n - 1])
    middle(*steps[-1])
    for d in range(1, C):
        peer = (c + C - d) % C
        remote(ss.at[peer], ss.at[peer], ss_s.at[d], ss_r.at[peer], peer, h).wait_recv()
    squares = sum(ss[k] for k in range(C))
    inverse_rms = lax.rsqrt(squares[:, :1] / (C * width) + norm_epsilon)
    loads[3].wait()
    for i in range(tiles):
        finish(i, inverse_rms)
        if i:
            forward(i - 1)
    forward(tiles - 1)
    for i in range(tiles):
        down(i)
    part[...] = acc[...].reshape(C, R, acc.shape[1]).astype(bf16)

    for d in range(1, C):
        peer = (c + d) % C
        send(part.at[peer], part_in.at[c], part_s.at[d], part_r.at[c], peer, h)
    part_in[c] = part[c]
    for j in range(bph):
        source = h * bph + j
        arrival = remote(own_st.at[j], own_st.at[j], st_s.at[0], st_r.at[j], source, c // rb)
        pl.when(jnp.logical_or(source != c, c // rb != h))(arrival.wait_recv)
    own_ref[...] = own_st[...]
    for d in range(1, C):
        peer = (c + C - d) % C
        remote(part_in.at[peer], part_in.at[peer], part_s.at[d], part_r.at[peer], peer, h).wait_recv()
    mlp_ref[...] = sum(part_in[k].astype(f32) for k in range(C))
    for copy in sent:
        copy.wait_send()
    for condition, copy in kept:
        pl.when(condition)(copy.wait_send)


def tail(C, H, mixture, stats, residual_in, norm_gain, out_weight, gate_weight, up_weight, down_weight):
    rows, query_width = mixture.shape
    R = rows // C
    width = out_weight.shape[1]
    hidden = gate_weight.shape[1]
    out_width = down_weight.shape[1]
    out_weight = out_weight.T
    down_weight = down_weight.T
    rb = C // H
    bph = C // H
    Y = H // CORES
    head_rows = rows // H
    tile = column_tile(hidden)
    tiles = hidden // tile
    bf16 = jnp.bfloat16
    vmem = pl.BlockSpec(memory_space=pltpu.VMEM)
    hbm = pl.BlockSpec(memory_space=pl.ANY)
    V = pltpu.VMEM
    S = pltpu.SemaphoreType.DMA
    return pl.pallas_call(
        functools.partial(tail_kernel, C, H),
        out_shape=(
            jax.ShapeDtypeStruct((R, out_width), jnp.float32),
            jax.ShapeDtypeStruct((bph, R, width), bf16),
        ),
        in_specs=[vmem] * 4 + [hbm] * 4,
        out_specs=(vmem, vmem),
        scratch_shapes=[
            V(out_weight.shape, bf16),
            V(gate_weight.shape, bf16),
            V(up_weight.shape, bf16),
            V(down_weight.shape, bf16),
            V((C, R, query_width), bf16),
            V((C, R, 128), jnp.float32),
            V((C, R, query_width), bf16),
            V((H, head_rows, width), bf16),
            V((H, head_rows, width), bf16),
            V((rb, R, width), bf16),
            V((rb, R, width), bf16),
            V((C, head_rows, 128), jnp.float32),
            V((bph, C, R, width), bf16),
            V((bph, R, width), bf16),
            V((tiles, 2, CORES, Y, head_rows, tile), bf16),
            V((tiles, 2, Y, head_rows, tile), bf16),
            V((tiles, 2, Y, head_rows, tile), bf16),
            V((tiles, 2, Y, head_rows, tile), bf16),
            V((tiles, H, head_rows, tile), bf16),
            V((rows, out_width), jnp.float32),
            V((C, R, out_width), bf16),
            V((C, R, out_width), bf16),
            S((4,)),
            S((C,)),
            S((C,)),
            S((C,)),
            S((C,)),
            S((C,)),
            S((C,)),
            S((H,)),
            S((H,)),
            S((C,)),
            S((bph, H)),
            S((rb,)),
            S((bph,)),
            S((C,)),
            S((C,)),
            S((tiles, 2)),
            S((tiles, 2)),
            S((tiles, 2, Y)),
            S((tiles, 2, Y)),
            S((tiles, Y)),
            S((tiles, H)),
            S((tiles, Y)),
            S((C,)),
            S((C,)),
        ],
        compiler_params=pltpu.CompilerParams(
            has_side_effects=True, vmem_limit_bytes=60 * 2**20
        ),
    )(
        mixture.reshape(C, R, query_width),
        stats.reshape(C, R, 128),
        residual_in,
        norm_gain.reshape(1, width),
        out_weight,
        gate_weight,
        up_weight,
        down_weight,
    )


LOG2E = 1.4426950408889634


def fused_kernel(
    C,
    H,
    NP,
    map_ref,
    sel_ref,
    q_ref,
    res_ref,
    gain_ref,
    k_hbm,
    v_hbm,
    ow_hbm,
    gw_hbm,
    uw_hbm,
    dw_hbm,
    out_ref,
    k_buf,
    v_buf,
    ow,
    gw,
    uw,
    dw,
    mix_out,
    mix_in,
    lse_out,
    lse_in,
    att,
    po_out,
    po_in,
    res_in,
    st,
    u,
    ss_out,
    ss_in,
    ss_mid,
    ss_last,
    first,
    first_in,
    second,
    second_in,
    hid,
    acc,
    part,
    part_in,
    kv_sem,
    w_sem,
    mix_s,
    mix_r,
    lse_s,
    lse_r,
    att_s,
    att_r,
    po_s,
    po_r,
    res_s,
    res_r,
    u_s,
    u_r,
    ss_s,
    ss_r,
    f_s,
    f_r,
    g_s,
    g_r,
    h_s,
    h_r,
    fw_s,
    part_s,
    part_r,
):
    c = lax.axis_index("ctx")
    h = lax.axis_index("head")
    X = C // H
    Z = C // X
    z = c // X
    x = c % X
    Y = H // CORES
    y = h // CORES
    core = h % CORES
    partner = y * CORES + (CORES - 1 - core)
    _, NQ, RC, query_width = q_ref.shape
    rows = C * RC
    hr = rows // H
    kv, pages, page_len, _ = k_buf.shape
    group = query_width // (kv * HEAD_SIZE)
    gw_cols = group * HEAD_SIZE
    tile_count = sel_ref.shape[0]
    tile_rows = NQ * rows // tile_count
    offset = page_len - NQ * rows
    page_total = map_ref.shape[0]
    width = ow.shape[0]
    tile = first.shape[-1]
    tiles = first.shape[1]
    RP = rows // NP
    f32 = jnp.float32
    bf16 = jnp.bfloat16
    owner = h == z
    visitor = h != z

    def remote(src, dst, send_sem, recv_sem, ctx, head):
        return pltpu.make_async_remote_copy(
            src_ref=src,
            dst_ref=dst,
            send_sem=send_sem,
            recv_sem=recv_sem,
            device_id=(ctx, head),
            device_id_type=MESH,
        )

    sent = []
    kept = []

    def send(*args):
        copy = remote(*args)
        copy.start()
        sent.append(copy)

    def send_if(condition, *args):
        copy = remote(*args)
        pl.when(condition)(copy.start)
        kept.append((condition, copy))

    def kv_load(j):
        lanes = pl.ds(pl.multiple_of(j * HEAD_SIZE, HEAD_SIZE), HEAD_SIZE)
        return (
            pltpu.make_async_copy(k_hbm.at[:, :, lanes], k_buf.at[j], kv_sem.at[0, j]),
            pltpu.make_async_copy(v_hbm.at[:, :, lanes], v_buf.at[j], kv_sem.at[1, j]),
        )

    for j in range(kv):
        for load in kv_load(j):
            load.start()
    loads = [
        pltpu.make_async_copy(src, dst, w_sem.at[i])
        for i, (src, dst) in enumerate(
            ((ow_hbm, ow), (gw_hbm, gw), (uw_hbm, uw), (dw_hbm, dw))
        )
    ]
    for load in loads:
        load.start()

    send_if(visitor, res_ref, res_in.at[h], res_s.at[0], res_r.at[h], c, z)
    res_in[h] = res_ref[...]

    facts = []
    for p in range(pages):
        slot = c * pages + p
        logical = jnp.int32(0)
        for j in range(page_total):
            logical = logical + jnp.where(map_ref[j] == slot, j, 0)
        picks = []
        for t in range(tile_count):
            hits = jnp.int32(0)
            for i in range(sel_ref.shape[1]):
                hits = hits + jnp.where(sel_ref[t, i] == logical, 1, 0)
            picks.append(jnp.where(hits > 0, 0.0, masked_score).astype(f32))
        reach = jnp.where(logical == page_total - 1, 0, page_len)
        facts.append((reach, picks))

    index = lax.broadcasted_iota(jnp.int32, (group * rows, 1), 0) & (rows - 1)
    shift = RC.bit_length() - 1
    base_row = (index >> shift) * (NQ * RC) + (index & (RC - 1))
    eye = lax.broadcasted_iota(jnp.int32, (rows, rows), 0) == lax.broadcasted_iota(
        jnp.int32, (rows, rows), 1
    )
    unit = score_scale * LOG2E

    def attend(n):
        q = n // kv
        j = n % kv

        @pl.when(n < kv)
        def _():
            for load in kv_load(j):
                load.wait()

        lanes = pl.ds(pl.multiple_of(j * gw_cols, gw_cols), gw_cols)
        block = q_ref[:, q, :, lanes].reshape(rows, gw_cols)
        lhs = jnp.concatenate(
            [block[:, g * HEAD_SIZE : (g + 1) * HEAD_SIZE] for g in range(group)], axis=0
        )
        row = base_row + q * RC
        key = offset + lax.broadcasted_iota(jnp.int32, (group * rows, page_len - offset), 1)
        tops, sums, outs = [], [], []
        for p in range(pages):
            reach, picks = facts[p]
            bias = jnp.zeros((group * rows, 1), f32)
            for t in range(tile_count):
                inside = jnp.logical_and(row >= t * tile_rows, row < (t + 1) * tile_rows)
                bias = jnp.where(inside, picks[t], bias)
            scores = lax.dot_general(
                lhs, k_buf[j, p], (((1,), (1,)), ((), ())), preferred_element_type=f32
            )
            late = jnp.where(key <= offset + row + reach, scores[:, offset:], masked_score)
            scores = jnp.concatenate([scores[:, :offset], late], axis=1)
            top = jnp.max(scores, axis=1, keepdims=True)
            weights = jnp.exp2((scores - top) * unit)
            sums.append(jnp.sum(weights, axis=1, keepdims=True))
            outs.append(
                jnp.dot(weights.astype(bf16), v_buf[j, p], preferred_element_type=f32)
            )
            tops.append(top * unit + bias)
        best = functools.reduce(jnp.maximum, tops)
        scales = [jnp.exp2(top - best) for top in tops]
        total = sum(s * e for s, e in zip(sums, scales))
        mixed = sum(o * (e / total) for o, e in zip(outs, scales))
        lse = best + jnp.log2(total)
        for g in range(group):
            part_rows = slice(g * rows, (g + 1) * rows)
            mix_out[n, :, :, g * HEAD_SIZE : (g + 1) * HEAD_SIZE] = (
                mixed[part_rows].reshape(C, RC, HEAD_SIZE).astype(bf16)
            )
            lse_out[n, g : g + 1] = jnp.sum(
                jnp.where(eye, lse[part_rows], 0.0), axis=0, keepdims=True
            )
        for copy in mix_sends(n):
            copy.start()
        mix_in[n, c] = mix_out[n, c]
        lse_in[n, c] = lse_out[n]

    def mix_sends(n):
        copies = []
        for d in range(1, C):
            peer = (c + d) % C
            copies.append(
                remote(mix_out.at[n, peer], mix_in.at[n, c], mix_s.at[n, d], mix_r.at[n, c], peer, h)
            )
            copies.append(
                remote(lse_out.at[n], lse_in.at[n, c], lse_s.at[n, d], lse_r.at[n, c], peer, h)
            )
        return copies

    def att_sends(n):
        copies = []
        for d in range(1, C):
            peer = (c + d) % C
            copies.append(
                remote(att.at[n, c], att.at[n, c], att_s.at[n, d], att_r.at[n, c], peer, h)
            )
        return copies

    def combine(n):
        for d in range(1, C):
            peer = (c + C - d) % C
            block = lse_in.at[n, peer]
            remote(block, block, lse_s.at[n, d], lse_r.at[n, peer], peer, h).wait_recv()
            block = mix_in.at[n, peer]
            remote(block, block, mix_s.at[n, d], mix_r.at[n, peer], peer, h).wait_recv()
        logs = [lse_in[n, k] for k in range(C)]
        best = functools.reduce(jnp.maximum, logs)
        scales = [jnp.exp2(value - best) for value in logs]
        inverse = 1.0 / sum(scales)
        lane = lax.broadcasted_iota(jnp.int32, (RC, rows), 1)
        mine = lane == c * RC + lax.broadcasted_iota(jnp.int32, (RC, rows), 0)
        for g in range(group):
            cols = slice(g * HEAD_SIZE, (g + 1) * HEAD_SIZE)
            value = jnp.zeros((RC, HEAD_SIZE), f32)
            for k in range(C):
                share = (scales[k] * inverse)[g : g + 1]
                share = jnp.sum(jnp.where(mine, share, 0.0), axis=1, keepdims=True)
                value = value + share * mix_in[n, k, :, cols].astype(f32)
            att[n, c, :, cols] = value.astype(bf16)
        for copy in att_sends(n):
            copy.start()

    def project(q):
        for j in range(kv):
            n = q * kv + j
            for d in range(1, C):
                peer = (c + C - d) % C
                block = att.at[n, peer]
                remote(block, block, att_s.at[n, d], att_r.at[n, peer], peer, h).wait_recv()
        if q == 0:
            loads[0].wait()
        value = None
        for j in range(kv):
            term = lax.dot_general(
                att[q * kv + j].reshape(rows, gw_cols),
                ow[:, j * gw_cols : (j + 1) * gw_cols],
                (((1,), (1,)), ((), ())),
                preferred_element_type=f32,
            )
            value = term if value is None else value + term
        po_out[q] = value.astype(bf16)
        for i in range(NP):
            piece = pl.ds(i * RP, RP)
            send_if(
                visitor,
                po_out.at[q, piece],
                po_in.at[q, h, piece],
                po_s.at[q, i],
                po_r.at[q, h, i],
                c,
                z,
            )
        po_in[q, h] = po_out[q]

    def own(q, i):
        if q == 0 and i == 0:
            for d in range(1, H):
                peer = (h + d) % H
                block = res_in.at[peer]
                remote(block, block, res_s.at[0], res_r.at[peer], c, peer).wait_recv()
        for d in range(1, H):
            peer = (h + d) % H
            block = po_in.at[q, peer, pl.ds(i * RP, RP)]
            remote(block, block, po_s.at[q, i], po_r.at[q, peer, i], c, peer).wait_recv()
        spare = u.shape[-1] - width
        lane = lax.broadcasted_iota(jnp.int32, (hr, spare), 1)
        for b in range(i * RP // hr, (i + 1) * RP // hr):
            span = slice(b * hr, (b + 1) * hr)
            value = res_in[b, :, q].reshape(hr, width).astype(f32)
            added = sum(po_in[q, k, span].astype(f32) for k in range(H))
            stream = (value + added).astype(bf16)
            st[q, span] = stream
            stream = stream.astype(f32)
            u[q, x, span, :width] = (stream * gain_ref[...]).astype(bf16)
            squares = jnp.sum(stream * stream, axis=1, keepdims=True)
            high = squares.astype(bf16).astype(f32)
            mid = (squares - high).astype(bf16).astype(f32)
            low = squares - high - mid
            packed = jnp.where(lane == 0, high, jnp.where(lane == 1, mid, low))
            packed = jnp.where(lane < 3, packed, 0.0)
            u[q, x, span, width:] = packed.astype(bf16)

    def relay(q, i):
        piece = u.at[q, x, pl.ds(i * RP, RP)]
        pl.when(visitor)(remote(piece, piece, u_s.at[q, i, 0], u_r.at[q, x, i], c, h).wait_recv)
        up = jnp.logical_and(z >= h, z < Z - 1)
        down = jnp.logical_and(z <= h, z > 0)
        above = jnp.minimum(z + 1, Z - 1) * X + x
        below = jnp.maximum(z - 1, 0) * X + x
        send_if(up, piece, piece, u_s.at[q, i, 0], u_r.at[q, x, i], above, h)
        send_if(down, piece, piece, u_s.at[q, i, 1], u_r.at[q, x, i], below, h)
        for d in range(1, X):
            peer = z * X + (x + d) % X
            send(piece, piece, u_s.at[q, i, 1 + d], u_r.at[q, x, i], peer, h)

    def spread(q):
        for i in range(NP):
            pl.when(owner)(functools.partial(own, q, i))
            relay(q, i)

    def gather(q):
        for d in range(1, X):
            source = (x + d) % X
            for i in range(NP):
                block = u.at[q, source, pl.ds(i * RP, RP)]
                remote(block, block, u_s.at[q, i, 1 + d], u_r.at[q, source, i], c, h).wait_recv()
        if q == 0:
            loads[1].wait()
            loads[2].wait()
        squares = 0.0
        for k in range(X):
            split = u[q, k, :, width:].astype(f32)
            squares = squares + jnp.sum(split, axis=1, keepdims=True)
        squares = jnp.broadcast_to(squares, (rows, 128)).reshape(Y, CORES, hr, 128)
        ss_out[q] = squares.swapaxes(0, 1)
        send(ss_out.at[q, CORES - 1 - core], ss_in.at[q], ss_s.at[q, 0], ss_r.at[q, 0], c, partner)

    def matmul(q, i, which):
        weight = (gw, uw)[which]
        cols = slice(i * tile, (i + 1) * tile)
        value = None
        for k in range(X):
            term = jnp.dot(
                u[q, k, :, :width],
                weight[k * width : (k + 1) * width, cols],
                preferred_element_type=f32,
            )
            value = term if value is None else value + term
        value = value.reshape(Y, CORES, hr, tile).swapaxes(0, 1).astype(bf16)
        first[q, i, which] = value
        send(
            first.at[q, i, which, CORES - 1 - core],
            first_in.at[q, i, which],
            f_s.at[q, i, which],
            f_r.at[q, i, which],
            c,
            partner,
        )

    def middle(q, i, which):
        block = first_in.at[q, i, which]
        remote(block, block, f_s.at[q, i, which], f_r.at[q, i, which], c, partner).wait_recv()
        both = first[q, i, which, core].astype(f32) + first_in[q, i, which].astype(f32)
        second[q, i, which] = both.astype(bf16)
        for d in range(1, Y):
            peer = (y + d) % Y
            send(
                second.at[q, i, which, peer],
                second_in.at[q, i, which, y],
                g_s.at[q, i, which, d],
                g_r.at[q, i, which, y],
                c,
                peer * CORES + core,
            )

    def middle_squares(q):
        block = ss_in.at[q]
        remote(block, block, ss_s.at[q, 0], ss_r.at[q, 0], c, partner).wait_recv()
        ss_mid[q] = ss_out[q, core] + ss_in[q]
        for d in range(1, Y):
            peer = (y + d) % Y
            send(
                ss_mid.at[q, peer],
                ss_last.at[q, y],
                ss_s.at[q, d],
                ss_r.at[q, 1 + y],
                c,
                peer * CORES + core,
            )

    def inverse_rms(q):
        total = ss_mid[q, y]
        for d in range(1, Y):
            peer = (y + Y - d) % Y
            block = ss_last.at[q, peer]
            remote(
                block, block, ss_s.at[q, d], ss_r.at[q, 1 + peer], c, peer * CORES + core
            ).wait_recv()
            total = total + ss_last[q, peer]
        return lax.rsqrt(total[:, :1] / (C * width) + norm_epsilon)

    def finish(q, i, inverse):
        sums = []
        for which in range(2):
            value = second[q, i, which, y].astype(f32)
            for d in range(1, Y):
                peer = (y + Y - d) % Y
                block = second_in.at[q, i, which, peer]
                remote(
                    block,
                    block,
                    g_s.at[q, i, which, d],
                    g_r.at[q, i, which, peer],
                    c,
                    peer * CORES + core,
                ).wait_recv()
                value = value + second_in[q, i, which, peer].astype(f32)
            sums.append(value * inverse)
        hid[q, i, h] = (jax.nn.gelu(sums[0], approximate=True) * sums[1]).astype(bf16)
        block = hid.at[q, i, h]
        for d in range(1, Y):
            peer = ((y + d) % Y) * CORES + core
            send(block, block, h_s.at[q, i, d], h_r.at[q, i, h], c, peer)
        send(block, block, h_s.at[q, i, 0], h_r.at[q, i, h], c, partner)

    def forward(q, i):
        for d in range(1, Y):
            origin = ((y + Y - d) % Y) * CORES + core
            block = hid.at[q, i, origin]
            remote(block, block, h_s.at[q, i, d], h_r.at[q, i, origin], c, origin).wait_recv()
            send(block, block, fw_s.at[q, i, d], h_r.at[q, i, origin], c, partner)

    def down(q, i):
        for d in range(Y):
            origin = ((y + Y - d) % Y) * CORES + (CORES - 1 - core)
            block = hid.at[q, i, origin]
            remote(block, block, h_s.at[q, i, 0], h_r.at[q, i, origin], c, partner).wait_recv()
        if q == 0 and i == 0:
            loads[3].wait()
        term = lax.dot_general(
            hid[q, i].reshape(rows, tile),
            dw[:, i * tile : (i + 1) * tile],
            (((1,), (1,)), ((), ())),
            preferred_element_type=f32,
        )
        if i == 0:
            acc[...] = term
        else:
            acc[...] += term

    def scatter(q):
        for k in range(X):

            @pl.when(jnp.logical_and(owner, x == k))
            def _(k=k):
                acc[:, k * width : (k + 1) * width] += st[q].astype(f32)

        part[q] = acc[...].reshape(C, RC, acc.shape[1]).astype(bf16)
        for d in range(1, C):
            peer = (c + d) % C
            send(part.at[q, peer], part_in.at[q, c], part_s.at[q, d], part_r.at[q, c], peer, h)
        part_in[q, c] = part[q, c]

    def collect(q):
        for d in range(1, C):
            peer = (c + C - d) % C
            block = part_in.at[q, peer]
            remote(block, block, part_s.at[q, d], part_r.at[q, peer], peer, h).wait_recv()
        out_ref[q] = sum(part_in[q, k].astype(f32) for k in range(C)).astype(bf16)

    steps = NQ * kv
    lag = 2

    def loop(n, carry):
        attend(n)

        @pl.when(n >= lag)
        def _():
            combine(n - lag)

        return carry

    lax.fori_loop(0, steps, loop, 0)
    project(0)
    for n in range(steps - lag, steps):
        combine(n)

    pairs = [(i, which) for i in range(tiles) for which in range(2)]

    def expand(q):
        gather(q)
        for n, (i, which) in enumerate(pairs):
            matmul(q, i, which)
            if n == 1:
                middle_squares(q)
            if n:
                middle(q, *pairs[n - 1])
        middle(q, *pairs[-1])

    def contract(q):
        inverse = inverse_rms(q)
        for i in range(tiles):
            finish(q, i, inverse)
            if i:
                forward(q, i - 1)
        forward(q, tiles - 1)

    spread(0)
    for q in range(1, NQ):
        project(q)
    for q in range(NQ):
        expand(q)
        if q + 1 < NQ:
            spread(q + 1)
        contract(q)
        for i in range(tiles):
            down(q, i)
        scatter(q)
    for q in range(NQ):
        collect(q)

    def drain(n, carry):
        for copy in mix_sends(n) + att_sends(n):
            copy.wait_send()
        return carry

    lax.fori_loop(0, steps, drain, 0)
    for copy in sent:
        copy.wait_send()
    for condition, copy in kept:
        pl.when(condition)(copy.wait_send)


def fused(
    C,
    H,
    queries,
    keys,
    values,
    page_map,
    selected,
    residual_in,
    out_weight,
    norm_gain,
    gate_weight,
    up_weight,
    down_weight,
):
    row_count, query_width = queries.shape
    pages, page_len, kv_width = keys.shape
    kv = kv_width // HEAD_SIZE
    group = query_width // kv_width
    NQ = row_count // 128
    RC = row_count // C // NQ
    rows = C * RC
    NP = 2
    X = C // H
    Y = H // CORES
    hr = rows // H
    width = out_weight.shape[1]
    hidden = gate_weight.shape[1]
    out_width = down_weight.shape[1]
    tile = column_tile(hidden)
    tiles = hidden // tile
    steps = NQ * kv
    u_width = (width + 127) // 128 * 128
    bf16 = jnp.bfloat16
    f32 = jnp.float32
    vmem = pl.BlockSpec(memory_space=pltpu.VMEM)
    smem = pl.BlockSpec(memory_space=pltpu.SMEM)
    hbm = pl.BlockSpec(memory_space=pl.ANY)
    V = pltpu.VMEM
    S = pltpu.SemaphoreType.DMA
    out_weight = out_weight.T
    down_weight = down_weight.T
    mixes = V((steps, C, RC, group * HEAD_SIZE), bf16)
    return pl.pallas_call(
        functools.partial(fused_kernel, C, H, NP),
        out_shape=jax.ShapeDtypeStruct((NQ, RC, out_width), bf16),
        in_specs=[smem] * 2 + [vmem] * 3 + [hbm] * 6,
        out_specs=vmem,
        scratch_shapes=[
            V((kv, pages, page_len, HEAD_SIZE), bf16),
            V((kv, pages, page_len, HEAD_SIZE), bf16),
            V(out_weight.shape, bf16),
            V(gate_weight.shape, bf16),
            V(up_weight.shape, bf16),
            V(down_weight.shape, bf16),
            mixes,
            mixes,
            V((steps, group, rows), f32),
            V((steps, C, group, rows), f32),
            mixes,
            V((NQ, rows, width), bf16),
            V((NQ, H, rows, width), bf16),
            V((H, X, NQ, RC, width), bf16),
            V((NQ, rows, width), bf16),
            V((NQ, X, rows, u_width), bf16),
            V((NQ, CORES, Y, hr, 128), f32),
            V((NQ, Y, hr, 128), f32),
            V((NQ, Y, hr, 128), f32),
            V((NQ, Y, hr, 128), f32),
            V((NQ, tiles, 2, CORES, Y, hr, tile), bf16),
            V((NQ, tiles, 2, Y, hr, tile), bf16),
            V((NQ, tiles, 2, Y, hr, tile), bf16),
            V((NQ, tiles, 2, Y, hr, tile), bf16),
            V((NQ, tiles, H, hr, tile), bf16),
            V((rows, out_width), f32),
            V((NQ, C, RC, out_width), bf16),
            V((NQ, C, RC, out_width), bf16),
            S((2, kv)),
            S((4,)),
            S((steps, C)),
            S((steps, C)),
            S((steps, C)),
            S((steps, C)),
            S((steps, C)),
            S((steps, C)),
            S((NQ, NP)),
            S((NQ, H, NP)),
            S((1,)),
            S((H,)),
            S((NQ, NP, 1 + X)),
            S((NQ, X, NP)),
            S((NQ, Y)),
            S((NQ, 1 + Y)),
            S((NQ, tiles, 2)),
            S((NQ, tiles, 2)),
            S((NQ, tiles, 2, Y)),
            S((NQ, tiles, 2, Y)),
            S((NQ, tiles, Y)),
            S((NQ, tiles, H)),
            S((NQ, tiles, Y)),
            S((NQ, C)),
            S((NQ, C)),
        ],
        compiler_params=pltpu.CompilerParams(
            has_side_effects=True, vmem_limit_bytes=63 * 2**20
        ),
    )(
        page_map,
        selected,
        queries.reshape(C, NQ, RC, query_width),
        residual_in.reshape(X, NQ, RC, width),
        norm_gain.reshape(1, width),
        keys,
        values,
        out_weight,
        gate_weight,
        up_weight,
        down_weight,
    ).reshape(row_count // C, out_width)


def fits(C, H, queries, keys, selected, out_weight, gate_weight):
    rows = queries.shape[0]
    width = out_weight.shape[1]
    if rows % 128:
        return False
    chunks = rows // 128
    return (
        C % H == 0
        and (C // H) * H == C
        and rows % (C * chunks) == 0
        and rows // (C * chunks) % 16 == 0
        and rows % selected.shape[0] == 0
        and (keys.shape[1] - rows) % 128 == 0
        and keys.shape[1] > rows
        and width % 16 == 0
        and width % 128 <= 125
        and width % 128 > 0
        and gate_weight.shape[1] % 128 == 0
    )


def shards(
    queries,
    keys,
    values,
    page_map,
    selected,
    residual_in,
    out_weight,
    norm_gain,
    gate_weight,
    up_weight,
    down_weight,
):
    ctx_index = lax.axis_index("ctx")
    C = lax.axis_size("ctx")
    H = lax.axis_size("head")
    if fits(C, H, queries, keys, selected, out_weight, gate_weight):
        return fused(
            C,
            H,
            queries,
            keys,
            values,
            page_map,
            selected,
            residual_in,
            out_weight,
            norm_gain,
            gate_weight,
            up_weight,
            down_weight,
        )
    row_max, row_total, mixture = owner_pass(
        queries, keys, values, page_map, selected, ctx_index, C
    )
    stats = jnp.concatenate([row_max, row_total], axis=1)
    stats = jnp.pad(stats, ((0, 0), (0, 128 - stats.shape[1])))
    mlp_out, own_stream = tail(
        C,
        H,
        mixture.astype(jnp.bfloat16),
        stats,
        residual_in,
        norm_gain,
        out_weight,
        gate_weight,
        up_weight,
        down_weight,
    )
    own_stream = jnp.concatenate([own_stream[j] for j in range(own_stream.shape[0])], axis=1)
    return (own_stream.astype(jnp.float32) + mlp_out).astype(jnp.bfloat16)


def solution(mesh):
    in_specs = (
        P(None, "head"),
        P("ctx", None, "head"),
        P("ctx", None, "head"),
        P(),
        P(),
        P("head", "ctx"),
        P("head", "ctx"),
        P("ctx"),
        P("head", "ctx"),
        P("head", "ctx"),
        P("ctx", "head"),
    )
    out_specs = P("ctx", "head")
    return jax.shard_map(shards, mesh=mesh, in_specs=in_specs, out_specs=out_specs, check_vma=False)
```

```python
import jax
import jax.numpy as jnp
import functools
from jax import lax
from jax.experimental import pallas as pl
from jax.experimental.pallas import tpu as pltpu
from jax.sharding import PartitionSpec as P

D = 5376
HEAD_SIZE = 128


score_scale = 168.0 ** (-0.5)
masked_score = -1e30
norm_epsilon = 1e-06


def attention_kernel(
    logical_ref, chosen_ref, page_total, q_ref, k_ref, v_ref, mix_ref, m_ref, l_ref, acc, top, total
):
    page = pl.program_id(1)
    tile_count = chosen_ref.shape[0]
    tile_rows = q_ref.shape[0] // tile_count
    group = q_ref.shape[1] // k_ref.shape[2]
    page_len = k_ref.shape[1]
    offset = page_len - q_ref.shape[0]
    f32 = jnp.float32

    @pl.when(page == 0)
    def _():
        acc[...] = jnp.zeros_like(acc)
        top[...] = jnp.full_like(top, masked_score)
        total[...] = jnp.zeros_like(total)

    causal = logical_ref[page] == page_total - 1

    def visit(t, masked):
        rows = slice(t * tile_rows, (t + 1) * tile_rows)
        for g in range(group):
            cols = slice(g * HEAD_SIZE, (g + 1) * HEAD_SIZE)
            scores = (
                lax.dot_general(
                    q_ref[rows, cols],
                    k_ref[0],
                    (((1,), (1,)), ((), ())),
                    preferred_element_type=f32,
                )
                * score_scale
            )
            if masked:
                position = offset + t * tile_rows + lax.broadcasted_iota(jnp.int32, scores.shape, 0)
                key = lax.broadcasted_iota(jnp.int32, scores.shape, 1)
                scores = jnp.where(key <= position, scores, masked_score)
            old = top[g, rows, :1]
            new = jnp.maximum(old, jnp.max(scores, axis=1, keepdims=True))
            weights = jnp.exp(scores - new)
            keep = jnp.exp(old - new)
            total[g, rows] = total[g, rows] * keep + jnp.sum(weights, axis=1, keepdims=True)
            top[g, rows] = jnp.broadcast_to(new, (tile_rows, 128))
            acc[rows, cols] = acc[rows, cols] * keep + jnp.dot(
                weights.astype(jnp.bfloat16), v_ref[0], preferred_element_type=f32
            )

    for t in range(tile_count):
        picked = chosen_ref[t, page] != 0
        pl.when(jnp.logical_and(picked, causal))(functools.partial(visit, t, True))
        pl.when(jnp.logical_and(picked, jnp.logical_not(causal)))(
            functools.partial(visit, t, False)
        )

    @pl.when(page == pl.num_programs(1) - 1)
    def _():
        mix_ref[...] = acc[...].astype(jnp.bfloat16)
        lane = lax.broadcasted_iota(jnp.int32, m_ref.shape[1:], 1)
        maxima = jnp.zeros(m_ref.shape[1:], f32)
        sums = jnp.zeros(m_ref.shape[1:], f32)
        for g in range(group):
            maxima = jnp.where(lane == g, top[g], maxima)
            sums = jnp.where(lane == g, total[g], sums)
        m_ref[0] = maxima
        l_ref[0] = sums


def owner_pass(queries, keys, values, page_map, selected, ctx_index, ctx_count):
    pages_local, page_len, kv_width = keys.shape
    row_count, query_width = queries.shape
    kv_local = kv_width // HEAD_SIZE
    group = query_width // kv_width
    tile_count = selected.shape[0]
    page_total = pages_local * ctx_count
    slot_ids = ctx_index * pages_local + jnp.arange(pages_local, dtype=jnp.int32)
    all_pages = jnp.arange(page_total, dtype=jnp.int32)
    logical = jnp.sum(
        jnp.where(page_map[None, :] == slot_ids[:, None], all_pages[None, :], 0), axis=1
    )
    chosen = jnp.any(selected[:, None, :] == logical[None, :, None], axis=2).astype(jnp.int32)
    stat = jax.ShapeDtypeStruct((kv_local, row_count, 128), jnp.float32)
    stat_spec = pl.BlockSpec((1, row_count, 128), lambda k, p, a, b: (k, 0, 0))
    kv_spec = pl.BlockSpec((1, page_len, HEAD_SIZE), lambda k, p, a, b: (p, 0, k))
    q_spec = pl.BlockSpec((row_count, group * HEAD_SIZE), lambda k, p, a, b: (0, k))

    def kernel(logical_ref, chosen_ref, *refs):
        attention_kernel(logical_ref, chosen_ref, page_total, *refs)

    mixture, top, total = pl.pallas_call(
        kernel,
        grid_spec=pltpu.PrefetchScalarGridSpec(
            num_scalar_prefetch=2,
            grid=(kv_local, pages_local),
            in_specs=[q_spec, kv_spec, kv_spec],
            out_specs=(q_spec, stat_spec, stat_spec),
            scratch_shapes=[
                pltpu.VMEM((row_count, group * HEAD_SIZE), jnp.float32),
                pltpu.VMEM((group, row_count, 128), jnp.float32),
                pltpu.VMEM((group, row_count, 128), jnp.float32),
            ],
        ),
        out_shape=(jax.ShapeDtypeStruct((row_count, query_width), jnp.bfloat16), stat, stat),
    )(logical.astype(jnp.int32), chosen, queries, keys, values)

    def heads(stacked):
        return stacked[:, :, :group].transpose(1, 0, 2).reshape(row_count, kv_local * group)

    return heads(top), heads(total), mixture


MESH = pl.DeviceIdType.MESH
CORES = 2


def column_tile(width):
    for tile in (896, 768, 640, 512, 384, 256, 128):
        if width % tile == 0:
            return tile
    return width


def flat(block, rows):
    if block.shape[1] % 16:
        return block.astype(jnp.float32).reshape(rows, -1).astype(jnp.bfloat16)
    return block.reshape(rows, -1)


def tail_kernel(
    C,
    H,
    mix_ref,
    stat_ref,
    res_ref,
    gain_ref,
    ow_hbm,
    gw_hbm,
    uw_hbm,
    dw_hbm,
    mlp_ref,
    own_ref,
    ow,
    gw,
    uw,
    dw,
    mix_in,
    stat_in,
    att,
    po,
    po_in,
    u_out,
    st_out,
    ss,
    ublk,
    own_st,
    first,
    first_in,
    second,
    second_in,
    hid,
    acc,
    part,
    part_in,
    w_sem,
    mix_s,
    mix_r,
    stat_s,
    stat_r,
    att_s,
    att_r,
    po_s,
    po_r,
    u_s,
    u_r,
    st_s,
    st_r,
    ss_s,
    ss_r,
    f_s,
    f_r,
    g_s,
    g_r,
    h_s,
    h_r,
    fw_s,
    part_s,
    part_r,
):
    c = lax.axis_index("ctx")
    h = lax.axis_index("head")
    Y = H // CORES
    y = h // CORES
    core = h % CORES
    partner = y * CORES + (CORES - 1 - core)
    R = mix_ref.shape[1]
    rows = C * R
    rb = C // H
    bph = C // H
    width = ow.shape[0]
    head_rows = rows // H
    heads = mix_ref.shape[2] // HEAD_SIZE
    tiles, _, _, _, _, tile = first.shape
    f32 = jnp.float32
    bf16 = jnp.bfloat16

    def remote(src, dst, send_sem, recv_sem, ctx, head):
        return pltpu.make_async_remote_copy(
            src_ref=src,
            dst_ref=dst,
            send_sem=send_sem,
            recv_sem=recv_sem,
            device_id=(ctx, head),
            device_id_type=MESH,
        )

    sent = []

    def send(*args):
        copy = remote(*args)
        copy.start()
        sent.append(copy)

    loads = [
        pltpu.make_async_copy(src, dst, w_sem.at[i])
        for i, (src, dst) in enumerate(
            ((ow_hbm, ow), (gw_hbm, gw), (uw_hbm, uw), (dw_hbm, dw))
        )
    ]
    for load in loads:
        load.start()

    for d in range(1, C):
        peer = (c + d) % C
        send(stat_ref.at[peer], stat_in.at[c], stat_s.at[d], stat_r.at[c], peer, h)
        send(mix_ref.at[peer], mix_in.at[c], mix_s.at[d], mix_r.at[c], peer, h)
    stat_in[c] = stat_ref[c]
    mix_in[c] = mix_ref[c]
    for d in range(1, C):
        peer = (c + C - d) % C
        remote(stat_in.at[peer], stat_in.at[peer], stat_s.at[d], stat_r.at[peer], peer, h).wait_recv()
        remote(mix_in.at[peer], mix_in.at[peer], mix_s.at[d], mix_r.at[peer], peer, h).wait_recv()
    maxima = [stat_in[k][:, :heads] for k in range(C)]
    top = functools.reduce(jnp.maximum, maxima)
    scales = [jnp.exp(m - top) for m in maxima]
    total = sum(stat_in[k][:, heads : 2 * heads] * scales[k] for k in range(C))
    inverse = 1.0 / total
    for g in range(heads):
        cols = slice(g * HEAD_SIZE, (g + 1) * HEAD_SIZE)
        mixed = sum(mix_in[k, :, cols].astype(f32) * scales[k][:, g : g + 1] for k in range(C))
        att[c, :, cols] = (mixed * inverse[:, g : g + 1]).astype(bf16)

    for d in range(1, C):
        peer = (c + d) % C
        send(att.at[c], att.at[c], att_s.at[d], att_r.at[c], peer, h)
    loads[0].wait()
    for d in range(1, C):
        peer = (c + C - d) % C
        remote(att.at[peer], att.at[peer], att_s.at[d], att_r.at[peer], peer, h).wait_recv()
    projected = lax.dot_general(
        flat(att[...], rows), ow[...], (((1,), (1,)), ((), ())), preferred_element_type=f32
    )
    po[...] = projected.reshape(H, head_rows, width).astype(bf16)

    for d in range(1, H):
        peer = (h + d) % H
        send(po.at[peer], po_in.at[h], po_s.at[d], po_r.at[h], c, peer)
    po_in[h] = po[h]
    for d in range(1, H):
        peer = (h + H - d) % H
        remote(po_in.at[peer], po_in.at[peer], po_s.at[d], po_r.at[peer], c, peer).wait_recv()
    projected = sum(po_in[k].astype(f32) for k in range(H))
    stream = (res_ref[...].astype(f32) + projected).astype(bf16).astype(f32)
    st_out[...] = stream.reshape(rb, R, width).astype(bf16)
    u_out[...] = (stream * gain_ref[...]).reshape(rb, R, width).astype(bf16)
    squares = jnp.sum(stream * stream, axis=1, keepdims=True)
    ss[c] = jnp.broadcast_to(squares, (head_rows, 128))

    block_head = c // bph
    block_part = c % bph
    u_dst = ublk.at[block_part, pl.ds(h * rb, rb)]
    kept = []
    for d in range(C):
        peer = (c + d) % C
        copy = remote(u_out, u_dst, u_s.at[d], u_r.at[block_part, h], peer, block_head)
        if d == 0:
            kept.append((block_head != h, copy))
            pl.when(block_head != h)(copy.start)

            @pl.when(block_head == h)
            def _():
                ublk[block_part, pl.ds(h * rb, rb)] = u_out[...]

        else:
            copy.start()
            sent.append(copy)
    for d in range(1, C):
        peer = (c + d) % C
        send(ss.at[c], ss.at[c], ss_s.at[d], ss_r.at[c], peer, h)
    for i in range(rb):
        owner = h * rb + i
        other = jnp.logical_or(owner != c, block_head != h)
        copy = remote(
            st_out.at[i], own_st.at[block_part], st_s.at[i], st_r.at[block_part], owner, block_head
        )
        kept.append((other, copy))
        pl.when(other)(copy.start)

        @pl.when(jnp.logical_not(other))
        def _(i=i):
            own_st[block_part] = st_out[i]

    for j in range(bph):
        for k in range(H):
            source = h * bph + j
            block = ublk.at[j, pl.ds(k * rb, rb)]
            arrival = remote(block, block, u_s.at[0], u_r.at[j, k], source, k)
            pl.when(jnp.logical_or(source != c, h != k))(arrival.wait_recv)
    loads[1].wait()
    loads[2].wait()

    def matmul(i, which, weight):
        cols = slice(i * tile, (i + 1) * tile)
        value = None
        for j in range(bph):
            term = jnp.dot(
                flat(ublk[j], rows),
                weight[j * width : (j + 1) * width, cols],
                preferred_element_type=f32,
            )
            value = term if value is None else value + term
        first[i, which] = value.reshape(Y, CORES, head_rows, tile).swapaxes(0, 1).astype(bf16)
        send(
            first.at[i, which, CORES - 1 - core],
            first_in.at[i, which],
            f_s.at[i, which],
            f_r.at[i, which],
            c,
            partner,
        )

    def middle(i, which):
        remote(
            first_in.at[i, which], first_in.at[i, which], f_s.at[i, which], f_r.at[i, which], c, partner
        ).wait_recv()
        both = first[i, which, core].astype(f32) + first_in[i, which].astype(f32)
        second[i, which] = both.astype(bf16)
        for d in range(1, Y):
            peer = (y + d) % Y
            send(
                second.at[i, which, peer],
                second_in.at[i, which, y],
                g_s.at[i, which, d],
                g_r.at[i, which, y],
                c,
                peer * CORES + core,
            )

    def finish(i, inverse_rms):
        sums = []
        for which in range(2):
            value = second[i, which, y].astype(f32)
            for d in range(1, Y):
                peer = (y + Y - d) % Y
                slot = second_in.at[i, which, peer]
                remote(
                    slot, slot, g_s.at[i, which, d], g_r.at[i, which, peer], c, peer * CORES + core
                ).wait_recv()
                value = value + second_in[i, which, peer].astype(f32)
            sums.append(value * inverse_rms)
        hid[i, h] = (jax.nn.gelu(sums[0], approximate=True) * sums[1]).astype(bf16)
        send(hid.at[i, h], hid.at[i, h], h_s.at[i, 0], h_r.at[i, h], c, partner)
        for d in range(1, Y):
            peer = ((y + d) % Y) * CORES + core
            send(hid.at[i, h], hid.at[i, h], h_s.at[i, d], h_r.at[i, h], c, peer)

    def forward(i):
        for d in range(1, Y):
            origin = ((y + Y - d) % Y) * CORES + core
            slot = hid.at[i, origin]
            remote(slot, slot, h_s.at[i, d], h_r.at[i, origin], c, origin).wait_recv()
            send(slot, slot, fw_s.at[i, d], h_r.at[i, origin], c, partner)

    def down(i):
        for d in range(Y):
            origin = ((y + Y - d) % Y) * CORES + (CORES - 1 - core)
            slot = hid.at[i, origin]
            remote(slot, slot, h_s.at[i, 0], h_r.at[i, origin], c, partner).wait_recv()
        term = lax.dot_general(
            flat(hid[i], rows),
            dw[:, i * tile : (i + 1) * tile],
            (((1,), (1,)), ((), ())),
            preferred_element_type=f32,
        )
        if i == 0:
            acc[...] = term
        else:
            acc[...] += term

    steps = [(i, which) for i in range(tiles) for which in range(2)]
    for n, (i, which) in enumerate(steps):
        matmul(i, which, (gw, uw)[which])
        if n:
            middle(*steps[n - 1])
    middle(*steps[-1])
    for d in range(1, C):
        peer = (c + C - d) % C
        remote(ss.at[peer], ss.at[peer], ss_s.at[d], ss_r.at[peer], peer, h).wait_recv()
    squares = sum(ss[k] for k in range(C))
    inverse_rms = lax.rsqrt(squares[:, :1] / (C * width) + norm_epsilon)
    loads[3].wait()
    for i in range(tiles):
        finish(i, inverse_rms)
        if i:
            forward(i - 1)
    forward(tiles - 1)
    for i in range(tiles):
        down(i)
    part[...] = acc[...].reshape(C, R, acc.shape[1]).astype(bf16)

    for d in range(1, C):
        peer = (c + d) % C
        send(part.at[peer], part_in.at[c], part_s.at[d], part_r.at[c], peer, h)
    part_in[c] = part[c]
    for j in range(bph):
        source = h * bph + j
        arrival = remote(own_st.at[j], own_st.at[j], st_s.at[0], st_r.at[j], source, c // rb)
        pl.when(jnp.logical_or(source != c, c // rb != h))(arrival.wait_recv)
    own_ref[...] = own_st[...]
    for d in range(1, C):
        peer = (c + C - d) % C
        remote(part_in.at[peer], part_in.at[peer], part_s.at[d], part_r.at[peer], peer, h).wait_recv()
    mlp_ref[...] = sum(part_in[k].astype(f32) for k in range(C))
    for copy in sent:
        copy.wait_send()
    for condition, copy in kept:
        pl.when(condition)(copy.wait_send)


def tail(C, H, mixture, stats, residual_in, norm_gain, out_weight, gate_weight, up_weight, down_weight):
    rows, query_width = mixture.shape
    R = rows // C
    width = out_weight.shape[1]
    hidden = gate_weight.shape[1]
    out_width = down_weight.shape[1]
    out_weight = out_weight.T
    down_weight = down_weight.T
    rb = C // H
    bph = C // H
    Y = H // CORES
    head_rows = rows // H
    tile = column_tile(hidden)
    tiles = hidden // tile
    bf16 = jnp.bfloat16
    vmem = pl.BlockSpec(memory_space=pltpu.VMEM)
    hbm = pl.BlockSpec(memory_space=pl.ANY)
    V = pltpu.VMEM
    S = pltpu.SemaphoreType.DMA
    return pl.pallas_call(
        functools.partial(tail_kernel, C, H),
        out_shape=(
            jax.ShapeDtypeStruct((R, out_width), jnp.float32),
            jax.ShapeDtypeStruct((bph, R, width), bf16),
        ),
        in_specs=[vmem] * 4 + [hbm] * 4,
        out_specs=(vmem, vmem),
        scratch_shapes=[
            V(out_weight.shape, bf16),
            V(gate_weight.shape, bf16),
            V(up_weight.shape, bf16),
            V(down_weight.shape, bf16),
            V((C, R, query_width), bf16),
            V((C, R, 128), jnp.float32),
            V((C, R, query_width), bf16),
            V((H, head_rows, width), bf16),
            V((H, head_rows, width), bf16),
            V((rb, R, width), bf16),
            V((rb, R, width), bf16),
            V((C, head_rows, 128), jnp.float32),
            V((bph, C, R, width), bf16),
            V((bph, R, width), bf16),
            V((tiles, 2, CORES, Y, head_rows, tile), bf16),
            V((tiles, 2, Y, head_rows, tile), bf16),
            V((tiles, 2, Y, head_rows, tile), bf16),
            V((tiles, 2, Y, head_rows, tile), bf16),
            V((tiles, H, head_rows, tile), bf16),
            V((rows, out_width), jnp.float32),
            V((C, R, out_width), bf16),
            V((C, R, out_width), bf16),
            S((4,)),
            S((C,)),
            S((C,)),
            S((C,)),
            S((C,)),
            S((C,)),
            S((C,)),
            S((H,)),
            S((H,)),
            S((C,)),
            S((bph, H)),
            S((rb,)),
            S((bph,)),
            S((C,)),
            S((C,)),
            S((tiles, 2)),
            S((tiles, 2)),
            S((tiles, 2, Y)),
            S((tiles, 2, Y)),
            S((tiles, Y)),
            S((tiles, H)),
            S((tiles, Y)),
            S((C,)),
            S((C,)),
        ],
        compiler_params=pltpu.CompilerParams(
            has_side_effects=True, vmem_limit_bytes=60 * 2**20
        ),
    )(
        mixture.reshape(C, R, query_width),
        stats.reshape(C, R, 128),
        residual_in,
        norm_gain.reshape(1, width),
        out_weight,
        gate_weight,
        up_weight,
        down_weight,
    )


LOG2E = 1.4426950408889634


def fused_kernel(
    C,
    H,
    NP,
    map_hbm,
    sel_hbm,
    q_hbm,
    res_hbm,
    gain_hbm,
    k_hbm,
    v_hbm,
    ow_hbm,
    gw_hbm,
    uw_hbm,
    dw_hbm,
    out_ref,
    map_ref,
    sel_ref,
    q_ref,
    res_ref,
    gain_ref,
    k_buf,
    v_buf,
    ow,
    gw,
    uw,
    dw,
    mix_out,
    mix_in,
    lse_out,
    lse_in,
    att,
    po_out,
    po_in,
    res_in,
    st,
    u,
    ss_out,
    ss_in,
    ss_mid,
    ss_last,
    first,
    first_in,
    second,
    second_in,
    hid,
    acc,
    part,
    part_in,
    in_sem,
    kv_sem,
    w_sem,
    mix_s,
    mix_r,
    lse_s,
    lse_r,
    att_s,
    att_r,
    po_s,
    po_r,
    res_s,
    res_r,
    u_s,
    u_r,
    ss_s,
    ss_r,
    f_s,
    f_r,
    g_s,
    g_r,
    h_s,
    h_r,
    part_s,
    part_r,
):
    c = lax.axis_index("ctx")
    h = lax.axis_index("head")
    X = C // H
    Z = C // X
    z = c // X
    x = c % X
    Y = H // CORES
    y = h // CORES
    core = h % CORES
    partner = y * CORES + (CORES - 1 - core)
    _, NQ, RC, query_width = q_ref.shape
    rows = C * RC
    hr = rows // H
    kv, pages, page_len, _ = k_buf.shape
    group = query_width // (kv * HEAD_SIZE)
    gw_cols = group * HEAD_SIZE
    tile_count = sel_ref.shape[0]
    tile_rows = NQ * rows // tile_count
    offset = page_len - NQ * rows
    page_total = map_ref.shape[0]
    width = ow.shape[0]
    tile = first.shape[-1]
    tiles = first.shape[1]
    RP = rows // NP
    f32 = jnp.float32
    bf16 = jnp.bfloat16
    owner = h == z
    visitor = h != z

    def remote(src, dst, send_sem, recv_sem, ctx, head):
        return pltpu.make_async_remote_copy(
            src_ref=src,
            dst_ref=dst,
            send_sem=send_sem,
            recv_sem=recv_sem,
            device_id=(ctx, head),
            device_id_type=MESH,
        )

    sent = []
    kept = []

    def start(*args):
        remote(*args).start()

    def send(*args):
        copy = remote(*args)
        copy.start()
        sent.append(copy)

    def send_if(condition, *args):
        copy = remote(*args)
        pl.when(condition)(copy.start)
        kept.append((condition, copy))

    def kv_load(j):
        lanes = pl.ds(pl.multiple_of(j * HEAD_SIZE, HEAD_SIZE), HEAD_SIZE)
        return (
            pltpu.make_async_copy(k_hbm.at[:, :, lanes], k_buf.at[j], kv_sem.at[0, j]),
            pltpu.make_async_copy(v_hbm.at[:, :, lanes], v_buf.at[j], kv_sem.at[1, j]),
        )

    barrier = pltpu.get_barrier_semaphore()
    for d in range(1, C):
        pl.semaphore_signal(
            barrier, inc=1, device_id=((c + d) % C, h), device_id_type=MESH
        )
    for d in range(1, H):
        pl.semaphore_signal(
            barrier, inc=1, device_id=(c, (h + d) % H), device_id_type=MESH
        )
    inputs = [
        pltpu.make_async_copy(src, dst, in_sem.at[i])
        for i, (src, dst) in enumerate(
            (
                (map_hbm, map_ref),
                (sel_hbm, sel_ref),
                (q_hbm, q_ref),
                (res_hbm, res_ref),
                (gain_hbm, gain_ref.at[0]),
            )
        )
    ]
    for load in inputs:
        load.start()
    for j in range(kv):
        for load in kv_load(j):
            load.start()
    loads = [
        pltpu.make_async_copy(src, dst, w_sem.at[i])
        for i, (src, dst) in enumerate(
            ((ow_hbm, ow), (gw_hbm, gw), (uw_hbm, uw), (dw_hbm, dw))
        )
    ]
    for load in inputs:
        load.wait()

    facts = []
    for p in range(pages):
        slot = c * pages + p
        logical = jnp.int32(0)
        for j in range(page_total):
            logical = logical + jnp.where(map_ref[j] == slot, j, 0)
        picks = []
        for t in range(tile_count):
            hits = jnp.int32(0)
            for i in range(sel_ref.shape[1]):
                hits = hits + jnp.where(sel_ref[t, i] == logical, 1, 0)
            picks.append(jnp.where(hits > 0, 0.0, masked_score).astype(f32))
        reach = jnp.where(logical == page_total - 1, 0, page_len)
        facts.append((reach, picks))

    index = lax.broadcasted_iota(jnp.int32, (group * rows, 1), 0) & (rows - 1)
    shift = RC.bit_length() - 1
    base_row = (index >> shift) * (NQ * RC) + (index & (RC - 1))
    eye = lax.broadcasted_iota(jnp.int32, (rows, rows), 0) == lax.broadcasted_iota(
        jnp.int32, (rows, rows), 1
    )
    unit = score_scale * LOG2E

    def attend(n):
        q = n // kv
        j = n % kv

        @pl.when(n < kv)
        def _():
            for load in kv_load(j):
                load.wait()

        @pl.when(n == 0)
        def _():
            for load in loads:
                load.start()

        lanes = pl.ds(pl.multiple_of(j * gw_cols, gw_cols), gw_cols)
        block = q_ref[:, q, :, lanes].reshape(rows, gw_cols)
        lhs = jnp.concatenate(
            [block[:, g * HEAD_SIZE : (g + 1) * HEAD_SIZE] for g in range(group)], axis=0
        )
        row = base_row + q * RC
        key = offset + lax.broadcasted_iota(jnp.int32, (group * rows, page_len - offset), 1)
        tops, sums, outs = [], [], []
        for p in range(pages):
            reach, picks = facts[p]
            bias = jnp.zeros((group * rows, 1), f32)
            for t in range(tile_count):
                inside = jnp.logical_and(row >= t * tile_rows, row < (t + 1) * tile_rows)
                bias = jnp.where(inside, picks[t], bias)
            scores = lax.dot_general(
                lhs, k_buf[j, p], (((1,), (1,)), ((), ())), preferred_element_type=f32
            )
            late = jnp.where(key <= offset + row + reach, scores[:, offset:], masked_score)
            scores = jnp.concatenate([scores[:, :offset], late], axis=1)
            top = jnp.max(scores, axis=1, keepdims=True)
            weights = jnp.exp2((scores - top) * unit)
            sums.append(jnp.sum(weights, axis=1, keepdims=True))
            outs.append(
                jnp.dot(weights.astype(bf16), v_buf[j, p], preferred_element_type=f32)
            )
            tops.append(top * unit + bias)
        best = functools.reduce(jnp.maximum, tops)
        scales = [jnp.exp2(top - best) for top in tops]
        total = sum(s * e for s, e in zip(sums, scales))
        mixed = sum(o * (e / total) for o, e in zip(outs, scales))
        lse = best + jnp.log2(total)
        for g in range(group):
            part_rows = slice(g * rows, (g + 1) * rows)
            mix_out[n, :, :, g * HEAD_SIZE : (g + 1) * HEAD_SIZE] = (
                mixed[part_rows].reshape(C, RC, HEAD_SIZE).astype(bf16)
            )
            lse_out[n, g : g + 1] = jnp.sum(
                jnp.where(eye, lse[part_rows], 0.0), axis=0, keepdims=True
            )
        mix_in[n, c] = mix_out[n, c]
        lse_in[n, c] = lse_out[n]

    def mix_sends(n):
        for d in range(1, C):
            peer = (c + d) % C
            remote(mix_out.at[n, peer], mix_in.at[n, c], mix_s.at[0], mix_r.at[n], peer, h).start()
            remote(lse_out.at[n], lse_in.at[n, c], lse_s.at[0], lse_r.at[n], peer, h).start()

    def att_sends(n):
        for d in range(1, C):
            peer = (c + d) % C
            remote(att.at[n, c], att.at[n, c], att_s.at[0], att_r.at[n], peer, h).start()

    def arrived(block, recv_sem):
        remote(block, block, recv_sem, recv_sem, c, partner).wait_recv()

    def left(block, send_sem):
        remote(block, block, send_sem, send_sem, c, partner).wait_send()

    def combine(n):
        arrived(lse_in.at[n, pl.ds(0, C - 1)], lse_r.at[n])
        arrived(mix_in.at[n, pl.ds(0, C - 1)], mix_r.at[n])
        logs = [lse_in[n, k] for k in range(C)]
        best = functools.reduce(jnp.maximum, logs)
        scales = [jnp.exp2(value - best) for value in logs]
        inverse = 1.0 / sum(scales)
        lane = lax.broadcasted_iota(jnp.int32, (RC, rows), 1)
        mine = lane == c * RC + lax.broadcasted_iota(jnp.int32, (RC, rows), 0)
        for g in range(group):
            cols = slice(g * HEAD_SIZE, (g + 1) * HEAD_SIZE)
            value = jnp.zeros((RC, HEAD_SIZE), f32)
            for k in range(C):
                share = (scales[k] * inverse)[g : g + 1]
                share = jnp.sum(jnp.where(mine, share, 0.0), axis=1, keepdims=True)
                value = value + share * mix_in[n, k, :, cols].astype(f32)
            att[n, c, :, cols] = value.astype(bf16)
        att_sends(n)

    def project(q):
        for j in range(kv):
            n = q * kv + j
            arrived(att.at[n, pl.ds(0, C - 1)], att_r.at[n])
        if q == 0:
            loads[0].wait()
        value = None
        for j in range(kv):
            term = lax.dot_general(
                att[q * kv + j].reshape(rows, gw_cols),
                ow[:, j * gw_cols : (j + 1) * gw_cols],
                (((1,), (1,)), ((), ())),
                preferred_element_type=f32,
            )
            value = term if value is None else value + term
        po_out[q] = value.astype(bf16)
        for i in range(NP):
            piece = pl.ds(i * RP, RP)
            copy = remote(
                po_out.at[q, piece], po_in.at[q, h, piece], po_s.at[q], po_r.at[q, i], c, z
            )
            pl.when(visitor)(copy.start)
        po_in[q, h] = po_out[q]

    def own(q, i):
        if q == 0 and i == 0:
            arrived(res_in.at[pl.ds(0, H - 1)], res_r.at[0])
        arrived(po_in.at[q, pl.ds(0, H - 1), pl.ds(i * RP, RP)], po_r.at[q, i])
        spare = u.shape[-1] - width
        lane = lax.broadcasted_iota(jnp.int32, (hr, spare), 1)
        for b in range(i * RP // hr, (i + 1) * RP // hr):
            span = slice(b * hr, (b + 1) * hr)
            value = res_in[b, :, q].reshape(hr, width).astype(f32)
            added = sum(po_in[q, k, span].astype(f32) for k in range(H))
            stream = (value + added).astype(bf16)
            st[q, span] = stream
            stream = stream.astype(f32)
            u[q, x, span, :width] = (stream * gain_ref[...]).astype(bf16)
            squares = jnp.sum(stream * stream, axis=1, keepdims=True)
            high = squares.astype(bf16).astype(f32)
            mid = (squares - high).astype(bf16).astype(f32)
            low = squares - high - mid
            packed = jnp.where(lane == 0, high, jnp.where(lane == 1, mid, low))
            packed = jnp.where(lane < 3, packed, 0.0)
            u[q, x, span, width:] = packed.astype(bf16)

    def relay(q, i, here):
        piece = u.at[q, x, pl.ds(i * RP, RP)]
        recv = u_r.at[q, x, i]
        pl.when(jnp.logical_and(here, visitor))(functools.partial(arrived, piece, recv))
        up = jnp.logical_and(here, jnp.logical_and(z >= h, z < Z - 1))
        down = jnp.logical_and(here, jnp.logical_and(z <= h, z > 0))
        above = jnp.minimum(z + 1, Z - 1) * X + x
        below = jnp.maximum(z - 1, 0) * X + x
        send_if(up, piece, piece, u_s.at[q, i, 0], recv, above, h)
        send_if(down, piece, piece, u_s.at[q, i, 1], recv, below, h)
        for d in range(1, X):
            peer = z * X + (x + d) % X
            send_if(here, piece, piece, u_s.at[q, i, 1 + d], recv, peer, h)

    def spread(q, here):
        for i in range(NP):
            pl.when(jnp.logical_and(here, owner))(functools.partial(own, q, i))
            relay(q, i, here)

    def gather(q):
        for d in range(1, X):
            source = (x + d) % X
            for i in range(NP):
                block = u.at[q, source, pl.ds(i * RP, RP)]
                arrived(block, u_r.at[q, source, i])
        if q == 0:
            loads[1].wait()
            loads[2].wait()
        squares = 0.0
        for k in range(X):
            split = u[q, k, :, width:].astype(f32)
            squares = squares + jnp.sum(split, axis=1, keepdims=True)
        squares = jnp.broadcast_to(squares, (rows, 128)).reshape(Y, CORES, hr, 128)
        ss_out[q] = squares.swapaxes(0, 1)
        send(ss_out.at[q, CORES - 1 - core], ss_in.at[q], ss_s.at[q, 0], ss_r.at[q, 0], c, partner)

    def matmul(q, i, which):
        weight = (gw, uw)[which]
        cols = slice(i * tile, (i + 1) * tile)
        value = None
        for k in range(X):
            term = jnp.dot(
                u[q, k, :, :width],
                weight[k * width : (k + 1) * width, cols],
                preferred_element_type=f32,
            )
            value = term if value is None else value + term
        value = value.reshape(Y, CORES, hr, tile).swapaxes(0, 1).astype(bf16)
        first[q, i, which] = value
        start(
            first.at[q, i, which, CORES - 1 - core],
            first_in.at[q, i, which],
            f_s.at[0],
            f_r.at[q, i, which],
            c,
            partner,
        )

    def middle(q, i, which):
        block = first_in.at[q, i, which]
        arrived(block, f_r.at[q, i, which])
        both = first[q, i, which, core].astype(f32) + first_in[q, i, which].astype(f32)
        second[q, i, which] = both.astype(bf16)
        for d in range(1, Y):
            peer = (y + d) % Y
            start(
                second.at[q, i, which, peer],
                second_in.at[q, i, which, y],
                g_s.at[0],
                g_r.at[q, i, which, y],
                c,
                peer * CORES + core,
            )

    def middle_squares(q):
        block = ss_in.at[q]
        remote(block, block, ss_s.at[q, 0], ss_r.at[q, 0], c, partner).wait_recv()
        ss_mid[q] = ss_out[q, core] + ss_in[q]
        for d in range(1, Y):
            peer = (y + d) % Y
            send(
                ss_mid.at[q, peer],
                ss_last.at[q, y],
                ss_s.at[q, d],
                ss_r.at[q, 1 + y],
                c,
                peer * CORES + core,
            )

    def inverse_rms(q):
        total = ss_mid[q, y]
        for d in range(1, Y):
            peer = (y + Y - d) % Y
            block = ss_last.at[q, peer]
            remote(
                block, block, ss_s.at[q, d], ss_r.at[q, 1 + peer], c, peer * CORES + core
            ).wait_recv()
            total = total + ss_last[q, peer]
        return lax.rsqrt(total[:, :1] / (C * width) + norm_epsilon)

    def finish(q, i, inverse):
        sums = []
        for which in range(2):
            value = second[q, i, which, y].astype(f32)
            for d in range(1, Y):
                peer = (y + Y - d) % Y
                block = second_in.at[q, i, which, peer]
                remote(
                    block,
                    block,
                    g_s.at[0],
                    g_r.at[q, i, which, peer],
                    c,
                    peer * CORES + core,
                ).wait_recv()
                value = value + second_in[q, i, which, peer].astype(f32)
            sums.append(value * inverse)
        hid[q, i, h] = (jax.nn.gelu(sums[0], approximate=True) * sums[1]).astype(bf16)
        block = hid.at[q, i, h]
        for d in range(1, Y):
            peer = ((y + d) % Y) * CORES + core
            start(block, block, h_s.at[0], h_r.at[q, i, h], c, peer)
        start(block, block, h_s.at[0], h_r.at[q, i, h], c, partner)

    def forward(q, i):
        for d in range(1, Y):
            origin = ((y + Y - d) % Y) * CORES + core
            block = hid.at[q, i, origin]
            arrived(block, h_r.at[q, i, origin])
            start(block, block, h_s.at[0], h_r.at[q, i, origin], c, partner)

    def down(q, i):
        for d in range(Y):
            origin = ((y + Y - d) % Y) * CORES + (CORES - 1 - core)
            block = hid.at[q, i, origin]
            arrived(block, h_r.at[q, i, origin])
        if q == 0 and i == 0:
            loads[3].wait()
        term = lax.dot_general(
            hid[q, i].reshape(rows, tile),
            dw[:, i * tile : (i + 1) * tile],
            (((1,), (1,)), ((), ())),
            preferred_element_type=f32,
        )
        if i == 0:
            acc[...] = term
        else:
            acc[...] += term

    def scatter(q):
        for k in range(X):

            @pl.when(jnp.logical_and(owner, x == k))
            def _(k=k):
                acc[:, k * width : (k + 1) * width] += st[q].astype(f32)

        part[q] = acc[...].reshape(C, RC, acc.shape[1]).astype(bf16)
        for d in range(1, C):
            peer = (c + d) % C
            start(part.at[q, peer], part_in.at[q, c], part_s.at[0], part_r.at[q], peer, h)
        part_in[q, c] = part[q, c]

    def collect(q):
        arrived(part_in.at[q, pl.ds(0, C - 1)], part_r.at[q])
        out_ref[q] = sum(part_in[q, k].astype(f32) for k in range(C)).astype(bf16)

    pl.semaphore_wait(barrier, C + H - 2)
    send_if(visitor, res_ref, res_in.at[h], res_s.at[0], res_r.at[0], c, z)
    res_in[h] = res_ref[...]

    steps = NQ * kv
    lag = 3

    def loop(n, carry):
        attend(n)
        pl.when(jnp.logical_or(n < kv, n >= kv + lag))(functools.partial(mix_sends, n))

        @pl.when(jnp.logical_and(n >= lag, n < kv + lag))
        def _():
            combine(n - lag)

        @pl.when(n == kv + lag - 1)
        def _():
            for k in range(kv, kv + lag):
                mix_sends(k)

        return carry

    lax.fori_loop(0, steps, loop, 0)
    project(0)
    for n in range(kv, steps):
        combine(n)

    pairs = [(i, which) for i in range(tiles) for which in range(2)]

    def expand(q):
        gather(q)
        for n, (i, which) in enumerate(pairs):
            matmul(q, i, which)
            if n == 1:
                middle_squares(q)
            if n:
                middle(q, *pairs[n - 1])
        middle(q, *pairs[-1])

    def contract(q):
        inverse = inverse_rms(q)
        for i in range(tiles):
            finish(q, i, inverse)
            if i:
                forward(q, i - 1)
        forward(q, tiles - 1)

    near = jnp.logical_and(z - h <= 1, h - z <= 1)
    always = z >= 0
    spread(0, near)
    project(1)
    spread(0, jnp.logical_not(near))
    expand(0)
    spread(1, always)
    expand(1)
    for q in range(NQ):
        contract(q)
        for i in range(tiles):
            down(q, i)
        scatter(q)
    for q in range(NQ):
        collect(q)

    left(mix_out.at[:, pl.ds(0, C - 1)], mix_s.at[0])
    left(lse_in.at[:, pl.ds(0, C - 1)], lse_s.at[0])
    left(att.at[:, pl.ds(0, C - 1)], att_s.at[0])
    left(first_in, f_s.at[0])
    left(second.at[:, :, :, pl.ds(0, Y - 1)], g_s.at[0])
    left(hid.at[:, :, pl.ds(0, 2 * Y - 1)], h_s.at[0])
    left(part.at[:, pl.ds(0, C - 1)], part_s.at[0])
    for q in range(NQ):
        pl.when(visitor)(functools.partial(left, po_out.at[q], po_s.at[q]))
    for copy in sent:
        copy.wait_send()
    for condition, copy in kept:
        pl.when(condition)(copy.wait_send)


def fused(
    C,
    H,
    queries,
    keys,
    values,
    page_map,
    selected,
    residual_in,
    out_weight,
    norm_gain,
    gate_weight,
    up_weight,
    down_weight,
):
    row_count, query_width = queries.shape
    pages, page_len, kv_width = keys.shape
    kv = kv_width // HEAD_SIZE
    group = query_width // kv_width
    NQ = row_count // 128
    RC = row_count // C // NQ
    rows = C * RC
    NP = 2
    X = C // H
    Y = H // CORES
    hr = rows // H
    width = out_weight.shape[1]
    hidden = gate_weight.shape[1]
    out_width = down_weight.shape[1]
    tile = column_tile(hidden)
    tiles = hidden // tile
    steps = NQ * kv
    u_width = (width + 127) // 128 * 128
    bf16 = jnp.bfloat16
    f32 = jnp.float32
    vmem = pl.BlockSpec(memory_space=pltpu.VMEM)
    hbm = pl.BlockSpec(memory_space=pl.ANY)
    V = pltpu.VMEM
    S = pltpu.SemaphoreType.DMA
    out_weight = out_weight.T
    down_weight = down_weight.T
    mixes = V((steps, C, RC, group * HEAD_SIZE), bf16)
    return pl.pallas_call(
        functools.partial(fused_kernel, C, H, NP),
        out_shape=jax.ShapeDtypeStruct((NQ, RC, out_width), bf16),
        in_specs=[hbm] * 11,
        out_specs=vmem,
        scratch_shapes=[
            pltpu.SMEM(page_map.shape, jnp.int32),
            pltpu.SMEM(selected.shape, jnp.int32),
            V((C, NQ, RC, query_width), bf16),
            V((X, NQ, RC, width), bf16),
            V((1, width), f32),
            V((kv, pages, page_len, HEAD_SIZE), bf16),
            V((kv, pages, page_len, HEAD_SIZE), bf16),
            V(out_weight.shape, bf16),
            V(gate_weight.shape, bf16),
            V(up_weight.shape, bf16),
            V(down_weight.shape, bf16),
            mixes,
            mixes,
            V((steps, group, rows), f32),
            V((steps, C, group, rows), f32),
            mixes,
            V((NQ, rows, width), bf16),
            V((NQ, H, rows, width), bf16),
            V((H, X, NQ, RC, width), bf16),
            V((NQ, rows, width), bf16),
            V((NQ, X, rows, u_width), bf16),
            V((NQ, CORES, Y, hr, 128), f32),
            V((NQ, Y, hr, 128), f32),
            V((NQ, Y, hr, 128), f32),
            V((NQ, Y, hr, 128), f32),
            V((NQ, tiles, 2, CORES, Y, hr, tile), bf16),
            V((NQ, tiles, 2, Y, hr, tile), bf16),
            V((NQ, tiles, 2, Y, hr, tile), bf16),
            V((NQ, tiles, 2, Y, hr, tile), bf16),
            V((NQ, tiles, H, hr, tile), bf16),
            V((rows, out_width), f32),
            V((NQ, C, RC, out_width), bf16),
            V((NQ, C, RC, out_width), bf16),
            S((5,)),
            S((2, kv)),
            S((4,)),
            S((1,)),
            S((steps,)),
            S((1,)),
            S((steps,)),
            S((1,)),
            S((steps,)),
            S((NQ,)),
            S((NQ, NP)),
            S((1,)),
            S((1,)),
            S((NQ, NP, 1 + X)),
            S((NQ, X, NP)),
            S((NQ, Y)),
            S((NQ, 1 + Y)),
            S((1,)),
            S((NQ, tiles, 2)),
            S((1,)),
            S((NQ, tiles, 2, Y)),
            S((1,)),
            S((NQ, tiles, H)),
            S((1,)),
            S((NQ,)),
        ],
        compiler_params=pltpu.CompilerParams(
            collective_id=0, has_side_effects=True, vmem_limit_bytes=63 * 2**20
        ),
    )(
        page_map,
        selected,
        queries.reshape(C, NQ, RC, query_width),
        residual_in.reshape(X, NQ, RC, width),
        norm_gain,
        keys,
        values,
        out_weight,
        gate_weight,
        up_weight,
        down_weight,
    ).reshape(row_count // C, out_width)


def fits(C, H, queries, keys, selected, out_weight, gate_weight):
    rows = queries.shape[0]
    width = out_weight.shape[1]
    if rows % 128:
        return False
    chunks = rows // 128
    return (
        chunks == 2
        and C % H == 0
        and (C // H) * H == C
        and rows % (C * chunks) == 0
        and rows // (C * chunks) % 16 == 0
        and rows % selected.shape[0] == 0
        and keys.shape[2] // HEAD_SIZE > 3
        and (keys.shape[1] - rows) % 128 == 0
        and keys.shape[1] > rows
        and width % 16 == 0
        and width % 128 <= 125
        and width % 128 > 0
        and gate_weight.shape[1] % 128 == 0
    )


def shards(
    queries,
    keys,
    values,
    page_map,
    selected,
    residual_in,
    out_weight,
    norm_gain,
    gate_weight,
    up_weight,
    down_weight,
):
    ctx_index = lax.axis_index("ctx")
    C = lax.axis_size("ctx")
    H = lax.axis_size("head")
    if fits(C, H, queries, keys, selected, out_weight, gate_weight):
        return fused(
            C,
            H,
            queries,
            keys,
            values,
            page_map,
            selected,
            residual_in,
            out_weight,
            norm_gain,
            gate_weight,
            up_weight,
            down_weight,
        )
    row_max, row_total, mixture = owner_pass(
        queries, keys, values, page_map, selected, ctx_index, C
    )
    stats = jnp.concatenate([row_max, row_total], axis=1)
    stats = jnp.pad(stats, ((0, 0), (0, 128 - stats.shape[1])))
    mlp_out, own_stream = tail(
        C,
        H,
        mixture.astype(jnp.bfloat16),
        stats,
        residual_in,
        norm_gain,
        out_weight,
        gate_weight,
        up_weight,
        down_weight,
    )
    own_stream = jnp.concatenate([own_stream[j] for j in range(own_stream.shape[0])], axis=1)
    return (own_stream.astype(jnp.float32) + mlp_out).astype(jnp.bfloat16)


def solution(mesh):
    in_specs = (
        P(None, "head"),
        P("ctx", None, "head"),
        P("ctx", None, "head"),
        P(),
        P(),
        P("head", "ctx"),
        P("head", "ctx"),
        P("ctx"),
        P("head", "ctx"),
        P("head", "ctx"),
        P("ctx", "head"),
    )
    out_specs = P("ctx", "head")
    return jax.shard_map(shards, mesh=mesh, in_specs=in_specs, out_specs=out_specs, check_vma=False)
```

```python
import jax
import jax.numpy as jnp
import functools
from jax import lax
from jax.experimental import pallas as pl
from jax.experimental.pallas import tpu as pltpu
from jax.sharding import PartitionSpec as P

D = 5376
HEAD_SIZE = 128


score_scale = 168.0 ** (-0.5)
masked_score = -1e30
norm_epsilon = 1e-06


def attention_kernel(
    logical_ref, chosen_ref, page_total, q_ref, k_ref, v_ref, mix_ref, m_ref, l_ref, acc, top, total
):
    page = pl.program_id(1)
    tile_count = chosen_ref.shape[0]
    tile_rows = q_ref.shape[0] // tile_count
    group = q_ref.shape[1] // k_ref.shape[2]
    page_len = k_ref.shape[1]
    offset = page_len - q_ref.shape[0]
    f32 = jnp.float32

    @pl.when(page == 0)
    def _():
        acc[...] = jnp.zeros_like(acc)
        top[...] = jnp.full_like(top, masked_score)
        total[...] = jnp.zeros_like(total)

    causal = logical_ref[page] == page_total - 1

    def visit(t, masked):
        rows = slice(t * tile_rows, (t + 1) * tile_rows)
        for g in range(group):
            cols = slice(g * HEAD_SIZE, (g + 1) * HEAD_SIZE)
            scores = (
                lax.dot_general(
                    q_ref[rows, cols],
                    k_ref[0],
                    (((1,), (1,)), ((), ())),
                    preferred_element_type=f32,
                )
                * score_scale
            )
            if masked:
                position = offset + t * tile_rows + lax.broadcasted_iota(jnp.int32, scores.shape, 0)
                key = lax.broadcasted_iota(jnp.int32, scores.shape, 1)
                scores = jnp.where(key <= position, scores, masked_score)
            old = top[g, rows, :1]
            new = jnp.maximum(old, jnp.max(scores, axis=1, keepdims=True))
            weights = jnp.exp(scores - new)
            keep = jnp.exp(old - new)
            total[g, rows] = total[g, rows] * keep + jnp.sum(weights, axis=1, keepdims=True)
            top[g, rows] = jnp.broadcast_to(new, (tile_rows, 128))
            acc[rows, cols] = acc[rows, cols] * keep + jnp.dot(
                weights.astype(jnp.bfloat16), v_ref[0], preferred_element_type=f32
            )

    for t in range(tile_count):
        picked = chosen_ref[t, page] != 0
        pl.when(jnp.logical_and(picked, causal))(functools.partial(visit, t, True))
        pl.when(jnp.logical_and(picked, jnp.logical_not(causal)))(
            functools.partial(visit, t, False)
        )

    @pl.when(page == pl.num_programs(1) - 1)
    def _():
        mix_ref[...] = acc[...].astype(jnp.bfloat16)
        lane = lax.broadcasted_iota(jnp.int32, m_ref.shape[1:], 1)
        maxima = jnp.zeros(m_ref.shape[1:], f32)
        sums = jnp.zeros(m_ref.shape[1:], f32)
        for g in range(group):
            maxima = jnp.where(lane == g, top[g], maxima)
            sums = jnp.where(lane == g, total[g], sums)
        m_ref[0] = maxima
        l_ref[0] = sums


def owner_pass(queries, keys, values, page_map, selected, ctx_index, ctx_count):
    pages_local, page_len, kv_width = keys.shape
    row_count, query_width = queries.shape
    kv_local = kv_width // HEAD_SIZE
    group = query_width // kv_width
    tile_count = selected.shape[0]
    page_total = pages_local * ctx_count
    slot_ids = ctx_index * pages_local + jnp.arange(pages_local, dtype=jnp.int32)
    all_pages = jnp.arange(page_total, dtype=jnp.int32)
    logical = jnp.sum(
        jnp.where(page_map[None, :] == slot_ids[:, None], all_pages[None, :], 0), axis=1
    )
    chosen = jnp.any(selected[:, None, :] == logical[None, :, None], axis=2).astype(jnp.int32)
    stat = jax.ShapeDtypeStruct((kv_local, row_count, 128), jnp.float32)
    stat_spec = pl.BlockSpec((1, row_count, 128), lambda k, p, a, b: (k, 0, 0))
    kv_spec = pl.BlockSpec((1, page_len, HEAD_SIZE), lambda k, p, a, b: (p, 0, k))
    q_spec = pl.BlockSpec((row_count, group * HEAD_SIZE), lambda k, p, a, b: (0, k))

    def kernel(logical_ref, chosen_ref, *refs):
        attention_kernel(logical_ref, chosen_ref, page_total, *refs)

    mixture, top, total = pl.pallas_call(
        kernel,
        grid_spec=pltpu.PrefetchScalarGridSpec(
            num_scalar_prefetch=2,
            grid=(kv_local, pages_local),
            in_specs=[q_spec, kv_spec, kv_spec],
            out_specs=(q_spec, stat_spec, stat_spec),
            scratch_shapes=[
                pltpu.VMEM((row_count, group * HEAD_SIZE), jnp.float32),
                pltpu.VMEM((group, row_count, 128), jnp.float32),
                pltpu.VMEM((group, row_count, 128), jnp.float32),
            ],
        ),
        out_shape=(jax.ShapeDtypeStruct((row_count, query_width), jnp.bfloat16), stat, stat),
    )(logical.astype(jnp.int32), chosen, queries, keys, values)

    def heads(stacked):
        return stacked[:, :, :group].transpose(1, 0, 2).reshape(row_count, kv_local * group)

    return heads(top), heads(total), mixture


MESH = pl.DeviceIdType.MESH
CORES = 2


def column_tile(width):
    for tile in (896, 768, 640, 512, 384, 256, 128):
        if width % tile == 0:
            return tile
    return width


def flat(block, rows):
    if block.shape[1] % 16:
        return block.astype(jnp.float32).reshape(rows, -1).astype(jnp.bfloat16)
    return block.reshape(rows, -1)


def tail_kernel(
    C,
    H,
    mix_ref,
    stat_ref,
    res_ref,
    gain_ref,
    ow_hbm,
    gw_hbm,
    uw_hbm,
    dw_hbm,
    mlp_ref,
    own_ref,
    ow,
    gw,
    uw,
    dw,
    mix_in,
    stat_in,
    att,
    po,
    po_in,
    u_out,
    st_out,
    ss,
    ublk,
    own_st,
    first,
    first_in,
    second,
    second_in,
    hid,
    acc,
    part,
    part_in,
    w_sem,
    mix_s,
    mix_r,
    stat_s,
    stat_r,
    att_s,
    att_r,
    po_s,
    po_r,
    u_s,
    u_r,
    st_s,
    st_r,
    ss_s,
    ss_r,
    f_s,
    f_r,
    g_s,
    g_r,
    h_s,
    h_r,
    fw_s,
    part_s,
    part_r,
):
    c = lax.axis_index("ctx")
    h = lax.axis_index("head")
    Y = H // CORES
    y = h // CORES
    core = h % CORES
    partner = y * CORES + (CORES - 1 - core)
    R = mix_ref.shape[1]
    rows = C * R
    rb = C // H
    bph = C // H
    width = ow.shape[0]
    head_rows = rows // H
    heads = mix_ref.shape[2] // HEAD_SIZE
    tiles, _, _, _, _, tile = first.shape
    f32 = jnp.float32
    bf16 = jnp.bfloat16

    def remote(src, dst, send_sem, recv_sem, ctx, head):
        return pltpu.make_async_remote_copy(
            src_ref=src,
            dst_ref=dst,
            send_sem=send_sem,
            recv_sem=recv_sem,
            device_id=(ctx, head),
            device_id_type=MESH,
        )

    sent = []

    def send(*args):
        copy = remote(*args)
        copy.start()
        sent.append(copy)

    loads = [
        pltpu.make_async_copy(src, dst, w_sem.at[i])
        for i, (src, dst) in enumerate(
            ((ow_hbm, ow), (gw_hbm, gw), (uw_hbm, uw), (dw_hbm, dw))
        )
    ]
    for load in loads:
        load.start()

    for d in range(1, C):
        peer = (c + d) % C
        send(stat_ref.at[peer], stat_in.at[c], stat_s.at[d], stat_r.at[c], peer, h)
        send(mix_ref.at[peer], mix_in.at[c], mix_s.at[d], mix_r.at[c], peer, h)
    stat_in[c] = stat_ref[c]
    mix_in[c] = mix_ref[c]
    for d in range(1, C):
        peer = (c + C - d) % C
        remote(stat_in.at[peer], stat_in.at[peer], stat_s.at[d], stat_r.at[peer], peer, h).wait_recv()
        remote(mix_in.at[peer], mix_in.at[peer], mix_s.at[d], mix_r.at[peer], peer, h).wait_recv()
    maxima = [stat_in[k][:, :heads] for k in range(C)]
    top = functools.reduce(jnp.maximum, maxima)
    scales = [jnp.exp(m - top) for m in maxima]
    total = sum(stat_in[k][:, heads : 2 * heads] * scales[k] for k in range(C))
    inverse = 1.0 / total
    for g in range(heads):
        cols = slice(g * HEAD_SIZE, (g + 1) * HEAD_SIZE)
        mixed = sum(mix_in[k, :, cols].astype(f32) * scales[k][:, g : g + 1] for k in range(C))
        att[c, :, cols] = (mixed * inverse[:, g : g + 1]).astype(bf16)

    for d in range(1, C):
        peer = (c + d) % C
        send(att.at[c], att.at[c], att_s.at[d], att_r.at[c], peer, h)
    loads[0].wait()
    for d in range(1, C):
        peer = (c + C - d) % C
        remote(att.at[peer], att.at[peer], att_s.at[d], att_r.at[peer], peer, h).wait_recv()
    projected = lax.dot_general(
        flat(att[...], rows), ow[...], (((1,), (1,)), ((), ())), preferred_element_type=f32
    )
    po[...] = projected.reshape(H, head_rows, width).astype(bf16)

    for d in range(1, H):
        peer = (h + d) % H
        send(po.at[peer], po_in.at[h], po_s.at[d], po_r.at[h], c, peer)
    po_in[h] = po[h]
    for d in range(1, H):
        peer = (h + H - d) % H
        remote(po_in.at[peer], po_in.at[peer], po_s.at[d], po_r.at[peer], c, peer).wait_recv()
    projected = sum(po_in[k].astype(f32) for k in range(H))
    stream = (res_ref[...].astype(f32) + projected).astype(bf16).astype(f32)
    st_out[...] = stream.reshape(rb, R, width).astype(bf16)
    u_out[...] = (stream * gain_ref[...]).reshape(rb, R, width).astype(bf16)
    squares = jnp.sum(stream * stream, axis=1, keepdims=True)
    ss[c] = jnp.broadcast_to(squares, (head_rows, 128))

    block_head = c // bph
    block_part = c % bph
    u_dst = ublk.at[block_part, pl.ds(h * rb, rb)]
    kept = []
    for d in range(C):
        peer = (c + d) % C
        copy = remote(u_out, u_dst, u_s.at[d], u_r.at[block_part, h], peer, block_head)
        if d == 0:
            kept.append((block_head != h, copy))
            pl.when(block_head != h)(copy.start)

            @pl.when(block_head == h)
            def _():
                ublk[block_part, pl.ds(h * rb, rb)] = u_out[...]

        else:
            copy.start()
            sent.append(copy)
    for d in range(1, C):
        peer = (c + d) % C
        send(ss.at[c], ss.at[c], ss_s.at[d], ss_r.at[c], peer, h)
    for i in range(rb):
        owner = h * rb + i
        other = jnp.logical_or(owner != c, block_head != h)
        copy = remote(
            st_out.at[i], own_st.at[block_part], st_s.at[i], st_r.at[block_part], owner, block_head
        )
        kept.append((other, copy))
        pl.when(other)(copy.start)

        @pl.when(jnp.logical_not(other))
        def _(i=i):
            own_st[block_part] = st_out[i]

    for j in range(bph):
        for k in range(H):
            source = h * bph + j
            block = ublk.at[j, pl.ds(k * rb, rb)]
            arrival = remote(block, block, u_s.at[0], u_r.at[j, k], source, k)
            pl.when(jnp.logical_or(source != c, h != k))(arrival.wait_recv)
    loads[1].wait()
    loads[2].wait()

    def matmul(i, which, weight):
        cols = slice(i * tile, (i + 1) * tile)
        value = None
        for j in range(bph):
            term = jnp.dot(
                flat(ublk[j], rows),
                weight[j * width : (j + 1) * width, cols],
                preferred_element_type=f32,
            )
            value = term if value is None else value + term
        first[i, which] = value.reshape(Y, CORES, head_rows, tile).swapaxes(0, 1).astype(bf16)
        send(
            first.at[i, which, CORES - 1 - core],
            first_in.at[i, which],
            f_s.at[i, which],
            f_r.at[i, which],
            c,
            partner,
        )

    def middle(i, which):
        remote(
            first_in.at[i, which], first_in.at[i, which], f_s.at[i, which], f_r.at[i, which], c, partner
        ).wait_recv()
        both = first[i, which, core].astype(f32) + first_in[i, which].astype(f32)
        second[i, which] = both.astype(bf16)
        for d in range(1, Y):
            peer = (y + d) % Y
            send(
                second.at[i, which, peer],
                second_in.at[i, which, y],
                g_s.at[i, which, d],
                g_r.at[i, which, y],
                c,
                peer * CORES + core,
            )

    def finish(i, inverse_rms):
        sums = []
        for which in range(2):
            value = second[i, which, y].astype(f32)
            for d in range(1, Y):
                peer = (y + Y - d) % Y
                slot = second_in.at[i, which, peer]
                remote(
                    slot, slot, g_s.at[i, which, d], g_r.at[i, which, peer], c, peer * CORES + core
                ).wait_recv()
                value = value + second_in[i, which, peer].astype(f32)
            sums.append(value * inverse_rms)
        hid[i, h] = (jax.nn.gelu(sums[0], approximate=True) * sums[1]).astype(bf16)
        send(hid.at[i, h], hid.at[i, h], h_s.at[i, 0], h_r.at[i, h], c, partner)
        for d in range(1, Y):
            peer = ((y + d) % Y) * CORES + core
            send(hid.at[i, h], hid.at[i, h], h_s.at[i, d], h_r.at[i, h], c, peer)

    def forward(i):
        for d in range(1, Y):
            origin = ((y + Y - d) % Y) * CORES + core
            slot = hid.at[i, origin]
            remote(slot, slot, h_s.at[i, d], h_r.at[i, origin], c, origin).wait_recv()
            send(slot, slot, fw_s.at[i, d], h_r.at[i, origin], c, partner)

    def down(i):
        for d in range(Y):
            origin = ((y + Y - d) % Y) * CORES + (CORES - 1 - core)
            slot = hid.at[i, origin]
            remote(slot, slot, h_s.at[i, 0], h_r.at[i, origin], c, partner).wait_recv()
        term = lax.dot_general(
            flat(hid[i], rows),
            dw[:, i * tile : (i + 1) * tile],
            (((1,), (1,)), ((), ())),
            preferred_element_type=f32,
        )
        if i == 0:
            acc[...] = term
        else:
            acc[...] += term

    steps = [(i, which) for i in range(tiles) for which in range(2)]
    for n, (i, which) in enumerate(steps):
        matmul(i, which, (gw, uw)[which])
        if n:
            middle(*steps[n - 1])
    middle(*steps[-1])
    for d in range(1, C):
        peer = (c + C - d) % C
        remote(ss.at[peer], ss.at[peer], ss_s.at[d], ss_r.at[peer], peer, h).wait_recv()
    squares = sum(ss[k] for k in range(C))
    inverse_rms = lax.rsqrt(squares[:, :1] / (C * width) + norm_epsilon)
    loads[3].wait()
    for i in range(tiles):
        finish(i, inverse_rms)
        if i:
            forward(i - 1)
    forward(tiles - 1)
    for i in range(tiles):
        down(i)
    part[...] = acc[...].reshape(C, R, acc.shape[1]).astype(bf16)

    for d in range(1, C):
        peer = (c + d) % C
        send(part.at[peer], part_in.at[c], part_s.at[d], part_r.at[c], peer, h)
    part_in[c] = part[c]
    for j in range(bph):
        source = h * bph + j
        arrival = remote(own_st.at[j], own_st.at[j], st_s.at[0], st_r.at[j], source, c // rb)
        pl.when(jnp.logical_or(source != c, c // rb != h))(arrival.wait_recv)
    own_ref[...] = own_st[...]
    for d in range(1, C):
        peer = (c + C - d) % C
        remote(part_in.at[peer], part_in.at[peer], part_s.at[d], part_r.at[peer], peer, h).wait_recv()
    mlp_ref[...] = sum(part_in[k].astype(f32) for k in range(C))
    for copy in sent:
        copy.wait_send()
    for condition, copy in kept:
        pl.when(condition)(copy.wait_send)


def tail(C, H, mixture, stats, residual_in, norm_gain, out_weight, gate_weight, up_weight, down_weight):
    rows, query_width = mixture.shape
    R = rows // C
    width = out_weight.shape[1]
    hidden = gate_weight.shape[1]
    out_width = down_weight.shape[1]
    out_weight = out_weight.T
    down_weight = down_weight.T
    rb = C // H
    bph = C // H
    Y = H // CORES
    head_rows = rows // H
    tile = column_tile(hidden)
    tiles = hidden // tile
    bf16 = jnp.bfloat16
    vmem = pl.BlockSpec(memory_space=pltpu.VMEM)
    hbm = pl.BlockSpec(memory_space=pl.ANY)
    V = pltpu.VMEM
    S = pltpu.SemaphoreType.DMA
    return pl.pallas_call(
        functools.partial(tail_kernel, C, H),
        out_shape=(
            jax.ShapeDtypeStruct((R, out_width), jnp.float32),
            jax.ShapeDtypeStruct((bph, R, width), bf16),
        ),
        in_specs=[vmem] * 4 + [hbm] * 4,
        out_specs=(vmem, vmem),
        scratch_shapes=[
            V(out_weight.shape, bf16),
            V(gate_weight.shape, bf16),
            V(up_weight.shape, bf16),
            V(down_weight.shape, bf16),
            V((C, R, query_width), bf16),
            V((C, R, 128), jnp.float32),
            V((C, R, query_width), bf16),
            V((H, head_rows, width), bf16),
            V((H, head_rows, width), bf16),
            V((rb, R, width), bf16),
            V((rb, R, width), bf16),
            V((C, head_rows, 128), jnp.float32),
            V((bph, C, R, width), bf16),
            V((bph, R, width), bf16),
            V((tiles, 2, CORES, Y, head_rows, tile), bf16),
            V((tiles, 2, Y, head_rows, tile), bf16),
            V((tiles, 2, Y, head_rows, tile), bf16),
            V((tiles, 2, Y, head_rows, tile), bf16),
            V((tiles, H, head_rows, tile), bf16),
            V((rows, out_width), jnp.float32),
            V((C, R, out_width), bf16),
            V((C, R, out_width), bf16),
            S((4,)),
            S((C,)),
            S((C,)),
            S((C,)),
            S((C,)),
            S((C,)),
            S((C,)),
            S((H,)),
            S((H,)),
            S((C,)),
            S((bph, H)),
            S((rb,)),
            S((bph,)),
            S((C,)),
            S((C,)),
            S((tiles, 2)),
            S((tiles, 2)),
            S((tiles, 2, Y)),
            S((tiles, 2, Y)),
            S((tiles, Y)),
            S((tiles, H)),
            S((tiles, Y)),
            S((C,)),
            S((C,)),
        ],
        compiler_params=pltpu.CompilerParams(
            has_side_effects=True, vmem_limit_bytes=60 * 2**20
        ),
    )(
        mixture.reshape(C, R, query_width),
        stats.reshape(C, R, 128),
        residual_in,
        norm_gain.reshape(1, width),
        out_weight,
        gate_weight,
        up_weight,
        down_weight,
    )


LOG2E = 1.4426950408889634


def fused_kernel(
    C,
    H,
    NP,
    map_hbm,
    sel_hbm,
    q_hbm,
    res_hbm,
    gain_hbm,
    k_hbm,
    v_hbm,
    ow_hbm,
    gw_hbm,
    uw_hbm,
    dw_hbm,
    out_ref,
    map_ref,
    sel_ref,
    q_ref,
    res_ref,
    gain_ref,
    k_buf,
    v_buf,
    ow,
    gw,
    uw,
    dw,
    mix_out,
    mix_in,
    lse_out,
    lse_in,
    att,
    po_out,
    po_in,
    res_in,
    st,
    u,
    ss_out,
    ss_in,
    ss_mid,
    ss_last,
    scale,
    first,
    first_in,
    second,
    second_in,
    hid,
    acc,
    part,
    part_in,
    in_sem,
    kv_sem,
    w_sem,
    mix_s,
    mix_r,
    lse_s,
    lse_r,
    att_s,
    att_r,
    po_s,
    po_r,
    res_s,
    res_r,
    u_s,
    u_r,
    ss_s,
    ss_r,
    f_s,
    f_r,
    g_s,
    g_r,
    h_s,
    h_r,
    part_s,
    part_r,
):
    c = lax.axis_index("ctx")
    h = lax.axis_index("head")
    X = C // H
    Z = C // X
    z = c // X
    x = c % X
    Y = H // CORES
    y = h // CORES
    core = h % CORES
    partner = y * CORES + (CORES - 1 - core)
    _, NQ, RC, query_width = q_ref.shape
    rows = C * RC
    hr = rows // H
    kv, pages, page_len, _ = k_buf.shape
    group = query_width // (kv * HEAD_SIZE)
    gw_cols = group * HEAD_SIZE
    tile_count = sel_ref.shape[0]
    tile_rows = NQ * rows // tile_count
    offset = page_len - NQ * rows
    page_total = map_ref.shape[0]
    width = ow.shape[0]
    tile = first.shape[-1]
    tiles = first.shape[1]
    RP = rows // NP
    f32 = jnp.float32
    bf16 = jnp.bfloat16
    owner = h == z
    visitor = h != z

    def remote(src, dst, send_sem, recv_sem, ctx, head):
        return pltpu.make_async_remote_copy(
            src_ref=src,
            dst_ref=dst,
            send_sem=send_sem,
            recv_sem=recv_sem,
            device_id=(ctx, head),
            device_id_type=MESH,
        )

    sent = []
    kept = []

    def start(*args):
        remote(*args).start()

    def send(*args):
        copy = remote(*args)
        copy.start()
        sent.append(copy)

    def send_if(condition, *args):
        copy = remote(*args)
        pl.when(condition)(copy.start)
        kept.append((condition, copy))

    def kv_load(j):
        lanes = pl.ds(pl.multiple_of(j * HEAD_SIZE, HEAD_SIZE), HEAD_SIZE)
        return (
            pltpu.make_async_copy(k_hbm.at[:, :, lanes], k_buf.at[j], kv_sem.at[0, j]),
            pltpu.make_async_copy(v_hbm.at[:, :, lanes], v_buf.at[j], kv_sem.at[1, j]),
        )

    barrier = pltpu.get_barrier_semaphore()
    for d in range(1, C):
        pl.semaphore_signal(
            barrier, inc=1, device_id=((c + d) % C, h), device_id_type=MESH
        )
    for d in range(1, H):
        pl.semaphore_signal(
            barrier, inc=1, device_id=(c, (h + d) % H), device_id_type=MESH
        )
    inputs = [
        pltpu.make_async_copy(src, dst, in_sem.at[i])
        for i, (src, dst) in enumerate(
            (
                (map_hbm, map_ref),
                (sel_hbm, sel_ref),
                (q_hbm, q_ref),
                (res_hbm, res_ref),
                (gain_hbm, gain_ref.at[0]),
            )
        )
    ]
    for load in inputs:
        load.start()
    for j in range(kv):
        for load in kv_load(j):
            load.start()
    loads = [
        pltpu.make_async_copy(src, dst, w_sem.at[i])
        for i, (src, dst) in enumerate(
            ((ow_hbm, ow), (gw_hbm, gw), (uw_hbm, uw), (dw_hbm, dw))
        )
    ]
    for load in inputs:
        load.wait()

    facts = []
    for p in range(pages):
        slot = c * pages + p
        logical = jnp.int32(0)
        for j in range(page_total):
            logical = logical + jnp.where(map_ref[j] == slot, j, 0)
        picks = []
        for t in range(tile_count):
            hits = jnp.int32(0)
            for i in range(sel_ref.shape[1]):
                hits = hits + jnp.where(sel_ref[t, i] == logical, 1, 0)
            picks.append(jnp.where(hits > 0, 0.0, masked_score).astype(f32))
        reach = jnp.where(logical == page_total - 1, 0, page_len)
        facts.append((reach, picks))

    index = lax.broadcasted_iota(jnp.int32, (group * rows, 1), 0) & (rows - 1)
    shift = RC.bit_length() - 1
    base_row = (index >> shift) * (NQ * RC) + (index & (RC - 1))
    eye = lax.broadcasted_iota(jnp.int32, (rows, rows), 0) == lax.broadcasted_iota(
        jnp.int32, (rows, rows), 1
    )
    unit = score_scale * LOG2E

    def attend(n):
        q = n // kv
        j = n % kv

        @pl.when(n < kv)
        def _():
            for load in kv_load(j):
                load.wait()

        @pl.when(n == 0)
        def _():
            for load in loads:
                load.start()

        lanes = pl.ds(pl.multiple_of(j * gw_cols, gw_cols), gw_cols)
        block = q_ref[:, q, :, lanes].reshape(rows, gw_cols)
        lhs = jnp.concatenate(
            [block[:, g * HEAD_SIZE : (g + 1) * HEAD_SIZE] for g in range(group)], axis=0
        )
        row = base_row + q * RC
        key = offset + lax.broadcasted_iota(jnp.int32, (group * rows, page_len - offset), 1)
        tops, sums, outs = [], [], []
        for p in range(pages):
            reach, picks = facts[p]
            bias = jnp.zeros((group * rows, 1), f32)
            for t in range(tile_count):
                inside = jnp.logical_and(row >= t * tile_rows, row < (t + 1) * tile_rows)
                bias = jnp.where(inside, picks[t], bias)
            scores = lax.dot_general(
                lhs, k_buf[j, p], (((1,), (1,)), ((), ())), preferred_element_type=f32
            )
            late = jnp.where(key <= offset + row + reach, scores[:, offset:], masked_score)
            scores = jnp.concatenate([scores[:, :offset], late], axis=1)
            top = jnp.max(scores, axis=1, keepdims=True)
            weights = jnp.exp2((scores - top) * unit)
            sums.append(jnp.sum(weights, axis=1, keepdims=True))
            outs.append(
                jnp.dot(weights.astype(bf16), v_buf[j, p], preferred_element_type=f32)
            )
            tops.append(top * unit + bias)
        best = functools.reduce(jnp.maximum, tops)
        scales = [jnp.exp2(top - best) for top in tops]
        total = sum(s * e for s, e in zip(sums, scales))
        mixed = sum(o * (e / total) for o, e in zip(outs, scales))
        lse = best + jnp.log2(total)
        for g in range(group):
            part_rows = slice(g * rows, (g + 1) * rows)
            mix_out[n, :, :, g * HEAD_SIZE : (g + 1) * HEAD_SIZE] = (
                mixed[part_rows].reshape(C, RC, HEAD_SIZE).astype(bf16)
            )
            lse_out[n, g : g + 1] = jnp.sum(
                jnp.where(eye, lse[part_rows], 0.0), axis=0, keepdims=True
            )
        mix_in[n, c] = mix_out[n, c]
        lse_in[n, c] = lse_out[n]

    def mix_sends(n):
        for d in range(1, C):
            peer = (c + d) % C
            remote(mix_out.at[n, peer], mix_in.at[n, c], mix_s.at[0], mix_r.at[n], peer, h).start()
            remote(lse_out.at[n], lse_in.at[n, c], lse_s.at[0], lse_r.at[n], peer, h).start()

    def att_sends(n):
        for d in range(1, C):
            peer = (c + d) % C
            remote(att.at[n, c], att.at[n, c], att_s.at[0], att_r.at[n], peer, h).start()

    def arrived(block, recv_sem):
        remote(block, block, recv_sem, recv_sem, c, partner).wait_recv()

    def left(block, send_sem):
        remote(block, block, send_sem, send_sem, c, partner).wait_send()

    def combine(n):
        arrived(lse_in.at[n, pl.ds(0, C - 1)], lse_r.at[n])
        arrived(mix_in.at[n, pl.ds(0, C - 1)], mix_r.at[n])
        logs = [lse_in[n, k] for k in range(C)]
        best = functools.reduce(jnp.maximum, logs)
        scales = [jnp.exp2(value - best) for value in logs]
        inverse = 1.0 / sum(scales)
        lane = lax.broadcasted_iota(jnp.int32, (RC, rows), 1)
        mine = lane == c * RC + lax.broadcasted_iota(jnp.int32, (RC, rows), 0)
        for g in range(group):
            cols = slice(g * HEAD_SIZE, (g + 1) * HEAD_SIZE)
            value = jnp.zeros((RC, HEAD_SIZE), f32)
            for k in range(C):
                share = (scales[k] * inverse)[g : g + 1]
                share = jnp.sum(jnp.where(mine, share, 0.0), axis=1, keepdims=True)
                value = value + share * mix_in[n, k, :, cols].astype(f32)
            att[n, c, :, cols] = value.astype(bf16)
        att_sends(n)

    def project(q):
        for j in range(kv):
            n = q * kv + j
            arrived(att.at[n, pl.ds(0, C - 1)], att_r.at[n])
        if q == 0:
            loads[0].wait()
        value = None
        for j in range(kv):
            term = lax.dot_general(
                att[q * kv + j].reshape(rows, gw_cols),
                ow[:, j * gw_cols : (j + 1) * gw_cols],
                (((1,), (1,)), ((), ())),
                preferred_element_type=f32,
            )
            value = term if value is None else value + term
        po_out[q] = value.astype(bf16)
        for i in range(NP):
            piece = pl.ds(i * RP, RP)
            copy = remote(
                po_out.at[q, piece], po_in.at[q, h, piece], po_s.at[q], po_r.at[q, i], c, z
            )
            pl.when(visitor)(copy.start)
        po_in[q, h] = po_out[q]

    def own(q, i):
        if q == 0 and i == 0:
            arrived(res_in.at[pl.ds(0, H - 1)], res_r.at[0])
        arrived(po_in.at[q, pl.ds(0, H - 1), pl.ds(i * RP, RP)], po_r.at[q, i])
        spare = u.shape[-1] - width
        lane = lax.broadcasted_iota(jnp.int32, (hr, spare), 1)
        for b in range(i * RP // hr, (i + 1) * RP // hr):
            span = slice(b * hr, (b + 1) * hr)
            value = res_in[b, :, q].reshape(hr, width).astype(f32)
            added = sum(po_in[q, k, span].astype(f32) for k in range(H))
            stream = (value + added).astype(bf16)
            st[q, span] = stream
            stream = stream.astype(f32)
            u[q, x, span, :width] = (stream * gain_ref[...]).astype(bf16)
            squares = jnp.sum(stream * stream, axis=1, keepdims=True)
            high = squares.astype(bf16).astype(f32)
            mid = (squares - high).astype(bf16).astype(f32)
            low = squares - high - mid
            packed = jnp.where(lane == 0, high, jnp.where(lane == 1, mid, low))
            packed = jnp.where(lane < 3, packed, 0.0)
            u[q, x, span, width:] = packed.astype(bf16)

    def relay(q, i, here):
        piece = u.at[q, x, pl.ds(i * RP, RP)]
        recv = u_r.at[q, x, i]
        pl.when(jnp.logical_and(here, visitor))(functools.partial(arrived, piece, recv))
        up = jnp.logical_and(here, jnp.logical_and(z >= h, z < Z - 1))
        down = jnp.logical_and(here, jnp.logical_and(z <= h, z > 0))
        above = jnp.minimum(z + 1, Z - 1) * X + x
        below = jnp.maximum(z - 1, 0) * X + x
        send_if(up, piece, piece, u_s.at[q, i, 0], recv, above, h)
        send_if(down, piece, piece, u_s.at[q, i, 1], recv, below, h)
        for d in range(1, X):
            peer = z * X + (x + d) % X
            send_if(here, piece, piece, u_s.at[q, i, 1 + d], recv, peer, h)

    def spread(q, here):
        for i in range(NP):
            pl.when(jnp.logical_and(here, owner))(functools.partial(own, q, i))
            relay(q, i, here)

    def gather(q):
        for d in range(1, X):
            source = (x + d) % X
            for i in range(NP):
                block = u.at[q, source, pl.ds(i * RP, RP)]
                arrived(block, u_r.at[q, source, i])
        if q == 0:
            loads[1].wait()
            loads[2].wait()
        squares = 0.0
        for k in range(X):
            split = u[q, k, :, width:].astype(f32)
            squares = squares + jnp.sum(split, axis=1, keepdims=True)
        squares = jnp.broadcast_to(squares, (rows, 128)).reshape(Y, CORES, hr, 128)
        ss_out[q] = squares.swapaxes(0, 1)
        send(ss_out.at[q, CORES - 1 - core], ss_in.at[q], ss_s.at[q, 0], ss_r.at[q, 0], c, partner)

    def matmul(q, i, which):
        weight = (gw, uw)[which]
        cols = slice(i * tile, (i + 1) * tile)
        value = None
        for k in range(X):
            term = jnp.dot(
                u[q, k, :, :width],
                weight[k * width : (k + 1) * width, cols],
                preferred_element_type=f32,
            )
            value = term if value is None else value + term
        value = value.reshape(Y, CORES, hr, tile).swapaxes(0, 1).astype(bf16)
        first[q, i, which] = value
        start(
            first.at[q, i, which, CORES - 1 - core],
            first_in.at[q, i, which],
            f_s.at[0],
            f_r.at[q, i, which],
            c,
            partner,
        )

    def middle(q, i, which):
        block = first_in.at[q, i, which]
        arrived(block, f_r.at[q, i, which])
        both = first[q, i, which, core].astype(f32) + first_in[q, i, which].astype(f32)
        second[q, i, which] = both.astype(bf16)
        for d in range(1, Y):
            peer = (y + d) % Y
            start(
                second.at[q, i, which, peer],
                second_in.at[q, i, which, y],
                g_s.at[0],
                g_r.at[q, i, which, y],
                c,
                peer * CORES + core,
            )

    def middle_squares(q):
        block = ss_in.at[q]
        remote(block, block, ss_s.at[q, 0], ss_r.at[q, 0], c, partner).wait_recv()
        ss_mid[q] = ss_out[q, core] + ss_in[q]
        for d in range(1, Y):
            peer = (y + d) % Y
            send(
                ss_mid.at[q, peer],
                ss_last.at[q, y],
                ss_s.at[q, d],
                ss_r.at[q, 1 + y],
                c,
                peer * CORES + core,
            )

    def inverse_rms(q):
        total = ss_mid[q, y]
        for d in range(1, Y):
            peer = (y + Y - d) % Y
            block = ss_last.at[q, peer]
            remote(
                block, block, ss_s.at[q, d], ss_r.at[q, 1 + peer], c, peer * CORES + core
            ).wait_recv()
            total = total + ss_last[q, peer]
        scale[q] = lax.rsqrt(total / (C * width) + norm_epsilon)

    def finish(q, i):
        inverse = scale[q][:, :1]
        sums = []
        for which in range(2):
            value = second[q, i, which, y].astype(f32)
            for d in range(1, Y):
                peer = (y + Y - d) % Y
                block = second_in.at[q, i, which, peer]
                remote(
                    block,
                    block,
                    g_s.at[0],
                    g_r.at[q, i, which, peer],
                    c,
                    peer * CORES + core,
                ).wait_recv()
                value = value + second_in[q, i, which, peer].astype(f32)
            sums.append(value * inverse)
        hid[q, i, h] = (jax.nn.gelu(sums[0], approximate=True) * sums[1]).astype(bf16)
        block = hid.at[q, i, h]
        for d in range(1, Y):
            peer = ((y + d) % Y) * CORES + core
            start(block, block, h_s.at[0], h_r.at[q, i, h], c, peer)
        start(block, block, h_s.at[0], h_r.at[q, i, h], c, partner)

    def forward(q, i):
        for d in range(1, Y):
            origin = ((y + Y - d) % Y) * CORES + core
            block = hid.at[q, i, origin]
            arrived(block, h_r.at[q, i, origin])
            start(block, block, h_s.at[0], h_r.at[q, i, origin], c, partner)

    def down(q, i):
        for d in range(Y):
            origin = ((y + Y - d) % Y) * CORES + (CORES - 1 - core)
            block = hid.at[q, i, origin]
            arrived(block, h_r.at[q, i, origin])
        if q == 0 and i == 0:
            loads[3].wait()
        term = lax.dot_general(
            hid[q, i].reshape(rows, tile),
            dw[:, i * tile : (i + 1) * tile],
            (((1,), (1,)), ((), ())),
            preferred_element_type=f32,
        )
        if i == 0:
            acc[...] = term
        else:
            acc[...] += term

    def scatter(q):
        for k in range(X):

            @pl.when(jnp.logical_and(owner, x == k))
            def _(k=k):
                acc[:, k * width : (k + 1) * width] += st[q].astype(f32)

        part[q] = acc[...].reshape(C, RC, acc.shape[1]).astype(bf16)
        for d in range(1, C):
            peer = (c + d) % C
            start(part.at[q, peer], part_in.at[q, c], part_s.at[0], part_r.at[q], peer, h)
        part_in[q, c] = part[q, c]

    def collect(q):
        arrived(part_in.at[q, pl.ds(0, C - 1)], part_r.at[q])
        out_ref[q] = sum(part_in[q, k].astype(f32) for k in range(C)).astype(bf16)

    pl.semaphore_wait(barrier, C + H - 2)
    send_if(visitor, res_ref, res_in.at[h], res_s.at[0], res_r.at[0], c, z)
    res_in[h] = res_ref[...]

    steps = NQ * kv
    lag = 3

    def loop(n, carry):
        attend(n)
        pl.when(jnp.logical_or(n < kv, n >= kv + lag))(functools.partial(mix_sends, n))

        @pl.when(jnp.logical_and(n >= lag, n < kv + lag))
        def _():
            combine(n - lag)

        @pl.when(n == kv + lag - 1)
        def _():
            for k in range(kv, kv + lag):
                mix_sends(k)

        return carry

    lax.fori_loop(0, steps, loop, 0)
    pairs = [(i, which) for i in range(tiles) for which in range(2)]

    def expand(q, extra=None):
        gather(q)
        for n, (i, which) in enumerate(pairs):
            matmul(q, i, which)
            if n == 1:
                middle_squares(q)
            if n:
                middle(q, *pairs[n - 1])
            if extra is not None and which:
                extra(i)
        middle(q, *pairs[-1])

    def finish_if(here, q, i):
        @pl.when(here)
        def _():
            if i == 0:
                inverse_rms(q)
            finish(q, i)

    def contract(q):
        forward(q, 0)
        for i in range(tiles):
            if i + 1 < tiles:
                forward(q, i + 1)
            down(q, i)
        scatter(q)

    always = z >= 0
    far = jnp.maximum(z - h, h - z)
    early = z // CORES == y
    late = z // CORES != y
    project(0)
    for n in range(kv, steps):
        combine(n)
    spread(0, far < 2)
    spread(0, far == 2)
    project(1)
    spread(0, far > 2)
    expand(0)
    for i in range(tiles):
        finish_if(late, 0, i)
    spread(1, always)
    expand(1, functools.partial(finish_if, early, 0))
    contract(0)
    for i in range(tiles):
        finish_if(always, 1, i)
    contract(1)
    for q in range(NQ):
        collect(q)

    left(mix_out.at[:, pl.ds(0, C - 1)], mix_s.at[0])
    left(lse_in.at[:, pl.ds(0, C - 1)], lse_s.at[0])
    left(att.at[:, pl.ds(0, C - 1)], att_s.at[0])
    left(first_in, f_s.at[0])
    left(second.at[:, :, :, pl.ds(0, Y - 1)], g_s.at[0])
    left(hid.at[:, :, pl.ds(0, 2 * Y - 1)], h_s.at[0])
    left(part.at[:, pl.ds(0, C - 1)], part_s.at[0])
    for q in range(NQ):
        pl.when(visitor)(functools.partial(left, po_out.at[q], po_s.at[q]))
    for copy in sent:
        copy.wait_send()
    for condition, copy in kept:
        pl.when(condition)(copy.wait_send)


def fused(
    C,
    H,
    queries,
    keys,
    values,
    page_map,
    selected,
    residual_in,
    out_weight,
    norm_gain,
    gate_weight,
    up_weight,
    down_weight,
):
    row_count, query_width = queries.shape
    pages, page_len, kv_width = keys.shape
    kv = kv_width // HEAD_SIZE
    group = query_width // kv_width
    NQ = row_count // 128
    RC = row_count // C // NQ
    rows = C * RC
    NP = 4
    X = C // H
    Y = H // CORES
    hr = rows // H
    width = out_weight.shape[1]
    hidden = gate_weight.shape[1]
    out_width = down_weight.shape[1]
    tile = column_tile(hidden)
    tiles = hidden // tile
    steps = NQ * kv
    u_width = (width + 127) // 128 * 128
    bf16 = jnp.bfloat16
    f32 = jnp.float32
    vmem = pl.BlockSpec(memory_space=pltpu.VMEM)
    hbm = pl.BlockSpec(memory_space=pl.ANY)
    V = pltpu.VMEM
    S = pltpu.SemaphoreType.DMA
    out_weight = out_weight.T
    down_weight = down_weight.T
    mixes = V((steps, C, RC, group * HEAD_SIZE), bf16)
    return pl.pallas_call(
        functools.partial(fused_kernel, C, H, NP),
        out_shape=jax.ShapeDtypeStruct((NQ, RC, out_width), bf16),
        in_specs=[hbm] * 11,
        out_specs=vmem,
        scratch_shapes=[
            pltpu.SMEM(page_map.shape, jnp.int32),
            pltpu.SMEM(selected.shape, jnp.int32),
            V((C, NQ, RC, query_width), bf16),
            V((X, NQ, RC, width), bf16),
            V((1, width), f32),
            V((kv, pages, page_len, HEAD_SIZE), bf16),
            V((kv, pages, page_len, HEAD_SIZE), bf16),
            V(out_weight.shape, bf16),
            V(gate_weight.shape, bf16),
            V(up_weight.shape, bf16),
            V(down_weight.shape, bf16),
            mixes,
            mixes,
            V((steps, group, rows), f32),
            V((steps, C, group, rows), f32),
            mixes,
            V((NQ, rows, width), bf16),
            V((NQ, H, rows, width), bf16),
            V((H, X, NQ, RC, width), bf16),
            V((NQ, rows, width), bf16),
            V((NQ, X, rows, u_width), bf16),
            V((NQ, CORES, Y, hr, 128), f32),
            V((NQ, Y, hr, 128), f32),
            V((NQ, Y, hr, 128), f32),
            V((NQ, Y, hr, 128), f32),
            V((NQ, hr, 128), f32),
            V((NQ, tiles, 2, CORES, Y, hr, tile), bf16),
            V((NQ, tiles, 2, Y, hr, tile), bf16),
            V((NQ, tiles, 2, Y, hr, tile), bf16),
            V((NQ, tiles, 2, Y, hr, tile), bf16),
            V((NQ, tiles, H, hr, tile), bf16),
            V((rows, out_width), f32),
            V((NQ, C, RC, out_width), bf16),
            V((NQ, C, RC, out_width), bf16),
            S((5,)),
            S((2, kv)),
            S((4,)),
            S((1,)),
            S((steps,)),
            S((1,)),
            S((steps,)),
            S((1,)),
            S((steps,)),
            S((NQ,)),
            S((NQ, NP)),
            S((1,)),
            S((1,)),
            S((NQ, NP, 1 + X)),
            S((NQ, X, NP)),
            S((NQ, Y)),
            S((NQ, 1 + Y)),
            S((1,)),
            S((NQ, tiles, 2)),
            S((1,)),
            S((NQ, tiles, 2, Y)),
            S((1,)),
            S((NQ, tiles, H)),
            S((1,)),
            S((NQ,)),
        ],
        compiler_params=pltpu.CompilerParams(
            collective_id=0, has_side_effects=True, vmem_limit_bytes=63 * 2**20
        ),
    )(
        page_map,
        selected,
        queries.reshape(C, NQ, RC, query_width),
        residual_in.reshape(X, NQ, RC, width),
        norm_gain,
        keys,
        values,
        out_weight,
        gate_weight,
        up_weight,
        down_weight,
    ).reshape(row_count // C, out_width)


def fits(C, H, queries, keys, selected, out_weight, gate_weight):
    rows = queries.shape[0]
    width = out_weight.shape[1]
    if rows % 128:
        return False
    chunks = rows // 128
    return (
        chunks == 2
        and C % H == 0
        and (C // H) * H == C
        and rows % (C * chunks) == 0
        and rows // (C * chunks) % 16 == 0
        and rows % selected.shape[0] == 0
        and keys.shape[2] // HEAD_SIZE > 3
        and (keys.shape[1] - rows) % 128 == 0
        and keys.shape[1] > rows
        and width % 16 == 0
        and width % 128 <= 125
        and width % 128 > 0
        and gate_weight.shape[1] % 128 == 0
    )


def shards(
    queries,
    keys,
    values,
    page_map,
    selected,
    residual_in,
    out_weight,
    norm_gain,
    gate_weight,
    up_weight,
    down_weight,
):
    ctx_index = lax.axis_index("ctx")
    C = lax.axis_size("ctx")
    H = lax.axis_size("head")
    if fits(C, H, queries, keys, selected, out_weight, gate_weight):
        return fused(
            C,
            H,
            queries,
            keys,
            values,
            page_map,
            selected,
            residual_in,
            out_weight,
            norm_gain,
            gate_weight,
            up_weight,
            down_weight,
        )
    row_max, row_total, mixture = owner_pass(
        queries, keys, values, page_map, selected, ctx_index, C
    )
    stats = jnp.concatenate([row_max, row_total], axis=1)
    stats = jnp.pad(stats, ((0, 0), (0, 128 - stats.shape[1])))
    mlp_out, own_stream = tail(
        C,
        H,
        mixture.astype(jnp.bfloat16),
        stats,
        residual_in,
        norm_gain,
        out_weight,
        gate_weight,
        up_weight,
        down_weight,
    )
    own_stream = jnp.concatenate([own_stream[j] for j in range(own_stream.shape[0])], axis=1)
    return (own_stream.astype(jnp.float32) + mlp_out).astype(jnp.bfloat16)


def solution(mesh):
    in_specs = (
        P(None, "head"),
        P("ctx", None, "head"),
        P("ctx", None, "head"),
        P(),
        P(),
        P("head", "ctx"),
        P("head", "ctx"),
        P("ctx"),
        P("head", "ctx"),
        P("head", "ctx"),
        P("ctx", "head"),
    )
    out_specs = P("ctx", "head")
    return jax.shard_map(shards, mesh=mesh, in_specs=in_specs, out_specs=out_specs, check_vma=False)
```

```python
import jax
import jax.numpy as jnp
import functools
from jax import lax
from jax.experimental import pallas as pl
from jax.experimental.pallas import tpu as pltpu
from jax.sharding import PartitionSpec as P

D = 5376
HEAD_SIZE = 128


score_scale = 168.0 ** (-0.5)
masked_score = -1e30
norm_epsilon = 1e-06


def attention_kernel(
    logical_ref, chosen_ref, page_total, q_ref, k_ref, v_ref, mix_ref, m_ref, l_ref, acc, top, total
):
    page = pl.program_id(1)
    tile_count = chosen_ref.shape[0]
    tile_rows = q_ref.shape[0] // tile_count
    group = q_ref.shape[1] // k_ref.shape[2]
    page_len = k_ref.shape[1]
    offset = page_len - q_ref.shape[0]
    f32 = jnp.float32

    @pl.when(page == 0)
    def _():
        acc[...] = jnp.zeros_like(acc)
        top[...] = jnp.full_like(top, masked_score)
        total[...] = jnp.zeros_like(total)

    causal = logical_ref[page] == page_total - 1

    def visit(t, masked):
        rows = slice(t * tile_rows, (t + 1) * tile_rows)
        for g in range(group):
            cols = slice(g * HEAD_SIZE, (g + 1) * HEAD_SIZE)
            scores = (
                lax.dot_general(
                    q_ref[rows, cols],
                    k_ref[0],
                    (((1,), (1,)), ((), ())),
                    preferred_element_type=f32,
                )
                * score_scale
            )
            if masked:
                position = offset + t * tile_rows + lax.broadcasted_iota(jnp.int32, scores.shape, 0)
                key = lax.broadcasted_iota(jnp.int32, scores.shape, 1)
                scores = jnp.where(key <= position, scores, masked_score)
            old = top[g, rows, :1]
            new = jnp.maximum(old, jnp.max(scores, axis=1, keepdims=True))
            weights = jnp.exp(scores - new)
            keep = jnp.exp(old - new)
            total[g, rows] = total[g, rows] * keep + jnp.sum(weights, axis=1, keepdims=True)
            top[g, rows] = jnp.broadcast_to(new, (tile_rows, 128))
            acc[rows, cols] = acc[rows, cols] * keep + jnp.dot(
                weights.astype(jnp.bfloat16), v_ref[0], preferred_element_type=f32
            )

    for t in range(tile_count):
        picked = chosen_ref[t, page] != 0
        pl.when(jnp.logical_and(picked, causal))(functools.partial(visit, t, True))
        pl.when(jnp.logical_and(picked, jnp.logical_not(causal)))(
            functools.partial(visit, t, False)
        )

    @pl.when(page == pl.num_programs(1) - 1)
    def _():
        mix_ref[...] = acc[...].astype(jnp.bfloat16)
        lane = lax.broadcasted_iota(jnp.int32, m_ref.shape[1:], 1)
        maxima = jnp.zeros(m_ref.shape[1:], f32)
        sums = jnp.zeros(m_ref.shape[1:], f32)
        for g in range(group):
            maxima = jnp.where(lane == g, top[g], maxima)
            sums = jnp.where(lane == g, total[g], sums)
        m_ref[0] = maxima
        l_ref[0] = sums


def owner_pass(queries, keys, values, page_map, selected, ctx_index, ctx_count):
    pages_local, page_len, kv_width = keys.shape
    row_count, query_width = queries.shape
    kv_local = kv_width // HEAD_SIZE
    group = query_width // kv_width
    tile_count = selected.shape[0]
    page_total = pages_local * ctx_count
    slot_ids = ctx_index * pages_local + jnp.arange(pages_local, dtype=jnp.int32)
    all_pages = jnp.arange(page_total, dtype=jnp.int32)
    logical = jnp.sum(
        jnp.where(page_map[None, :] == slot_ids[:, None], all_pages[None, :], 0), axis=1
    )
    chosen = jnp.any(selected[:, None, :] == logical[None, :, None], axis=2).astype(jnp.int32)
    stat = jax.ShapeDtypeStruct((kv_local, row_count, 128), jnp.float32)
    stat_spec = pl.BlockSpec((1, row_count, 128), lambda k, p, a, b: (k, 0, 0))
    kv_spec = pl.BlockSpec((1, page_len, HEAD_SIZE), lambda k, p, a, b: (p, 0, k))
    q_spec = pl.BlockSpec((row_count, group * HEAD_SIZE), lambda k, p, a, b: (0, k))

    def kernel(logical_ref, chosen_ref, *refs):
        attention_kernel(logical_ref, chosen_ref, page_total, *refs)

    mixture, top, total = pl.pallas_call(
        kernel,
        grid_spec=pltpu.PrefetchScalarGridSpec(
            num_scalar_prefetch=2,
            grid=(kv_local, pages_local),
            in_specs=[q_spec, kv_spec, kv_spec],
            out_specs=(q_spec, stat_spec, stat_spec),
            scratch_shapes=[
                pltpu.VMEM((row_count, group * HEAD_SIZE), jnp.float32),
                pltpu.VMEM((group, row_count, 128), jnp.float32),
                pltpu.VMEM((group, row_count, 128), jnp.float32),
            ],
        ),
        out_shape=(jax.ShapeDtypeStruct((row_count, query_width), jnp.bfloat16), stat, stat),
    )(logical.astype(jnp.int32), chosen, queries, keys, values)

    def heads(stacked):
        return stacked[:, :, :group].transpose(1, 0, 2).reshape(row_count, kv_local * group)

    return heads(top), heads(total), mixture


MESH = pl.DeviceIdType.MESH
CORES = 2


def column_tile(width):
    for tile in (896, 768, 640, 512, 384, 256, 128):
        if width % tile == 0:
            return tile
    return width


def flat(block, rows):
    if block.shape[1] % 16:
        return block.astype(jnp.float32).reshape(rows, -1).astype(jnp.bfloat16)
    return block.reshape(rows, -1)


def tail_kernel(
    C,
    H,
    mix_ref,
    stat_ref,
    res_ref,
    gain_ref,
    ow_hbm,
    gw_hbm,
    uw_hbm,
    dw_hbm,
    mlp_ref,
    own_ref,
    ow,
    gw,
    uw,
    dw,
    mix_in,
    stat_in,
    att,
    po,
    po_in,
    u_out,
    st_out,
    ss,
    ublk,
    own_st,
    first,
    first_in,
    second,
    second_in,
    hid,
    acc,
    part,
    part_in,
    w_sem,
    mix_s,
    mix_r,
    stat_s,
    stat_r,
    att_s,
    att_r,
    po_s,
    po_r,
    u_s,
    u_r,
    st_s,
    st_r,
    ss_s,
    ss_r,
    f_s,
    f_r,
    g_s,
    g_r,
    h_s,
    h_r,
    fw_s,
    part_s,
    part_r,
):
    c = lax.axis_index("ctx")
    h = lax.axis_index("head")
    Y = H // CORES
    y = h // CORES
    core = h % CORES
    partner = y * CORES + (CORES - 1 - core)
    R = mix_ref.shape[1]
    rows = C * R
    rb = C // H
    bph = C // H
    width = ow.shape[0]
    head_rows = rows // H
    heads = mix_ref.shape[2] // HEAD_SIZE
    tiles, _, _, _, _, tile = first.shape
    f32 = jnp.float32
    bf16 = jnp.bfloat16

    def remote(src, dst, send_sem, recv_sem, ctx, head):
        return pltpu.make_async_remote_copy(
            src_ref=src,
            dst_ref=dst,
            send_sem=send_sem,
            recv_sem=recv_sem,
            device_id=(ctx, head),
            device_id_type=MESH,
        )

    sent = []

    def send(*args):
        copy = remote(*args)
        copy.start()
        sent.append(copy)

    loads = [
        pltpu.make_async_copy(src, dst, w_sem.at[i])
        for i, (src, dst) in enumerate(
            ((ow_hbm, ow), (gw_hbm, gw), (uw_hbm, uw), (dw_hbm, dw))
        )
    ]
    for load in loads:
        load.start()

    for d in range(1, C):
        peer = (c + d) % C
        send(stat_ref.at[peer], stat_in.at[c], stat_s.at[d], stat_r.at[c], peer, h)
        send(mix_ref.at[peer], mix_in.at[c], mix_s.at[d], mix_r.at[c], peer, h)
    stat_in[c] = stat_ref[c]
    mix_in[c] = mix_ref[c]
    for d in range(1, C):
        peer = (c + C - d) % C
        remote(stat_in.at[peer], stat_in.at[peer], stat_s.at[d], stat_r.at[peer], peer, h).wait_recv()
        remote(mix_in.at[peer], mix_in.at[peer], mix_s.at[d], mix_r.at[peer], peer, h).wait_recv()
    maxima = [stat_in[k][:, :heads] for k in range(C)]
    top = functools.reduce(jnp.maximum, maxima)
    scales = [jnp.exp(m - top) for m in maxima]
    total = sum(stat_in[k][:, heads : 2 * heads] * scales[k] for k in range(C))
    inverse = 1.0 / total
    for g in range(heads):
        cols = slice(g * HEAD_SIZE, (g + 1) * HEAD_SIZE)
        mixed = sum(mix_in[k, :, cols].astype(f32) * scales[k][:, g : g + 1] for k in range(C))
        att[c, :, cols] = (mixed * inverse[:, g : g + 1]).astype(bf16)

    for d in range(1, C):
        peer = (c + d) % C
        send(att.at[c], att.at[c], att_s.at[d], att_r.at[c], peer, h)
    loads[0].wait()
    for d in range(1, C):
        peer = (c + C - d) % C
        remote(att.at[peer], att.at[peer], att_s.at[d], att_r.at[peer], peer, h).wait_recv()
    projected = lax.dot_general(
        flat(att[...], rows), ow[...], (((1,), (1,)), ((), ())), preferred_element_type=f32
    )
    po[...] = projected.reshape(H, head_rows, width).astype(bf16)

    for d in range(1, H):
        peer = (h + d) % H
        send(po.at[peer], po_in.at[h], po_s.at[d], po_r.at[h], c, peer)
    po_in[h] = po[h]
    for d in range(1, H):
        peer = (h + H - d) % H
        remote(po_in.at[peer], po_in.at[peer], po_s.at[d], po_r.at[peer], c, peer).wait_recv()
    projected = sum(po_in[k].astype(f32) for k in range(H))
    stream = (res_ref[...].astype(f32) + projected).astype(bf16).astype(f32)
    st_out[...] = stream.reshape(rb, R, width).astype(bf16)
    u_out[...] = (stream * gain_ref[...]).reshape(rb, R, width).astype(bf16)
    squares = jnp.sum(stream * stream, axis=1, keepdims=True)
    ss[c] = jnp.broadcast_to(squares, (head_rows, 128))

    block_head = c // bph
    block_part = c % bph
    u_dst = ublk.at[block_part, pl.ds(h * rb, rb)]
    kept = []
    for d in range(C):
        peer = (c + d) % C
        copy = remote(u_out, u_dst, u_s.at[d], u_r.at[block_part, h], peer, block_head)
        if d == 0:
            kept.append((block_head != h, copy))
            pl.when(block_head != h)(copy.start)

            @pl.when(block_head == h)
            def _():
                ublk[block_part, pl.ds(h * rb, rb)] = u_out[...]

        else:
            copy.start()
            sent.append(copy)
    for d in range(1, C):
        peer = (c + d) % C
        send(ss.at[c], ss.at[c], ss_s.at[d], ss_r.at[c], peer, h)
    for i in range(rb):
        owner = h * rb + i
        other = jnp.logical_or(owner != c, block_head != h)
        copy = remote(
            st_out.at[i], own_st.at[block_part], st_s.at[i], st_r.at[block_part], owner, block_head
        )
        kept.append((other, copy))
        pl.when(other)(copy.start)

        @pl.when(jnp.logical_not(other))
        def _(i=i):
            own_st[block_part] = st_out[i]

    for j in range(bph):
        for k in range(H):
            source = h * bph + j
            block = ublk.at[j, pl.ds(k * rb, rb)]
            arrival = remote(block, block, u_s.at[0], u_r.at[j, k], source, k)
            pl.when(jnp.logical_or(source != c, h != k))(arrival.wait_recv)
    loads[1].wait()
    loads[2].wait()

    def matmul(i, which, weight):
        cols = slice(i * tile, (i + 1) * tile)
        value = None
        for j in range(bph):
            term = jnp.dot(
                flat(ublk[j], rows),
                weight[j * width : (j + 1) * width, cols],
                preferred_element_type=f32,
            )
            value = term if value is None else value + term
        first[i, which] = value.reshape(Y, CORES, head_rows, tile).swapaxes(0, 1).astype(bf16)
        send(
            first.at[i, which, CORES - 1 - core],
            first_in.at[i, which],
            f_s.at[i, which],
            f_r.at[i, which],
            c,
            partner,
        )

    def middle(i, which):
        remote(
            first_in.at[i, which], first_in.at[i, which], f_s.at[i, which], f_r.at[i, which], c, partner
        ).wait_recv()
        both = first[i, which, core].astype(f32) + first_in[i, which].astype(f32)
        second[i, which] = both.astype(bf16)
        for d in range(1, Y):
            peer = (y + d) % Y
            send(
                second.at[i, which, peer],
                second_in.at[i, which, y],
                g_s.at[i, which, d],
                g_r.at[i, which, y],
                c,
                peer * CORES + core,
            )

    def finish(i, inverse_rms):
        sums = []
        for which in range(2):
            value = second[i, which, y].astype(f32)
            for d in range(1, Y):
                peer = (y + Y - d) % Y
                slot = second_in.at[i, which, peer]
                remote(
                    slot, slot, g_s.at[i, which, d], g_r.at[i, which, peer], c, peer * CORES + core
                ).wait_recv()
                value = value + second_in[i, which, peer].astype(f32)
            sums.append(value * inverse_rms)
        hid[i, h] = (jax.nn.gelu(sums[0], approximate=True) * sums[1]).astype(bf16)
        send(hid.at[i, h], hid.at[i, h], h_s.at[i, 0], h_r.at[i, h], c, partner)
        for d in range(1, Y):
            peer = ((y + d) % Y) * CORES + core
            send(hid.at[i, h], hid.at[i, h], h_s.at[i, d], h_r.at[i, h], c, peer)

    def forward(i):
        for d in range(1, Y):
            origin = ((y + Y - d) % Y) * CORES + core
            slot = hid.at[i, origin]
            remote(slot, slot, h_s.at[i, d], h_r.at[i, origin], c, origin).wait_recv()
            send(slot, slot, fw_s.at[i, d], h_r.at[i, origin], c, partner)

    def down(i):
        for d in range(Y):
            origin = ((y + Y - d) % Y) * CORES + (CORES - 1 - core)
            slot = hid.at[i, origin]
            remote(slot, slot, h_s.at[i, 0], h_r.at[i, origin], c, partner).wait_recv()
        term = lax.dot_general(
            flat(hid[i], rows),
            dw[:, i * tile : (i + 1) * tile],
            (((1,), (1,)), ((), ())),
            preferred_element_type=f32,
        )
        if i == 0:
            acc[...] = term
        else:
            acc[...] += term

    steps = [(i, which) for i in range(tiles) for which in range(2)]
    for n, (i, which) in enumerate(steps):
        matmul(i, which, (gw, uw)[which])
        if n:
            middle(*steps[n - 1])
    middle(*steps[-1])
    for d in range(1, C):
        peer = (c + C - d) % C
        remote(ss.at[peer], ss.at[peer], ss_s.at[d], ss_r.at[peer], peer, h).wait_recv()
    squares = sum(ss[k] for k in range(C))
    inverse_rms = lax.rsqrt(squares[:, :1] / (C * width) + norm_epsilon)
    loads[3].wait()
    for i in range(tiles):
        finish(i, inverse_rms)
        if i:
            forward(i - 1)
    forward(tiles - 1)
    for i in range(tiles):
        down(i)
    part[...] = acc[...].reshape(C, R, acc.shape[1]).astype(bf16)

    for d in range(1, C):
        peer = (c + d) % C
        send(part.at[peer], part_in.at[c], part_s.at[d], part_r.at[c], peer, h)
    part_in[c] = part[c]
    for j in range(bph):
        source = h * bph + j
        arrival = remote(own_st.at[j], own_st.at[j], st_s.at[0], st_r.at[j], source, c // rb)
        pl.when(jnp.logical_or(source != c, c // rb != h))(arrival.wait_recv)
    own_ref[...] = own_st[...]
    for d in range(1, C):
        peer = (c + C - d) % C
        remote(part_in.at[peer], part_in.at[peer], part_s.at[d], part_r.at[peer], peer, h).wait_recv()
    mlp_ref[...] = sum(part_in[k].astype(f32) for k in range(C))
    for copy in sent:
        copy.wait_send()
    for condition, copy in kept:
        pl.when(condition)(copy.wait_send)


def tail(C, H, mixture, stats, residual_in, norm_gain, out_weight, gate_weight, up_weight, down_weight):
    rows, query_width = mixture.shape
    R = rows // C
    width = out_weight.shape[1]
    hidden = gate_weight.shape[1]
    out_width = down_weight.shape[1]
    out_weight = out_weight.T
    down_weight = down_weight.T
    rb = C // H
    bph = C // H
    Y = H // CORES
    head_rows = rows // H
    tile = column_tile(hidden)
    tiles = hidden // tile
    bf16 = jnp.bfloat16
    vmem = pl.BlockSpec(memory_space=pltpu.VMEM)
    hbm = pl.BlockSpec(memory_space=pl.ANY)
    V = pltpu.VMEM
    S = pltpu.SemaphoreType.DMA
    return pl.pallas_call(
        functools.partial(tail_kernel, C, H),
        out_shape=(
            jax.ShapeDtypeStruct((R, out_width), jnp.float32),
            jax.ShapeDtypeStruct((bph, R, width), bf16),
        ),
        in_specs=[vmem] * 4 + [hbm] * 4,
        out_specs=(vmem, vmem),
        scratch_shapes=[
            V(out_weight.shape, bf16),
            V(gate_weight.shape, bf16),
            V(up_weight.shape, bf16),
            V(down_weight.shape, bf16),
            V((C, R, query_width), bf16),
            V((C, R, 128), jnp.float32),
            V((C, R, query_width), bf16),
            V((H, head_rows, width), bf16),
            V((H, head_rows, width), bf16),
            V((rb, R, width), bf16),
            V((rb, R, width), bf16),
            V((C, head_rows, 128), jnp.float32),
            V((bph, C, R, width), bf16),
            V((bph, R, width), bf16),
            V((tiles, 2, CORES, Y, head_rows, tile), bf16),
            V((tiles, 2, Y, head_rows, tile), bf16),
            V((tiles, 2, Y, head_rows, tile), bf16),
            V((tiles, 2, Y, head_rows, tile), bf16),
            V((tiles, H, head_rows, tile), bf16),
            V((rows, out_width), jnp.float32),
            V((C, R, out_width), bf16),
            V((C, R, out_width), bf16),
            S((4,)),
            S((C,)),
            S((C,)),
            S((C,)),
            S((C,)),
            S((C,)),
            S((C,)),
            S((H,)),
            S((H,)),
            S((C,)),
            S((bph, H)),
            S((rb,)),
            S((bph,)),
            S((C,)),
            S((C,)),
            S((tiles, 2)),
            S((tiles, 2)),
            S((tiles, 2, Y)),
            S((tiles, 2, Y)),
            S((tiles, Y)),
            S((tiles, H)),
            S((tiles, Y)),
            S((C,)),
            S((C,)),
        ],
        compiler_params=pltpu.CompilerParams(
            has_side_effects=True, vmem_limit_bytes=60 * 2**20
        ),
    )(
        mixture.reshape(C, R, query_width),
        stats.reshape(C, R, 128),
        residual_in,
        norm_gain.reshape(1, width),
        out_weight,
        gate_weight,
        up_weight,
        down_weight,
    )


LOG2E = 1.4426950408889634


def fused_kernel(
    C,
    H,
    NP,
    map_hbm,
    sel_hbm,
    q_hbm,
    res_hbm,
    gain_hbm,
    k_hbm,
    v_hbm,
    ow_hbm,
    gw_hbm,
    uw_hbm,
    dw_hbm,
    out_ref,
    map_ref,
    sel_ref,
    q_ref,
    res_ref,
    gain_ref,
    k_buf,
    v_buf,
    ow,
    gw,
    uw,
    dw,
    mix_out,
    mix_in,
    lse_out,
    lse_in,
    att,
    po_out,
    po_in,
    res_in,
    st,
    u,
    ss_out,
    ss_in,
    ss_mid,
    ss_last,
    scale,
    begun,
    first,
    first_in,
    second,
    second_in,
    hid,
    acc,
    part,
    part_in,
    in_sem,
    kv_sem,
    w_sem,
    mix_s,
    mix_r,
    lse_s,
    lse_r,
    att_s,
    att_r,
    po_s,
    po_r,
    res_s,
    res_r,
    u_s,
    u_r,
    ss_s,
    ss_r,
    f_s,
    f_r,
    g_s,
    g_r,
    h_s,
    h_r,
    part_s,
    part_r,
):
    c = lax.axis_index("ctx")
    h = lax.axis_index("head")
    X = C // H
    Z = C // X
    z = c // X
    x = c % X
    Y = H // CORES
    y = h // CORES
    core = h % CORES
    partner = y * CORES + (CORES - 1 - core)
    _, NQ, RC, query_width = q_ref.shape
    rows = C * RC
    hr = rows // H
    kv, pages, page_len, _ = k_buf.shape
    group = query_width // (kv * HEAD_SIZE)
    gw_cols = group * HEAD_SIZE
    tile_count = sel_ref.shape[0]
    tile_rows = NQ * rows // tile_count
    offset = page_len - NQ * rows
    page_total = map_ref.shape[0]
    width = ow.shape[0]
    tile = first.shape[-1]
    tiles = first.shape[1]
    RP = rows // NP
    f32 = jnp.float32
    bf16 = jnp.bfloat16
    owner = h == z
    visitor = h != z

    def remote(src, dst, send_sem, recv_sem, ctx, head):
        return pltpu.make_async_remote_copy(
            src_ref=src,
            dst_ref=dst,
            send_sem=send_sem,
            recv_sem=recv_sem,
            device_id=(ctx, head),
            device_id_type=MESH,
        )

    sent = []
    kept = []

    def start(*args):
        remote(*args).start()

    def send(*args):
        copy = remote(*args)
        copy.start()
        sent.append(copy)

    def send_if(condition, *args):
        copy = remote(*args)
        pl.when(condition)(copy.start)
        kept.append((condition, copy))

    def kv_load(j):
        lanes = pl.ds(pl.multiple_of(j * HEAD_SIZE, HEAD_SIZE), HEAD_SIZE)
        return (
            pltpu.make_async_copy(k_hbm.at[:, :, lanes], k_buf.at[j], kv_sem.at[0, j]),
            pltpu.make_async_copy(v_hbm.at[:, :, lanes], v_buf.at[j], kv_sem.at[1, j]),
        )

    barrier = pltpu.get_barrier_semaphore()
    for d in range(1, C):
        pl.semaphore_signal(
            barrier, inc=1, device_id=((c + d) % C, h), device_id_type=MESH
        )
    for d in range(1, H):
        pl.semaphore_signal(
            barrier, inc=1, device_id=(c, (h + d) % H), device_id_type=MESH
        )
    inputs = [
        pltpu.make_async_copy(src, dst, in_sem.at[i])
        for i, (src, dst) in enumerate(
            (
                (map_hbm, map_ref),
                (sel_hbm, sel_ref),
                (q_hbm, q_ref),
                (res_hbm, res_ref),
                (gain_hbm, gain_ref.at[0]),
            )
        )
    ]
    for load in inputs:
        load.start()
    for j in range(kv):
        for load in kv_load(j):
            load.start()
    loads = [
        pltpu.make_async_copy(src, dst, w_sem.at[i])
        for i, (src, dst) in enumerate(
            ((ow_hbm, ow), (gw_hbm, gw), (uw_hbm, uw), (dw_hbm, dw))
        )
    ]
    for load in inputs[:3]:
        load.wait()

    facts = []
    for p in range(pages):
        slot = c * pages + p
        logical = jnp.int32(0)
        for j in range(page_total):
            logical = logical + jnp.where(map_ref[j] == slot, j, 0)
        picks = []
        for t in range(tile_count):
            hits = jnp.int32(0)
            for i in range(sel_ref.shape[1]):
                hits = hits + jnp.where(sel_ref[t, i] == logical, 1, 0)
            picks.append(jnp.where(hits > 0, 0.0, masked_score).astype(f32))
        reach = jnp.where(logical == page_total - 1, 0, page_len)
        facts.append((reach, picks))

    index = lax.broadcasted_iota(jnp.int32, (group * rows, 1), 0) & (rows - 1)
    shift = RC.bit_length() - 1
    base_row = (index >> shift) * (NQ * RC) + (index & (RC - 1))
    eye = lax.broadcasted_iota(jnp.int32, (rows, rows), 0) == lax.broadcasted_iota(
        jnp.int32, (rows, rows), 1
    )
    unit = score_scale * LOG2E

    def attend(n):
        q = n // kv
        j = n % kv

        @pl.when(n < kv)
        def _():
            for load in kv_load(j):
                load.wait()

        @pl.when(n == 0)
        def _():
            for load in loads:
                load.start()

        lanes = pl.ds(pl.multiple_of(j * gw_cols, gw_cols), gw_cols)
        block = q_ref[:, q, :, lanes].reshape(rows, gw_cols)
        lhs = jnp.concatenate(
            [block[:, g * HEAD_SIZE : (g + 1) * HEAD_SIZE] for g in range(group)], axis=0
        )
        row = base_row + q * RC
        key = offset + lax.broadcasted_iota(jnp.int32, (group * rows, page_len - offset), 1)
        tops, sums, outs = [], [], []
        for p in range(pages):
            reach, picks = facts[p]
            bias = jnp.zeros((group * rows, 1), f32)
            for t in range(tile_count):
                inside = jnp.logical_and(row >= t * tile_rows, row < (t + 1) * tile_rows)
                bias = jnp.where(inside, picks[t], bias)
            scores = lax.dot_general(
                lhs, k_buf[j, p], (((1,), (1,)), ((), ())), preferred_element_type=f32
            )
            late = jnp.where(key <= offset + row + reach, scores[:, offset:], masked_score)
            scores = jnp.concatenate([scores[:, :offset], late], axis=1)
            top = jnp.max(scores, axis=1, keepdims=True)
            weights = jnp.exp2((scores - top) * unit)
            sums.append(jnp.sum(weights, axis=1, keepdims=True))
            outs.append(
                jnp.dot(weights.astype(bf16), v_buf[j, p], preferred_element_type=f32)
            )
            tops.append(top * unit + bias)
        best = functools.reduce(jnp.maximum, tops)
        scales = [jnp.exp2(top - best) for top in tops]
        total = sum(s * e for s, e in zip(sums, scales))
        mixed = sum(o * (e / total) for o, e in zip(outs, scales))
        lse = best + jnp.log2(total)
        for g in range(group):
            part_rows = slice(g * rows, (g + 1) * rows)
            mix_out[n, :, :, g * HEAD_SIZE : (g + 1) * HEAD_SIZE] = (
                mixed[part_rows].reshape(C, RC, HEAD_SIZE).astype(bf16)
            )
            lse_out[n, g : g + 1] = jnp.sum(
                jnp.where(eye, lse[part_rows], 0.0), axis=0, keepdims=True
            )
        mix_in[n, c] = mix_out[n, c]
        lse_in[n, c] = lse_out[n]

    def mix_sends(n):
        for d in range(1, C):
            peer = (c + d) % C
            remote(mix_out.at[n, peer], mix_in.at[n, c], mix_s.at[0], mix_r.at[n], peer, h).start()
            remote(lse_out.at[n], lse_in.at[n, c], lse_s.at[0], lse_r.at[n], peer, h).start()

    def att_sends(n):
        for d in range(1, C):
            peer = (c + d) % C
            remote(att.at[n, c], att.at[n, c], att_s.at[0], att_r.at[n], peer, h).start()

    def arrived(block, recv_sem):
        remote(block, block, recv_sem, recv_sem, c, partner).wait_recv()

    def left(block, send_sem):
        remote(block, block, send_sem, send_sem, c, partner).wait_send()

    def combine(n):
        arrived(lse_in.at[n, pl.ds(0, C - 1)], lse_r.at[n])
        arrived(mix_in.at[n, pl.ds(0, C - 1)], mix_r.at[n])
        logs = [lse_in[n, k] for k in range(C)]
        best = functools.reduce(jnp.maximum, logs)
        scales = [jnp.exp2(value - best) for value in logs]
        inverse = 1.0 / sum(scales)
        lane = lax.broadcasted_iota(jnp.int32, (RC, rows), 1)
        mine = lane == c * RC + lax.broadcasted_iota(jnp.int32, (RC, rows), 0)
        for g in range(group):
            cols = slice(g * HEAD_SIZE, (g + 1) * HEAD_SIZE)
            value = jnp.zeros((RC, HEAD_SIZE), f32)
            for k in range(C):
                share = (scales[k] * inverse)[g : g + 1]
                share = jnp.sum(jnp.where(mine, share, 0.0), axis=1, keepdims=True)
                value = value + share * mix_in[n, k, :, cols].astype(f32)
            att[n, c, :, cols] = value.astype(bf16)
        att_sends(n)

    def project(q):
        for j in range(kv):
            n = q * kv + j
            arrived(att.at[n, pl.ds(0, C - 1)], att_r.at[n])
        if q == 0:
            loads[0].wait()
        value = None
        for j in range(kv):
            term = lax.dot_general(
                att[q * kv + j].reshape(rows, gw_cols),
                ow[:, j * gw_cols : (j + 1) * gw_cols],
                (((1,), (1,)), ((), ())),
                preferred_element_type=f32,
            )
            value = term if value is None else value + term
        po_out[q] = value.astype(bf16)
        for i in range(NP):
            piece = pl.ds(i * RP, RP)
            copy = remote(
                po_out.at[q, piece], po_in.at[q, h, piece], po_s.at[q], po_r.at[q, i], c, z
            )
            pl.when(visitor)(copy.start)
        po_in[q, h] = po_out[q]

    def own(q, i):
        if q == 0 and i == 0:
            arrived(res_in.at[pl.ds(0, H - 1)], res_r.at[0])
        arrived(po_in.at[q, pl.ds(0, H - 1), pl.ds(i * RP, RP)], po_r.at[q, i])
        spare = u.shape[-1] - width
        lane = lax.broadcasted_iota(jnp.int32, (hr, spare), 1)
        for b in range(i * RP // hr, (i + 1) * RP // hr):
            span = slice(b * hr, (b + 1) * hr)
            value = res_in[b, :, q].reshape(hr, width).astype(f32)
            added = sum(po_in[q, k, span].astype(f32) for k in range(H))
            stream = (value + added).astype(bf16)
            st[q, span] = stream
            stream = stream.astype(f32)
            u[q, x, span, :width] = (stream * gain_ref[...]).astype(bf16)
            squares = jnp.sum(stream * stream, axis=1, keepdims=True)
            high = squares.astype(bf16).astype(f32)
            mid = (squares - high).astype(bf16).astype(f32)
            low = squares - high - mid
            packed = jnp.where(lane == 0, high, jnp.where(lane == 1, mid, low))
            packed = jnp.where(lane < 3, packed, 0.0)
            u[q, x, span, width:] = packed.astype(bf16)

    def relay(q, i, here):
        piece = u.at[q, x, pl.ds(i * RP, RP)]
        recv = u_r.at[q, x, i]
        pl.when(jnp.logical_and(here, visitor))(functools.partial(arrived, piece, recv))
        up = jnp.logical_and(here, jnp.logical_and(z >= h, z < Z - 1))
        down = jnp.logical_and(here, jnp.logical_and(z <= h, z > 0))
        above = jnp.minimum(z + 1, Z - 1) * X + x
        below = jnp.maximum(z - 1, 0) * X + x
        send_if(up, piece, piece, u_s.at[q, i, 0], recv, above, h)
        send_if(down, piece, piece, u_s.at[q, i, 1], recv, below, h)
        for d in range(1, X):
            peer = z * X + (x + d) % X
            send_if(here, piece, piece, u_s.at[q, i, 1 + d], recv, peer, h)

    def spread(q, here):
        for i in range(NP):
            pl.when(jnp.logical_and(here, owner))(functools.partial(own, q, i))
            relay(q, i, here)

    def gather(q):
        for d in range(1, X):
            source = (x + d) % X
            for i in range(NP):
                block = u.at[q, source, pl.ds(i * RP, RP)]
                arrived(block, u_r.at[q, source, i])
        squares = 0.0
        for k in range(X):
            split = u[q, k, :, width:].astype(f32)
            squares = squares + jnp.sum(split, axis=1, keepdims=True)
        squares = jnp.broadcast_to(squares, (rows, 128)).reshape(Y, CORES, hr, 128)
        ss_out[q] = squares.swapaxes(0, 1)
        send(ss_out.at[q, CORES - 1 - core], ss_in.at[q], ss_s.at[q, 0], ss_r.at[q, 0], c, partner)

    def block_dot(q, k, i, which):
        weight = (gw, uw)[which]
        span = pl.ds(pl.multiple_of(k * width, 16), width)
        return jnp.dot(
            u[q, k, :, :width],
            weight[span, i * tile : (i + 1) * tile],
            preferred_element_type=f32,
        )

    def start_expand(q):
        if q == 0:
            loads[1].wait()
            loads[2].wait()
        for i in range(tiles):
            for which in range(2):
                begun[i, which] = block_dot(q, x, i, which)

    def matmul(q, i, which):
        value = begun[i, which]
        for d in range(1, X):
            value = value + block_dot(q, (x + d) % X, i, which)
        value = value.reshape(Y, CORES, hr, tile).swapaxes(0, 1).astype(bf16)
        first[q, i, which] = value
        start(
            first.at[q, i, which, CORES - 1 - core],
            first_in.at[q, i, which],
            f_s.at[0],
            f_r.at[q, i, which],
            c,
            partner,
        )

    def middle(q, i, which):
        block = first_in.at[q, i, which]
        arrived(block, f_r.at[q, i, which])
        both = first[q, i, which, core].astype(f32) + first_in[q, i, which].astype(f32)
        second[q, i, which] = both.astype(bf16)
        for d in range(1, Y):
            peer = (y + d) % Y
            start(
                second.at[q, i, which, peer],
                second_in.at[q, i, which, y],
                g_s.at[0],
                g_r.at[q, i, which, y],
                c,
                peer * CORES + core,
            )

    def middle_squares(q):
        block = ss_in.at[q]
        remote(block, block, ss_s.at[q, 0], ss_r.at[q, 0], c, partner).wait_recv()
        ss_mid[q] = ss_out[q, core] + ss_in[q]
        for d in range(1, Y):
            peer = (y + d) % Y
            send(
                ss_mid.at[q, peer],
                ss_last.at[q, y],
                ss_s.at[q, d],
                ss_r.at[q, 1 + y],
                c,
                peer * CORES + core,
            )

    def inverse_rms(q):
        total = ss_mid[q, y]
        for d in range(1, Y):
            peer = (y + Y - d) % Y
            block = ss_last.at[q, peer]
            remote(
                block, block, ss_s.at[q, d], ss_r.at[q, 1 + peer], c, peer * CORES + core
            ).wait_recv()
            total = total + ss_last[q, peer]
        scale[q] = lax.rsqrt(total / (C * width) + norm_epsilon)

    def finish(q, i):
        inverse = scale[q][:, :1]
        sums = []
        for which in range(2):
            value = second[q, i, which, y].astype(f32)
            for d in range(1, Y):
                peer = (y + Y - d) % Y
                block = second_in.at[q, i, which, peer]
                remote(
                    block,
                    block,
                    g_s.at[0],
                    g_r.at[q, i, which, peer],
                    c,
                    peer * CORES + core,
                ).wait_recv()
                value = value + second_in[q, i, which, peer].astype(f32)
            sums.append(value * inverse)
        hid[q, i, h] = (jax.nn.gelu(sums[0], approximate=True) * sums[1]).astype(bf16)
        block = hid.at[q, i, h]
        for d in range(1, Y):
            peer = ((y + d) % Y) * CORES + core
            start(block, block, h_s.at[0], h_r.at[q, i, h], c, peer)
        start(block, block, h_s.at[0], h_r.at[q, i, h], c, partner)

    def forward(q, i):
        for d in range(1, Y):
            origin = ((y + Y - d) % Y) * CORES + core
            block = hid.at[q, i, origin]
            arrived(block, h_r.at[q, i, origin])
            start(block, block, h_s.at[0], h_r.at[q, i, origin], c, partner)

    def down(q, i):
        for d in range(Y):
            origin = ((y + Y - d) % Y) * CORES + (CORES - 1 - core)
            block = hid.at[q, i, origin]
            arrived(block, h_r.at[q, i, origin])
        if q == 0 and i == 0:
            loads[3].wait()
        term = lax.dot_general(
            hid[q, i].reshape(rows, tile),
            dw[:, i * tile : (i + 1) * tile],
            (((1,), (1,)), ((), ())),
            preferred_element_type=f32,
        )
        if i == 0:
            acc[...] = term
        else:
            acc[...] += term

    def scatter(q):
        for k in range(X):

            @pl.when(jnp.logical_and(owner, x == k))
            def _(k=k):
                acc[:, k * width : (k + 1) * width] += st[q].astype(f32)

        part[q] = acc[...].reshape(C, RC, acc.shape[1]).astype(bf16)
        for d in range(1, C):
            peer = (c + d) % C
            start(part.at[q, peer], part_in.at[q, c], part_s.at[0], part_r.at[q], peer, h)
        part_in[q, c] = part[q, c]

    def collect(q):
        arrived(part_in.at[q, pl.ds(0, C - 1)], part_r.at[q])
        out_ref[q] = sum(part_in[q, k].astype(f32) for k in range(C)).astype(bf16)

    pl.semaphore_wait(barrier, C + H - 2)
    steps = NQ * kv
    lag = 3

    def loop(n, carry):
        attend(n)
        pl.when(jnp.logical_or(n < kv, n >= kv + lag))(functools.partial(mix_sends, n))

        @pl.when(jnp.logical_and(n >= lag, n < kv + lag))
        def _():
            combine(n - lag)

        @pl.when(n == kv + lag - 1)
        def _():
            for k in range(kv, kv + lag):
                mix_sends(k)

        return carry

    lax.fori_loop(0, steps, loop, 0)
    for load in inputs[3:]:
        load.wait()
    send_if(visitor, res_ref, res_in.at[h], res_s.at[0], res_r.at[0], c, z)
    res_in[h] = res_ref[...]
    pairs = [(i, which) for i in range(tiles) for which in range(2)]

    def expand(q, extra=None):
        start_expand(q)
        gather(q)
        for n, (i, which) in enumerate(pairs):
            matmul(q, i, which)
            if n == 1:
                middle_squares(q)
            if n:
                middle(q, *pairs[n - 1])
            if extra is not None and which:
                extra(i)
        middle(q, *pairs[-1])

    def finish_if(here, q, i):
        @pl.when(here)
        def _():
            if i == 0:
                inverse_rms(q)
            finish(q, i)

    def contract(q, done=0):
        forward(q, done)
        for i in range(done, tiles):
            if i + 1 < tiles:
                forward(q, i + 1)
            down(q, i)
        scatter(q)

    def between(i):
        finish_if(early, 0, i)
        if i:

            @pl.when(late)
            def _():
                forward(0, i - 1)
                down(0, i - 1)


    always = z >= 0
    far = jnp.maximum(z - h, h - z)
    early = z // CORES == y
    late = z // CORES != y
    project(0)
    for n in range(kv, steps - 2):
        combine(n)
    spread(0, far == 0)
    for n in range(steps - 2, steps):
        combine(n)
    spread(0, far == 1)
    project(1)
    spread(0, far > 1)
    expand(0)
    for i in range(tiles):
        finish_if(late, 0, i)
    spread(1, always)
    expand(1, between)
    pl.when(late)(lambda: contract(0, tiles - 1))
    pl.when(early)(lambda: contract(0))
    for i in range(tiles):
        finish_if(always, 1, i)
    contract(1)
    for q in range(NQ):
        collect(q)

    left(mix_out.at[:, pl.ds(0, C - 1)], mix_s.at[0])
    left(lse_in.at[:, pl.ds(0, C - 1)], lse_s.at[0])
    left(att.at[:, pl.ds(0, C - 1)], att_s.at[0])
    left(first_in, f_s.at[0])
    left(second.at[:, :, :, pl.ds(0, Y - 1)], g_s.at[0])
    left(hid.at[:, :, pl.ds(0, 2 * Y - 1)], h_s.at[0])
    left(part.at[:, pl.ds(0, C - 1)], part_s.at[0])
    for q in range(NQ):
        pl.when(visitor)(functools.partial(left, po_out.at[q], po_s.at[q]))
    for copy in sent:
        copy.wait_send()
    for condition, copy in kept:
        pl.when(condition)(copy.wait_send)


def fused(
    C,
    H,
    queries,
    keys,
    values,
    page_map,
    selected,
    residual_in,
    out_weight,
    norm_gain,
    gate_weight,
    up_weight,
    down_weight,
):
    row_count, query_width = queries.shape
    pages, page_len, kv_width = keys.shape
    kv = kv_width // HEAD_SIZE
    group = query_width // kv_width
    NQ = row_count // 128
    RC = row_count // C // NQ
    rows = C * RC
    NP = 4
    X = C // H
    Y = H // CORES
    hr = rows // H
    width = out_weight.shape[1]
    hidden = gate_weight.shape[1]
    out_width = down_weight.shape[1]
    tile = column_tile(hidden)
    tiles = hidden // tile
    steps = NQ * kv
    u_width = (width + 127) // 128 * 128
    bf16 = jnp.bfloat16
    f32 = jnp.float32
    vmem = pl.BlockSpec(memory_space=pltpu.VMEM)
    hbm = pl.BlockSpec(memory_space=pl.ANY)
    V = pltpu.VMEM
    S = pltpu.SemaphoreType.DMA
    out_weight = out_weight.T
    down_weight = down_weight.T
    mixes = V((steps, C, RC, group * HEAD_SIZE), bf16)
    return pl.pallas_call(
        functools.partial(fused_kernel, C, H, NP),
        out_shape=jax.ShapeDtypeStruct((NQ, RC, out_width), bf16),
        in_specs=[hbm] * 11,
        out_specs=vmem,
        scratch_shapes=[
            pltpu.SMEM(page_map.shape, jnp.int32),
            pltpu.SMEM(selected.shape, jnp.int32),
            V((C, NQ, RC, query_width), bf16),
            V((X, NQ, RC, width), bf16),
            V((1, width), f32),
            V((kv, pages, page_len, HEAD_SIZE), bf16),
            V((kv, pages, page_len, HEAD_SIZE), bf16),
            V(out_weight.shape, bf16),
            V(gate_weight.shape, bf16),
            V(up_weight.shape, bf16),
            V(down_weight.shape, bf16),
            mixes,
            mixes,
            V((steps, group, rows), f32),
            V((steps, C, group, rows), f32),
            mixes,
            V((NQ, rows, width), bf16),
            V((NQ, H, rows, width), bf16),
            V((H, X, NQ, RC, width), bf16),
            V((NQ, rows, width), bf16),
            V((NQ, X, rows, u_width), bf16),
            V((NQ, CORES, Y, hr, 128), f32),
            V((NQ, Y, hr, 128), f32),
            V((NQ, Y, hr, 128), f32),
            V((NQ, Y, hr, 128), f32),
            V((NQ, hr, 128), f32),
            V((tiles, 2, rows, tile), f32),
            V((NQ, tiles, 2, CORES, Y, hr, tile), bf16),
            V((NQ, tiles, 2, Y, hr, tile), bf16),
            V((NQ, tiles, 2, Y, hr, tile), bf16),
            V((NQ, tiles, 2, Y, hr, tile), bf16),
            V((NQ, tiles, H, hr, tile), bf16),
            V((rows, out_width), f32),
            V((NQ, C, RC, out_width), bf16),
            V((NQ, C, RC, out_width), bf16),
            S((5,)),
            S((2, kv)),
            S((4,)),
            S((1,)),
            S((steps,)),
            S((1,)),
            S((steps,)),
            S((1,)),
            S((steps,)),
            S((NQ,)),
            S((NQ, NP)),
            S((1,)),
            S((1,)),
            S((NQ, NP, 1 + X)),
            S((NQ, X, NP)),
            S((NQ, Y)),
            S((NQ, 1 + Y)),
            S((1,)),
            S((NQ, tiles, 2)),
            S((1,)),
            S((NQ, tiles, 2, Y)),
            S((1,)),
            S((NQ, tiles, H)),
            S((1,)),
            S((NQ,)),
        ],
        compiler_params=pltpu.CompilerParams(
            collective_id=0, has_side_effects=True, vmem_limit_bytes=63 * 2**20
        ),
    )(
        page_map,
        selected,
        queries.reshape(C, NQ, RC, query_width),
        residual_in.reshape(X, NQ, RC, width),
        norm_gain,
        keys,
        values,
        out_weight,
        gate_weight,
        up_weight,
        down_weight,
    ).reshape(row_count // C, out_width)


def fits(C, H, queries, keys, selected, out_weight, gate_weight):
    rows = queries.shape[0]
    width = out_weight.shape[1]
    if rows % 128:
        return False
    chunks = rows // 128
    return (
        chunks == 2
        and C % H == 0
        and (C // H) * H == C
        and rows % (C * chunks) == 0
        and rows // (C * chunks) % 16 == 0
        and rows % selected.shape[0] == 0
        and keys.shape[2] // HEAD_SIZE > 3
        and (keys.shape[1] - rows) % 128 == 0
        and keys.shape[1] > rows
        and width % 16 == 0
        and width % 128 <= 125
        and width % 128 > 0
        and gate_weight.shape[1] % 128 == 0
    )


def shards(
    queries,
    keys,
    values,
    page_map,
    selected,
    residual_in,
    out_weight,
    norm_gain,
    gate_weight,
    up_weight,
    down_weight,
):
    ctx_index = lax.axis_index("ctx")
    C = lax.axis_size("ctx")
    H = lax.axis_size("head")
    if fits(C, H, queries, keys, selected, out_weight, gate_weight):
        return fused(
            C,
            H,
            queries,
            keys,
            values,
            page_map,
            selected,
            residual_in,
            out_weight,
            norm_gain,
            gate_weight,
            up_weight,
            down_weight,
        )
    row_max, row_total, mixture = owner_pass(
        queries, keys, values, page_map, selected, ctx_index, C
    )
    stats = jnp.concatenate([row_max, row_total], axis=1)
    stats = jnp.pad(stats, ((0, 0), (0, 128 - stats.shape[1])))
    mlp_out, own_stream = tail(
        C,
        H,
        mixture.astype(jnp.bfloat16),
        stats,
        residual_in,
        norm_gain,
        out_weight,
        gate_weight,
        up_weight,
        down_weight,
    )
    own_stream = jnp.concatenate([own_stream[j] for j in range(own_stream.shape[0])], axis=1)
    return (own_stream.astype(jnp.float32) + mlp_out).astype(jnp.bfloat16)


def solution(mesh):
    in_specs = (
        P(None, "head"),
        P("ctx", None, "head"),
        P("ctx", None, "head"),
        P(),
        P(),
        P("head", "ctx"),
        P("head", "ctx"),
        P("ctx"),
        P("head", "ctx"),
        P("head", "ctx"),
        P("ctx", "head"),
    )
    out_specs = P("ctx", "head")
    return jax.shard_map(shards, mesh=mesh, in_specs=in_specs, out_specs=out_specs, check_vma=False)
```

```python
import jax
import jax.numpy as jnp
import functools
from jax import lax
from jax.experimental import pallas as pl
from jax.experimental.pallas import tpu as pltpu
from jax.sharding import PartitionSpec as P

D = 5376
HEAD_SIZE = 128


score_scale = 168.0 ** (-0.5)
masked_score = -1e30
norm_epsilon = 1e-06


def attention_kernel(
    logical_ref, chosen_ref, page_total, q_ref, k_ref, v_ref, mix_ref, m_ref, l_ref, acc, top, total
):
    page = pl.program_id(1)
    tile_count = chosen_ref.shape[0]
    tile_rows = q_ref.shape[0] // tile_count
    group = q_ref.shape[1] // k_ref.shape[2]
    page_len = k_ref.shape[1]
    offset = page_len - q_ref.shape[0]
    f32 = jnp.float32

    @pl.when(page == 0)
    def _():
        acc[...] = jnp.zeros_like(acc)
        top[...] = jnp.full_like(top, masked_score)
        total[...] = jnp.zeros_like(total)

    causal = logical_ref[page] == page_total - 1

    def visit(t, masked):
        rows = slice(t * tile_rows, (t + 1) * tile_rows)
        for g in range(group):
            cols = slice(g * HEAD_SIZE, (g + 1) * HEAD_SIZE)
            scores = (
                lax.dot_general(
                    q_ref[rows, cols],
                    k_ref[0],
                    (((1,), (1,)), ((), ())),
                    preferred_element_type=f32,
                )
                * score_scale
            )
            if masked:
                position = offset + t * tile_rows + lax.broadcasted_iota(jnp.int32, scores.shape, 0)
                key = lax.broadcasted_iota(jnp.int32, scores.shape, 1)
                scores = jnp.where(key <= position, scores, masked_score)
            old = top[g, rows, :1]
            new = jnp.maximum(old, jnp.max(scores, axis=1, keepdims=True))
            weights = jnp.exp(scores - new)
            keep = jnp.exp(old - new)
            total[g, rows] = total[g, rows] * keep + jnp.sum(weights, axis=1, keepdims=True)
            top[g, rows] = jnp.broadcast_to(new, (tile_rows, 128))
            acc[rows, cols] = acc[rows, cols] * keep + jnp.dot(
                weights.astype(jnp.bfloat16), v_ref[0], preferred_element_type=f32
            )

    for t in range(tile_count):
        picked = chosen_ref[t, page] != 0
        pl.when(jnp.logical_and(picked, causal))(functools.partial(visit, t, True))
        pl.when(jnp.logical_and(picked, jnp.logical_not(causal)))(
            functools.partial(visit, t, False)
        )

    @pl.when(page == pl.num_programs(1) - 1)
    def _():
        mix_ref[...] = acc[...].astype(jnp.bfloat16)
        lane = lax.broadcasted_iota(jnp.int32, m_ref.shape[1:], 1)
        maxima = jnp.zeros(m_ref.shape[1:], f32)
        sums = jnp.zeros(m_ref.shape[1:], f32)
        for g in range(group):
            maxima = jnp.where(lane == g, top[g], maxima)
            sums = jnp.where(lane == g, total[g], sums)
        m_ref[0] = maxima
        l_ref[0] = sums


def owner_pass(queries, keys, values, page_map, selected, ctx_index, ctx_count):
    pages_local, page_len, kv_width = keys.shape
    row_count, query_width = queries.shape
    kv_local = kv_width // HEAD_SIZE
    group = query_width // kv_width
    tile_count = selected.shape[0]
    page_total = pages_local * ctx_count
    slot_ids = ctx_index * pages_local + jnp.arange(pages_local, dtype=jnp.int32)
    all_pages = jnp.arange(page_total, dtype=jnp.int32)
    logical = jnp.sum(
        jnp.where(page_map[None, :] == slot_ids[:, None], all_pages[None, :], 0), axis=1
    )
    chosen = jnp.any(selected[:, None, :] == logical[None, :, None], axis=2).astype(jnp.int32)
    stat = jax.ShapeDtypeStruct((kv_local, row_count, 128), jnp.float32)
    stat_spec = pl.BlockSpec((1, row_count, 128), lambda k, p, a, b: (k, 0, 0))
    kv_spec = pl.BlockSpec((1, page_len, HEAD_SIZE), lambda k, p, a, b: (p, 0, k))
    q_spec = pl.BlockSpec((row_count, group * HEAD_SIZE), lambda k, p, a, b: (0, k))

    def kernel(logical_ref, chosen_ref, *refs):
        attention_kernel(logical_ref, chosen_ref, page_total, *refs)

    mixture, top, total = pl.pallas_call(
        kernel,
        grid_spec=pltpu.PrefetchScalarGridSpec(
            num_scalar_prefetch=2,
            grid=(kv_local, pages_local),
            in_specs=[q_spec, kv_spec, kv_spec],
            out_specs=(q_spec, stat_spec, stat_spec),
            scratch_shapes=[
                pltpu.VMEM((row_count, group * HEAD_SIZE), jnp.float32),
                pltpu.VMEM((group, row_count, 128), jnp.float32),
                pltpu.VMEM((group, row_count, 128), jnp.float32),
            ],
        ),
        out_shape=(jax.ShapeDtypeStruct((row_count, query_width), jnp.bfloat16), stat, stat),
    )(logical.astype(jnp.int32), chosen, queries, keys, values)

    def heads(stacked):
        return stacked[:, :, :group].transpose(1, 0, 2).reshape(row_count, kv_local * group)

    return heads(top), heads(total), mixture


MESH = pl.DeviceIdType.MESH
CORES = 2


def column_tile(width):
    for tile in (896, 768, 640, 512, 384, 256, 128):
        if width % tile == 0:
            return tile
    return width


def flat(block, rows):
    if block.shape[1] % 16:
        return block.astype(jnp.float32).reshape(rows, -1).astype(jnp.bfloat16)
    return block.reshape(rows, -1)


def tail_kernel(
    C,
    H,
    mix_ref,
    stat_ref,
    res_ref,
    gain_ref,
    ow_hbm,
    gw_hbm,
    uw_hbm,
    dw_hbm,
    mlp_ref,
    own_ref,
    ow,
    gw,
    uw,
    dw,
    mix_in,
    stat_in,
    att,
    po,
    po_in,
    u_out,
    st_out,
    ss,
    ublk,
    own_st,
    first,
    first_in,
    second,
    second_in,
    hid,
    acc,
    part,
    part_in,
    w_sem,
    mix_s,
    mix_r,
    stat_s,
    stat_r,
    att_s,
    att_r,
    po_s,
    po_r,
    u_s,
    u_r,
    st_s,
    st_r,
    ss_s,
    ss_r,
    f_s,
    f_r,
    g_s,
    g_r,
    h_s,
    h_r,
    fw_s,
    part_s,
    part_r,
):
    c = lax.axis_index("ctx")
    h = lax.axis_index("head")
    Y = H // CORES
    y = h // CORES
    core = h % CORES
    partner = y * CORES + (CORES - 1 - core)
    R = mix_ref.shape[1]
    rows = C * R
    rb = C // H
    bph = C // H
    width = ow.shape[0]
    head_rows = rows // H
    heads = mix_ref.shape[2] // HEAD_SIZE
    tiles, _, _, _, _, tile = first.shape
    f32 = jnp.float32
    bf16 = jnp.bfloat16

    def remote(src, dst, send_sem, recv_sem, ctx, head):
        return pltpu.make_async_remote_copy(
            src_ref=src,
            dst_ref=dst,
            send_sem=send_sem,
            recv_sem=recv_sem,
            device_id=(ctx, head),
            device_id_type=MESH,
        )

    sent = []

    def send(*args):
        copy = remote(*args)
        copy.start()
        sent.append(copy)

    loads = [
        pltpu.make_async_copy(src, dst, w_sem.at[i])
        for i, (src, dst) in enumerate(
            ((ow_hbm, ow), (gw_hbm, gw), (uw_hbm, uw), (dw_hbm, dw))
        )
    ]
    for load in loads:
        load.start()

    for d in range(1, C):
        peer = (c + d) % C
        send(stat_ref.at[peer], stat_in.at[c], stat_s.at[d], stat_r.at[c], peer, h)
        send(mix_ref.at[peer], mix_in.at[c], mix_s.at[d], mix_r.at[c], peer, h)
    stat_in[c] = stat_ref[c]
    mix_in[c] = mix_ref[c]
    for d in range(1, C):
        peer = (c + C - d) % C
        remote(stat_in.at[peer], stat_in.at[peer], stat_s.at[d], stat_r.at[peer], peer, h).wait_recv()
        remote(mix_in.at[peer], mix_in.at[peer], mix_s.at[d], mix_r.at[peer], peer, h).wait_recv()
    maxima = [stat_in[k][:, :heads] for k in range(C)]
    top = functools.reduce(jnp.maximum, maxima)
    scales = [jnp.exp(m - top) for m in maxima]
    total = sum(stat_in[k][:, heads : 2 * heads] * scales[k] for k in range(C))
    inverse = 1.0 / total
    for g in range(heads):
        cols = slice(g * HEAD_SIZE, (g + 1) * HEAD_SIZE)
        mixed = sum(mix_in[k, :, cols].astype(f32) * scales[k][:, g : g + 1] for k in range(C))
        att[c, :, cols] = (mixed * inverse[:, g : g + 1]).astype(bf16)

    for d in range(1, C):
        peer = (c + d) % C
        send(att.at[c], att.at[c], att_s.at[d], att_r.at[c], peer, h)
    loads[0].wait()
    for d in range(1, C):
        peer = (c + C - d) % C
        remote(att.at[peer], att.at[peer], att_s.at[d], att_r.at[peer], peer, h).wait_recv()
    projected = lax.dot_general(
        flat(att[...], rows), ow[...], (((1,), (1,)), ((), ())), preferred_element_type=f32
    )
    po[...] = projected.reshape(H, head_rows, width).astype(bf16)

    for d in range(1, H):
        peer = (h + d) % H
        send(po.at[peer], po_in.at[h], po_s.at[d], po_r.at[h], c, peer)
    po_in[h] = po[h]
    for d in range(1, H):
        peer = (h + H - d) % H
        remote(po_in.at[peer], po_in.at[peer], po_s.at[d], po_r.at[peer], c, peer).wait_recv()
    projected = sum(po_in[k].astype(f32) for k in range(H))
    stream = (res_ref[...].astype(f32) + projected).astype(bf16).astype(f32)
    st_out[...] = stream.reshape(rb, R, width).astype(bf16)
    u_out[...] = (stream * gain_ref[...]).reshape(rb, R, width).astype(bf16)
    squares = jnp.sum(stream * stream, axis=1, keepdims=True)
    ss[c] = jnp.broadcast_to(squares, (head_rows, 128))

    block_head = c // bph
    block_part = c % bph
    u_dst = ublk.at[block_part, pl.ds(h * rb, rb)]
    kept = []
    for d in range(C):
        peer = (c + d) % C
        copy = remote(u_out, u_dst, u_s.at[d], u_r.at[block_part, h], peer, block_head)
        if d == 0:
            kept.append((block_head != h, copy))
            pl.when(block_head != h)(copy.start)

            @pl.when(block_head == h)
            def _():
                ublk[block_part, pl.ds(h * rb, rb)] = u_out[...]

        else:
            copy.start()
            sent.append(copy)
    for d in range(1, C):
        peer = (c + d) % C
        send(ss.at[c], ss.at[c], ss_s.at[d], ss_r.at[c], peer, h)
    for i in range(rb):
        owner = h * rb + i
        other = jnp.logical_or(owner != c, block_head != h)
        copy = remote(
            st_out.at[i], own_st.at[block_part], st_s.at[i], st_r.at[block_part], owner, block_head
        )
        kept.append((other, copy))
        pl.when(other)(copy.start)

        @pl.when(jnp.logical_not(other))
        def _(i=i):
            own_st[block_part] = st_out[i]

    for j in range(bph):
        for k in range(H):
            source = h * bph + j
            block = ublk.at[j, pl.ds(k * rb, rb)]
            arrival = remote(block, block, u_s.at[0], u_r.at[j, k], source, k)
            pl.when(jnp.logical_or(source != c, h != k))(arrival.wait_recv)
    loads[1].wait()
    loads[2].wait()

    def matmul(i, which, weight):
        cols = slice(i * tile, (i + 1) * tile)
        value = None
        for j in range(bph):
            term = jnp.dot(
                flat(ublk[j], rows),
                weight[j * width : (j + 1) * width, cols],
                preferred_element_type=f32,
            )
            value = term if value is None else value + term
        first[i, which] = value.reshape(Y, CORES, head_rows, tile).swapaxes(0, 1).astype(bf16)
        send(
            first.at[i, which, CORES - 1 - core],
            first_in.at[i, which],
            f_s.at[i, which],
            f_r.at[i, which],
            c,
            partner,
        )

    def middle(i, which):
        remote(
            first_in.at[i, which], first_in.at[i, which], f_s.at[i, which], f_r.at[i, which], c, partner
        ).wait_recv()
        both = first[i, which, core].astype(f32) + first_in[i, which].astype(f32)
        second[i, which] = both.astype(bf16)
        for d in range(1, Y):
            peer = (y + d) % Y
            send(
                second.at[i, which, peer],
                second_in.at[i, which, y],
                g_s.at[i, which, d],
                g_r.at[i, which, y],
                c,
                peer * CORES + core,
            )

    def finish(i, inverse_rms):
        sums = []
        for which in range(2):
            value = second[i, which, y].astype(f32)
            for d in range(1, Y):
                peer = (y + Y - d) % Y
                slot = second_in.at[i, which, peer]
                remote(
                    slot, slot, g_s.at[i, which, d], g_r.at[i, which, peer], c, peer * CORES + core
                ).wait_recv()
                value = value + second_in[i, which, peer].astype(f32)
            sums.append(value * inverse_rms)
        hid[i, h] = (jax.nn.gelu(sums[0], approximate=True) * sums[1]).astype(bf16)
        send(hid.at[i, h], hid.at[i, h], h_s.at[i, 0], h_r.at[i, h], c, partner)
        for d in range(1, Y):
            peer = ((y + d) % Y) * CORES + core
            send(hid.at[i, h], hid.at[i, h], h_s.at[i, d], h_r.at[i, h], c, peer)

    def forward(i):
        for d in range(1, Y):
            origin = ((y + Y - d) % Y) * CORES + core
            slot = hid.at[i, origin]
            remote(slot, slot, h_s.at[i, d], h_r.at[i, origin], c, origin).wait_recv()
            send(slot, slot, fw_s.at[i, d], h_r.at[i, origin], c, partner)

    def down(i):
        for d in range(Y):
            origin = ((y + Y - d) % Y) * CORES + (CORES - 1 - core)
            slot = hid.at[i, origin]
            remote(slot, slot, h_s.at[i, 0], h_r.at[i, origin], c, partner).wait_recv()
        term = lax.dot_general(
            flat(hid[i], rows),
            dw[:, i * tile : (i + 1) * tile],
            (((1,), (1,)), ((), ())),
            preferred_element_type=f32,
        )
        if i == 0:
            acc[...] = term
        else:
            acc[...] += term

    steps = [(i, which) for i in range(tiles) for which in range(2)]
    for n, (i, which) in enumerate(steps):
        matmul(i, which, (gw, uw)[which])
        if n:
            middle(*steps[n - 1])
    middle(*steps[-1])
    for d in range(1, C):
        peer = (c + C - d) % C
        remote(ss.at[peer], ss.at[peer], ss_s.at[d], ss_r.at[peer], peer, h).wait_recv()
    squares = sum(ss[k] for k in range(C))
    inverse_rms = lax.rsqrt(squares[:, :1] / (C * width) + norm_epsilon)
    loads[3].wait()
    for i in range(tiles):
        finish(i, inverse_rms)
        if i:
            forward(i - 1)
    forward(tiles - 1)
    for i in range(tiles):
        down(i)
    part[...] = acc[...].reshape(C, R, acc.shape[1]).astype(bf16)

    for d in range(1, C):
        peer = (c + d) % C
        send(part.at[peer], part_in.at[c], part_s.at[d], part_r.at[c], peer, h)
    part_in[c] = part[c]
    for j in range(bph):
        source = h * bph + j
        arrival = remote(own_st.at[j], own_st.at[j], st_s.at[0], st_r.at[j], source, c // rb)
        pl.when(jnp.logical_or(source != c, c // rb != h))(arrival.wait_recv)
    own_ref[...] = own_st[...]
    for d in range(1, C):
        peer = (c + C - d) % C
        remote(part_in.at[peer], part_in.at[peer], part_s.at[d], part_r.at[peer], peer, h).wait_recv()
    mlp_ref[...] = sum(part_in[k].astype(f32) for k in range(C))
    for copy in sent:
        copy.wait_send()
    for condition, copy in kept:
        pl.when(condition)(copy.wait_send)


def tail(C, H, mixture, stats, residual_in, norm_gain, out_weight, gate_weight, up_weight, down_weight):
    rows, query_width = mixture.shape
    R = rows // C
    width = out_weight.shape[1]
    hidden = gate_weight.shape[1]
    out_width = down_weight.shape[1]
    out_weight = out_weight.T
    down_weight = down_weight.T
    rb = C // H
    bph = C // H
    Y = H // CORES
    head_rows = rows // H
    tile = column_tile(hidden)
    tiles = hidden // tile
    bf16 = jnp.bfloat16
    vmem = pl.BlockSpec(memory_space=pltpu.VMEM)
    hbm = pl.BlockSpec(memory_space=pl.ANY)
    V = pltpu.VMEM
    S = pltpu.SemaphoreType.DMA
    return pl.pallas_call(
        functools.partial(tail_kernel, C, H),
        out_shape=(
            jax.ShapeDtypeStruct((R, out_width), jnp.float32),
            jax.ShapeDtypeStruct((bph, R, width), bf16),
        ),
        in_specs=[vmem] * 4 + [hbm] * 4,
        out_specs=(vmem, vmem),
        scratch_shapes=[
            V(out_weight.shape, bf16),
            V(gate_weight.shape, bf16),
            V(up_weight.shape, bf16),
            V(down_weight.shape, bf16),
            V((C, R, query_width), bf16),
            V((C, R, 128), jnp.float32),
            V((C, R, query_width), bf16),
            V((H, head_rows, width), bf16),
            V((H, head_rows, width), bf16),
            V((rb, R, width), bf16),
            V((rb, R, width), bf16),
            V((C, head_rows, 128), jnp.float32),
            V((bph, C, R, width), bf16),
            V((bph, R, width), bf16),
            V((tiles, 2, CORES, Y, head_rows, tile), bf16),
            V((tiles, 2, Y, head_rows, tile), bf16),
            V((tiles, 2, Y, head_rows, tile), bf16),
            V((tiles, 2, Y, head_rows, tile), bf16),
            V((tiles, H, head_rows, tile), bf16),
            V((rows, out_width), jnp.float32),
            V((C, R, out_width), bf16),
            V((C, R, out_width), bf16),
            S((4,)),
            S((C,)),
            S((C,)),
            S((C,)),
            S((C,)),
            S((C,)),
            S((C,)),
            S((H,)),
            S((H,)),
            S((C,)),
            S((bph, H)),
            S((rb,)),
            S((bph,)),
            S((C,)),
            S((C,)),
            S((tiles, 2)),
            S((tiles, 2)),
            S((tiles, 2, Y)),
            S((tiles, 2, Y)),
            S((tiles, Y)),
            S((tiles, H)),
            S((tiles, Y)),
            S((C,)),
            S((C,)),
        ],
        compiler_params=pltpu.CompilerParams(
            has_side_effects=True, vmem_limit_bytes=60 * 2**20
        ),
    )(
        mixture.reshape(C, R, query_width),
        stats.reshape(C, R, 128),
        residual_in,
        norm_gain.reshape(1, width),
        out_weight,
        gate_weight,
        up_weight,
        down_weight,
    )


LOG2E = 1.4426950408889634


def fused_kernel(
    C,
    H,
    NP,
    map_hbm,
    sel_hbm,
    q_hbm,
    res_hbm,
    gain_hbm,
    k_hbm,
    v_hbm,
    ow_hbm,
    gw_hbm,
    uw_hbm,
    dw_hbm,
    out_ref,
    map_ref,
    sel_ref,
    q_ref,
    res_ref,
    gain_ref,
    k_buf,
    v_buf,
    ow,
    gw,
    uw,
    dw,
    mix_out,
    mix_in,
    lse_out,
    lse_in,
    att,
    po_out,
    po_in,
    res_in,
    st,
    u,
    ss_out,
    ss_in,
    ss_mid,
    ss_last,
    scale,
    begun,
    first,
    first_in,
    second,
    second_in,
    hid,
    acc,
    part,
    part_in,
    in_sem,
    kv_sem,
    w_sem,
    mix_s,
    mix_r,
    lse_s,
    lse_r,
    att_s,
    att_r,
    cross_r,
    po_s,
    po_r,
    res_s,
    res_r,
    u_s,
    u_r,
    ss_s,
    ss_r,
    f_s,
    f_r,
    g_s,
    g_r,
    h_s,
    h_r,
    part_s,
    part_r,
):
    c = lax.axis_index("ctx")
    h = lax.axis_index("head")
    X = C // H
    Z = C // X
    z = c // X
    x = c % X
    Y = H // CORES
    y = h // CORES
    core = h % CORES
    partner = y * CORES + (CORES - 1 - core)
    _, NQ, RC, query_width = q_ref.shape
    rows = C * RC
    hr = rows // H
    kv, pages, page_len, _ = k_buf.shape
    group = query_width // (kv * HEAD_SIZE)
    gw_cols = group * HEAD_SIZE
    tile_count = sel_ref.shape[0]
    tile_rows = NQ * rows // tile_count
    offset = page_len - NQ * rows
    page_total = map_ref.shape[0]
    width = ow.shape[0]
    tile = first.shape[-1]
    tiles = first.shape[1]
    RP = rows // NP
    f32 = jnp.float32
    bf16 = jnp.bfloat16
    owner = h == z
    visitor = h != z

    def remote(src, dst, send_sem, recv_sem, ctx, head):
        return pltpu.make_async_remote_copy(
            src_ref=src,
            dst_ref=dst,
            send_sem=send_sem,
            recv_sem=recv_sem,
            device_id=(ctx, head),
            device_id_type=MESH,
        )

    sent = []
    kept = []

    def start(*args):
        remote(*args).start()

    def send(*args):
        copy = remote(*args)
        copy.start()
        sent.append(copy)

    def send_if(condition, *args):
        copy = remote(*args)
        pl.when(condition)(copy.start)
        kept.append((condition, copy))

    def kv_load(j):
        lanes = pl.ds(pl.multiple_of(j * HEAD_SIZE, HEAD_SIZE), HEAD_SIZE)
        return (
            pltpu.make_async_copy(k_hbm.at[:, :, lanes], k_buf.at[j], kv_sem.at[0, j]),
            pltpu.make_async_copy(v_hbm.at[:, :, lanes], v_buf.at[j], kv_sem.at[1, j]),
        )

    barrier = pltpu.get_barrier_semaphore()
    for d in range(1, C):
        pl.semaphore_signal(
            barrier, inc=1, device_id=((c + d) % C, h), device_id_type=MESH
        )
    for d in range(1, H):
        pl.semaphore_signal(
            barrier, inc=1, device_id=(c, (h + d) % H), device_id_type=MESH
        )
    inputs = [
        pltpu.make_async_copy(src, dst, in_sem.at[i])
        for i, (src, dst) in enumerate(
            (
                (map_hbm, map_ref),
                (sel_hbm, sel_ref),
                (q_hbm, q_ref),
                (res_hbm, res_ref),
                (gain_hbm, gain_ref.at[0]),
            )
        )
    ]
    for load in inputs:
        load.start()
    for load in kv_load(0):
        load.start()
    loads = [
        pltpu.make_async_copy(src, dst, w_sem.at[i])
        for i, (src, dst) in enumerate(
            ((ow_hbm, ow), (gw_hbm, gw), (uw_hbm, uw), (dw_hbm, dw))
        )
    ]
    for load in inputs[:3]:
        load.wait()

    facts = []
    for p in range(pages):
        slot = c * pages + p
        logical = jnp.int32(0)
        for j in range(page_total):
            logical = logical + jnp.where(map_ref[j] == slot, j, 0)
        picks = []
        for t in range(tile_count):
            hits = jnp.int32(0)
            for i in range(sel_ref.shape[1]):
                hits = hits + jnp.where(sel_ref[t, i] == logical, 1, 0)
            picks.append(jnp.where(hits > 0, 0.0, masked_score).astype(f32))
        reach = jnp.where(logical == page_total - 1, 0, page_len)
        facts.append((reach, picks))

    index = lax.broadcasted_iota(jnp.int32, (group * rows, 1), 0) & (rows - 1)
    shift = RC.bit_length() - 1
    base_row = (index >> shift) * (NQ * RC) + (index & (RC - 1))
    eye = lax.broadcasted_iota(jnp.int32, (rows, rows), 0) == lax.broadcasted_iota(
        jnp.int32, (rows, rows), 1
    )
    unit = score_scale * LOG2E

    def attend(n):
        q = n // kv
        j = n % kv

        @pl.when(n < kv)
        def _():
            for load in kv_load(j):
                load.wait()

        @pl.when(n == 0)
        def _():
            for k in range(1, kv):
                for load in kv_load(k):
                    load.start()
            for load in loads:
                load.start()

        lanes = pl.ds(pl.multiple_of(j * gw_cols, gw_cols), gw_cols)
        block = q_ref[:, q, :, lanes].reshape(rows, gw_cols)
        lhs = jnp.concatenate(
            [block[:, g * HEAD_SIZE : (g + 1) * HEAD_SIZE] for g in range(group)], axis=0
        )
        row = base_row + q * RC
        key = offset + lax.broadcasted_iota(jnp.int32, (group * rows, page_len - offset), 1)
        tops, sums, outs = [], [], []
        for p in range(pages):
            reach, picks = facts[p]
            bias = jnp.zeros((group * rows, 1), f32)
            for t in range(tile_count):
                inside = jnp.logical_and(row >= t * tile_rows, row < (t + 1) * tile_rows)
                bias = jnp.where(inside, picks[t], bias)
            scores = lax.dot_general(
                lhs, k_buf[j, p], (((1,), (1,)), ((), ())), preferred_element_type=f32
            )
            late = jnp.where(key <= offset + row + reach, scores[:, offset:], masked_score)
            scores = jnp.concatenate([scores[:, :offset], late], axis=1)
            top = jnp.max(scores, axis=1, keepdims=True)
            weights = jnp.exp2((scores - top) * unit)
            sums.append(jnp.sum(weights, axis=1, keepdims=True))
            outs.append(
                jnp.dot(weights.astype(bf16), v_buf[j, p], preferred_element_type=f32)
            )
            tops.append(top * unit + bias)
        best = functools.reduce(jnp.maximum, tops)
        scales = [jnp.exp2(top - best) for top in tops]
        total = sum(s * e for s, e in zip(sums, scales))
        mixed = sum(o * (e / total) for o, e in zip(outs, scales))
        lse = best + jnp.log2(total)
        for g in range(group):
            part_rows = slice(g * rows, (g + 1) * rows)
            mix_out[n, :, :, g * HEAD_SIZE : (g + 1) * HEAD_SIZE] = (
                mixed[part_rows].reshape(C, RC, HEAD_SIZE).astype(bf16)
            )
            lse_out[n, g : g + 1] = jnp.sum(
                jnp.where(eye, lse[part_rows], 0.0), axis=0, keepdims=True
            )
        mix_in[n, c] = mix_out[n, c]
        lse_in[n, c] = lse_out[n]

    def mix_sends(n):
        for d in range(1, C):
            peer = (c + d) % C
            remote(mix_out.at[n, peer], mix_in.at[n, c], mix_s.at[0], mix_r.at[n], peer, h).start()
            remote(lse_out.at[n], lse_in.at[n, c], lse_s.at[0], lse_r.at[n], peer, h).start()

    def att_sends(n, direct):
        block = att.at[n, c]
        if direct:
            for d in range(1, C):
                start(block, block, att_s.at[0], att_r.at[n], (c + d) % C, h)
        else:
            for d in range(1, Z):
                start(block, block, att_s.at[0], att_r.at[n], (z + d) % Z * X + x, h)
            for d in range(1, X):
                start(block, block, att_s.at[0], cross_r.at[n - kv], z * X + (x + d) % X, h)

    def att_relay(n):
        arrived(att.at[n, pl.ds(0, Z - 1)], att_r.at[n])
        for e in range(1, Z):
            block = att.at[n, (z + e) % Z * X + x]
            for d in range(1, X):
                start(block, block, att_s.at[0], cross_r.at[n - kv], z * X + (x + d) % X, h)

    def arrived(block, recv_sem):
        remote(block, block, recv_sem, recv_sem, c, partner).wait_recv()

    def left(block, send_sem):
        remote(block, block, send_sem, send_sem, c, partner).wait_send()

    def combine(n, direct):
        arrived(lse_in.at[n, pl.ds(0, C - 1)], lse_r.at[n])
        arrived(mix_in.at[n, pl.ds(0, C - 1)], mix_r.at[n])
        logs = [lse_in[n, k] for k in range(C)]
        best = functools.reduce(jnp.maximum, logs)
        scales = [jnp.exp2(value - best) for value in logs]
        inverse = 1.0 / sum(scales)
        lane = lax.broadcasted_iota(jnp.int32, (RC, rows), 1)
        mine = lane == c * RC + lax.broadcasted_iota(jnp.int32, (RC, rows), 0)
        for g in range(group):
            cols = slice(g * HEAD_SIZE, (g + 1) * HEAD_SIZE)
            value = jnp.zeros((RC, HEAD_SIZE), f32)
            for k in range(C):
                share = (scales[k] * inverse)[g : g + 1]
                share = jnp.sum(jnp.where(mine, share, 0.0), axis=1, keepdims=True)
                value = value + share * mix_in[n, k, :, cols].astype(f32)
            att[n, c, :, cols] = value.astype(bf16)
        att_sends(n, direct)

    def project(q):
        for j in range(kv):
            n = q * kv + j
            if q == 0:
                arrived(att.at[n, pl.ds(0, C - 1)], att_r.at[n])
            else:
                arrived(att.at[n, pl.ds(0, (X - 1) * Z)], cross_r.at[n - kv])
        if q == 0:
            loads[0].wait()
        value = None
        for j in range(kv):
            term = lax.dot_general(
                att[q * kv + j].reshape(rows, gw_cols),
                ow[:, j * gw_cols : (j + 1) * gw_cols],
                (((1,), (1,)), ((), ())),
                preferred_element_type=f32,
            )
            value = term if value is None else value + term
        po_out[q] = value.astype(bf16)
        for i in range(NP):
            piece = pl.ds(i * RP, RP)
            copy = remote(
                po_out.at[q, piece], po_in.at[q, h, piece], po_s.at[q], po_r.at[q, i], c, z
            )
            pl.when(visitor)(copy.start)
        po_in[q, h] = po_out[q]

    def own(q, i):
        if q == 0 and i == 0:
            arrived(res_in.at[pl.ds(0, H - 1)], res_r.at[0])
        arrived(po_in.at[q, pl.ds(0, H - 1), pl.ds(i * RP, RP)], po_r.at[q, i])
        spare = u.shape[-1] - width
        lane = lax.broadcasted_iota(jnp.int32, (hr, spare), 1)
        for b in range(i * RP // hr, (i + 1) * RP // hr):
            span = slice(b * hr, (b + 1) * hr)
            value = res_in[b, :, q].reshape(hr, width).astype(f32)
            added = sum(po_in[q, k, span].astype(f32) for k in range(H))
            stream = (value + added).astype(bf16)
            st[q, span] = stream
            stream = stream.astype(f32)
            u[q, x, span, :width] = (stream * gain_ref[...]).astype(bf16)
            squares = jnp.sum(stream * stream, axis=1, keepdims=True)
            high = squares.astype(bf16).astype(f32)
            mid = (squares - high).astype(bf16).astype(f32)
            low = squares - high - mid
            packed = jnp.where(lane == 0, high, jnp.where(lane == 1, mid, low))
            packed = jnp.where(lane < 3, packed, 0.0)
            u[q, x, span, width:] = packed.astype(bf16)

    def relay(q, i, here):
        piece = u.at[q, x, pl.ds(i * RP, RP)]
        recv = u_r.at[q, x, i]
        pl.when(jnp.logical_and(here, visitor))(functools.partial(arrived, piece, recv))
        for way, ahead in enumerate((Z - 1 - z, z)):
            step = 1 - 2 * way
            go = jnp.logical_and(jnp.logical_and(here, step * (z - h) >= 0), ahead > 0)
            target = jnp.clip(z + step, 0, Z - 1) * X + x
            copy = remote(piece, piece, u_s.at[way], recv, target, h)
            pl.when(go)(copy.start)
            kept.append((go, copy))
        for d in range(1, X):
            peer = z * X + (x + d) % X
            copy = remote(piece, piece, u_s.at[1 + d], recv, peer, h)
            pl.when(here)(copy.start)
            kept.append((here, copy))

    def spread(q, here):
        for i in range(NP):
            pl.when(jnp.logical_and(here, owner))(functools.partial(own, q, i))
            relay(q, i, here)

    def gather(q):
        for d in range(1, X):
            source = (x + d) % X
            for i in range(NP):
                block = u.at[q, source, pl.ds(i * RP, RP)]
                arrived(block, u_r.at[q, source, i])
        squares = 0.0
        for k in range(X):
            split = u[q, k, :, width:].astype(f32)
            squares = squares + jnp.sum(split, axis=1, keepdims=True)
        squares = jnp.broadcast_to(squares, (rows, 128)).reshape(Y, CORES, hr, 128)
        ss_out[q] = squares.swapaxes(0, 1)
        send(ss_out.at[q, CORES - 1 - core], ss_in.at[q], ss_s.at[q, 0], ss_r.at[q, 0], c, partner)

    def block_dot(q, k, i, which):
        weight = (gw, uw)[which]
        span = pl.ds(pl.multiple_of(k * width, 16), width)
        return jnp.dot(
            u[q, k, :, :width],
            weight[span, i * tile : (i + 1) * tile],
            preferred_element_type=f32,
        )

    def start_expand(q):
        if q == 0:
            loads[1].wait()
            loads[2].wait()
        for i in range(tiles):
            for which in range(2):
                begun[i, which] = block_dot(q, x, i, which)

    def matmul(q, i, which):
        value = begun[i, which]
        for d in range(1, X):
            value = value + block_dot(q, (x + d) % X, i, which)
        value = value.reshape(Y, CORES, hr, tile).swapaxes(0, 1).astype(bf16)
        first[q, i, which] = value
        start(
            first.at[q, i, which, CORES - 1 - core],
            first_in.at[q, i, which],
            f_s.at[0],
            f_r.at[q, i, which],
            c,
            partner,
        )

    def middle(q, i, which):
        block = first_in.at[q, i, which]
        arrived(block, f_r.at[q, i, which])
        both = first[q, i, which, core].astype(f32) + first_in[q, i, which].astype(f32)
        second[q, i, which] = both.astype(bf16)
        for d in range(1, Y):
            peer = (y + d) % Y
            start(
                second.at[q, i, which, peer],
                second_in.at[q, i, which, y],
                g_s.at[0],
                g_r.at[q, i, which, y],
                c,
                peer * CORES + core,
            )

    def middle_squares(q):
        block = ss_in.at[q]
        remote(block, block, ss_s.at[q, 0], ss_r.at[q, 0], c, partner).wait_recv()
        ss_mid[q] = ss_out[q, core] + ss_in[q]
        for d in range(1, Y):
            peer = (y + d) % Y
            send(
                ss_mid.at[q, peer],
                ss_last.at[q, y],
                ss_s.at[q, d],
                ss_r.at[q, 1 + y],
                c,
                peer * CORES + core,
            )

    def inverse_rms(q):
        total = ss_mid[q, y]
        for d in range(1, Y):
            peer = (y + Y - d) % Y
            block = ss_last.at[q, peer]
            remote(
                block, block, ss_s.at[q, d], ss_r.at[q, 1 + peer], c, peer * CORES + core
            ).wait_recv()
            total = total + ss_last[q, peer]
        scale[q] = lax.rsqrt(total / (C * width) + norm_epsilon)

    def finish(q, i):
        inverse = scale[q][:, :1]
        sums = []
        for which in range(2):
            value = second[q, i, which, y].astype(f32)
            for d in range(1, Y):
                peer = (y + Y - d) % Y
                block = second_in.at[q, i, which, peer]
                remote(
                    block,
                    block,
                    g_s.at[0],
                    g_r.at[q, i, which, peer],
                    c,
                    peer * CORES + core,
                ).wait_recv()
                value = value + second_in[q, i, which, peer].astype(f32)
            sums.append(value * inverse)
        hid[q, i, h] = (jax.nn.gelu(sums[0], approximate=True) * sums[1]).astype(bf16)
        block = hid.at[q, i, h]
        for d in range(1, Y):
            peer = ((y + d) % Y) * CORES + core
            start(block, block, h_s.at[0], h_r.at[q, i, h], c, peer)
        start(block, block, h_s.at[0], h_r.at[q, i, h], c, partner)

    def forward(q, i):
        for d in range(1, Y):
            origin = ((y + Y - d) % Y) * CORES + core
            block = hid.at[q, i, origin]
            arrived(block, h_r.at[q, i, origin])
            start(block, block, h_s.at[0], h_r.at[q, i, origin], c, partner)

    def down(q, i):
        for d in range(Y):
            origin = ((y + Y - d) % Y) * CORES + (CORES - 1 - core)
            block = hid.at[q, i, origin]
            arrived(block, h_r.at[q, i, origin])
        if q == 0 and i == 0:
            loads[3].wait()
        term = lax.dot_general(
            hid[q, i].reshape(rows, tile),
            dw[:, i * tile : (i + 1) * tile],
            (((1,), (1,)), ((), ())),
            preferred_element_type=f32,
        )
        if i == 0:
            acc[...] = term
        else:
            acc[...] += term

    def scatter(q):
        for k in range(X):

            @pl.when(jnp.logical_and(owner, x == k))
            def _(k=k):
                acc[:, k * width : (k + 1) * width] += st[q].astype(f32)

        part[q] = acc[...].reshape(C, RC, acc.shape[1]).astype(bf16)
        for d in range(1, C):
            peer = (c + d) % C
            start(part.at[q, peer], part_in.at[q, c], part_s.at[0], part_r.at[q], peer, h)
        part_in[q, c] = part[q, c]

    def collect(q):
        arrived(part_in.at[q, pl.ds(0, C - 1)], part_r.at[q])
        out_ref[q] = sum(part_in[q, k].astype(f32) for k in range(C)).astype(bf16)

    steps = NQ * kv
    lag = 3

    def loop(n, carry):
        attend(n)

        @pl.when(n == 1)
        def _():
            pl.semaphore_wait(barrier, C + H - 2)
            mix_sends(0)

        ready = jnp.logical_and(n >= 1, n < kv)
        pl.when(jnp.logical_or(ready, n >= kv + lag))(functools.partial(mix_sends, n))

        for k in range(kv):

            @pl.when(n == (kv + lag - 2 if k == kv - 1 else max(k + 2, lag)))
            def _(k=k):
                combine(k, True)

        @pl.when(n == kv + lag - 1)
        def _():
            for k in range(kv, kv + lag):
                mix_sends(k)

        return carry

    lax.fori_loop(0, steps, loop, 0)
    for load in inputs[3:]:
        load.wait()
    send_if(visitor, res_ref, res_in.at[h], res_s.at[0], res_r.at[0], c, z)
    res_in[h] = res_ref[...]
    pairs = [(i, which) for i in range(tiles) for which in range(2)]

    def expand(q, extra=None):
        start_expand(q)
        gather(q)
        for n, (i, which) in enumerate(pairs):
            matmul(q, i, which)
            if n == 1:
                middle_squares(q)
            if n:
                middle(q, *pairs[n - 1])
            if extra is not None and which:
                extra(i)
        middle(q, *pairs[-1])

    def finish_if(here, q, i):
        @pl.when(here)
        def _():
            if i == 0:
                inverse_rms(q)
            finish(q, i)

    def contract(q, done=0):
        forward(q, done)
        for i in range(done, tiles):
            if i + 1 < tiles:
                forward(q, i + 1)
            down(q, i)
        scatter(q)

    def between(i):
        finish_if(early, 0, i)
        if i:

            @pl.when(late)
            def _():
                forward(0, i - 1)
                down(0, i - 1)


    far = jnp.maximum(z - h, h - z)
    early = z // CORES == y
    late = z // CORES != y
    project(0)
    for n in range(kv, steps - 2):
        combine(n, False)
    spread(0, far == 0)
    for n in range(steps - 2, steps):
        combine(n, False)
    for n in range(kv, steps - 2):
        att_relay(n)
    spread(0, far == 1)
    for n in range(steps - 2, steps):
        att_relay(n)
    spread(0, far == 2)
    project(1)
    spread(0, far > 2)
    expand(0, lambda i: spread(1, far == 0) if i == tiles - 2 else None)
    first_on = jnp.logical_and(late, far <= 2)
    spread(1, first_on)
    for i in range(tiles):
        finish_if(late, 0, i)
    spread(1, jnp.logical_and(jnp.logical_not(first_on), far > 0))
    expand(1, between)
    for i in range(tiles - 1):
        finish_if(late, 1, i)
    pl.when(late)(lambda: contract(0, tiles - 1))
    finish_if(late, 1, tiles - 1)
    pl.when(early)(lambda: contract(0))
    for i in range(tiles):
        finish_if(early, 1, i)
    contract(1)
    for q in range(NQ):
        collect(q)

    left(mix_out.at[:, pl.ds(0, C - 1)], mix_s.at[0])
    left(lse_in.at[:, pl.ds(0, C - 1)], lse_s.at[0])
    left(att.at[:, pl.ds(0, C - 1)], att_s.at[0])
    left(first_in, f_s.at[0])
    left(second.at[:, :, :, pl.ds(0, Y - 1)], g_s.at[0])
    left(hid.at[:, :, pl.ds(0, 2 * Y - 1)], h_s.at[0])
    left(part.at[:, pl.ds(0, C - 1)], part_s.at[0])
    for q in range(NQ):
        pl.when(visitor)(functools.partial(left, po_out.at[q], po_s.at[q]))
    for copy in sent:
        copy.wait_send()
    for condition, copy in kept:
        pl.when(condition)(copy.wait_send)


def fused(
    C,
    H,
    queries,
    keys,
    values,
    page_map,
    selected,
    residual_in,
    out_weight,
    norm_gain,
    gate_weight,
    up_weight,
    down_weight,
):
    row_count, query_width = queries.shape
    pages, page_len, kv_width = keys.shape
    kv = kv_width // HEAD_SIZE
    group = query_width // kv_width
    NQ = row_count // 128
    RC = row_count // C // NQ
    rows = C * RC
    NP = 4
    X = C // H
    Y = H // CORES
    hr = rows // H
    width = out_weight.shape[1]
    hidden = gate_weight.shape[1]
    out_width = down_weight.shape[1]
    tile = column_tile(hidden)
    tiles = hidden // tile
    steps = NQ * kv
    u_width = (width + 127) // 128 * 128
    bf16 = jnp.bfloat16
    f32 = jnp.float32
    vmem = pl.BlockSpec(memory_space=pltpu.VMEM)
    hbm = pl.BlockSpec(memory_space=pl.ANY)
    V = pltpu.VMEM
    S = pltpu.SemaphoreType.DMA
    out_weight = out_weight.T
    down_weight = down_weight.T
    mixes = V((steps, C, RC, group * HEAD_SIZE), bf16)
    return pl.pallas_call(
        functools.partial(fused_kernel, C, H, NP),
        out_shape=jax.ShapeDtypeStruct((NQ, RC, out_width), bf16),
        in_specs=[hbm] * 11,
        out_specs=vmem,
        scratch_shapes=[
            pltpu.SMEM(page_map.shape, jnp.int32),
            pltpu.SMEM(selected.shape, jnp.int32),
            V((C, NQ, RC, query_width), bf16),
            V((X, NQ, RC, width), bf16),
            V((1, width), f32),
            V((kv, pages, page_len, HEAD_SIZE), bf16),
            V((kv, pages, page_len, HEAD_SIZE), bf16),
            V(out_weight.shape, bf16),
            V(gate_weight.shape, bf16),
            V(up_weight.shape, bf16),
            V(down_weight.shape, bf16),
            mixes,
            mixes,
            V((steps, group, rows), f32),
            V((steps, C, group, rows), f32),
            mixes,
            V((NQ, rows, width), bf16),
            V((NQ, H, rows, width), bf16),
            V((H, X, NQ, RC, width), bf16),
            V((NQ, rows, width), bf16),
            V((NQ, X, rows, u_width), bf16),
            V((NQ, CORES, Y, hr, 128), f32),
            V((NQ, Y, hr, 128), f32),
            V((NQ, Y, hr, 128), f32),
            V((NQ, Y, hr, 128), f32),
            V((NQ, hr, 128), f32),
            V((tiles, 2, rows, tile), f32),
            V((NQ, tiles, 2, CORES, Y, hr, tile), bf16),
            V((NQ, tiles, 2, Y, hr, tile), bf16),
            V((NQ, tiles, 2, Y, hr, tile), bf16),
            V((NQ, tiles, 2, Y, hr, tile), bf16),
            V((NQ, tiles, H, hr, tile), bf16),
            V((rows, out_width), f32),
            V((NQ, C, RC, out_width), bf16),
            V((NQ, C, RC, out_width), bf16),
            S((5,)),
            S((2, kv)),
            S((4,)),
            S((1,)),
            S((steps,)),
            S((1,)),
            S((steps,)),
            S((1,)),
            S((steps,)),
            S((kv,)),
            S((NQ,)),
            S((NQ, NP)),
            S((1,)),
            S((1,)),
            S((1 + X,)),
            S((NQ, X, NP)),
            S((NQ, Y)),
            S((NQ, 1 + Y)),
            S((1,)),
            S((NQ, tiles, 2)),
            S((1,)),
            S((NQ, tiles, 2, Y)),
            S((1,)),
            S((NQ, tiles, H)),
            S((1,)),
            S((NQ,)),
        ],
        compiler_params=pltpu.CompilerParams(
            collective_id=0, has_side_effects=True, vmem_limit_bytes=63 * 2**20
        ),
    )(
        page_map,
        selected,
        queries.reshape(C, NQ, RC, query_width),
        residual_in.reshape(X, NQ, RC, width),
        norm_gain,
        keys,
        values,
        out_weight,
        gate_weight,
        up_weight,
        down_weight,
    ).reshape(row_count // C, out_width)


def fits(C, H, queries, keys, selected, out_weight, gate_weight):
    rows = queries.shape[0]
    width = out_weight.shape[1]
    if rows % 128:
        return False
    chunks = rows // 128
    return (
        chunks == 2
        and C % H == 0
        and (C // H) * H == C
        and rows % (C * chunks) == 0
        and rows // (C * chunks) % 16 == 0
        and rows % selected.shape[0] == 0
        and keys.shape[2] // HEAD_SIZE > 3
        and (keys.shape[1] - rows) % 128 == 0
        and keys.shape[1] > rows
        and width % 16 == 0
        and width % 128 <= 125
        and width % 128 > 0
        and gate_weight.shape[1] % 128 == 0
    )


def shards(
    queries,
    keys,
    values,
    page_map,
    selected,
    residual_in,
    out_weight,
    norm_gain,
    gate_weight,
    up_weight,
    down_weight,
):
    ctx_index = lax.axis_index("ctx")
    C = lax.axis_size("ctx")
    H = lax.axis_size("head")
    if fits(C, H, queries, keys, selected, out_weight, gate_weight):
        return fused(
            C,
            H,
            queries,
            keys,
            values,
            page_map,
            selected,
            residual_in,
            out_weight,
            norm_gain,
            gate_weight,
            up_weight,
            down_weight,
        )
    row_max, row_total, mixture = owner_pass(
        queries, keys, values, page_map, selected, ctx_index, C
    )
    stats = jnp.concatenate([row_max, row_total], axis=1)
    stats = jnp.pad(stats, ((0, 0), (0, 128 - stats.shape[1])))
    mlp_out, own_stream = tail(
        C,
        H,
        mixture.astype(jnp.bfloat16),
        stats,
        residual_in,
        norm_gain,
        out_weight,
        gate_weight,
        up_weight,
        down_weight,
    )
    own_stream = jnp.concatenate([own_stream[j] for j in range(own_stream.shape[0])], axis=1)
    return (own_stream.astype(jnp.float32) + mlp_out).astype(jnp.bfloat16)


def solution(mesh):
    in_specs = (
        P(None, "head"),
        P("ctx", None, "head"),
        P("ctx", None, "head"),
        P(),
        P(),
        P("head", "ctx"),
        P("head", "ctx"),
        P("ctx"),
        P("head", "ctx"),
        P("head", "ctx"),
        P("ctx", "head"),
    )
    out_specs = P("ctx", "head")
    return jax.shard_map(shards, mesh=mesh, in_specs=in_specs, out_specs=out_specs, check_vma=False)
```

```python
import jax
import jax.numpy as jnp
import functools
from jax import lax
from jax.experimental import pallas as pl
from jax.experimental.pallas import tpu as pltpu
from jax.sharding import PartitionSpec as P

D = 5376
HEAD_SIZE = 128


score_scale = 168.0 ** (-0.5)
masked_score = -1e30
norm_epsilon = 1e-06


def attention_kernel(
    logical_ref, chosen_ref, page_total, q_ref, k_ref, v_ref, mix_ref, m_ref, l_ref, acc, top, total
):
    page = pl.program_id(1)
    tile_count = chosen_ref.shape[0]
    tile_rows = q_ref.shape[0] // tile_count
    group = q_ref.shape[1] // k_ref.shape[2]
    page_len = k_ref.shape[1]
    offset = page_len - q_ref.shape[0]
    f32 = jnp.float32

    @pl.when(page == 0)
    def _():
        acc[...] = jnp.zeros_like(acc)
        top[...] = jnp.full_like(top, masked_score)
        total[...] = jnp.zeros_like(total)

    causal = logical_ref[page] == page_total - 1

    def visit(t, masked):
        rows = slice(t * tile_rows, (t + 1) * tile_rows)
        for g in range(group):
            cols = slice(g * HEAD_SIZE, (g + 1) * HEAD_SIZE)
            scores = (
                lax.dot_general(
                    q_ref[rows, cols],
                    k_ref[0],
                    (((1,), (1,)), ((), ())),
                    preferred_element_type=f32,
                )
                * score_scale
            )
            if masked:
                position = offset + t * tile_rows + lax.broadcasted_iota(jnp.int32, scores.shape, 0)
                key = lax.broadcasted_iota(jnp.int32, scores.shape, 1)
                scores = jnp.where(key <= position, scores, masked_score)
            old = top[g, rows, :1]
            new = jnp.maximum(old, jnp.max(scores, axis=1, keepdims=True))
            weights = jnp.exp(scores - new)
            keep = jnp.exp(old - new)
            total[g, rows] = total[g, rows] * keep + jnp.sum(weights, axis=1, keepdims=True)
            top[g, rows] = jnp.broadcast_to(new, (tile_rows, 128))
            acc[rows, cols] = acc[rows, cols] * keep + jnp.dot(
                weights.astype(jnp.bfloat16), v_ref[0], preferred_element_type=f32
            )

    for t in range(tile_count):
        picked = chosen_ref[t, page] != 0
        pl.when(jnp.logical_and(picked, causal))(functools.partial(visit, t, True))
        pl.when(jnp.logical_and(picked, jnp.logical_not(causal)))(
            functools.partial(visit, t, False)
        )

    @pl.when(page == pl.num_programs(1) - 1)
    def _():
        mix_ref[...] = acc[...].astype(jnp.bfloat16)
        lane = lax.broadcasted_iota(jnp.int32, m_ref.shape[1:], 1)
        maxima = jnp.zeros(m_ref.shape[1:], f32)
        sums = jnp.zeros(m_ref.shape[1:], f32)
        for g in range(group):
            maxima = jnp.where(lane == g, top[g], maxima)
            sums = jnp.where(lane == g, total[g], sums)
        m_ref[0] = maxima
        l_ref[0] = sums


def owner_pass(queries, keys, values, page_map, selected, ctx_index, ctx_count):
    pages_local, page_len, kv_width = keys.shape
    row_count, query_width = queries.shape
    kv_local = kv_width // HEAD_SIZE
    group = query_width // kv_width
    tile_count = selected.shape[0]
    page_total = pages_local * ctx_count
    slot_ids = ctx_index * pages_local + jnp.arange(pages_local, dtype=jnp.int32)
    all_pages = jnp.arange(page_total, dtype=jnp.int32)
    logical = jnp.sum(
        jnp.where(page_map[None, :] == slot_ids[:, None], all_pages[None, :], 0), axis=1
    )
    chosen = jnp.any(selected[:, None, :] == logical[None, :, None], axis=2).astype(jnp.int32)
    stat = jax.ShapeDtypeStruct((kv_local, row_count, 128), jnp.float32)
    stat_spec = pl.BlockSpec((1, row_count, 128), lambda k, p, a, b: (k, 0, 0))
    kv_spec = pl.BlockSpec((1, page_len, HEAD_SIZE), lambda k, p, a, b: (p, 0, k))
    q_spec = pl.BlockSpec((row_count, group * HEAD_SIZE), lambda k, p, a, b: (0, k))

    def kernel(logical_ref, chosen_ref, *refs):
        attention_kernel(logical_ref, chosen_ref, page_total, *refs)

    mixture, top, total = pl.pallas_call(
        kernel,
        grid_spec=pltpu.PrefetchScalarGridSpec(
            num_scalar_prefetch=2,
            grid=(kv_local, pages_local),
            in_specs=[q_spec, kv_spec, kv_spec],
            out_specs=(q_spec, stat_spec, stat_spec),
            scratch_shapes=[
                pltpu.VMEM((row_count, group * HEAD_SIZE), jnp.float32),
                pltpu.VMEM((group, row_count, 128), jnp.float32),
                pltpu.VMEM((group, row_count, 128), jnp.float32),
            ],
        ),
        out_shape=(jax.ShapeDtypeStruct((row_count, query_width), jnp.bfloat16), stat, stat),
    )(logical.astype(jnp.int32), chosen, queries, keys, values)

    def heads(stacked):
        return stacked[:, :, :group].transpose(1, 0, 2).reshape(row_count, kv_local * group)

    return heads(top), heads(total), mixture


MESH = pl.DeviceIdType.MESH
CORES = 2


def column_tile(width):
    for tile in (896, 768, 640, 512, 384, 256, 128):
        if width % tile == 0:
            return tile
    return width


def flat(block, rows):
    if block.shape[1] % 16:
        return block.astype(jnp.float32).reshape(rows, -1).astype(jnp.bfloat16)
    return block.reshape(rows, -1)


def tail_kernel(
    C,
    H,
    mix_ref,
    stat_ref,
    res_ref,
    gain_ref,
    ow_hbm,
    gw_hbm,
    uw_hbm,
    dw_hbm,
    mlp_ref,
    own_ref,
    ow,
    gw,
    uw,
    dw,
    mix_in,
    stat_in,
    att,
    po,
    po_in,
    u_out,
    st_out,
    ss,
    ublk,
    own_st,
    first,
    first_in,
    second,
    second_in,
    hid,
    acc,
    part,
    part_in,
    w_sem,
    mix_s,
    mix_r,
    stat_s,
    stat_r,
    att_s,
    att_r,
    po_s,
    po_r,
    u_s,
    u_r,
    st_s,
    st_r,
    ss_s,
    ss_r,
    f_s,
    f_r,
    g_s,
    g_r,
    h_s,
    h_r,
    fw_s,
    part_s,
    part_r,
):
    c = lax.axis_index("ctx")
    h = lax.axis_index("head")
    Y = H // CORES
    y = h // CORES
    core = h % CORES
    partner = y * CORES + (CORES - 1 - core)
    R = mix_ref.shape[1]
    rows = C * R
    rb = C // H
    bph = C // H
    width = ow.shape[0]
    head_rows = rows // H
    heads = mix_ref.shape[2] // HEAD_SIZE
    tiles, _, _, _, _, tile = first.shape
    f32 = jnp.float32
    bf16 = jnp.bfloat16

    def remote(src, dst, send_sem, recv_sem, ctx, head):
        return pltpu.make_async_remote_copy(
            src_ref=src,
            dst_ref=dst,
            send_sem=send_sem,
            recv_sem=recv_sem,
            device_id=(ctx, head),
            device_id_type=MESH,
        )

    sent = []

    def send(*args):
        copy = remote(*args)
        copy.start()
        sent.append(copy)

    loads = [
        pltpu.make_async_copy(src, dst, w_sem.at[i])
        for i, (src, dst) in enumerate(
            ((ow_hbm, ow), (gw_hbm, gw), (uw_hbm, uw), (dw_hbm, dw))
        )
    ]
    for load in loads:
        load.start()

    for d in range(1, C):
        peer = (c + d) % C
        send(stat_ref.at[peer], stat_in.at[c], stat_s.at[d], stat_r.at[c], peer, h)
        send(mix_ref.at[peer], mix_in.at[c], mix_s.at[d], mix_r.at[c], peer, h)
    stat_in[c] = stat_ref[c]
    mix_in[c] = mix_ref[c]
    for d in range(1, C):
        peer = (c + C - d) % C
        remote(stat_in.at[peer], stat_in.at[peer], stat_s.at[d], stat_r.at[peer], peer, h).wait_recv()
        remote(mix_in.at[peer], mix_in.at[peer], mix_s.at[d], mix_r.at[peer], peer, h).wait_recv()
    maxima = [stat_in[k][:, :heads] for k in range(C)]
    top = functools.reduce(jnp.maximum, maxima)
    scales = [jnp.exp(m - top) for m in maxima]
    total = sum(stat_in[k][:, heads : 2 * heads] * scales[k] for k in range(C))
    inverse = 1.0 / total
    for g in range(heads):
        cols = slice(g * HEAD_SIZE, (g + 1) * HEAD_SIZE)
        mixed = sum(mix_in[k, :, cols].astype(f32) * scales[k][:, g : g + 1] for k in range(C))
        att[c, :, cols] = (mixed * inverse[:, g : g + 1]).astype(bf16)

    for d in range(1, C):
        peer = (c + d) % C
        send(att.at[c], att.at[c], att_s.at[d], att_r.at[c], peer, h)
    loads[0].wait()
    for d in range(1, C):
        peer = (c + C - d) % C
        remote(att.at[peer], att.at[peer], att_s.at[d], att_r.at[peer], peer, h).wait_recv()
    projected = lax.dot_general(
        flat(att[...], rows), ow[...], (((1,), (1,)), ((), ())), preferred_element_type=f32
    )
    po[...] = projected.reshape(H, head_rows, width).astype(bf16)

    for d in range(1, H):
        peer = (h + d) % H
        send(po.at[peer], po_in.at[h], po_s.at[d], po_r.at[h], c, peer)
    po_in[h] = po[h]
    for d in range(1, H):
        peer = (h + H - d) % H
        remote(po_in.at[peer], po_in.at[peer], po_s.at[d], po_r.at[peer], c, peer).wait_recv()
    projected = sum(po_in[k].astype(f32) for k in range(H))
    stream = (res_ref[...].astype(f32) + projected).astype(bf16).astype(f32)
    st_out[...] = stream.reshape(rb, R, width).astype(bf16)
    u_out[...] = (stream * gain_ref[...]).reshape(rb, R, width).astype(bf16)
    squares = jnp.sum(stream * stream, axis=1, keepdims=True)
    ss[c] = jnp.broadcast_to(squares, (head_rows, 128))

    block_head = c // bph
    block_part = c % bph
    u_dst = ublk.at[block_part, pl.ds(h * rb, rb)]
    kept = []
    for d in range(C):
        peer = (c + d) % C
        copy = remote(u_out, u_dst, u_s.at[d], u_r.at[block_part, h], peer, block_head)
        if d == 0:
            kept.append((block_head != h, copy))
            pl.when(block_head != h)(copy.start)

            @pl.when(block_head == h)
            def _():
                ublk[block_part, pl.ds(h * rb, rb)] = u_out[...]

        else:
            copy.start()
            sent.append(copy)
    for d in range(1, C):
        peer = (c + d) % C
        send(ss.at[c], ss.at[c], ss_s.at[d], ss_r.at[c], peer, h)
    for i in range(rb):
        owner = h * rb + i
        other = jnp.logical_or(owner != c, block_head != h)
        copy = remote(
            st_out.at[i], own_st.at[block_part], st_s.at[i], st_r.at[block_part], owner, block_head
        )
        kept.append((other, copy))
        pl.when(other)(copy.start)

        @pl.when(jnp.logical_not(other))
        def _(i=i):
            own_st[block_part] = st_out[i]

    for j in range(bph):
        for k in range(H):
            source = h * bph + j
            block = ublk.at[j, pl.ds(k * rb, rb)]
            arrival = remote(block, block, u_s.at[0], u_r.at[j, k], source, k)
            pl.when(jnp.logical_or(source != c, h != k))(arrival.wait_recv)
    loads[1].wait()
    loads[2].wait()

    def matmul(i, which, weight):
        cols = slice(i * tile, (i + 1) * tile)
        value = None
        for j in range(bph):
            term = jnp.dot(
                flat(ublk[j], rows),
                weight[j * width : (j + 1) * width, cols],
                preferred_element_type=f32,
            )
            value = term if value is None else value + term
        first[i, which] = value.reshape(Y, CORES, head_rows, tile).swapaxes(0, 1).astype(bf16)
        send(
            first.at[i, which, CORES - 1 - core],
            first_in.at[i, which],
            f_s.at[i, which],
            f_r.at[i, which],
            c,
            partner,
        )

    def middle(i, which):
        remote(
            first_in.at[i, which], first_in.at[i, which], f_s.at[i, which], f_r.at[i, which], c, partner
        ).wait_recv()
        both = first[i, which, core].astype(f32) + first_in[i, which].astype(f32)
        second[i, which] = both.astype(bf16)
        for d in range(1, Y):
            peer = (y + d) % Y
            send(
                second.at[i, which, peer],
                second_in.at[i, which, y],
                g_s.at[i, which, d],
                g_r.at[i, which, y],
                c,
                peer * CORES + core,
            )

    def finish(i, inverse_rms):
        sums = []
        for which in range(2):
            value = second[i, which, y].astype(f32)
            for d in range(1, Y):
                peer = (y + Y - d) % Y
                slot = second_in.at[i, which, peer]
                remote(
                    slot, slot, g_s.at[i, which, d], g_r.at[i, which, peer], c, peer * CORES + core
                ).wait_recv()
                value = value + second_in[i, which, peer].astype(f32)
            sums.append(value * inverse_rms)
        hid[i, h] = (jax.nn.gelu(sums[0], approximate=True) * sums[1]).astype(bf16)
        send(hid.at[i, h], hid.at[i, h], h_s.at[i, 0], h_r.at[i, h], c, partner)
        for d in range(1, Y):
            peer = ((y + d) % Y) * CORES + core
            send(hid.at[i, h], hid.at[i, h], h_s.at[i, d], h_r.at[i, h], c, peer)

    def forward(i):
        for d in range(1, Y):
            origin = ((y + Y - d) % Y) * CORES + core
            slot = hid.at[i, origin]
            remote(slot, slot, h_s.at[i, d], h_r.at[i, origin], c, origin).wait_recv()
            send(slot, slot, fw_s.at[i, d], h_r.at[i, origin], c, partner)

    def down(i):
        for d in range(Y):
            origin = ((y + Y - d) % Y) * CORES + (CORES - 1 - core)
            slot = hid.at[i, origin]
            remote(slot, slot, h_s.at[i, 0], h_r.at[i, origin], c, partner).wait_recv()
        term = lax.dot_general(
            flat(hid[i], rows),
            dw[:, i * tile : (i + 1) * tile],
            (((1,), (1,)), ((), ())),
            preferred_element_type=f32,
        )
        if i == 0:
            acc[...] = term
        else:
            acc[...] += term

    steps = [(i, which) for i in range(tiles) for which in range(2)]
    for n, (i, which) in enumerate(steps):
        matmul(i, which, (gw, uw)[which])
        if n:
            middle(*steps[n - 1])
    middle(*steps[-1])
    for d in range(1, C):
        peer = (c + C - d) % C
        remote(ss.at[peer], ss.at[peer], ss_s.at[d], ss_r.at[peer], peer, h).wait_recv()
    squares = sum(ss[k] for k in range(C))
    inverse_rms = lax.rsqrt(squares[:, :1] / (C * width) + norm_epsilon)
    loads[3].wait()
    for i in range(tiles):
        finish(i, inverse_rms)
        if i:
            forward(i - 1)
    forward(tiles - 1)
    for i in range(tiles):
        down(i)
    part[...] = acc[...].reshape(C, R, acc.shape[1]).astype(bf16)

    for d in range(1, C):
        peer = (c + d) % C
        send(part.at[peer], part_in.at[c], part_s.at[d], part_r.at[c], peer, h)
    part_in[c] = part[c]
    for j in range(bph):
        source = h * bph + j
        arrival = remote(own_st.at[j], own_st.at[j], st_s.at[0], st_r.at[j], source, c // rb)
        pl.when(jnp.logical_or(source != c, c // rb != h))(arrival.wait_recv)
    own_ref[...] = own_st[...]
    for d in range(1, C):
        peer = (c + C - d) % C
        remote(part_in.at[peer], part_in.at[peer], part_s.at[d], part_r.at[peer], peer, h).wait_recv()
    mlp_ref[...] = sum(part_in[k].astype(f32) for k in range(C))
    for copy in sent:
        copy.wait_send()
    for condition, copy in kept:
        pl.when(condition)(copy.wait_send)


def tail(C, H, mixture, stats, residual_in, norm_gain, out_weight, gate_weight, up_weight, down_weight):
    rows, query_width = mixture.shape
    R = rows // C
    width = out_weight.shape[1]
    hidden = gate_weight.shape[1]
    out_width = down_weight.shape[1]
    out_weight = out_weight.T
    down_weight = down_weight.T
    rb = C // H
    bph = C // H
    Y = H // CORES
    head_rows = rows // H
    tile = column_tile(hidden)
    tiles = hidden // tile
    bf16 = jnp.bfloat16
    vmem = pl.BlockSpec(memory_space=pltpu.VMEM)
    hbm = pl.BlockSpec(memory_space=pl.ANY)
    V = pltpu.VMEM
    S = pltpu.SemaphoreType.DMA
    return pl.pallas_call(
        functools.partial(tail_kernel, C, H),
        out_shape=(
            jax.ShapeDtypeStruct((R, out_width), jnp.float32),
            jax.ShapeDtypeStruct((bph, R, width), bf16),
        ),
        in_specs=[vmem] * 4 + [hbm] * 4,
        out_specs=(vmem, vmem),
        scratch_shapes=[
            V(out_weight.shape, bf16),
            V(gate_weight.shape, bf16),
            V(up_weight.shape, bf16),
            V(down_weight.shape, bf16),
            V((C, R, query_width), bf16),
            V((C, R, 128), jnp.float32),
            V((C, R, query_width), bf16),
            V((H, head_rows, width), bf16),
            V((H, head_rows, width), bf16),
            V((rb, R, width), bf16),
            V((rb, R, width), bf16),
            V((C, head_rows, 128), jnp.float32),
            V((bph, C, R, width), bf16),
            V((bph, R, width), bf16),
            V((tiles, 2, CORES, Y, head_rows, tile), bf16),
            V((tiles, 2, Y, head_rows, tile), bf16),
            V((tiles, 2, Y, head_rows, tile), bf16),
            V((tiles, 2, Y, head_rows, tile), bf16),
            V((tiles, H, head_rows, tile), bf16),
            V((rows, out_width), jnp.float32),
            V((C, R, out_width), bf16),
            V((C, R, out_width), bf16),
            S((4,)),
            S((C,)),
            S((C,)),
            S((C,)),
            S((C,)),
            S((C,)),
            S((C,)),
            S((H,)),
            S((H,)),
            S((C,)),
            S((bph, H)),
            S((rb,)),
            S((bph,)),
            S((C,)),
            S((C,)),
            S((tiles, 2)),
            S((tiles, 2)),
            S((tiles, 2, Y)),
            S((tiles, 2, Y)),
            S((tiles, Y)),
            S((tiles, H)),
            S((tiles, Y)),
            S((C,)),
            S((C,)),
        ],
        compiler_params=pltpu.CompilerParams(
            has_side_effects=True, vmem_limit_bytes=60 * 2**20
        ),
    )(
        mixture.reshape(C, R, query_width),
        stats.reshape(C, R, 128),
        residual_in,
        norm_gain.reshape(1, width),
        out_weight,
        gate_weight,
        up_weight,
        down_weight,
    )


LOG2E = 1.4426950408889634


def fused_kernel(
    C,
    H,
    NP,
    map_hbm,
    sel_hbm,
    q_hbm,
    res_hbm,
    gain_hbm,
    k_hbm,
    v_hbm,
    ow_hbm,
    gw_hbm,
    uw_hbm,
    dw_hbm,
    out_ref,
    map_ref,
    sel_ref,
    q_ref,
    res_ref,
    gain_ref,
    k_buf,
    v_buf,
    ow,
    gw,
    uw,
    dw,
    mix_out,
    mix_in,
    lse_out,
    lse_in,
    att,
    po_out,
    po_in,
    res_in,
    st,
    u,
    ss_out,
    ss_in,
    ss_mid,
    ss_last,
    scale,
    begun,
    first,
    first_in,
    second,
    second_in,
    hid,
    acc,
    part,
    part_in,
    in_sem,
    kv_sem,
    w_sem,
    mix_s,
    mix_r,
    lse_s,
    lse_r,
    att_s,
    att_r,
    cross_r,
    po_s,
    po_r,
    res_s,
    res_r,
    u_s,
    u_r,
    ss_s,
    ss_r,
    f_s,
    f_r,
    g_s,
    g_r,
    h_s,
    h_r,
    part_s,
    part_r,
):
    c = lax.axis_index("ctx")
    h = lax.axis_index("head")
    X = C // H
    Z = C // X
    z = c // X
    x = c % X
    Y = H // CORES
    y = h // CORES
    core = h % CORES
    partner = y * CORES + (CORES - 1 - core)
    _, NQ, RC, query_width = q_ref.shape
    rows = C * RC
    hr = rows // H
    kv, pages, page_len, _ = k_buf.shape
    group = query_width // (kv * HEAD_SIZE)
    gw_cols = group * HEAD_SIZE
    tile_count = sel_ref.shape[0]
    tile_rows = NQ * rows // tile_count
    offset = page_len - NQ * rows
    page_total = map_ref.shape[0]
    width = ow.shape[0]
    tile = first.shape[-1]
    tiles = first.shape[1]
    RP = rows // NP
    f32 = jnp.float32
    bf16 = jnp.bfloat16
    owner = h == z
    visitor = h != z

    def remote(src, dst, send_sem, recv_sem, ctx, head):
        return pltpu.make_async_remote_copy(
            src_ref=src,
            dst_ref=dst,
            send_sem=send_sem,
            recv_sem=recv_sem,
            device_id=(ctx, head),
            device_id_type=MESH,
        )

    sent = []
    kept = []

    def start(*args):
        remote(*args).start()

    def send(*args):
        copy = remote(*args)
        copy.start()
        sent.append(copy)

    def send_if(condition, *args):
        copy = remote(*args)
        pl.when(condition)(copy.start)
        kept.append((condition, copy))

    def kv_load(j):
        lanes = pl.ds(pl.multiple_of(j * HEAD_SIZE, HEAD_SIZE), HEAD_SIZE)
        return (
            pltpu.make_async_copy(k_hbm.at[:, :, lanes], k_buf.at[j], kv_sem.at[0, j]),
            pltpu.make_async_copy(v_hbm.at[:, :, lanes], v_buf.at[j], kv_sem.at[1, j]),
        )

    barrier = pltpu.get_barrier_semaphore()
    for d in range(1, C):
        pl.semaphore_signal(
            barrier, inc=1, device_id=((c + d) % C, h), device_id_type=MESH
        )
    for d in range(1, H):
        pl.semaphore_signal(
            barrier, inc=1, device_id=(c, (h + d) % H), device_id_type=MESH
        )
    inputs = [
        pltpu.make_async_copy(src, dst, in_sem.at[i])
        for i, (src, dst) in enumerate(
            (
                (map_hbm, map_ref),
                (sel_hbm, sel_ref),
                (q_hbm, q_ref),
                (res_hbm, res_ref),
                (gain_hbm, gain_ref.at[0]),
            )
        )
    ]
    for load in inputs:
        load.start()
    for load in kv_load(0):
        load.start()
    loads = [
        pltpu.make_async_copy(src, dst, w_sem.at[i])
        for i, (src, dst) in enumerate(
            ((ow_hbm, ow), (gw_hbm, gw), (uw_hbm, uw), (dw_hbm, dw))
        )
    ]
    for load in inputs[:3]:
        load.wait()

    facts = []
    for p in range(pages):
        slot = c * pages + p
        logical = jnp.int32(0)
        for j in range(page_total):
            logical = logical + jnp.where(map_ref[j] == slot, j, 0)
        picks = []
        for t in range(tile_count):
            hits = jnp.int32(0)
            for i in range(sel_ref.shape[1]):
                hits = hits + jnp.where(sel_ref[t, i] == logical, 1, 0)
            picks.append(jnp.where(hits > 0, 0.0, masked_score).astype(f32))
        reach = jnp.where(logical == page_total - 1, 0, page_len)
        facts.append((reach, picks))

    index = lax.broadcasted_iota(jnp.int32, (group * rows, 1), 0) & (rows - 1)
    shift = RC.bit_length() - 1
    base_row = (index >> shift) * (NQ * RC) + (index & (RC - 1))
    eye = lax.broadcasted_iota(jnp.int32, (rows, rows), 0) == lax.broadcasted_iota(
        jnp.int32, (rows, rows), 1
    )
    unit = score_scale * LOG2E

    def attend(n):
        q = n // kv
        j = n % kv

        @pl.when(n < kv)
        def _():
            for load in kv_load(j):
                load.wait()

        @pl.when(n == 0)
        def _():
            for k in range(1, kv):
                for load in kv_load(k):
                    load.start()
            for load in loads:
                load.start()

        lanes = pl.ds(pl.multiple_of(j * gw_cols, gw_cols), gw_cols)
        block = q_ref[:, q, :, lanes].reshape(rows, gw_cols)
        lhs = jnp.concatenate(
            [block[:, g * HEAD_SIZE : (g + 1) * HEAD_SIZE] for g in range(group)], axis=0
        )
        row = base_row + q * RC
        key = offset + lax.broadcasted_iota(jnp.int32, (group * rows, page_len - offset), 1)
        tops, sums, outs = [], [], []
        for p in range(pages):
            reach, picks = facts[p]
            bias = jnp.zeros((group * rows, 1), f32)
            for t in range(tile_count):
                inside = jnp.logical_and(row >= t * tile_rows, row < (t + 1) * tile_rows)
                bias = jnp.where(inside, picks[t], bias)
            scores = lax.dot_general(
                lhs, k_buf[j, p], (((1,), (1,)), ((), ())), preferred_element_type=f32
            )
            late = jnp.where(key <= offset + row + reach, scores[:, offset:], masked_score)
            scores = jnp.concatenate([scores[:, :offset], late], axis=1)
            top = jnp.max(scores, axis=1, keepdims=True)
            weights = jnp.exp2((scores - top) * unit)
            sums.append(jnp.sum(weights, axis=1, keepdims=True))
            outs.append(
                jnp.dot(weights.astype(bf16), v_buf[j, p], preferred_element_type=f32)
            )
            tops.append(top * unit + bias)
        best = functools.reduce(jnp.maximum, tops)
        scales = [jnp.exp2(top - best) for top in tops]
        total = sum(s * e for s, e in zip(sums, scales))
        mixed = sum(o * (e / total) for o, e in zip(outs, scales))
        lse = best + jnp.log2(total)
        for g in range(group):
            part_rows = slice(g * rows, (g + 1) * rows)
            mix_out[n, :, :, g * HEAD_SIZE : (g + 1) * HEAD_SIZE] = (
                mixed[part_rows].reshape(C, RC, HEAD_SIZE).astype(bf16)
            )
            lse_out[n, g : g + 1] = jnp.sum(
                jnp.where(eye, lse[part_rows], 0.0), axis=0, keepdims=True
            )
        mix_in[n, c] = mix_out[n, c]
        lse_in[n, c] = lse_out[n]

    def mix_sends(n):
        for d in range(1, C):
            peer = (c + d) % C
            remote(mix_out.at[n, peer], mix_in.at[n, c], mix_s.at[0], mix_r.at[n], peer, h).start()
            remote(lse_out.at[n], lse_in.at[n, c], lse_s.at[0], lse_r.at[n], peer, h).start()

    def att_sends(n, direct):
        block = att.at[n, c]
        if direct:
            for d in range(1, C):
                start(block, block, att_s.at[0], att_r.at[n], (c + d) % C, h)
        else:
            for d in range(1, Z):
                start(block, block, att_s.at[0], att_r.at[n], (z + d) % Z * X + x, h)
            for d in range(1, X):
                start(block, block, att_s.at[0], cross_r.at[n - kv], z * X + (x + d) % X, h)

    def att_relay(n):
        arrived(att.at[n, pl.ds(0, Z - 1)], att_r.at[n])
        for e in range(1, Z):
            block = att.at[n, (z + e) % Z * X + x]
            for d in range(1, X):
                start(block, block, att_s.at[0], cross_r.at[n - kv], z * X + (x + d) % X, h)

    def arrived(block, recv_sem):
        remote(block, block, recv_sem, recv_sem, c, partner).wait_recv()

    def left(block, send_sem):
        remote(block, block, send_sem, send_sem, c, partner).wait_send()

    def combine(n, direct):
        arrived(lse_in.at[n, pl.ds(0, C - 1)], lse_r.at[n])
        arrived(mix_in.at[n, pl.ds(0, C - 1)], mix_r.at[n])
        logs = [lse_in[n, k] for k in range(C)]
        best = functools.reduce(jnp.maximum, logs)
        scales = [jnp.exp2(value - best) for value in logs]
        inverse = 1.0 / sum(scales)
        lane = lax.broadcasted_iota(jnp.int32, (RC, rows), 1)
        mine = lane == c * RC + lax.broadcasted_iota(jnp.int32, (RC, rows), 0)
        for g in range(group):
            cols = slice(g * HEAD_SIZE, (g + 1) * HEAD_SIZE)
            value = jnp.zeros((RC, HEAD_SIZE), f32)
            for k in range(C):
                share = (scales[k] * inverse)[g : g + 1]
                share = jnp.sum(jnp.where(mine, share, 0.0), axis=1, keepdims=True)
                value = value + share * mix_in[n, k, :, cols].astype(f32)
            att[n, c, :, cols] = value.astype(bf16)
        att_sends(n, direct)

    def project(q):
        for j in range(kv):
            n = q * kv + j
            if q == 0:
                arrived(att.at[n, pl.ds(0, C - 1)], att_r.at[n])
            else:
                arrived(att.at[n, pl.ds(0, (X - 1) * Z)], cross_r.at[n - kv])
        if q == 0:
            loads[0].wait()
        value = None
        for j in range(kv):
            term = lax.dot_general(
                att[q * kv + j].reshape(rows, gw_cols),
                ow[:, j * gw_cols : (j + 1) * gw_cols],
                (((1,), (1,)), ((), ())),
                preferred_element_type=f32,
            )
            value = term if value is None else value + term
        po_out[q] = value.astype(bf16)
        for i in range(NP):
            piece = pl.ds(i * RP, RP)
            copy = remote(
                po_out.at[q, piece], po_in.at[q, h, piece], po_s.at[q], po_r.at[q, i], c, z
            )
            pl.when(visitor)(copy.start)
        po_in[q, h] = po_out[q]

    def own(q, i):
        if q == 0 and i == 0:
            arrived(res_in.at[pl.ds(0, H - 1)], res_r.at[0])
        arrived(po_in.at[q, pl.ds(0, H - 1), pl.ds(i * RP, RP)], po_r.at[q, i])
        spare = u.shape[-1] - width
        lane = lax.broadcasted_iota(jnp.int32, (hr, spare), 1)
        for b in range(i * RP // hr, (i + 1) * RP // hr):
            span = slice(b * hr, (b + 1) * hr)
            value = res_in[b, :, q].reshape(hr, width).astype(f32)
            added = sum(po_in[q, k, span].astype(f32) for k in range(H))
            stream = (value + added).astype(bf16)
            st[q, span] = stream
            stream = stream.astype(f32)
            u[q, x, span, :width] = (stream * gain_ref[...]).astype(bf16)
            squares = jnp.sum(stream * stream, axis=1, keepdims=True)
            high = squares.astype(bf16).astype(f32)
            mid = (squares - high).astype(bf16).astype(f32)
            low = squares - high - mid
            packed = jnp.where(lane == 0, high, jnp.where(lane == 1, mid, low))
            packed = jnp.where(lane < 3, packed, 0.0)
            u[q, x, span, width:] = packed.astype(bf16)

    def relay(q, i, here):
        piece = u.at[q, x, pl.ds(i * RP, RP)]
        recv = u_r.at[q, x, i]
        pl.when(jnp.logical_and(here, visitor))(functools.partial(arrived, piece, recv))
        for way, ahead in enumerate((Z - 1 - z, z)):
            step = 1 - 2 * way
            go = jnp.logical_and(jnp.logical_and(here, step * (z - h) >= 0), ahead > 0)
            target = jnp.clip(z + step, 0, Z - 1) * X + x
            copy = remote(piece, piece, u_s.at[way], recv, target, h)
            pl.when(go)(copy.start)
            kept.append((go, copy))
        for d in range(1, X):
            peer = z * X + (x + d) % X
            copy = remote(piece, piece, u_s.at[1 + d], recv, peer, h)
            pl.when(here)(copy.start)
            kept.append((here, copy))

    def spread(q, here):
        for i in range(NP):
            pl.when(jnp.logical_and(here, owner))(functools.partial(own, q, i))
            relay(q, i, here)

    def gather(q):
        for d in range(1, X):
            source = (x + d) % X
            for i in range(NP):
                block = u.at[q, source, pl.ds(i * RP, RP)]
                arrived(block, u_r.at[q, source, i])
        squares = 0.0
        for k in range(X):
            split = u[q, k, :, width:].astype(f32)
            squares = squares + jnp.sum(split, axis=1, keepdims=True)
        squares = jnp.broadcast_to(squares, (rows, 128)).reshape(Y, CORES, hr, 128)
        ss_out[q] = squares.swapaxes(0, 1)
        send(ss_out.at[q, CORES - 1 - core], ss_in.at[q], ss_s.at[q, 0], ss_r.at[q, 0], c, partner)

    def block_dot(q, k, i, which):
        weight = (gw, uw)[which]
        span = pl.ds(pl.multiple_of(k * width, 16), width)
        return jnp.dot(
            u[q, k, :, :width],
            weight[span, i * tile : (i + 1) * tile],
            preferred_element_type=f32,
        )

    def start_expand(q):
        if q == 0:
            loads[1].wait()
            loads[2].wait()
        for i in range(tiles):
            for which in range(2):
                begun[i, which] = block_dot(q, x, i, which)

    def matmul(q, i, which):
        value = begun[i, which]
        for d in range(1, X):
            value = value + block_dot(q, (x + d) % X, i, which)
        value = value.reshape(Y, CORES, hr, tile).swapaxes(0, 1).astype(bf16)
        first[q, i, which] = value
        start(
            first.at[q, i, which, CORES - 1 - core],
            first_in.at[q, i, which],
            f_s.at[0],
            f_r.at[q, i, which],
            c,
            partner,
        )

    def middle(q, i, which):
        block = first_in.at[q, i, which]
        arrived(block, f_r.at[q, i, which])
        both = first[q, i, which, core].astype(f32) + first_in[q, i, which].astype(f32)
        second[q, i, which] = both.astype(bf16)
        for d in range(1, Y):
            peer = (y + d) % Y
            start(
                second.at[q, i, which, peer],
                second_in.at[q, i, which, y],
                g_s.at[0],
                g_r.at[q, i, which, y],
                c,
                peer * CORES + core,
            )

    def middle_squares(q):
        block = ss_in.at[q]
        remote(block, block, ss_s.at[q, 0], ss_r.at[q, 0], c, partner).wait_recv()
        ss_mid[q] = ss_out[q, core] + ss_in[q]
        for d in range(1, Y):
            peer = (y + d) % Y
            send(
                ss_mid.at[q, peer],
                ss_last.at[q, y],
                ss_s.at[q, d],
                ss_r.at[q, 1 + y],
                c,
                peer * CORES + core,
            )

    def inverse_rms(q):
        total = ss_mid[q, y]
        for d in range(1, Y):
            peer = (y + Y - d) % Y
            block = ss_last.at[q, peer]
            remote(
                block, block, ss_s.at[q, d], ss_r.at[q, 1 + peer], c, peer * CORES + core
            ).wait_recv()
            total = total + ss_last[q, peer]
        scale[q] = lax.rsqrt(total / (C * width) + norm_epsilon)

    def finish(q, i):
        inverse = scale[q][:, :1]
        sums = []
        for which in range(2):
            value = second[q, i, which, y].astype(f32)
            for d in range(1, Y):
                peer = (y + Y - d) % Y
                block = second_in.at[q, i, which, peer]
                remote(
                    block,
                    block,
                    g_s.at[0],
                    g_r.at[q, i, which, peer],
                    c,
                    peer * CORES + core,
                ).wait_recv()
                value = value + second_in[q, i, which, peer].astype(f32)
            sums.append(value * inverse)
        hid[q, i, h] = (jax.nn.gelu(sums[0], approximate=True) * sums[1]).astype(bf16)
        block = hid.at[q, i, h]
        for d in range(1, Y):
            peer = ((y + d) % Y) * CORES + core
            start(block, block, h_s.at[0], h_r.at[q, i, h], c, peer)
        start(block, block, h_s.at[0], h_r.at[q, i, h], c, partner)

    def forward(q, i):
        for d in range(1, Y):
            origin = ((y + Y - d) % Y) * CORES + core
            block = hid.at[q, i, origin]
            arrived(block, h_r.at[q, i, origin])
            start(block, block, h_s.at[0], h_r.at[q, i, origin], c, partner)

    def down(q, i):
        for d in range(Y):
            origin = ((y + Y - d) % Y) * CORES + (CORES - 1 - core)
            block = hid.at[q, i, origin]
            arrived(block, h_r.at[q, i, origin])
        if q == 0 and i == 0:
            loads[3].wait()
        term = lax.dot_general(
            hid[q, i].reshape(rows, tile),
            dw[:, i * tile : (i + 1) * tile],
            (((1,), (1,)), ((), ())),
            preferred_element_type=f32,
        )
        if i == 0:
            acc[...] = term
        else:
            acc[...] += term

    def scatter(q):
        for k in range(X):

            @pl.when(jnp.logical_and(owner, x == k))
            def _(k=k):
                acc[:, k * width : (k + 1) * width] += st[q].astype(f32)

        part[q] = acc[...].reshape(C, RC, acc.shape[1]).astype(bf16)
        for d in range(1, C):
            peer = (c + d) % C
            start(part.at[q, peer], part_in.at[q, c], part_s.at[0], part_r.at[q], peer, h)
        part_in[q, c] = part[q, c]

    def collect(q):
        arrived(part_in.at[q, pl.ds(0, C - 1)], part_r.at[q])
        out_ref[q] = sum(part_in[q, k].astype(f32) for k in range(C)).astype(bf16)

    steps = NQ * kv
    lag = 3

    def loop(n, carry):
        attend(n)

        @pl.when(n == 1)
        def _():
            pl.semaphore_wait(barrier, C + H - 2)
            mix_sends(0)

        ready = jnp.logical_and(n >= 1, n < kv)
        pl.when(jnp.logical_or(ready, n >= kv + lag))(functools.partial(mix_sends, n))

        for k in range(kv):

            @pl.when(n == (kv + lag - 2 if k == kv - 1 else max(k + 2, lag)))
            def _(k=k):
                combine(k, True)

        @pl.when(n == kv + lag - 1)
        def _():
            for k in range(kv, kv + lag):
                mix_sends(k)

        return carry

    lax.fori_loop(0, steps, loop, 0)
    for load in inputs[3:]:
        load.wait()
    send_if(visitor, res_ref, res_in.at[h], res_s.at[0], res_r.at[0], c, z)
    res_in[h] = res_ref[...]
    pairs = [(i, which) for i in range(tiles) for which in range(2)]

    def expand(q, extra=None):
        gather(q)
        for n, (i, which) in enumerate(pairs):
            matmul(q, i, which)
            if n == 1:
                middle_squares(q)
            if n:
                middle(q, *pairs[n - 1])
            if extra is not None and which:
                extra(i)
        middle(q, *pairs[-1])

    def finish_if(here, q, i):
        @pl.when(here)
        def _():
            if i == 0:
                inverse_rms(q)
            finish(q, i)

    def contract(q, done=0):
        forward(q, done)
        for i in range(done, tiles):
            if i + 1 < tiles:
                forward(q, i + 1)
            down(q, i)
        scatter(q)

    def between(i):
        finish_if(early, 0, i)
        if i:

            @pl.when(late)
            def _():
                forward(0, i - 1)
                down(0, i - 1)


    far = jnp.maximum(z - h, h - z)
    early = z // CORES == y
    late = z // CORES != y
    project(0)
    for n in range(kv, steps - 2):
        combine(n, False)
    spread(0, far == 0)
    for n in range(steps - 2, steps):
        combine(n, False)
    for n in range(kv, steps - 2):
        att_relay(n)
    spread(0, far == 1)
    for n in range(steps - 2, steps):
        att_relay(n)
    pl.when(far <= 1)(lambda: start_expand(0))
    spread(0, far == 2)
    project(1)
    spread(0, far > 2)
    pl.when(far > 1)(lambda: start_expand(0))
    expand(0, lambda i: spread(1, far == 0) if i == tiles - 1 else None)
    first_on = jnp.logical_and(late, far <= 2)
    spread(1, first_on)
    for i in range(tiles):
        finish_if(late, 0, i)
    spread(1, jnp.logical_and(jnp.logical_not(first_on), far > 0))
    start_expand(1)
    expand(1, between)
    for i in range(tiles - 1):
        finish_if(late, 1, i)
    pl.when(late)(lambda: contract(0, tiles - 1))
    finish_if(late, 1, tiles - 1)
    pl.when(early)(lambda: contract(0))
    for i in range(tiles):
        finish_if(early, 1, i)
    contract(1)
    for q in range(NQ):
        collect(q)

    left(mix_out.at[:, pl.ds(0, C - 1)], mix_s.at[0])
    left(lse_in.at[:, pl.ds(0, C - 1)], lse_s.at[0])
    left(att.at[:, pl.ds(0, C - 1)], att_s.at[0])
    left(first_in, f_s.at[0])
    left(second.at[:, :, :, pl.ds(0, Y - 1)], g_s.at[0])
    left(hid.at[:, :, pl.ds(0, 2 * Y - 1)], h_s.at[0])
    left(part.at[:, pl.ds(0, C - 1)], part_s.at[0])
    for q in range(NQ):
        pl.when(visitor)(functools.partial(left, po_out.at[q], po_s.at[q]))
    for copy in sent:
        copy.wait_send()
    for condition, copy in kept:
        pl.when(condition)(copy.wait_send)


def fused(
    C,
    H,
    queries,
    keys,
    values,
    page_map,
    selected,
    residual_in,
    out_weight,
    norm_gain,
    gate_weight,
    up_weight,
    down_weight,
):
    row_count, query_width = queries.shape
    pages, page_len, kv_width = keys.shape
    kv = kv_width // HEAD_SIZE
    group = query_width // kv_width
    NQ = row_count // 128
    RC = row_count // C // NQ
    rows = C * RC
    NP = 4
    X = C // H
    Y = H // CORES
    hr = rows // H
    width = out_weight.shape[1]
    hidden = gate_weight.shape[1]
    out_width = down_weight.shape[1]
    tile = column_tile(hidden)
    tiles = hidden // tile
    steps = NQ * kv
    u_width = (width + 127) // 128 * 128
    bf16 = jnp.bfloat16
    f32 = jnp.float32
    vmem = pl.BlockSpec(memory_space=pltpu.VMEM)
    hbm = pl.BlockSpec(memory_space=pl.ANY)
    V = pltpu.VMEM
    S = pltpu.SemaphoreType.DMA
    out_weight = out_weight.T
    down_weight = down_weight.T
    mixes = V((steps, C, RC, group * HEAD_SIZE), bf16)
    return pl.pallas_call(
        functools.partial(fused_kernel, C, H, NP),
        out_shape=pltpu.VMEM((NQ, RC, out_width), bf16),
        in_specs=[hbm] * 11,
        out_specs=vmem,
        scratch_shapes=[
            pltpu.SMEM(page_map.shape, jnp.int32),
            pltpu.SMEM(selected.shape, jnp.int32),
            V((C, NQ, RC, query_width), bf16),
            V((X, NQ, RC, width), bf16),
            V((1, width), f32),
            V((kv, pages, page_len, HEAD_SIZE), bf16),
            V((kv, pages, page_len, HEAD_SIZE), bf16),
            V(out_weight.shape, bf16),
            V(gate_weight.shape, bf16),
            V(up_weight.shape, bf16),
            V(down_weight.shape, bf16),
            mixes,
            mixes,
            V((steps, group, rows), f32),
            V((steps, C, group, rows), f32),
            mixes,
            V((NQ, rows, width), bf16),
            V((NQ, H, rows, width), bf16),
            V((H, X, NQ, RC, width), bf16),
            V((NQ, rows, width), bf16),
            V((NQ, X, rows, u_width), bf16),
            V((NQ, CORES, Y, hr, 128), f32),
            V((NQ, Y, hr, 128), f32),
            V((NQ, Y, hr, 128), f32),
            V((NQ, Y, hr, 128), f32),
            V((NQ, hr, 128), f32),
            V((tiles, 2, rows, tile), f32),
            V((NQ, tiles, 2, CORES, Y, hr, tile), bf16),
            V((NQ, tiles, 2, Y, hr, tile), bf16),
            V((NQ, tiles, 2, Y, hr, tile), bf16),
            V((NQ, tiles, 2, Y, hr, tile), bf16),
            V((NQ, tiles, H, hr, tile), bf16),
            V((rows, out_width), f32),
            V((NQ, C, RC, out_width), bf16),
            V((NQ, C, RC, out_width), bf16),
            S((5,)),
            S((2, kv)),
            S((4,)),
            S((1,)),
            S((steps,)),
            S((1,)),
            S((steps,)),
            S((1,)),
            S((steps,)),
            S((kv,)),
            S((NQ,)),
            S((NQ, NP)),
            S((1,)),
            S((1,)),
            S((1 + X,)),
            S((NQ, X, NP)),
            S((NQ, Y)),
            S((NQ, 1 + Y)),
            S((1,)),
            S((NQ, tiles, 2)),
            S((1,)),
            S((NQ, tiles, 2, Y)),
            S((1,)),
            S((NQ, tiles, H)),
            S((1,)),
            S((NQ,)),
        ],
        compiler_params=pltpu.CompilerParams(
            collective_id=0, has_side_effects=True, vmem_limit_bytes=63 * 2**20
        ),
    )(
        page_map,
        selected,
        queries.reshape(C, NQ, RC, query_width),
        residual_in.reshape(X, NQ, RC, width),
        norm_gain,
        keys,
        values,
        out_weight,
        gate_weight,
        up_weight,
        down_weight,
    ).reshape(row_count // C, out_width)


def fits(C, H, queries, keys, selected, out_weight, gate_weight):
    rows = queries.shape[0]
    width = out_weight.shape[1]
    if rows % 128:
        return False
    chunks = rows // 128
    return (
        chunks == 2
        and C % H == 0
        and (C // H) * H == C
        and rows % (C * chunks) == 0
        and rows // (C * chunks) % 16 == 0
        and rows % selected.shape[0] == 0
        and keys.shape[2] // HEAD_SIZE > 3
        and (keys.shape[1] - rows) % 128 == 0
        and keys.shape[1] > rows
        and width % 16 == 0
        and width % 128 <= 125
        and width % 128 > 0
        and gate_weight.shape[1] % 128 == 0
    )


def shards(
    queries,
    keys,
    values,
    page_map,
    selected,
    residual_in,
    out_weight,
    norm_gain,
    gate_weight,
    up_weight,
    down_weight,
):
    ctx_index = lax.axis_index("ctx")
    C = lax.axis_size("ctx")
    H = lax.axis_size("head")
    if fits(C, H, queries, keys, selected, out_weight, gate_weight):
        return fused(
            C,
            H,
            queries,
            keys,
            values,
            page_map,
            selected,
            residual_in,
            out_weight,
            norm_gain,
            gate_weight,
            up_weight,
            down_weight,
        )
    row_max, row_total, mixture = owner_pass(
        queries, keys, values, page_map, selected, ctx_index, C
    )
    stats = jnp.concatenate([row_max, row_total], axis=1)
    stats = jnp.pad(stats, ((0, 0), (0, 128 - stats.shape[1])))
    mlp_out, own_stream = tail(
        C,
        H,
        mixture.astype(jnp.bfloat16),
        stats,
        residual_in,
        norm_gain,
        out_weight,
        gate_weight,
        up_weight,
        down_weight,
    )
    own_stream = jnp.concatenate([own_stream[j] for j in range(own_stream.shape[0])], axis=1)
    return (own_stream.astype(jnp.float32) + mlp_out).astype(jnp.bfloat16)


def solution(mesh):
    in_specs = (
        P(None, "head"),
        P("ctx", None, "head"),
        P("ctx", None, "head"),
        P(),
        P(),
        P("head", "ctx"),
        P("head", "ctx"),
        P("ctx"),
        P("head", "ctx"),
        P("head", "ctx"),
        P("ctx", "head"),
    )
    out_specs = P("ctx", "head")
    return jax.shard_map(shards, mesh=mesh, in_specs=in_specs, out_specs=out_specs, check_vma=False)
```

```python
import jax
import jax.numpy as jnp
import functools
from jax import lax
from jax.experimental import pallas as pl
from jax.experimental.pallas import tpu as pltpu
from jax.sharding import PartitionSpec as P

D = 5376
HEAD_SIZE = 128


score_scale = 168.0 ** (-0.5)
masked_score = -1e30
norm_epsilon = 1e-06


def attention_kernel(
    logical_ref, chosen_ref, page_total, q_ref, k_ref, v_ref, mix_ref, m_ref, l_ref, acc, top, total
):
    page = pl.program_id(1)
    tile_count = chosen_ref.shape[0]
    tile_rows = q_ref.shape[0] // tile_count
    group = q_ref.shape[1] // k_ref.shape[2]
    page_len = k_ref.shape[1]
    offset = page_len - q_ref.shape[0]
    f32 = jnp.float32

    @pl.when(page == 0)
    def _():
        acc[...] = jnp.zeros_like(acc)
        top[...] = jnp.full_like(top, masked_score)
        total[...] = jnp.zeros_like(total)

    causal = logical_ref[page] == page_total - 1

    def visit(t, masked):
        rows = slice(t * tile_rows, (t + 1) * tile_rows)
        for g in range(group):
            cols = slice(g * HEAD_SIZE, (g + 1) * HEAD_SIZE)
            scores = (
                lax.dot_general(
                    q_ref[rows, cols],
                    k_ref[0],
                    (((1,), (1,)), ((), ())),
                    preferred_element_type=f32,
                )
                * score_scale
            )
            if masked:
                position = offset + t * tile_rows + lax.broadcasted_iota(jnp.int32, scores.shape, 0)
                key = lax.broadcasted_iota(jnp.int32, scores.shape, 1)
                scores = jnp.where(key <= position, scores, masked_score)
            old = top[g, rows, :1]
            new = jnp.maximum(old, jnp.max(scores, axis=1, keepdims=True))
            weights = jnp.exp(scores - new)
            keep = jnp.exp(old - new)
            total[g, rows] = total[g, rows] * keep + jnp.sum(weights, axis=1, keepdims=True)
            top[g, rows] = jnp.broadcast_to(new, (tile_rows, 128))
            acc[rows, cols] = acc[rows, cols] * keep + jnp.dot(
                weights.astype(jnp.bfloat16), v_ref[0], preferred_element_type=f32
            )

    for t in range(tile_count):
        picked = chosen_ref[t, page] != 0
        pl.when(jnp.logical_and(picked, causal))(functools.partial(visit, t, True))
        pl.when(jnp.logical_and(picked, jnp.logical_not(causal)))(
            functools.partial(visit, t, False)
        )

    @pl.when(page == pl.num_programs(1) - 1)
    def _():
        mix_ref[...] = acc[...].astype(jnp.bfloat16)
        lane = lax.broadcasted_iota(jnp.int32, m_ref.shape[1:], 1)
        maxima = jnp.zeros(m_ref.shape[1:], f32)
        sums = jnp.zeros(m_ref.shape[1:], f32)
        for g in range(group):
            maxima = jnp.where(lane == g, top[g], maxima)
            sums = jnp.where(lane == g, total[g], sums)
        m_ref[0] = maxima
        l_ref[0] = sums


def owner_pass(queries, keys, values, page_map, selected, ctx_index, ctx_count):
    pages_local, page_len, kv_width = keys.shape
    row_count, query_width = queries.shape
    kv_local = kv_width // HEAD_SIZE
    group = query_width // kv_width
    tile_count = selected.shape[0]
    page_total = pages_local * ctx_count
    slot_ids = ctx_index * pages_local + jnp.arange(pages_local, dtype=jnp.int32)
    all_pages = jnp.arange(page_total, dtype=jnp.int32)
    logical = jnp.sum(
        jnp.where(page_map[None, :] == slot_ids[:, None], all_pages[None, :], 0), axis=1
    )
    chosen = jnp.any(selected[:, None, :] == logical[None, :, None], axis=2).astype(jnp.int32)
    stat = jax.ShapeDtypeStruct((kv_local, row_count, 128), jnp.float32)
    stat_spec = pl.BlockSpec((1, row_count, 128), lambda k, p, a, b: (k, 0, 0))
    kv_spec = pl.BlockSpec((1, page_len, HEAD_SIZE), lambda k, p, a, b: (p, 0, k))
    q_spec = pl.BlockSpec((row_count, group * HEAD_SIZE), lambda k, p, a, b: (0, k))

    def kernel(logical_ref, chosen_ref, *refs):
        attention_kernel(logical_ref, chosen_ref, page_total, *refs)

    mixture, top, total = pl.pallas_call(
        kernel,
        grid_spec=pltpu.PrefetchScalarGridSpec(
            num_scalar_prefetch=2,
            grid=(kv_local, pages_local),
            in_specs=[q_spec, kv_spec, kv_spec],
            out_specs=(q_spec, stat_spec, stat_spec),
            scratch_shapes=[
                pltpu.VMEM((row_count, group * HEAD_SIZE), jnp.float32),
                pltpu.VMEM((group, row_count, 128), jnp.float32),
                pltpu.VMEM((group, row_count, 128), jnp.float32),
            ],
        ),
        out_shape=(jax.ShapeDtypeStruct((row_count, query_width), jnp.bfloat16), stat, stat),
    )(logical.astype(jnp.int32), chosen, queries, keys, values)

    def heads(stacked):
        return stacked[:, :, :group].transpose(1, 0, 2).reshape(row_count, kv_local * group)

    return heads(top), heads(total), mixture


MESH = pl.DeviceIdType.MESH
CORES = 2


def column_tile(width):
    for tile in (896, 768, 640, 512, 384, 256, 128):
        if width % tile == 0:
            return tile
    return width


def flat(block, rows):
    if block.shape[1] % 16:
        return block.astype(jnp.float32).reshape(rows, -1).astype(jnp.bfloat16)
    return block.reshape(rows, -1)


def tail_kernel(
    C,
    H,
    mix_ref,
    stat_ref,
    res_ref,
    gain_ref,
    ow_hbm,
    gw_hbm,
    uw_hbm,
    dw_hbm,
    mlp_ref,
    own_ref,
    ow,
    gw,
    uw,
    dw,
    mix_in,
    stat_in,
    att,
    po,
    po_in,
    u_out,
    st_out,
    ss,
    ublk,
    own_st,
    first,
    first_in,
    second,
    second_in,
    hid,
    acc,
    part,
    part_in,
    w_sem,
    mix_s,
    mix_r,
    stat_s,
    stat_r,
    att_s,
    att_r,
    po_s,
    po_r,
    u_s,
    u_r,
    st_s,
    st_r,
    ss_s,
    ss_r,
    f_s,
    f_r,
    g_s,
    g_r,
    h_s,
    h_r,
    fw_s,
    part_s,
    part_r,
):
    c = lax.axis_index("ctx")
    h = lax.axis_index("head")
    Y = H // CORES
    y = h // CORES
    core = h % CORES
    partner = y * CORES + (CORES - 1 - core)
    R = mix_ref.shape[1]
    rows = C * R
    rb = C // H
    bph = C // H
    width = ow.shape[0]
    head_rows = rows // H
    heads = mix_ref.shape[2] // HEAD_SIZE
    tiles, _, _, _, _, tile = first.shape
    f32 = jnp.float32
    bf16 = jnp.bfloat16

    def remote(src, dst, send_sem, recv_sem, ctx, head):
        return pltpu.make_async_remote_copy(
            src_ref=src,
            dst_ref=dst,
            send_sem=send_sem,
            recv_sem=recv_sem,
            device_id=(ctx, head),
            device_id_type=MESH,
        )

    sent = []

    def send(*args):
        copy = remote(*args)
        copy.start()
        sent.append(copy)

    loads = [
        pltpu.make_async_copy(src, dst, w_sem.at[i])
        for i, (src, dst) in enumerate(
            ((ow_hbm, ow), (gw_hbm, gw), (uw_hbm, uw), (dw_hbm, dw))
        )
    ]
    for load in loads:
        load.start()

    for d in range(1, C):
        peer = (c + d) % C
        send(stat_ref.at[peer], stat_in.at[c], stat_s.at[d], stat_r.at[c], peer, h)
        send(mix_ref.at[peer], mix_in.at[c], mix_s.at[d], mix_r.at[c], peer, h)
    stat_in[c] = stat_ref[c]
    mix_in[c] = mix_ref[c]
    for d in range(1, C):
        peer = (c + C - d) % C
        remote(stat_in.at[peer], stat_in.at[peer], stat_s.at[d], stat_r.at[peer], peer, h).wait_recv()
        remote(mix_in.at[peer], mix_in.at[peer], mix_s.at[d], mix_r.at[peer], peer, h).wait_recv()
    maxima = [stat_in[k][:, :heads] for k in range(C)]
    top = functools.reduce(jnp.maximum, maxima)
    scales = [jnp.exp(m - top) for m in maxima]
    total = sum(stat_in[k][:, heads : 2 * heads] * scales[k] for k in range(C))
    inverse = 1.0 / total
    for g in range(heads):
        cols = slice(g * HEAD_SIZE, (g + 1) * HEAD_SIZE)
        mixed = sum(mix_in[k, :, cols].astype(f32) * scales[k][:, g : g + 1] for k in range(C))
        att[c, :, cols] = (mixed * inverse[:, g : g + 1]).astype(bf16)

    for d in range(1, C):
        peer = (c + d) % C
        send(att.at[c], att.at[c], att_s.at[d], att_r.at[c], peer, h)
    loads[0].wait()
    for d in range(1, C):
        peer = (c + C - d) % C
        remote(att.at[peer], att.at[peer], att_s.at[d], att_r.at[peer], peer, h).wait_recv()
    projected = lax.dot_general(
        flat(att[...], rows), ow[...], (((1,), (1,)), ((), ())), preferred_element_type=f32
    )
    po[...] = projected.reshape(H, head_rows, width).astype(bf16)

    for d in range(1, H):
        peer = (h + d) % H
        send(po.at[peer], po_in.at[h], po_s.at[d], po_r.at[h], c, peer)
    po_in[h] = po[h]
    for d in range(1, H):
        peer = (h + H - d) % H
        remote(po_in.at[peer], po_in.at[peer], po_s.at[d], po_r.at[peer], c, peer).wait_recv()
    projected = sum(po_in[k].astype(f32) for k in range(H))
    stream = (res_ref[...].astype(f32) + projected).astype(bf16).astype(f32)
    st_out[...] = stream.reshape(rb, R, width).astype(bf16)
    u_out[...] = (stream * gain_ref[...]).reshape(rb, R, width).astype(bf16)
    squares = jnp.sum(stream * stream, axis=1, keepdims=True)
    ss[c] = jnp.broadcast_to(squares, (head_rows, 128))

    block_head = c // bph
    block_part = c % bph
    u_dst = ublk.at[block_part, pl.ds(h * rb, rb)]
    kept = []
    for d in range(C):
        peer = (c + d) % C
        copy = remote(u_out, u_dst, u_s.at[d], u_r.at[block_part, h], peer, block_head)
        if d == 0:
            kept.append((block_head != h, copy))
            pl.when(block_head != h)(copy.start)

            @pl.when(block_head == h)
            def _():
                ublk[block_part, pl.ds(h * rb, rb)] = u_out[...]

        else:
            copy.start()
            sent.append(copy)
    for d in range(1, C):
        peer = (c + d) % C
        send(ss.at[c], ss.at[c], ss_s.at[d], ss_r.at[c], peer, h)
    for i in range(rb):
        owner = h * rb + i
        other = jnp.logical_or(owner != c, block_head != h)
        copy = remote(
            st_out.at[i], own_st.at[block_part], st_s.at[i], st_r.at[block_part], owner, block_head
        )
        kept.append((other, copy))
        pl.when(other)(copy.start)

        @pl.when(jnp.logical_not(other))
        def _(i=i):
            own_st[block_part] = st_out[i]

    for j in range(bph):
        for k in range(H):
            source = h * bph + j
            block = ublk.at[j, pl.ds(k * rb, rb)]
            arrival = remote(block, block, u_s.at[0], u_r.at[j, k], source, k)
            pl.when(jnp.logical_or(source != c, h != k))(arrival.wait_recv)
    loads[1].wait()
    loads[2].wait()

    def matmul(i, which, weight):
        cols = slice(i * tile, (i + 1) * tile)
        value = None
        for j in range(bph):
            term = jnp.dot(
                flat(ublk[j], rows),
                weight[j * width : (j + 1) * width, cols],
                preferred_element_type=f32,
            )
            value = term if value is None else value + term
        first[i, which] = value.reshape(Y, CORES, head_rows, tile).swapaxes(0, 1).astype(bf16)
        send(
            first.at[i, which, CORES - 1 - core],
            first_in.at[i, which],
            f_s.at[i, which],
            f_r.at[i, which],
            c,
            partner,
        )

    def middle(i, which):
        remote(
            first_in.at[i, which], first_in.at[i, which], f_s.at[i, which], f_r.at[i, which], c, partner
        ).wait_recv()
        both = first[i, which, core].astype(f32) + first_in[i, which].astype(f32)
        second[i, which] = both.astype(bf16)
        for d in range(1, Y):
            peer = (y + d) % Y
            send(
                second.at[i, which, peer],
                second_in.at[i, which, y],
                g_s.at[i, which, d],
                g_r.at[i, which, y],
                c,
                peer * CORES + core,
            )

    def finish(i, inverse_rms):
        sums = []
        for which in range(2):
            value = second[i, which, y].astype(f32)
            for d in range(1, Y):
                peer = (y + Y - d) % Y
                slot = second_in.at[i, which, peer]
                remote(
                    slot, slot, g_s.at[i, which, d], g_r.at[i, which, peer], c, peer * CORES + core
                ).wait_recv()
                value = value + second_in[i, which, peer].astype(f32)
            sums.append(value * inverse_rms)
        hid[i, h] = (jax.nn.gelu(sums[0], approximate=True) * sums[1]).astype(bf16)
        send(hid.at[i, h], hid.at[i, h], h_s.at[i, 0], h_r.at[i, h], c, partner)
        for d in range(1, Y):
            peer = ((y + d) % Y) * CORES + core
            send(hid.at[i, h], hid.at[i, h], h_s.at[i, d], h_r.at[i, h], c, peer)

    def forward(i):
        for d in range(1, Y):
            origin = ((y + Y - d) % Y) * CORES + core
            slot = hid.at[i, origin]
            remote(slot, slot, h_s.at[i, d], h_r.at[i, origin], c, origin).wait_recv()
            send(slot, slot, fw_s.at[i, d], h_r.at[i, origin], c, partner)

    def down(i):
        for d in range(Y):
            origin = ((y + Y - d) % Y) * CORES + (CORES - 1 - core)
            slot = hid.at[i, origin]
            remote(slot, slot, h_s.at[i, 0], h_r.at[i, origin], c, partner).wait_recv()
        term = lax.dot_general(
            flat(hid[i], rows),
            dw[:, i * tile : (i + 1) * tile],
            (((1,), (1,)), ((), ())),
            preferred_element_type=f32,
        )
        if i == 0:
            acc[...] = term
        else:
            acc[...] += term

    steps = [(i, which) for i in range(tiles) for which in range(2)]
    for n, (i, which) in enumerate(steps):
        matmul(i, which, (gw, uw)[which])
        if n:
            middle(*steps[n - 1])
    middle(*steps[-1])
    for d in range(1, C):
        peer = (c + C - d) % C
        remote(ss.at[peer], ss.at[peer], ss_s.at[d], ss_r.at[peer], peer, h).wait_recv()
    squares = sum(ss[k] for k in range(C))
    inverse_rms = lax.rsqrt(squares[:, :1] / (C * width) + norm_epsilon)
    loads[3].wait()
    for i in range(tiles):
        finish(i, inverse_rms)
        if i:
            forward(i - 1)
    forward(tiles - 1)
    for i in range(tiles):
        down(i)
    part[...] = acc[...].reshape(C, R, acc.shape[1]).astype(bf16)

    for d in range(1, C):
        peer = (c + d) % C
        send(part.at[peer], part_in.at[c], part_s.at[d], part_r.at[c], peer, h)
    part_in[c] = part[c]
    for j in range(bph):
        source = h * bph + j
        arrival = remote(own_st.at[j], own_st.at[j], st_s.at[0], st_r.at[j], source, c // rb)
        pl.when(jnp.logical_or(source != c, c // rb != h))(arrival.wait_recv)
    own_ref[...] = own_st[...]
    for d in range(1, C):
        peer = (c + C - d) % C
        remote(part_in.at[peer], part_in.at[peer], part_s.at[d], part_r.at[peer], peer, h).wait_recv()
    mlp_ref[...] = sum(part_in[k].astype(f32) for k in range(C))
    for copy in sent:
        copy.wait_send()
    for condition, copy in kept:
        pl.when(condition)(copy.wait_send)


def tail(C, H, mixture, stats, residual_in, norm_gain, out_weight, gate_weight, up_weight, down_weight):
    rows, query_width = mixture.shape
    R = rows // C
    width = out_weight.shape[1]
    hidden = gate_weight.shape[1]
    out_width = down_weight.shape[1]
    out_weight = out_weight.T
    down_weight = down_weight.T
    rb = C // H
    bph = C // H
    Y = H // CORES
    head_rows = rows // H
    tile = column_tile(hidden)
    tiles = hidden // tile
    bf16 = jnp.bfloat16
    vmem = pl.BlockSpec(memory_space=pltpu.VMEM)
    hbm = pl.BlockSpec(memory_space=pl.ANY)
    V = pltpu.VMEM
    S = pltpu.SemaphoreType.DMA
    return pl.pallas_call(
        functools.partial(tail_kernel, C, H),
        out_shape=(
            jax.ShapeDtypeStruct((R, out_width), jnp.float32),
            jax.ShapeDtypeStruct((bph, R, width), bf16),
        ),
        in_specs=[vmem] * 4 + [hbm] * 4,
        out_specs=(vmem, vmem),
        scratch_shapes=[
            V(out_weight.shape, bf16),
            V(gate_weight.shape, bf16),
            V(up_weight.shape, bf16),
            V(down_weight.shape, bf16),
            V((C, R, query_width), bf16),
            V((C, R, 128), jnp.float32),
            V((C, R, query_width), bf16),
            V((H, head_rows, width), bf16),
            V((H, head_rows, width), bf16),
            V((rb, R, width), bf16),
            V((rb, R, width), bf16),
            V((C, head_rows, 128), jnp.float32),
            V((bph, C, R, width), bf16),
            V((bph, R, width), bf16),
            V((tiles, 2, CORES, Y, head_rows, tile), bf16),
            V((tiles, 2, Y, head_rows, tile), bf16),
            V((tiles, 2, Y, head_rows, tile), bf16),
            V((tiles, 2, Y, head_rows, tile), bf16),
            V((tiles, H, head_rows, tile), bf16),
            V((rows, out_width), jnp.float32),
            V((C, R, out_width), bf16),
            V((C, R, out_width), bf16),
            S((4,)),
            S((C,)),
            S((C,)),
            S((C,)),
            S((C,)),
            S((C,)),
            S((C,)),
            S((H,)),
            S((H,)),
            S((C,)),
            S((bph, H)),
            S((rb,)),
            S((bph,)),
            S((C,)),
            S((C,)),
            S((tiles, 2)),
            S((tiles, 2)),
            S((tiles, 2, Y)),
            S((tiles, 2, Y)),
            S((tiles, Y)),
            S((tiles, H)),
            S((tiles, Y)),
            S((C,)),
            S((C,)),
        ],
        compiler_params=pltpu.CompilerParams(
            has_side_effects=True, vmem_limit_bytes=60 * 2**20
        ),
    )(
        mixture.reshape(C, R, query_width),
        stats.reshape(C, R, 128),
        residual_in,
        norm_gain.reshape(1, width),
        out_weight,
        gate_weight,
        up_weight,
        down_weight,
    )


LOG2E = 1.4426950408889634


def fused_kernel(
    C,
    H,
    NP,
    map_hbm,
    sel_hbm,
    q_hbm,
    res_hbm,
    gain_hbm,
    k_hbm,
    v_hbm,
    ow_hbm,
    gw_hbm,
    uw_hbm,
    dw_hbm,
    out_ref,
    map_ref,
    sel_ref,
    q_ref,
    res_ref,
    gain_ref,
    k_buf,
    v_buf,
    ow,
    gw,
    uw,
    dw,
    mix_out,
    mix_in,
    lse_out,
    lse_in,
    att,
    po_out,
    po_in,
    res_in,
    st,
    u,
    ss_out,
    ss_in,
    ss_mid,
    ss_last,
    scale,
    begun,
    first,
    first_in,
    second,
    second_in,
    hid,
    acc,
    part,
    part_in,
    in_sem,
    kv_sem,
    w_sem,
    mix_s,
    mix_r,
    lse_s,
    lse_r,
    att_s,
    att_r,
    cross_r,
    po_s,
    po_r,
    res_s,
    res_r,
    u_s,
    u_r,
    ss_s,
    ss_r,
    f_s,
    f_r,
    g_s,
    g_r,
    h_s,
    h_r,
    part_s,
    part_r,
):
    c = lax.axis_index("ctx")
    h = lax.axis_index("head")
    X = C // H
    Z = C // X
    z = c // X
    x = c % X
    Y = H // CORES
    y = h // CORES
    core = h % CORES
    partner = y * CORES + (CORES - 1 - core)
    _, NQ, RC, query_width = q_ref.shape
    rows = C * RC
    hr = rows // H
    kv, pages, page_len, _ = k_buf.shape
    group = query_width // (kv * HEAD_SIZE)
    gw_cols = group * HEAD_SIZE
    tile_count = sel_ref.shape[0]
    tile_rows = NQ * rows // tile_count
    offset = page_len - NQ * rows
    page_total = map_ref.shape[0]
    width = ow.shape[0]
    tile = first.shape[-1]
    tiles = first.shape[1]
    RP = rows // NP
    f32 = jnp.float32
    bf16 = jnp.bfloat16
    owner = h == z
    visitor = h != z

    def remote(src, dst, send_sem, recv_sem, ctx, head):
        return pltpu.make_async_remote_copy(
            src_ref=src,
            dst_ref=dst,
            send_sem=send_sem,
            recv_sem=recv_sem,
            device_id=(ctx, head),
            device_id_type=MESH,
        )

    sent = []
    kept = []

    def start(*args):
        remote(*args).start()

    def send(*args):
        copy = remote(*args)
        copy.start()
        sent.append(copy)

    def send_if(condition, *args):
        copy = remote(*args)
        pl.when(condition)(copy.start)
        kept.append((condition, copy))

    def kv_load(j):
        lanes = pl.ds(pl.multiple_of(j * HEAD_SIZE, HEAD_SIZE), HEAD_SIZE)
        return (
            pltpu.make_async_copy(k_hbm.at[:, :, lanes], k_buf.at[j], kv_sem.at[0, j]),
            pltpu.make_async_copy(v_hbm.at[:, :, lanes], v_buf.at[j], kv_sem.at[1, j]),
        )

    barrier = pltpu.get_barrier_semaphore()
    for d in range(1, C):
        pl.semaphore_signal(
            barrier, inc=1, device_id=((c + d) % C, h), device_id_type=MESH
        )
    for d in range(1, H):
        pl.semaphore_signal(
            barrier, inc=1, device_id=(c, (h + d) % H), device_id_type=MESH
        )
    inputs = [
        pltpu.make_async_copy(src, dst, in_sem.at[i])
        for i, (src, dst) in enumerate(
            (
                (map_hbm, map_ref),
                (sel_hbm, sel_ref),
                (q_hbm, q_ref),
                (res_hbm, res_ref),
                (gain_hbm, gain_ref.at[0]),
            )
        )
    ]
    for load in inputs:
        load.start()
    for load in kv_load(0):
        load.start()
    loads = [
        pltpu.make_async_copy(src, dst, w_sem.at[i])
        for i, (src, dst) in enumerate(
            ((ow_hbm, ow), (gw_hbm, gw), (uw_hbm, uw), (dw_hbm, dw))
        )
    ]
    for load in inputs[:3]:
        load.wait()

    facts = []
    for p in range(pages):
        slot = c * pages + p
        logical = jnp.int32(0)
        for j in range(page_total):
            logical = logical + jnp.where(map_ref[j] == slot, j, 0)
        picks = []
        for t in range(tile_count):
            hits = jnp.int32(0)
            for i in range(sel_ref.shape[1]):
                hits = hits + jnp.where(sel_ref[t, i] == logical, 1, 0)
            picks.append(jnp.where(hits > 0, 0.0, masked_score).astype(f32))
        reach = jnp.where(logical == page_total - 1, 0, page_len)
        facts.append((reach, picks))

    index = lax.broadcasted_iota(jnp.int32, (group * rows, 1), 0) & (rows - 1)
    shift = RC.bit_length() - 1
    base_row = (index >> shift) * (NQ * RC) + (index & (RC - 1))
    eye = lax.broadcasted_iota(jnp.int32, (rows, rows), 0) == lax.broadcasted_iota(
        jnp.int32, (rows, rows), 1
    )
    unit = score_scale * LOG2E

    def attend(n):
        q = n // kv
        j = n % kv

        @pl.when(n < kv)
        def _():
            for load in kv_load(j):
                load.wait()

        @pl.when(n == 0)
        def _():
            for k in range(1, kv):
                for load in kv_load(k):
                    load.start()
            for load in loads:
                load.start()

        lanes = pl.ds(pl.multiple_of(j * gw_cols, gw_cols), gw_cols)
        block = q_ref[:, q, :, lanes].reshape(rows, gw_cols)
        lhs = jnp.concatenate(
            [block[:, g * HEAD_SIZE : (g + 1) * HEAD_SIZE] for g in range(group)], axis=0
        )
        row = base_row + q * RC
        key = offset + lax.broadcasted_iota(jnp.int32, (group * rows, page_len - offset), 1)
        tops, sums, outs = [], [], []
        for p in range(pages):
            reach, picks = facts[p]
            bias = jnp.zeros((group * rows, 1), f32)
            for t in range(tile_count):
                inside = jnp.logical_and(row >= t * tile_rows, row < (t + 1) * tile_rows)
                bias = jnp.where(inside, picks[t], bias)
            scores = lax.dot_general(
                lhs, k_buf[j, p], (((1,), (1,)), ((), ())), preferred_element_type=f32
            )
            late = jnp.where(key <= offset + row + reach, scores[:, offset:], masked_score)
            scores = jnp.concatenate([scores[:, :offset], late], axis=1)
            top = jnp.max(scores, axis=1, keepdims=True)
            weights = jnp.exp2((scores - top) * unit)
            sums.append(jnp.sum(weights, axis=1, keepdims=True))
            outs.append(
                jnp.dot(weights.astype(bf16), v_buf[j, p], preferred_element_type=f32)
            )
            tops.append(top * unit + bias)
        best = functools.reduce(jnp.maximum, tops)
        scales = [jnp.exp2(top - best) for top in tops]
        total = sum(s * e for s, e in zip(sums, scales))
        mixed = sum(o * (e / total) for o, e in zip(outs, scales))
        lse = best + jnp.log2(total)
        for g in range(group):
            part_rows = slice(g * rows, (g + 1) * rows)
            mix_out[n, :, :, g * HEAD_SIZE : (g + 1) * HEAD_SIZE] = (
                mixed[part_rows].reshape(C, RC, HEAD_SIZE).astype(bf16)
            )
            lse_out[n, g : g + 1] = jnp.sum(
                jnp.where(eye, lse[part_rows], 0.0), axis=0, keepdims=True
            )
        mix_in[n, c] = mix_out[n, c]
        lse_in[n, c] = lse_out[n]

    def mix_sends(n):
        for d in range(1, C):
            peer = (c + d) % C
            remote(mix_out.at[n, peer], mix_in.at[n, c], mix_s.at[0], mix_r.at[n], peer, h).start()
            remote(lse_out.at[n], lse_in.at[n, c], lse_s.at[0], lse_r.at[n], peer, h).start()

    def att_sends(n, direct):
        block = att.at[n, c]
        if direct:
            for d in range(1, C):
                start(block, block, att_s.at[0], att_r.at[n], (c + d) % C, h)
        else:
            for d in range(1, Z):
                start(block, block, att_s.at[0], att_r.at[n], (z + d) % Z * X + x, h)
            for d in range(1, X):
                start(block, block, att_s.at[0], cross_r.at[n - kv], z * X + (x + d) % X, h)

    def att_relay(n):
        arrived(att.at[n, pl.ds(0, Z - 1)], att_r.at[n])
        for e in range(1, Z):
            block = att.at[n, (z + e) % Z * X + x]
            for d in range(1, X):
                start(block, block, att_s.at[0], cross_r.at[n - kv], z * X + (x + d) % X, h)

    def arrived(block, recv_sem):
        remote(block, block, recv_sem, recv_sem, c, partner).wait_recv()

    def left(block, send_sem):
        remote(block, block, send_sem, send_sem, c, partner).wait_send()

    def combine(n, direct):
        arrived(lse_in.at[n, pl.ds(0, C - 1)], lse_r.at[n])
        arrived(mix_in.at[n, pl.ds(0, C - 1)], mix_r.at[n])
        logs = [lse_in[n, k] for k in range(C)]
        best = functools.reduce(jnp.maximum, logs)
        scales = [jnp.exp2(value - best) for value in logs]
        inverse = 1.0 / sum(scales)
        lane = lax.broadcasted_iota(jnp.int32, (RC, rows), 1)
        mine = lane == c * RC + lax.broadcasted_iota(jnp.int32, (RC, rows), 0)
        for g in range(group):
            cols = slice(g * HEAD_SIZE, (g + 1) * HEAD_SIZE)
            value = jnp.zeros((RC, HEAD_SIZE), f32)
            for k in range(C):
                share = (scales[k] * inverse)[g : g + 1]
                share = jnp.sum(jnp.where(mine, share, 0.0), axis=1, keepdims=True)
                value = value + share * mix_in[n, k, :, cols].astype(f32)
            att[n, c, :, cols] = value.astype(bf16)
        att_sends(n, direct)

    def project(q):
        for j in range(kv):
            n = q * kv + j
            if q == 0:
                arrived(att.at[n, pl.ds(0, C - 1)], att_r.at[n])
            else:
                arrived(att.at[n, pl.ds(0, (X - 1) * Z)], cross_r.at[n - kv])
        if q == 0:
            loads[0].wait()
        value = None
        for j in range(kv):
            term = lax.dot_general(
                att[q * kv + j].reshape(rows, gw_cols),
                ow[:, j * gw_cols : (j + 1) * gw_cols],
                (((1,), (1,)), ((), ())),
                preferred_element_type=f32,
            )
            value = term if value is None else value + term
        po_out[q] = value.astype(bf16)
        for i in range(NP):
            piece = pl.ds(i * RP, RP)
            copy = remote(
                po_out.at[q, piece], po_in.at[q, h, piece], po_s.at[q], po_r.at[q, i], c, z
            )
            pl.when(visitor)(copy.start)
        po_in[q, h] = po_out[q]

    def own(q, i):
        if q == 0 and i == 0:
            arrived(res_in.at[pl.ds(0, H - 1)], res_r.at[0])
        arrived(po_in.at[q, pl.ds(0, H - 1), pl.ds(i * RP, RP)], po_r.at[q, i])
        spare = u.shape[-1] - width
        lane = lax.broadcasted_iota(jnp.int32, (RC, spare), 1)
        for b in range(i * RP // RC, (i + 1) * RP // RC):
            span = slice(b * RC, (b + 1) * RC)
            value = res_in[b // X, b % X, q].astype(f32)
            added = sum(po_in[q, k, span].astype(f32) for k in range(H))
            stream = (value + added).astype(bf16)
            st[q, span] = stream
            stream = stream.astype(f32)
            u[q, x, span, :width] = (stream * gain_ref[...]).astype(bf16)
            squares = jnp.sum(stream * stream, axis=1, keepdims=True)
            high = squares.astype(bf16).astype(f32)
            mid = (squares - high).astype(bf16).astype(f32)
            low = squares - high - mid
            packed = jnp.where(lane == 0, high, jnp.where(lane == 1, mid, low))
            packed = jnp.where(lane < 3, packed, 0.0)
            u[q, x, span, width:] = packed.astype(bf16)

    def relay(q, i, here):
        piece = u.at[q, x, pl.ds(i * RP, RP)]
        recv = u_r.at[q, x, i]
        pl.when(jnp.logical_and(here, visitor))(functools.partial(arrived, piece, recv))
        for way, ahead in enumerate((Z - 1 - z, z)):
            step = 1 - 2 * way
            go = jnp.logical_and(jnp.logical_and(here, step * (z - h) >= 0), ahead > 0)
            target = jnp.clip(z + step, 0, Z - 1) * X + x
            copy = remote(piece, piece, u_s.at[way], recv, target, h)
            pl.when(go)(copy.start)
            kept.append((go, copy))
        for d in range(1, X):
            peer = z * X + (x + d) % X
            copy = remote(piece, piece, u_s.at[1 + d], recv, peer, h)
            pl.when(here)(copy.start)
            kept.append((here, copy))

    def spread(q, here):
        for i in range(NP):
            pl.when(jnp.logical_and(here, owner))(functools.partial(own, q, i))
            relay(q, i, here)

    def gather(q):
        for d in range(1, X):
            source = (x + d) % X
            for i in range(NP):
                block = u.at[q, source, pl.ds(i * RP, RP)]
                arrived(block, u_r.at[q, source, i])
        squares = 0.0
        for k in range(X):
            split = u[q, k, :, width:].astype(f32)
            squares = squares + jnp.sum(split, axis=1, keepdims=True)
        squares = jnp.broadcast_to(squares, (rows, 128)).reshape(Y, CORES, hr, 128)
        ss_out[q] = squares.swapaxes(0, 1)
        send(ss_out.at[q, CORES - 1 - core], ss_in.at[q], ss_s.at[q, 0], ss_r.at[q, 0], c, partner)

    def block_dot(q, k, i, which):
        weight = (gw, uw)[which]
        span = pl.ds(pl.multiple_of(k * width, 16), width)
        return jnp.dot(
            u[q, k, :, :width],
            weight[span, i * tile : (i + 1) * tile],
            preferred_element_type=f32,
        )

    def start_expand(q):
        if q == 0:
            loads[1].wait()
            loads[2].wait()
        for i in range(tiles):
            for which in range(2):
                begun[i, which] = block_dot(q, x, i, which)

    def matmul(q, i, which):
        value = begun[i, which]
        for d in range(1, X):
            value = value + block_dot(q, (x + d) % X, i, which)
        value = value.reshape(Y, CORES, hr, tile).swapaxes(0, 1).astype(bf16)
        first[q, i, which] = value
        start(
            first.at[q, i, which, CORES - 1 - core],
            first_in.at[q, i, which],
            f_s.at[0],
            f_r.at[q, i, which],
            c,
            partner,
        )

    def middle(q, i, which):
        block = first_in.at[q, i, which]
        arrived(block, f_r.at[q, i, which])
        both = first[q, i, which, core].astype(f32) + first_in[q, i, which].astype(f32)
        second[q, i, which] = both.astype(bf16)
        for d in range(1, Y):
            peer = (y + d) % Y
            start(
                second.at[q, i, which, peer],
                second_in.at[q, i, which, y],
                g_s.at[0],
                g_r.at[q, i, which, y],
                c,
                peer * CORES + core,
            )

    def middle_squares(q):
        block = ss_in.at[q]
        remote(block, block, ss_s.at[q, 0], ss_r.at[q, 0], c, partner).wait_recv()
        ss_mid[q] = ss_out[q, core] + ss_in[q]
        for d in range(1, Y):
            peer = (y + d) % Y
            send(
                ss_mid.at[q, peer],
                ss_last.at[q, y],
                ss_s.at[q, d],
                ss_r.at[q, 1 + y],
                c,
                peer * CORES + core,
            )

    def inverse_rms(q):
        total = ss_mid[q, y]
        for d in range(1, Y):
            peer = (y + Y - d) % Y
            block = ss_last.at[q, peer]
            remote(
                block, block, ss_s.at[q, d], ss_r.at[q, 1 + peer], c, peer * CORES + core
            ).wait_recv()
            total = total + ss_last[q, peer]
        scale[q] = lax.rsqrt(total / (C * width) + norm_epsilon)

    def finish(q, i):
        inverse = scale[q][:, :1]
        sums = []
        for which in range(2):
            value = second[q, i, which, y].astype(f32)
            for d in range(1, Y):
                peer = (y + Y - d) % Y
                block = second_in.at[q, i, which, peer]
                remote(
                    block,
                    block,
                    g_s.at[0],
                    g_r.at[q, i, which, peer],
                    c,
                    peer * CORES + core,
                ).wait_recv()
                value = value + second_in[q, i, which, peer].astype(f32)
            sums.append(value * inverse)
        hid[q, i, h] = (jax.nn.gelu(sums[0], approximate=True) * sums[1]).astype(bf16)
        block = hid.at[q, i, h]
        for d in range(1, Y):
            peer = ((y + d) % Y) * CORES + core
            start(block, block, h_s.at[0], h_r.at[q, i, h], c, peer)
        start(block, block, h_s.at[0], h_r.at[q, i, h], c, partner)

    def forward(q, i):
        for d in range(1, Y):
            origin = ((y + Y - d) % Y) * CORES + core
            block = hid.at[q, i, origin]
            arrived(block, h_r.at[q, i, origin])
            start(block, block, h_s.at[0], h_r.at[q, i, origin], c, partner)

    def down(q, i):
        for d in range(Y):
            origin = ((y + Y - d) % Y) * CORES + (CORES - 1 - core)
            block = hid.at[q, i, origin]
            arrived(block, h_r.at[q, i, origin])
        if q == 0 and i == 0:
            loads[3].wait()
        term = lax.dot_general(
            hid[q, i].reshape(rows, tile),
            dw[:, i * tile : (i + 1) * tile],
            (((1,), (1,)), ((), ())),
            preferred_element_type=f32,
        )
        if i == 0:
            acc[...] = term
        else:
            acc[...] += term

    def scatter(q):
        for k in range(X):

            @pl.when(jnp.logical_and(owner, x == k))
            def _(k=k):
                acc[:, k * width : (k + 1) * width] += st[q].astype(f32)

        part[q] = acc[...].reshape(C, RC, acc.shape[1]).astype(bf16)
        for d in range(1, C):
            peer = (c + d) % C
            start(part.at[q, peer], part_in.at[q, c], part_s.at[0], part_r.at[q], peer, h)
        part_in[q, c] = part[q, c]

    def collect(q):
        arrived(part_in.at[q, pl.ds(0, C - 1)], part_r.at[q])
        out_ref[q] = sum(part_in[q, k].astype(f32) for k in range(C)).astype(bf16)

    steps = NQ * kv
    lag = 3

    def loop(n, carry):
        attend(n)

        @pl.when(n == 1)
        def _():
            pl.semaphore_wait(barrier, C + H - 2)
            mix_sends(0)

        ready = jnp.logical_and(n >= 1, n < kv)
        pl.when(jnp.logical_or(ready, n >= kv + lag - 1))(functools.partial(mix_sends, n))

        for k in range(kv):

            @pl.when(n == (kv + lag - 2 if k == kv - 1 else max(k + 2, lag)))
            def _(k=k):
                combine(k, True)

        @pl.when(n == kv + lag - 2)
        def _():
            for k in range(kv, kv + lag - 1):
                mix_sends(k)

        return carry

    lax.fori_loop(0, steps, loop, 0)
    for load in inputs[3:]:
        load.wait()
    send_if(visitor, res_ref, res_in.at[h], res_s.at[0], res_r.at[0], c, z)
    res_in[h] = res_ref[...]
    pairs = [(i, which) for i in range(tiles) for which in range(2)]

    def expand(q, extra=None):
        gather(q)
        for n, (i, which) in enumerate(pairs):
            matmul(q, i, which)
            if n == 1:
                middle_squares(q)
            if n:
                middle(q, *pairs[n - 1])
            if extra is not None and which:
                extra(i)
        middle(q, *pairs[-1])

    def finish_if(here, q, i):
        @pl.when(here)
        def _():
            if i == 0:
                inverse_rms(q)
            finish(q, i)

    def contract(q, done=0):
        forward(q, done)
        for i in range(done, tiles):
            if i + 1 < tiles:
                forward(q, i + 1)
            down(q, i)
        scatter(q)

    def between(i):
        finish_if(early, 0, i)
        if i:

            @pl.when(late)
            def _():
                forward(0, i - 1)
                down(0, i - 1)


    far = jnp.maximum(z - h, h - z)
    early = z // CORES == y
    late = z // CORES != y
    project(0)
    for n in range(kv, steps - 2):
        combine(n, False)
    spread(0, far == 0)
    for n in range(steps - 2, steps):
        combine(n, False)
    for n in range(kv, steps - 2):
        att_relay(n)
    spread(0, far == 1)
    for n in range(steps - 2, steps):
        att_relay(n)
    pl.when(far <= 1)(lambda: start_expand(0))
    spread(0, far == 2)
    project(1)
    spread(0, far > 2)
    pl.when(far > 1)(lambda: start_expand(0))
    expand(0, lambda i: spread(1, far == 0) if i == tiles - 1 else None)
    first_on = jnp.logical_and(late, far <= 2)
    spread(1, first_on)
    for i in range(tiles):
        finish_if(late, 0, i)
    spread(1, jnp.logical_and(jnp.logical_not(first_on), far > 0))
    start_expand(1)
    expand(1, between)
    for i in range(tiles - 1):
        finish_if(late, 1, i)
    pl.when(late)(lambda: contract(0, tiles - 1))
    finish_if(late, 1, tiles - 1)
    pl.when(early)(lambda: contract(0))
    for i in range(tiles):
        finish_if(early, 1, i)
    contract(1)
    for q in range(NQ):
        collect(q)

    left(mix_out.at[:, pl.ds(0, C - 1)], mix_s.at[0])
    left(lse_in.at[:, pl.ds(0, C - 1)], lse_s.at[0])
    left(att.at[:, pl.ds(0, C - 1)], att_s.at[0])
    left(first_in, f_s.at[0])
    left(second.at[:, :, :, pl.ds(0, Y - 1)], g_s.at[0])
    left(hid.at[:, :, pl.ds(0, 2 * Y - 1)], h_s.at[0])
    left(part.at[:, pl.ds(0, C - 1)], part_s.at[0])
    for q in range(NQ):
        pl.when(visitor)(functools.partial(left, po_out.at[q], po_s.at[q]))
    for copy in sent:
        copy.wait_send()
    for condition, copy in kept:
        pl.when(condition)(copy.wait_send)


def fused(
    C,
    H,
    queries,
    keys,
    values,
    page_map,
    selected,
    residual_in,
    out_weight,
    norm_gain,
    gate_weight,
    up_weight,
    down_weight,
):
    row_count, query_width = queries.shape
    pages, page_len, kv_width = keys.shape
    kv = kv_width // HEAD_SIZE
    group = query_width // kv_width
    NQ = row_count // 128
    RC = row_count // C // NQ
    rows = C * RC
    NP = 8
    X = C // H
    Y = H // CORES
    hr = rows // H
    width = out_weight.shape[1]
    hidden = gate_weight.shape[1]
    out_width = down_weight.shape[1]
    tile = column_tile(hidden)
    tiles = hidden // tile
    steps = NQ * kv
    u_width = (width + 127) // 128 * 128
    bf16 = jnp.bfloat16
    f32 = jnp.float32
    vmem = pl.BlockSpec(memory_space=pltpu.VMEM)
    hbm = pl.BlockSpec(memory_space=pl.ANY)
    V = pltpu.VMEM
    S = pltpu.SemaphoreType.DMA
    out_weight = out_weight.T
    down_weight = down_weight.T
    mixes = V((steps, C, RC, group * HEAD_SIZE), bf16)
    return pl.pallas_call(
        functools.partial(fused_kernel, C, H, NP),
        out_shape=pltpu.VMEM((NQ, RC, out_width), bf16),
        in_specs=[hbm] * 11,
        out_specs=vmem,
        scratch_shapes=[
            pltpu.SMEM(page_map.shape, jnp.int32),
            pltpu.SMEM(selected.shape, jnp.int32),
            V((C, NQ, RC, query_width), bf16),
            V((X, NQ, RC, width), bf16),
            V((1, width), f32),
            V((kv, pages, page_len, HEAD_SIZE), bf16),
            V((kv, pages, page_len, HEAD_SIZE), bf16),
            V(out_weight.shape, bf16),
            V(gate_weight.shape, bf16),
            V(up_weight.shape, bf16),
            V(down_weight.shape, bf16),
            mixes,
            mixes,
            V((steps, group, rows), f32),
            V((steps, C, group, rows), f32),
            mixes,
            V((NQ, rows, width), bf16),
            V((NQ, H, rows, width), bf16),
            V((H, X, NQ, RC, width), bf16),
            V((NQ, rows, width), bf16),
            V((NQ, X, rows, u_width), bf16),
            V((NQ, CORES, Y, hr, 128), f32),
            V((NQ, Y, hr, 128), f32),
            V((NQ, Y, hr, 128), f32),
            V((NQ, Y, hr, 128), f32),
            V((NQ, hr, 128), f32),
            V((tiles, 2, rows, tile), f32),
            V((NQ, tiles, 2, CORES, Y, hr, tile), bf16),
            V((NQ, tiles, 2, Y, hr, tile), bf16),
            V((NQ, tiles, 2, Y, hr, tile), bf16),
            V((NQ, tiles, 2, Y, hr, tile), bf16),
            V((NQ, tiles, H, hr, tile), bf16),
            V((rows, out_width), f32),
            V((NQ, C, RC, out_width), bf16),
            V((NQ, C, RC, out_width), bf16),
            S((5,)),
            S((2, kv)),
            S((4,)),
            S((1,)),
            S((steps,)),
            S((1,)),
            S((steps,)),
            S((1,)),
            S((steps,)),
            S((kv,)),
            S((NQ,)),
            S((NQ, NP)),
            S((1,)),
            S((1,)),
            S((1 + X,)),
            S((NQ, X, NP)),
            S((NQ, Y)),
            S((NQ, 1 + Y)),
            S((1,)),
            S((NQ, tiles, 2)),
            S((1,)),
            S((NQ, tiles, 2, Y)),
            S((1,)),
            S((NQ, tiles, H)),
            S((1,)),
            S((NQ,)),
        ],
        compiler_params=pltpu.CompilerParams(
            collective_id=0, has_side_effects=True, vmem_limit_bytes=63 * 2**20
        ),
    )(
        page_map,
        selected,
        queries.reshape(C, NQ, RC, query_width),
        residual_in.reshape(X, NQ, RC, width),
        norm_gain,
        keys,
        values,
        out_weight,
        gate_weight,
        up_weight,
        down_weight,
    ).reshape(row_count // C, out_width)


def fits(C, H, queries, keys, selected, out_weight, gate_weight):
    rows = queries.shape[0]
    width = out_weight.shape[1]
    if rows % 128:
        return False
    chunks = rows // 128
    return (
        chunks == 2
        and C % H == 0
        and (C // H) * H == C
        and rows % (C * chunks) == 0
        and rows // (C * chunks) % 16 == 0
        and rows % selected.shape[0] == 0
        and keys.shape[2] // HEAD_SIZE > 3
        and (keys.shape[1] - rows) % 128 == 0
        and keys.shape[1] > rows
        and width % 16 == 0
        and width % 128 <= 125
        and width % 128 > 0
        and gate_weight.shape[1] % 128 == 0
    )


def shards(
    queries,
    keys,
    values,
    page_map,
    selected,
    residual_in,
    out_weight,
    norm_gain,
    gate_weight,
    up_weight,
    down_weight,
):
    ctx_index = lax.axis_index("ctx")
    C = lax.axis_size("ctx")
    H = lax.axis_size("head")
    if fits(C, H, queries, keys, selected, out_weight, gate_weight):
        return fused(
            C,
            H,
            queries,
            keys,
            values,
            page_map,
            selected,
            residual_in,
            out_weight,
            norm_gain,
            gate_weight,
            up_weight,
            down_weight,
        )
    row_max, row_total, mixture = owner_pass(
        queries, keys, values, page_map, selected, ctx_index, C
    )
    stats = jnp.concatenate([row_max, row_total], axis=1)
    stats = jnp.pad(stats, ((0, 0), (0, 128 - stats.shape[1])))
    mlp_out, own_stream = tail(
        C,
        H,
        mixture.astype(jnp.bfloat16),
        stats,
        residual_in,
        norm_gain,
        out_weight,
        gate_weight,
        up_weight,
        down_weight,
    )
    own_stream = jnp.concatenate([own_stream[j] for j in range(own_stream.shape[0])], axis=1)
    return (own_stream.astype(jnp.float32) + mlp_out).astype(jnp.bfloat16)


def solution(mesh):
    in_specs = (
        P(None, "head"),
        P("ctx", None, "head"),
        P("ctx", None, "head"),
        P(),
        P(),
        P("head", "ctx"),
        P("head", "ctx"),
        P("ctx"),
        P("head", "ctx"),
        P("head", "ctx"),
        P("ctx", "head"),
    )
    out_specs = P("ctx", "head")
    return jax.shard_map(shards, mesh=mesh, in_specs=in_specs, out_specs=out_specs, check_vma=False)
```

```python
import jax
import jax.numpy as jnp
import functools
from jax import lax
from jax.experimental import pallas as pl
from jax.experimental.pallas import tpu as pltpu
from jax.sharding import PartitionSpec as P

D = 5376
HEAD_SIZE = 128


score_scale = 168.0 ** (-0.5)
masked_score = -1e30
norm_epsilon = 1e-06


def attention_kernel(
    logical_ref, chosen_ref, page_total, q_ref, k_ref, v_ref, mix_ref, m_ref, l_ref, acc, top, total
):
    page = pl.program_id(1)
    tile_count = chosen_ref.shape[0]
    tile_rows = q_ref.shape[0] // tile_count
    group = q_ref.shape[1] // k_ref.shape[2]
    page_len = k_ref.shape[1]
    offset = page_len - q_ref.shape[0]
    f32 = jnp.float32

    @pl.when(page == 0)
    def _():
        acc[...] = jnp.zeros_like(acc)
        top[...] = jnp.full_like(top, masked_score)
        total[...] = jnp.zeros_like(total)

    causal = logical_ref[page] == page_total - 1

    def visit(t, masked):
        rows = slice(t * tile_rows, (t + 1) * tile_rows)
        for g in range(group):
            cols = slice(g * HEAD_SIZE, (g + 1) * HEAD_SIZE)
            scores = (
                lax.dot_general(
                    q_ref[rows, cols],
                    k_ref[0],
                    (((1,), (1,)), ((), ())),
                    preferred_element_type=f32,
                )
                * score_scale
            )
            if masked:
                position = offset + t * tile_rows + lax.broadcasted_iota(jnp.int32, scores.shape, 0)
                key = lax.broadcasted_iota(jnp.int32, scores.shape, 1)
                scores = jnp.where(key <= position, scores, masked_score)
            old = top[g, rows, :1]
            new = jnp.maximum(old, jnp.max(scores, axis=1, keepdims=True))
            weights = jnp.exp(scores - new)
            keep = jnp.exp(old - new)
            total[g, rows] = total[g, rows] * keep + jnp.sum(weights, axis=1, keepdims=True)
            top[g, rows] = jnp.broadcast_to(new, (tile_rows, 128))
            acc[rows, cols] = acc[rows, cols] * keep + jnp.dot(
                weights.astype(jnp.bfloat16), v_ref[0], preferred_element_type=f32
            )

    for t in range(tile_count):
        picked = chosen_ref[t, page] != 0
        pl.when(jnp.logical_and(picked, causal))(functools.partial(visit, t, True))
        pl.when(jnp.logical_and(picked, jnp.logical_not(causal)))(
            functools.partial(visit, t, False)
        )

    @pl.when(page == pl.num_programs(1) - 1)
    def _():
        mix_ref[...] = acc[...].astype(jnp.bfloat16)
        lane = lax.broadcasted_iota(jnp.int32, m_ref.shape[1:], 1)
        maxima = jnp.zeros(m_ref.shape[1:], f32)
        sums = jnp.zeros(m_ref.shape[1:], f32)
        for g in range(group):
            maxima = jnp.where(lane == g, top[g], maxima)
            sums = jnp.where(lane == g, total[g], sums)
        m_ref[0] = maxima
        l_ref[0] = sums


def owner_pass(queries, keys, values, page_map, selected, ctx_index, ctx_count):
    pages_local, page_len, kv_width = keys.shape
    row_count, query_width = queries.shape
    kv_local = kv_width // HEAD_SIZE
    group = query_width // kv_width
    tile_count = selected.shape[0]
    page_total = pages_local * ctx_count
    slot_ids = ctx_index * pages_local + jnp.arange(pages_local, dtype=jnp.int32)
    all_pages = jnp.arange(page_total, dtype=jnp.int32)
    logical = jnp.sum(
        jnp.where(page_map[None, :] == slot_ids[:, None], all_pages[None, :], 0), axis=1
    )
    chosen = jnp.any(selected[:, None, :] == logical[None, :, None], axis=2).astype(jnp.int32)
    stat = jax.ShapeDtypeStruct((kv_local, row_count, 128), jnp.float32)
    stat_spec = pl.BlockSpec((1, row_count, 128), lambda k, p, a, b: (k, 0, 0))
    kv_spec = pl.BlockSpec((1, page_len, HEAD_SIZE), lambda k, p, a, b: (p, 0, k))
    q_spec = pl.BlockSpec((row_count, group * HEAD_SIZE), lambda k, p, a, b: (0, k))

    def kernel(logical_ref, chosen_ref, *refs):
        attention_kernel(logical_ref, chosen_ref, page_total, *refs)

    mixture, top, total = pl.pallas_call(
        kernel,
        grid_spec=pltpu.PrefetchScalarGridSpec(
            num_scalar_prefetch=2,
            grid=(kv_local, pages_local),
            in_specs=[q_spec, kv_spec, kv_spec],
            out_specs=(q_spec, stat_spec, stat_spec),
            scratch_shapes=[
                pltpu.VMEM((row_count, group * HEAD_SIZE), jnp.float32),
                pltpu.VMEM((group, row_count, 128), jnp.float32),
                pltpu.VMEM((group, row_count, 128), jnp.float32),
            ],
        ),
        out_shape=(jax.ShapeDtypeStruct((row_count, query_width), jnp.bfloat16), stat, stat),
    )(logical.astype(jnp.int32), chosen, queries, keys, values)

    def heads(stacked):
        return stacked[:, :, :group].transpose(1, 0, 2).reshape(row_count, kv_local * group)

    return heads(top), heads(total), mixture


MESH = pl.DeviceIdType.MESH
CORES = 2


def column_tile(width):
    for tile in (896, 768, 640, 512, 384, 256, 128):
        if width % tile == 0:
            return tile
    return width


def flat(block, rows):
    if block.shape[1] % 16:
        return block.astype(jnp.float32).reshape(rows, -1).astype(jnp.bfloat16)
    return block.reshape(rows, -1)


def tail_kernel(
    C,
    H,
    mix_ref,
    stat_ref,
    res_ref,
    gain_ref,
    ow_hbm,
    gw_hbm,
    uw_hbm,
    dw_hbm,
    mlp_ref,
    own_ref,
    ow,
    gw,
    uw,
    dw,
    mix_in,
    stat_in,
    att,
    po,
    po_in,
    u_out,
    st_out,
    ss,
    ublk,
    own_st,
    first,
    first_in,
    second,
    second_in,
    hid,
    acc,
    part,
    part_in,
    w_sem,
    mix_s,
    mix_r,
    stat_s,
    stat_r,
    att_s,
    att_r,
    po_s,
    po_r,
    u_s,
    u_r,
    st_s,
    st_r,
    ss_s,
    ss_r,
    f_s,
    f_r,
    g_s,
    g_r,
    h_s,
    h_r,
    fw_s,
    part_s,
    part_r,
):
    c = lax.axis_index("ctx")
    h = lax.axis_index("head")
    Y = H // CORES
    y = h // CORES
    core = h % CORES
    partner = y * CORES + (CORES - 1 - core)
    R = mix_ref.shape[1]
    rows = C * R
    rb = C // H
    bph = C // H
    width = ow.shape[0]
    head_rows = rows // H
    heads = mix_ref.shape[2] // HEAD_SIZE
    tiles, _, _, _, _, tile = first.shape
    f32 = jnp.float32
    bf16 = jnp.bfloat16

    def remote(src, dst, send_sem, recv_sem, ctx, head):
        return pltpu.make_async_remote_copy(
            src_ref=src,
            dst_ref=dst,
            send_sem=send_sem,
            recv_sem=recv_sem,
            device_id=(ctx, head),
            device_id_type=MESH,
        )

    sent = []

    def send(*args):
        copy = remote(*args)
        copy.start()
        sent.append(copy)

    loads = [
        pltpu.make_async_copy(src, dst, w_sem.at[i])
        for i, (src, dst) in enumerate(
            ((ow_hbm, ow), (gw_hbm, gw), (uw_hbm, uw), (dw_hbm, dw))
        )
    ]
    for load in loads:
        load.start()

    for d in range(1, C):
        peer = (c + d) % C
        send(stat_ref.at[peer], stat_in.at[c], stat_s.at[d], stat_r.at[c], peer, h)
        send(mix_ref.at[peer], mix_in.at[c], mix_s.at[d], mix_r.at[c], peer, h)
    stat_in[c] = stat_ref[c]
    mix_in[c] = mix_ref[c]
    for d in range(1, C):
        peer = (c + C - d) % C
        remote(stat_in.at[peer], stat_in.at[peer], stat_s.at[d], stat_r.at[peer], peer, h).wait_recv()
        remote(mix_in.at[peer], mix_in.at[peer], mix_s.at[d], mix_r.at[peer], peer, h).wait_recv()
    maxima = [stat_in[k][:, :heads] for k in range(C)]
    top = functools.reduce(jnp.maximum, maxima)
    scales = [jnp.exp(m - top) for m in maxima]
    total = sum(stat_in[k][:, heads : 2 * heads] * scales[k] for k in range(C))
    inverse = 1.0 / total
    for g in range(heads):
        cols = slice(g * HEAD_SIZE, (g + 1) * HEAD_SIZE)
        mixed = sum(mix_in[k, :, cols].astype(f32) * scales[k][:, g : g + 1] for k in range(C))
        att[c, :, cols] = (mixed * inverse[:, g : g + 1]).astype(bf16)

    for d in range(1, C):
        peer = (c + d) % C
        send(att.at[c], att.at[c], att_s.at[d], att_r.at[c], peer, h)
    loads[0].wait()
    for d in range(1, C):
        peer = (c + C - d) % C
        remote(att.at[peer], att.at[peer], att_s.at[d], att_r.at[peer], peer, h).wait_recv()
    projected = lax.dot_general(
        flat(att[...], rows), ow[...], (((1,), (1,)), ((), ())), preferred_element_type=f32
    )
    po[...] = projected.reshape(H, head_rows, width).astype(bf16)

    for d in range(1, H):
        peer = (h + d) % H
        send(po.at[peer], po_in.at[h], po_s.at[d], po_r.at[h], c, peer)
    po_in[h] = po[h]
    for d in range(1, H):
        peer = (h + H - d) % H
        remote(po_in.at[peer], po_in.at[peer], po_s.at[d], po_r.at[peer], c, peer).wait_recv()
    projected = sum(po_in[k].astype(f32) for k in range(H))
    stream = (res_ref[...].astype(f32) + projected).astype(bf16).astype(f32)
    st_out[...] = stream.reshape(rb, R, width).astype(bf16)
    u_out[...] = (stream * gain_ref[...]).reshape(rb, R, width).astype(bf16)
    squares = jnp.sum(stream * stream, axis=1, keepdims=True)
    ss[c] = jnp.broadcast_to(squares, (head_rows, 128))

    block_head = c // bph
    block_part = c % bph
    u_dst = ublk.at[block_part, pl.ds(h * rb, rb)]
    kept = []
    for d in range(C):
        peer = (c + d) % C
        copy = remote(u_out, u_dst, u_s.at[d], u_r.at[block_part, h], peer, block_head)
        if d == 0:
            kept.append((block_head != h, copy))
            pl.when(block_head != h)(copy.start)

            @pl.when(block_head == h)
            def _():
                ublk[block_part, pl.ds(h * rb, rb)] = u_out[...]

        else:
            copy.start()
            sent.append(copy)
    for d in range(1, C):
        peer = (c + d) % C
        send(ss.at[c], ss.at[c], ss_s.at[d], ss_r.at[c], peer, h)
    for i in range(rb):
        owner = h * rb + i
        other = jnp.logical_or(owner != c, block_head != h)
        copy = remote(
            st_out.at[i], own_st.at[block_part], st_s.at[i], st_r.at[block_part], owner, block_head
        )
        kept.append((other, copy))
        pl.when(other)(copy.start)

        @pl.when(jnp.logical_not(other))
        def _(i=i):
            own_st[block_part] = st_out[i]

    for j in range(bph):
        for k in range(H):
            source = h * bph + j
            block = ublk.at[j, pl.ds(k * rb, rb)]
            arrival = remote(block, block, u_s.at[0], u_r.at[j, k], source, k)
            pl.when(jnp.logical_or(source != c, h != k))(arrival.wait_recv)
    loads[1].wait()
    loads[2].wait()

    def matmul(i, which, weight):
        cols = slice(i * tile, (i + 1) * tile)
        value = None
        for j in range(bph):
            term = jnp.dot(
                flat(ublk[j], rows),
                weight[j * width : (j + 1) * width, cols],
                preferred_element_type=f32,
            )
            value = term if value is None else value + term
        first[i, which] = value.reshape(Y, CORES, head_rows, tile).swapaxes(0, 1).astype(bf16)
        send(
            first.at[i, which, CORES - 1 - core],
            first_in.at[i, which],
            f_s.at[i, which],
            f_r.at[i, which],
            c,
            partner,
        )

    def middle(i, which):
        remote(
            first_in.at[i, which], first_in.at[i, which], f_s.at[i, which], f_r.at[i, which], c, partner
        ).wait_recv()
        both = first[i, which, core].astype(f32) + first_in[i, which].astype(f32)
        second[i, which] = both.astype(bf16)
        for d in range(1, Y):
            peer = (y + d) % Y
            send(
                second.at[i, which, peer],
                second_in.at[i, which, y],
                g_s.at[i, which, d],
                g_r.at[i, which, y],
                c,
                peer * CORES + core,
            )

    def finish(i, inverse_rms):
        sums = []
        for which in range(2):
            value = second[i, which, y].astype(f32)
            for d in range(1, Y):
                peer = (y + Y - d) % Y
                slot = second_in.at[i, which, peer]
                remote(
                    slot, slot, g_s.at[i, which, d], g_r.at[i, which, peer], c, peer * CORES + core
                ).wait_recv()
                value = value + second_in[i, which, peer].astype(f32)
            sums.append(value * inverse_rms)
        hid[i, h] = (jax.nn.gelu(sums[0], approximate=True) * sums[1]).astype(bf16)
        send(hid.at[i, h], hid.at[i, h], h_s.at[i, 0], h_r.at[i, h], c, partner)
        for d in range(1, Y):
            peer = ((y + d) % Y) * CORES + core
            send(hid.at[i, h], hid.at[i, h], h_s.at[i, d], h_r.at[i, h], c, peer)

    def forward(i):
        for d in range(1, Y):
            origin = ((y + Y - d) % Y) * CORES + core
            slot = hid.at[i, origin]
            remote(slot, slot, h_s.at[i, d], h_r.at[i, origin], c, origin).wait_recv()
            send(slot, slot, fw_s.at[i, d], h_r.at[i, origin], c, partner)

    def down(i):
        for d in range(Y):
            origin = ((y + Y - d) % Y) * CORES + (CORES - 1 - core)
            slot = hid.at[i, origin]
            remote(slot, slot, h_s.at[i, 0], h_r.at[i, origin], c, partner).wait_recv()
        term = lax.dot_general(
            flat(hid[i], rows),
            dw[:, i * tile : (i + 1) * tile],
            (((1,), (1,)), ((), ())),
            preferred_element_type=f32,
        )
        if i == 0:
            acc[...] = term
        else:
            acc[...] += term

    steps = [(i, which) for i in range(tiles) for which in range(2)]
    for n, (i, which) in enumerate(steps):
        matmul(i, which, (gw, uw)[which])
        if n:
            middle(*steps[n - 1])
    middle(*steps[-1])
    for d in range(1, C):
        peer = (c + C - d) % C
        remote(ss.at[peer], ss.at[peer], ss_s.at[d], ss_r.at[peer], peer, h).wait_recv()
    squares = sum(ss[k] for k in range(C))
    inverse_rms = lax.rsqrt(squares[:, :1] / (C * width) + norm_epsilon)
    loads[3].wait()
    for i in range(tiles):
        finish(i, inverse_rms)
        if i:
            forward(i - 1)
    forward(tiles - 1)
    for i in range(tiles):
        down(i)
    part[...] = acc[...].reshape(C, R, acc.shape[1]).astype(bf16)

    for d in range(1, C):
        peer = (c + d) % C
        send(part.at[peer], part_in.at[c], part_s.at[d], part_r.at[c], peer, h)
    part_in[c] = part[c]
    for j in range(bph):
        source = h * bph + j
        arrival = remote(own_st.at[j], own_st.at[j], st_s.at[0], st_r.at[j], source, c // rb)
        pl.when(jnp.logical_or(source != c, c // rb != h))(arrival.wait_recv)
    own_ref[...] = own_st[...]
    for d in range(1, C):
        peer = (c + C - d) % C
        remote(part_in.at[peer], part_in.at[peer], part_s.at[d], part_r.at[peer], peer, h).wait_recv()
    mlp_ref[...] = sum(part_in[k].astype(f32) for k in range(C))
    for copy in sent:
        copy.wait_send()
    for condition, copy in kept:
        pl.when(condition)(copy.wait_send)


def tail(C, H, mixture, stats, residual_in, norm_gain, out_weight, gate_weight, up_weight, down_weight):
    rows, query_width = mixture.shape
    R = rows // C
    width = out_weight.shape[1]
    hidden = gate_weight.shape[1]
    out_width = down_weight.shape[1]
    out_weight = out_weight.T
    down_weight = down_weight.T
    rb = C // H
    bph = C // H
    Y = H // CORES
    head_rows = rows // H
    tile = column_tile(hidden)
    tiles = hidden // tile
    bf16 = jnp.bfloat16
    vmem = pl.BlockSpec(memory_space=pltpu.VMEM)
    hbm = pl.BlockSpec(memory_space=pl.ANY)
    V = pltpu.VMEM
    S = pltpu.SemaphoreType.DMA
    return pl.pallas_call(
        functools.partial(tail_kernel, C, H),
        out_shape=(
            jax.ShapeDtypeStruct((R, out_width), jnp.float32),
            jax.ShapeDtypeStruct((bph, R, width), bf16),
        ),
        in_specs=[vmem] * 4 + [hbm] * 4,
        out_specs=(vmem, vmem),
        scratch_shapes=[
            V(out_weight.shape, bf16),
            V(gate_weight.shape, bf16),
            V(up_weight.shape, bf16),
            V(down_weight.shape, bf16),
            V((C, R, query_width), bf16),
            V((C, R, 128), jnp.float32),
            V((C, R, query_width), bf16),
            V((H, head_rows, width), bf16),
            V((H, head_rows, width), bf16),
            V((rb, R, width), bf16),
            V((rb, R, width), bf16),
            V((C, head_rows, 128), jnp.float32),
            V((bph, C, R, width), bf16),
            V((bph, R, width), bf16),
            V((tiles, 2, CORES, Y, head_rows, tile), bf16),
            V((tiles, 2, Y, head_rows, tile), bf16),
            V((tiles, 2, Y, head_rows, tile), bf16),
            V((tiles, 2, Y, head_rows, tile), bf16),
            V((tiles, H, head_rows, tile), bf16),
            V((rows, out_width), jnp.float32),
            V((C, R, out_width), bf16),
            V((C, R, out_width), bf16),
            S((4,)),
            S((C,)),
            S((C,)),
            S((C,)),
            S((C,)),
            S((C,)),
            S((C,)),
            S((H,)),
            S((H,)),
            S((C,)),
            S((bph, H)),
            S((rb,)),
            S((bph,)),
            S((C,)),
            S((C,)),
            S((tiles, 2)),
            S((tiles, 2)),
            S((tiles, 2, Y)),
            S((tiles, 2, Y)),
            S((tiles, Y)),
            S((tiles, H)),
            S((tiles, Y)),
            S((C,)),
            S((C,)),
        ],
        compiler_params=pltpu.CompilerParams(
            has_side_effects=True, vmem_limit_bytes=60 * 2**20
        ),
    )(
        mixture.reshape(C, R, query_width),
        stats.reshape(C, R, 128),
        residual_in,
        norm_gain.reshape(1, width),
        out_weight,
        gate_weight,
        up_weight,
        down_weight,
    )


LOG2E = 1.4426950408889634


def fused_kernel(
    C,
    H,
    NP,
    map_hbm,
    sel_hbm,
    q_hbm,
    res_hbm,
    gain_hbm,
    k_hbm,
    v_hbm,
    ow_hbm,
    gw_hbm,
    uw_hbm,
    dw_hbm,
    out_ref,
    map_ref,
    sel_ref,
    q_ref,
    res_ref,
    gain_ref,
    k_buf,
    v_buf,
    ow,
    gw,
    uw,
    dw,
    mix_out,
    mix_in,
    lse_out,
    lse_in,
    att,
    po_out,
    po_in,
    res_in,
    st,
    u,
    ss_out,
    ss_in,
    ss_mid,
    ss_last,
    scale,
    begun,
    first,
    first_in,
    second,
    second_in,
    hid,
    acc,
    part,
    part_in,
    in_sem,
    kv_sem,
    w_sem,
    mix_s,
    mix_r,
    lse_s,
    lse_r,
    att_s,
    att_r,
    cross_r,
    po_s,
    po_r,
    res_s,
    res_r,
    u_s,
    u_r,
    ss_s,
    ss_r,
    f_s,
    f_r,
    g_s,
    g_r,
    h_s,
    h_r,
    part_s,
    part_r,
):
    c = lax.axis_index("ctx")
    h = lax.axis_index("head")
    X = C // H
    Z = C // X
    z = c // X
    x = c % X
    Y = H // CORES
    y = h // CORES
    core = h % CORES
    partner = y * CORES + (CORES - 1 - core)
    _, NQ, RC, query_width = q_ref.shape
    rows = C * RC
    hr = rows // H
    kv, pages, page_len, _ = k_buf.shape
    group = query_width // (kv * HEAD_SIZE)
    gw_cols = group * HEAD_SIZE
    tile_count = sel_ref.shape[0]
    tile_rows = NQ * rows // tile_count
    offset = page_len - NQ * rows
    page_total = map_ref.shape[0]
    width = ow.shape[0]
    tile = first.shape[-1]
    tiles = first.shape[1]
    RP = rows // NP
    f32 = jnp.float32
    bf16 = jnp.bfloat16
    owner = h == z
    visitor = h != z

    def remote(src, dst, send_sem, recv_sem, ctx, head):
        return pltpu.make_async_remote_copy(
            src_ref=src,
            dst_ref=dst,
            send_sem=send_sem,
            recv_sem=recv_sem,
            device_id=(ctx, head),
            device_id_type=MESH,
        )

    sent = []
    kept = []

    def start(*args):
        remote(*args).start()

    def send(*args):
        copy = remote(*args)
        copy.start()
        sent.append(copy)

    def send_if(condition, *args):
        copy = remote(*args)
        pl.when(condition)(copy.start)
        kept.append((condition, copy))

    def kv_load(j):
        lanes = pl.ds(pl.multiple_of(j * HEAD_SIZE, HEAD_SIZE), HEAD_SIZE)
        return (
            pltpu.make_async_copy(k_hbm.at[:, :, lanes], k_buf.at[j], kv_sem.at[0, j]),
            pltpu.make_async_copy(v_hbm.at[:, :, lanes], v_buf.at[j], kv_sem.at[1, j]),
        )

    barrier = pltpu.get_barrier_semaphore()
    for d in range(1, C):
        pl.semaphore_signal(
            barrier, inc=1, device_id=((c + d) % C, h), device_id_type=MESH
        )
    for d in range(1, H):
        pl.semaphore_signal(
            barrier, inc=1, device_id=(c, (h + d) % H), device_id_type=MESH
        )
    inputs = [
        pltpu.make_async_copy(src, dst, in_sem.at[i])
        for i, (src, dst) in enumerate(
            (
                (map_hbm, map_ref),
                (sel_hbm, sel_ref),
                (q_hbm, q_ref),
                (res_hbm, res_ref),
                (gain_hbm, gain_ref.at[0]),
            )
        )
    ]
    for load in inputs:
        load.start()
    for load in kv_load(0):
        load.start()
    loads = [
        pltpu.make_async_copy(src, dst, w_sem.at[i])
        for i, (src, dst) in enumerate(
            ((ow_hbm, ow), (gw_hbm, gw), (uw_hbm, uw), (dw_hbm, dw))
        )
    ]
    for load in inputs[:3]:
        load.wait()

    facts = []
    for p in range(pages):
        slot = c * pages + p
        logical = jnp.int32(0)
        for j in range(page_total):
            logical = logical + jnp.where(map_ref[j] == slot, j, 0)
        picks = []
        for t in range(tile_count):
            hits = jnp.int32(0)
            for i in range(sel_ref.shape[1]):
                hits = hits + jnp.where(sel_ref[t, i] == logical, 1, 0)
            picks.append(jnp.where(hits > 0, 0.0, masked_score).astype(f32))
        reach = jnp.where(logical == page_total - 1, 0, page_len)
        facts.append((reach, picks))

    index = lax.broadcasted_iota(jnp.int32, (group * rows, 1), 0) & (rows - 1)
    shift = RC.bit_length() - 1
    base_row = (index >> shift) * (NQ * RC) + (index & (RC - 1))
    eye = lax.broadcasted_iota(jnp.int32, (rows, rows), 0) == lax.broadcasted_iota(
        jnp.int32, (rows, rows), 1
    )
    unit = score_scale * LOG2E

    def attend(n):
        q = n // kv
        j = n % kv

        @pl.when(n < kv)
        def _():
            for load in kv_load(j):
                load.wait()

        @pl.when(n == 0)
        def _():
            for k in range(1, kv):
                for load in kv_load(k):
                    load.start()
            for load in loads:
                load.start()

        lanes = pl.ds(pl.multiple_of(j * gw_cols, gw_cols), gw_cols)
        block = q_ref[:, q, :, lanes].reshape(rows, gw_cols)
        lhs = jnp.concatenate(
            [block[:, g * HEAD_SIZE : (g + 1) * HEAD_SIZE] for g in range(group)], axis=0
        )
        row = base_row + q * RC
        key = offset + lax.broadcasted_iota(jnp.int32, (group * rows, page_len - offset), 1)
        tops, sums, outs = [], [], []
        for p in range(pages):
            reach, picks = facts[p]
            bias = jnp.zeros((group * rows, 1), f32)
            for t in range(tile_count):
                inside = jnp.logical_and(row >= t * tile_rows, row < (t + 1) * tile_rows)
                bias = jnp.where(inside, picks[t], bias)
            scores = lax.dot_general(
                lhs, k_buf[j, p], (((1,), (1,)), ((), ())), preferred_element_type=f32
            )
            late = jnp.where(key <= offset + row + reach, scores[:, offset:], masked_score)
            scores = jnp.concatenate([scores[:, :offset], late], axis=1)
            top = jnp.max(scores, axis=1, keepdims=True)
            weights = jnp.exp2((scores - top) * unit)
            sums.append(jnp.sum(weights, axis=1, keepdims=True))
            outs.append(
                jnp.dot(weights.astype(bf16), v_buf[j, p], preferred_element_type=f32)
            )
            tops.append(top * unit + bias)
        best = functools.reduce(jnp.maximum, tops)
        scales = [jnp.exp2(top - best) for top in tops]
        total = sum(s * e for s, e in zip(sums, scales))
        mixed = sum(o * (e / total) for o, e in zip(outs, scales))
        lse = best + jnp.log2(total)
        for g in range(group):
            part_rows = slice(g * rows, (g + 1) * rows)
            mix_out[n, :, :, g * HEAD_SIZE : (g + 1) * HEAD_SIZE] = (
                mixed[part_rows].reshape(C, RC, HEAD_SIZE).astype(bf16)
            )
            lse_out[n, g : g + 1] = jnp.sum(
                jnp.where(eye, lse[part_rows], 0.0), axis=0, keepdims=True
            )
        mix_in[n, c] = mix_out[n, c]
        lse_in[n, c] = lse_out[n]

    def mix_sends(n):
        for d in range(1, C):
            peer = (c + d) % C
            remote(mix_out.at[n, peer], mix_in.at[n, c], mix_s.at[0], mix_r.at[n], peer, h).start()
            remote(lse_out.at[n], lse_in.at[n, c], lse_s.at[0], lse_r.at[n], peer, h).start()

    def att_sends(n, direct):
        block = att.at[n, c]
        if direct:
            for d in range(1, C):
                start(block, block, att_s.at[0], att_r.at[n], (c + d) % C, h)
        else:
            for d in range(1, Z):
                start(block, block, att_s.at[0], att_r.at[n], (z + d) % Z * X + x, h)
            for d in range(1, X):
                start(block, block, att_s.at[0], cross_r.at[n - kv], z * X + (x + d) % X, h)

    def att_relay(n):
        arrived(att.at[n, pl.ds(0, Z - 1)], att_r.at[n])
        for e in range(1, Z):
            block = att.at[n, (z + e) % Z * X + x]
            for d in range(1, X):
                start(block, block, att_s.at[0], cross_r.at[n - kv], z * X + (x + d) % X, h)

    def arrived(block, recv_sem):
        remote(block, block, recv_sem, recv_sem, c, partner).wait_recv()

    def left(block, send_sem):
        remote(block, block, send_sem, send_sem, c, partner).wait_send()

    def combine(n, direct):
        arrived(lse_in.at[n, pl.ds(0, C - 1)], lse_r.at[n])
        arrived(mix_in.at[n, pl.ds(0, C - 1)], mix_r.at[n])
        logs = [lse_in[n, k] for k in range(C)]
        best = functools.reduce(jnp.maximum, logs)
        scales = [jnp.exp2(value - best) for value in logs]
        inverse = 1.0 / sum(scales)
        lane = lax.broadcasted_iota(jnp.int32, (RC, rows), 1)
        mine = lane == c * RC + lax.broadcasted_iota(jnp.int32, (RC, rows), 0)
        for g in range(group):
            cols = slice(g * HEAD_SIZE, (g + 1) * HEAD_SIZE)
            value = jnp.zeros((RC, HEAD_SIZE), f32)
            for k in range(C):
                share = (scales[k] * inverse)[g : g + 1]
                share = jnp.sum(jnp.where(mine, share, 0.0), axis=1, keepdims=True)
                value = value + share * mix_in[n, k, :, cols].astype(f32)
            att[n, c, :, cols] = value.astype(bf16)
        att_sends(n, direct)

    def project(q):
        for j in range(kv):
            n = q * kv + j
            if q == 0:
                arrived(att.at[n, pl.ds(0, C - 1)], att_r.at[n])
            else:
                arrived(att.at[n, pl.ds(0, (X - 1) * Z)], cross_r.at[n - kv])
        if q == 0:
            loads[0].wait()
        value = None
        for j in range(kv):
            term = lax.dot_general(
                att[q * kv + j].reshape(rows, gw_cols),
                ow[:, j * gw_cols : (j + 1) * gw_cols],
                (((1,), (1,)), ((), ())),
                preferred_element_type=f32,
            )
            value = term if value is None else value + term
        po_out[q] = value.astype(bf16)
        for i in range(NP):
            piece = pl.ds(i * RP, RP)
            copy = remote(
                po_out.at[q, piece], po_in.at[q, h, piece], po_s.at[q], po_r.at[q, i], c, z
            )
            pl.when(visitor)(copy.start)
        po_in[q, h] = po_out[q]

    def own(q, i):
        if q == 0 and i == 0:
            arrived(res_in.at[pl.ds(0, H - 1)], res_r.at[0])
        arrived(po_in.at[q, pl.ds(0, H - 1), pl.ds(i * RP, RP)], po_r.at[q, i])
        spare = u.shape[-1] - width
        lane = lax.broadcasted_iota(jnp.int32, (hr, spare), 1)
        for b in range(i * RP // hr, (i + 1) * RP // hr):
            span = slice(b * hr, (b + 1) * hr)
            value = res_in[b, :, q].reshape(hr, width).astype(f32)
            added = sum(po_in[q, k, span].astype(f32) for k in range(H))
            stream = (value + added).astype(bf16)
            st[q, span] = stream
            stream = stream.astype(f32)
            u[q, x, span, :width] = (stream * gain_ref[...]).astype(bf16)
            squares = jnp.sum(stream * stream, axis=1, keepdims=True)
            high = squares.astype(bf16).astype(f32)
            mid = (squares - high).astype(bf16).astype(f32)
            low = squares - high - mid
            packed = jnp.where(lane == 0, high, jnp.where(lane == 1, mid, low))
            packed = jnp.where(lane < 3, packed, 0.0)
            u[q, x, span, width:] = packed.astype(bf16)

    def relay(q, i, here):
        piece = u.at[q, x, pl.ds(i * RP, RP)]
        recv = u_r.at[q, x, i]
        pl.when(jnp.logical_and(here, visitor))(functools.partial(arrived, piece, recv))
        for way, ahead in enumerate((Z - 1 - z, z)):
            step = 1 - 2 * way
            go = jnp.logical_and(jnp.logical_and(here, step * (z - h) >= 0), ahead > 0)
            target = jnp.clip(z + step, 0, Z - 1) * X + x
            copy = remote(piece, piece, u_s.at[way], recv, target, h)
            pl.when(go)(copy.start)
            kept.append((go, copy))
        for d in range(1, X):
            peer = z * X + (x + d) % X
            copy = remote(piece, piece, u_s.at[1 + d], recv, peer, h)
            pl.when(here)(copy.start)
            kept.append((here, copy))

    def spread(q, here):
        for i in range(NP):
            pl.when(jnp.logical_and(here, owner))(functools.partial(own, q, i))
            relay(q, i, here)

    def gather(q):
        for d in range(1, X):
            source = (x + d) % X
            for i in range(NP):
                block = u.at[q, source, pl.ds(i * RP, RP)]
                arrived(block, u_r.at[q, source, i])
        squares = 0.0
        for k in range(X):
            split = u[q, k, :, width:].astype(f32)
            squares = squares + jnp.sum(split, axis=1, keepdims=True)
        squares = jnp.broadcast_to(squares, (rows, 128)).reshape(Y, CORES, hr, 128)
        ss_out[q] = squares.swapaxes(0, 1)
        send(ss_out.at[q, CORES - 1 - core], ss_in.at[q], ss_s.at[q, 0], ss_r.at[q, 0], c, partner)

    def block_dot(q, k, i, which):
        weight = (gw, uw)[which]
        span = pl.ds(pl.multiple_of(k * width, 16), width)
        return jnp.dot(
            u[q, k, :, :width],
            weight[span, i * tile : (i + 1) * tile],
            preferred_element_type=f32,
        )

    def start_expand(q):
        if q == 0:
            loads[1].wait()
            loads[2].wait()
        for i in range(tiles):
            for which in range(2):
                begun[i, which] = block_dot(q, x, i, which)

    def matmul(q, i, which):
        value = begun[i, which]
        for d in range(1, X):
            value = value + block_dot(q, (x + d) % X, i, which)
        value = value.reshape(Y, CORES, hr, tile).swapaxes(0, 1).astype(bf16)
        first[q, i, which] = value
        start(
            first.at[q, i, which, CORES - 1 - core],
            first_in.at[q, i, which],
            f_s.at[0],
            f_r.at[q, i, which],
            c,
            partner,
        )

    def middle(q, i, which):
        block = first_in.at[q, i, which]
        arrived(block, f_r.at[q, i, which])
        both = first[q, i, which, core].astype(f32) + first_in[q, i, which].astype(f32)
        second[q, i, which] = both.astype(bf16)
        for d in range(1, Y):
            peer = (y + d) % Y
            start(
                second.at[q, i, which, peer],
                second_in.at[q, i, which, y],
                g_s.at[0],
                g_r.at[q, i, which, y],
                c,
                peer * CORES + core,
            )

    def middle_squares(q):
        block = ss_in.at[q]
        remote(block, block, ss_s.at[q, 0], ss_r.at[q, 0], c, partner).wait_recv()
        ss_mid[q] = ss_out[q, core] + ss_in[q]
        for d in range(1, Y):
            peer = (y + d) % Y
            send(
                ss_mid.at[q, peer],
                ss_last.at[q, y],
                ss_s.at[q, d],
                ss_r.at[q, 1 + y],
                c,
                peer * CORES + core,
            )

    def inverse_rms(q):
        total = ss_mid[q, y]
        for d in range(1, Y):
            peer = (y + Y - d) % Y
            block = ss_last.at[q, peer]
            remote(
                block, block, ss_s.at[q, d], ss_r.at[q, 1 + peer], c, peer * CORES + core
            ).wait_recv()
            total = total + ss_last[q, peer]
        scale[q] = lax.rsqrt(total / (C * width) + norm_epsilon)

    def finish(q, i):
        inverse = scale[q][:, :1]
        sums = []
        for which in range(2):
            value = second[q, i, which, y].astype(f32)
            for d in range(1, Y):
                peer = (y + Y - d) % Y
                block = second_in.at[q, i, which, peer]
                remote(
                    block,
                    block,
                    g_s.at[0],
                    g_r.at[q, i, which, peer],
                    c,
                    peer * CORES + core,
                ).wait_recv()
                value = value + second_in[q, i, which, peer].astype(f32)
            sums.append(value * inverse)
        hid[q, i, h] = (jax.nn.gelu(sums[0], approximate=True) * sums[1]).astype(bf16)
        block = hid.at[q, i, h]
        for d in range(1, Y):
            peer = ((y + d) % Y) * CORES + core
            start(block, block, h_s.at[0], h_r.at[q, i, h], c, peer)
        start(block, block, h_s.at[0], h_r.at[q, i, h], c, partner)

    def forward(q, i):
        for d in range(1, Y):
            origin = ((y + Y - d) % Y) * CORES + core
            block = hid.at[q, i, origin]
            arrived(block, h_r.at[q, i, origin])
            start(block, block, h_s.at[0], h_r.at[q, i, origin], c, partner)

    def down(q, i):
        for d in range(Y):
            origin = ((y + Y - d) % Y) * CORES + (CORES - 1 - core)
            block = hid.at[q, i, origin]
            arrived(block, h_r.at[q, i, origin])
        if q == 0 and i == 0:
            loads[3].wait()
        term = lax.dot_general(
            hid[q, i].reshape(rows, tile),
            dw[:, i * tile : (i + 1) * tile],
            (((1,), (1,)), ((), ())),
            preferred_element_type=f32,
        )
        if i == 0:
            acc[...] = term
        else:
            acc[...] += term

    def scatter(q):
        for k in range(X):

            @pl.when(jnp.logical_and(owner, x == k))
            def _(k=k):
                acc[:, k * width : (k + 1) * width] += st[q].astype(f32)

        part[q] = acc[...].reshape(C, RC, acc.shape[1]).astype(bf16)
        for d in range(1, C):
            peer = (c + d) % C
            start(part.at[q, peer], part_in.at[q, c], part_s.at[0], part_r.at[q], peer, h)
        part_in[q, c] = part[q, c]

    def collect(q):
        arrived(part_in.at[q, pl.ds(0, C - 1)], part_r.at[q])
        out_ref[q] = sum(part_in[q, k].astype(f32) for k in range(C)).astype(bf16)

    steps = NQ * kv
    lag = 3

    def loop(n, carry):
        attend(n)

        @pl.when(n == 1)
        def _():
            pl.semaphore_wait(barrier, C + H - 2)
            mix_sends(0)

        ready = jnp.logical_and(n >= 1, n < kv)
        pl.when(jnp.logical_or(ready, n >= kv + lag - 1))(functools.partial(mix_sends, n))

        for k in range(kv):

            @pl.when(n == (kv + lag - 2 if k == kv - 1 else max(k + 2, lag)))
            def _(k=k):
                combine(k, True)

        @pl.when(n == kv + lag - 2)
        def _():
            for k in range(kv, kv + lag - 1):
                mix_sends(k)

        return carry

    lax.fori_loop(0, steps, loop, 0)
    for load in inputs[3:]:
        load.wait()
    send_if(visitor, res_ref, res_in.at[h], res_s.at[0], res_r.at[0], c, z)
    res_in[h] = res_ref[...]
    pairs = [(i, which) for i in range(tiles) for which in range(2)]

    def expand(q, extra=None):
        gather(q)
        for n, (i, which) in enumerate(pairs):
            matmul(q, i, which)
            if n == 1:
                middle_squares(q)
            if n:
                middle(q, *pairs[n - 1])
            if extra is not None and which:
                extra(i)
        middle(q, *pairs[-1])

    def finish_if(here, q, i):
        @pl.when(here)
        def _():
            if i == 0:
                inverse_rms(q)
            finish(q, i)

    def contract(q, done=0):
        forward(q, done)
        for i in range(done, tiles):
            if i + 1 < tiles:
                forward(q, i + 1)
            down(q, i)
        scatter(q)

    def between(i):
        finish_if(early, 0, i)
        if i:

            @pl.when(late)
            def _():
                forward(0, i - 1)
                down(0, i - 1)


    far = jnp.maximum(z - h, h - z)
    early = z // CORES == y
    late = z // CORES != y
    project(0)
    for n in range(kv, steps - 2):
        combine(n, False)
    spread(0, far == 0)
    for n in range(steps - 2, steps):
        combine(n, False)
    for n in range(kv, steps - 2):
        att_relay(n)
    spread(0, far == 1)
    for n in range(steps - 2, steps):
        att_relay(n)
    pl.when(far <= 1)(lambda: start_expand(0))
    spread(0, far == 2)
    project(1)
    spread(0, far > 2)
    pl.when(far > 1)(lambda: start_expand(0))
    expand(0, lambda i: spread(1, far == 0) if i == tiles - 1 else None)
    first_on = jnp.logical_and(late, far <= 2)
    spread(1, first_on)
    for i in range(tiles):
        finish_if(late, 0, i)
    spread(1, jnp.logical_and(jnp.logical_not(first_on), far > 0))
    start_expand(1)
    expand(1, between)
    for i in range(tiles - 1):
        finish_if(late, 1, i)
    pl.when(late)(lambda: contract(0, tiles - 1))
    finish_if(late, 1, tiles - 1)
    pl.when(early)(lambda: contract(0))
    for i in range(tiles):
        finish_if(early, 1, i)
    contract(1)
    for q in range(NQ):
        collect(q)

    left(mix_out.at[:, pl.ds(0, C - 1)], mix_s.at[0])
    left(lse_in.at[:, pl.ds(0, C - 1)], lse_s.at[0])
    left(att.at[:, pl.ds(0, C - 1)], att_s.at[0])
    left(first_in, f_s.at[0])
    left(second.at[:, :, :, pl.ds(0, Y - 1)], g_s.at[0])
    left(hid.at[:, :, pl.ds(0, 2 * Y - 1)], h_s.at[0])
    left(part.at[:, pl.ds(0, C - 1)], part_s.at[0])
    for q in range(NQ):
        pl.when(visitor)(functools.partial(left, po_out.at[q], po_s.at[q]))
    for copy in sent:
        copy.wait_send()
    for condition, copy in kept:
        pl.when(condition)(copy.wait_send)


def fused(
    C,
    H,
    queries,
    keys,
    values,
    page_map,
    selected,
    residual_in,
    out_weight,
    norm_gain,
    gate_weight,
    up_weight,
    down_weight,
):
    row_count, query_width = queries.shape
    pages, page_len, kv_width = keys.shape
    kv = kv_width // HEAD_SIZE
    group = query_width // kv_width
    NQ = row_count // 128
    RC = row_count // C // NQ
    rows = C * RC
    NP = 4
    X = C // H
    Y = H // CORES
    hr = rows // H
    width = out_weight.shape[1]
    hidden = gate_weight.shape[1]
    out_width = down_weight.shape[1]
    tile = column_tile(hidden)
    tiles = hidden // tile
    steps = NQ * kv
    u_width = (width + 127) // 128 * 128
    bf16 = jnp.bfloat16
    f32 = jnp.float32
    vmem = pl.BlockSpec(memory_space=pltpu.VMEM)
    hbm = pl.BlockSpec(memory_space=pl.ANY)
    V = pltpu.VMEM
    S = pltpu.SemaphoreType.DMA
    out_weight = out_weight.T
    down_weight = down_weight.T
    mixes = V((steps, C, RC, group * HEAD_SIZE), bf16)
    return pl.pallas_call(
        functools.partial(fused_kernel, C, H, NP),
        out_shape=pltpu.VMEM((NQ, RC, out_width), bf16),
        in_specs=[hbm] * 11,
        out_specs=vmem,
        scratch_shapes=[
            pltpu.SMEM(page_map.shape, jnp.int32),
            pltpu.SMEM(selected.shape, jnp.int32),
            V((C, NQ, RC, query_width), bf16),
            V((X, NQ, RC, width), bf16),
            V((1, width), f32),
            V((kv, pages, page_len, HEAD_SIZE), bf16),
            V((kv, pages, page_len, HEAD_SIZE), bf16),
            V(out_weight.shape, bf16),
            V(gate_weight.shape, bf16),
            V(up_weight.shape, bf16),
            V(down_weight.shape, bf16),
            mixes,
            mixes,
            V((steps, group, rows), f32),
            V((steps, C, group, rows), f32),
            mixes,
            V((NQ, rows, width), bf16),
            V((NQ, H, rows, width), bf16),
            V((H, X, NQ, RC, width), bf16),
            V((NQ, rows, width), bf16),
            V((NQ, X, rows, u_width), bf16),
            V((NQ, CORES, Y, hr, 128), f32),
            V((NQ, Y, hr, 128), f32),
            V((NQ, Y, hr, 128), f32),
            V((NQ, Y, hr, 128), f32),
            V((NQ, hr, 128), f32),
            V((tiles, 2, rows, tile), f32),
            V((NQ, tiles, 2, CORES, Y, hr, tile), bf16),
            V((NQ, tiles, 2, Y, hr, tile), bf16),
            V((NQ, tiles, 2, Y, hr, tile), bf16),
            V((NQ, tiles, 2, Y, hr, tile), bf16),
            V((NQ, tiles, H, hr, tile), bf16),
            V((rows, out_width), f32),
            V((NQ, C, RC, out_width), bf16),
            V((NQ, C, RC, out_width), bf16),
            S((5,)),
            S((2, kv)),
            S((4,)),
            S((1,)),
            S((steps,)),
            S((1,)),
            S((steps,)),
            S((1,)),
            S((steps,)),
            S((kv,)),
            S((NQ,)),
            S((NQ, NP)),
            S((1,)),
            S((1,)),
            S((1 + X,)),
            S((NQ, X, NP)),
            S((NQ, Y)),
            S((NQ, 1 + Y)),
            S((1,)),
            S((NQ, tiles, 2)),
            S((1,)),
            S((NQ, tiles, 2, Y)),
            S((1,)),
            S((NQ, tiles, H)),
            S((1,)),
            S((NQ,)),
        ],
        compiler_params=pltpu.CompilerParams(
            collective_id=0, has_side_effects=True, vmem_limit_bytes=63 * 2**20
        ),
    )(
        page_map,
        selected,
        queries.reshape(C, NQ, RC, query_width),
        residual_in.reshape(X, NQ, RC, width),
        norm_gain,
        keys,
        values,
        out_weight,
        gate_weight,
        up_weight,
        down_weight,
    ).reshape(row_count // C, out_width)


def fits(C, H, queries, keys, selected, out_weight, gate_weight):
    rows = queries.shape[0]
    width = out_weight.shape[1]
    if rows % 128:
        return False
    chunks = rows // 128
    return (
        chunks == 2
        and C % H == 0
        and (C // H) * H == C
        and rows % (C * chunks) == 0
        and rows // (C * chunks) % 16 == 0
        and rows % selected.shape[0] == 0
        and keys.shape[2] // HEAD_SIZE > 3
        and (keys.shape[1] - rows) % 128 == 0
        and keys.shape[1] > rows
        and width % 16 == 0
        and width % 128 <= 125
        and width % 128 > 0
        and gate_weight.shape[1] % 128 == 0
    )


def shards(
    queries,
    keys,
    values,
    page_map,
    selected,
    residual_in,
    out_weight,
    norm_gain,
    gate_weight,
    up_weight,
    down_weight,
):
    ctx_index = lax.axis_index("ctx")
    C = lax.axis_size("ctx")
    H = lax.axis_size("head")
    if fits(C, H, queries, keys, selected, out_weight, gate_weight):
        return fused(
            C,
            H,
            queries,
            keys,
            values,
            page_map,
            selected,
            residual_in,
            out_weight,
            norm_gain,
            gate_weight,
            up_weight,
            down_weight,
        )
    row_max, row_total, mixture = owner_pass(
        queries, keys, values, page_map, selected, ctx_index, C
    )
    stats = jnp.concatenate([row_max, row_total], axis=1)
    stats = jnp.pad(stats, ((0, 0), (0, 128 - stats.shape[1])))
    mlp_out, own_stream = tail(
        C,
        H,
        mixture.astype(jnp.bfloat16),
        stats,
        residual_in,
        norm_gain,
        out_weight,
        gate_weight,
        up_weight,
        down_weight,
    )
    own_stream = jnp.concatenate([own_stream[j] for j in range(own_stream.shape[0])], axis=1)
    return (own_stream.astype(jnp.float32) + mlp_out).astype(jnp.bfloat16)


def solution(mesh):
    in_specs = (
        P(None, "head"),
        P("ctx", None, "head"),
        P("ctx", None, "head"),
        P(),
        P(),
        P("head", "ctx"),
        P("head", "ctx"),
        P("ctx"),
        P("head", "ctx"),
        P("head", "ctx"),
        P("ctx", "head"),
    )
    out_specs = P("ctx", "head")
    return jax.shard_map(shards, mesh=mesh, in_specs=in_specs, out_specs=out_specs, check_vma=False)
```
